32 devices in a mesh: dp: 4 (over y, core), expert: 8 (over z, x).
Axes of the slice: x: 2, y: 2, z: 4, core: 2. Of those that a mesh axis runs over, the one named last changes fastest.
Arguments:
- inputs: bfloat16 [4096, 1536], P(('dp', 'expert')), may hold values from -6 to 6
- segment_ids: int32 [32, 128], P(('dp', 'expert')), may hold values from 0 to 3, never falling along the last dimension, each value on 1 to 64 neighbouring positions
- routes: int32 [4096, 8], P(('dp', 'expert')), may hold values from 0 to 39, all different within a row; in each aligned block of 128 rows (0 to 127, 128 to 255, ...) at most 28 rows name the same one
- expert_blocks: int32 [40], replicated, may hold values from 6 to 7, as said below
- norm1_gain: bfloat16 [1536], P('dp'), may hold values from 0.5 to 1.5
- q_weight: bfloat16 [1536, 1536], P('dp')
- k_weight: bfloat16 [1536, 512], P('dp')
- value_matrix: bfloat16 [1536, 512], P('dp'), may hold values from -0.15625 to 0.15625
- o_weight: bfloat16 [1536, 1536], P('dp'), may hold values from -3 to 3
- norm2_gain: bfloat16 [1536], P('dp'), may hold values from 0.5 to 1.5
- router_weight: bfloat16 [1536, 40], P('dp')
- expert_gate_up: bfloat16 [40, 1536, 1024], P('expert'), may hold values from -0.3125 to 0.3125
- expert_down: bfloat16 [40, 512, 1536], P('expert'), may hold values from -3 to 3
- out_grad: bfloat16 [4096, 1536], P(('dp', 'expert')), may hold values from -6 to 6
Outputs:
- output: bfloat16 [4096, 1536], P(('dp', 'expert'))
- grad_inputs: float32 [4096, 1536], P(('dp', 'expert'))
- grad_norm1_gain: float32 [1536], P('dp')
- grad_q_weight: float32 [1536, 1536], P('dp')
- grad_k_weight: float32 [1536, 512], P('dp')
- grad_v_weight: float32 [1536, 512], P('dp')
- grad_o_weight: float32 [1536, 1536], P('dp')
- grad_norm2_gain: float32 [1536], P('dp')
- grad_router_weight: float32 [1536, 40], P('dp')
- grad_expert_gate_up: float32 [40, 1536, 1024], P('expert', 'dp')
- grad_expert_down: float32 [40, 512, 1536], P('expert', None, 'dp')
The draws below stay inside these ranges and needn't reach their ends.
Inputs may be any that keep to these rules, and one draw needn't show every extreme that they name: `segment_ids`: in each sequence the ids never fall and take every value; a document spans 1 to 64 positions, and in every sequence one document spans exactly 64. The 8 routes of a token name different experts. Among the 128 tokens of one sequence no expert is named more than 28 times, and in some sequences one is named exactly 28 times. `expert_blocks`: both values occur.
All inputs are finite; a program needn't handle non-finite values.
Results may differ from the reference program's by a relative error of at most 0.015.
The reference program's roundings to bfloat16 on the way count: a program that leaves them out, or rounds other values in their place, can miss the bound.
Values may be sent and summed in bfloat16 or wider, within the bound.
A program may use at most 256 MiB of HBM per device.

```python
import math
import jax
import jax.numpy as jnp
import numpy as np
from jax import lax

MODEL_DIMENSION = 1536
QUERY_HEADS = 24
KEY_VALUE_HEADS = 8
HEAD_DIMENSION = 64
EXPERT_HIDDEN = 512
EXPERT_COUNT = 40
TOPK = 8
SEQ = 128
DOCS = 4
MAXB = 7
BLK = 4
CAP = 28
SLOTS = 5
SEQS = 32
TOKENS = 4096
N_EXPERT = 8


def draw_expert_blocks(key, part):
    key_one, key_two, key_three = jax.random.split(jax.random.fold_in(key, 11), 3)
    blocks = jax.random.randint(key_one, (EXPERT_COUNT,), MAXB - 1, MAXB + 1)
    full_at = jax.random.randint(key_two, (), 0, EXPERT_COUNT)
    short_at = (full_at + 1 + jax.random.randint(key_three, (), 0, EXPERT_COUNT - 1)) % EXPERT_COUNT
    expert_index = jnp.arange(EXPERT_COUNT)
    blocks = jnp.where(expert_index == full_at, MAXB, blocks)
    blocks = jnp.where(expert_index == short_at, MAXB - 1, blocks)
    return blocks.astype(jnp.int32)


def scaled_draw(key, shape, deviation):
    gaussian_sample = jax.random.normal(key, shape, jnp.float32)
    return (gaussian_sample * deviation).astype(jnp.bfloat16)


def draw_q_weight(key, part):
    return scaled_draw(jax.random.fold_in(key, 21), (MODEL_DIMENSION, QUERY_HEADS * HEAD_DIMENSION), 4.0 / math.sqrt(MODEL_DIMENSION))


def draw_k_weight(key, part):
    return scaled_draw(jax.random.fold_in(key, 31), (MODEL_DIMENSION, KEY_VALUE_HEADS * HEAD_DIMENSION), 4.0 / math.sqrt(MODEL_DIMENSION))


def draw_router_weight(key, part):
    return scaled_draw(jax.random.fold_in(key, 41), (MODEL_DIMENSION, EXPERT_COUNT), 1.5 / math.sqrt(MODEL_DIMENSION))


def shard_levels(rng, extent, pieces, smallest, top_value):
    factor_of, own = 1.0, jax.random.fold_in(rng, 6)
    for axis_at, parts in pieces:
        heights = jnp.exp(jax.random.uniform(jax.random.fold_in(own, axis_at), (parts,), jnp.float32, smallest / len(pieces), top_value / len(pieces)))
        factor_of = factor_of * jnp.repeat(heights, extent[axis_at] // parts).reshape([-1 if axis == axis_at else 1 for axis in range(len(extent))])
    return factor_of


def split_up(count, total, reach, lean):
    weights = [(1 << 20) // math.isqrt(standing ** lean) + 1 for standing in range(2, count + 1)]
    surplus, given = total - reach - (count - 1), [1] * (count - 1)
    while surplus > 0:
        movable = [i for i in range(count - 1) if given[i] < reach]
        whole, left = sum([weights[i] for i in movable]), surplus
        for i in movable:
            extra = min(reach - given[i], max(1, left * weights[i] // whole), surplus)
            given[i] = given[i] + extra
            surplus = surplus - extra
    return np.array([reach] + given)


def ragged_sizes(rng, number_of, total, reach, lean):
    if number_of == 2:
        one = jax.random.randint(rng, (), max(1, total - reach), min(reach, total - 1) + 1)
        return jnp.stack([one, total - one])
    sizes = jnp.asarray(split_up(number_of, total, reach, lean), jnp.int32)
    pairs = (number_of - 1) // 2
    donor, receiver = sizes[1:1 + 2 * pairs:2], sizes[2:2 + 2 * pairs:2]
    room = jnp.minimum(donor - 1, reach - receiver)
    passed = jax.random.randint(jax.random.fold_in(rng, 1), (pairs,), 0, 1 << 20) % (room + 1)
    sizes = sizes.at[1:1 + 2 * pairs:2].set(donor - passed).at[2:2 + 2 * pairs:2].set(receiver + passed)
    return sizes[jax.random.permutation(jax.random.fold_in(rng, 2), number_of)]


def assign_block(rng, own, number, rows, number_of, top, limit, skew):
    sequence = jax.random.permutation(rng, number_of)
    heavy_load, common = load_shares(number_of, rows * top, limit, skew, True), load_shares(number_of, rows * top, limit, skew, False)
    places = jnp.arange(number_of)

    def named(tallies, rotation):
        used = int((tallies > 0).sum())
        fixed = max(1, used // 4)
        passed = fixed + (places - fixed + rotation * (used - fixed)) % max(1, number_of - fixed)
        return jnp.zeros((number_of,), jnp.int32).at[sequence[jnp.where(places < fixed, places, passed)]].set(jnp.asarray(tallies, jnp.int32))

    tallies = jnp.where(number % 4 == 0, named(heavy_load, number // 4), named(common, number - number // 4 - 1))
    mixed = jax.random.permutation(jax.random.fold_in(own, 3), number_of)
    donor, taker = mixed[0:number_of // 2 * 2:2], mixed[1:number_of // 2 * 2:2]
    margin = jnp.minimum(tallies[donor] - 1, limit - tallies[taker]) // 2
    margin = jnp.where((donor == sequence[0]) | (taker == sequence[0]) | (tallies[taker] == 0), 0, jnp.maximum(margin, 0))
    passed = jax.random.randint(jax.random.fold_in(own, 4), (number_of // 2,), 0, 1 << 20) % (margin + 1)
    tallies = tallies.at[donor].add(-passed).at[taker].add(passed)
    labels = jnp.searchsorted(jnp.cumsum(tallies), jnp.arange(rows * top), side="right").astype(jnp.int32)
    listing = labels.reshape(top, rows).T
    listing = listing[jax.random.permutation(jax.random.fold_in(own, 1), rows)]
    rotation = jax.random.randint(jax.random.fold_in(own, 2), (rows, 1), 0, top)
    return jnp.take_along_axis(listing, (jnp.arange(top)[None, :] + rotation) % top, axis=1)


def load_shares(number_of, total, reach, lean, full):
    portions = [(1 << 20) // math.isqrt(rank ** lean) + 1 for rank in range(1, number_of + 1)]
    largest = reach if full else min(reach, max(-(-total // number_of), total * portions[0] // sum(portions)))
    least = 1 if total - largest >= number_of - 1 else 0
    holding, spare = [largest] + [least] * (number_of - 1), total - largest - least * (number_of - 1)
    while spare > 0:
        free = [i for i in range(1, number_of) if holding[i] < largest] or [i for i in range(1, number_of) if holding[i] < reach]
        pool, left = sum([portions[i] for i in free]), spare
        for i in free:
            extra = min(reach - holding[i], max(1, left * portions[i] // pool), spare)
            holding[i] = holding[i] + extra
            spare = spare - extra
    return np.array(holding)


def normal_values(key, dims, scale, reach, pieces=(), held_as=jnp.bfloat16):
    drawn = scale * jax.random.normal(key, dims, jnp.float32)
    if pieces:
        drawn = drawn * shard_levels(key, dims, pieces, -0.22, 0.18)
    return jnp.clip(drawn, -reach, reach).astype(held_as)


def setup_inputs(seed: int = 0) -> dict:
    key_list = jax.random.split(jax.random.key(seed), 15)
    inputs = normal_values(key_list[0], (TOKENS, MODEL_DIMENSION), 1.0, 6.0, ((0, 32),))
    segment_ids = jax.vmap(lambda own: jnp.searchsorted(jnp.cumsum(ragged_sizes(own, DOCS, SEQ, SEQ // 2, 1)), jnp.arange(SEQ), side="right"))(jax.random.split(key_list[1], SEQS)).reshape((SEQS, SEQ)).astype(jnp.int32)
    routes_keys = jax.random.split(jax.random.fold_in(key_list[2], 1), TOKENS // SEQ)
    routes_turns = jax.random.permutation(jax.random.fold_in(key_list[2], 3), TOKENS // SEQ)
    routes = jax.vmap(lambda own, number: assign_block(jax.random.fold_in(key_list[2], 2), own, number, SEQ, EXPERT_COUNT, TOPK, CAP, 2))(routes_keys, routes_turns).reshape((TOKENS, TOPK))
    expert_blocks = draw_expert_blocks(jax.random.fold_in(key_list[14], 71), 0)
    norm1_gain = jnp.clip(1.0 + 0.1 * jax.random.normal(key_list[4], (MODEL_DIMENSION,), jnp.float32), 0.5, 1.5).astype(jnp.bfloat16)
    q_weight = draw_q_weight(jax.random.fold_in(key_list[14], 71), 0)
    k_weight = draw_k_weight(jax.random.fold_in(key_list[14], 71), 0)
    value_matrix = normal_values(key_list[7], (MODEL_DIMENSION, KEY_VALUE_HEADS * HEAD_DIMENSION), MODEL_DIMENSION ** -0.5, 0.15625, ((0, 4),))
    o_weight = normal_values(key_list[8], (QUERY_HEADS * HEAD_DIMENSION, MODEL_DIMENSION), 4 ** -0.5, 3.0, ((0, 4),))
    norm2_gain = jnp.clip(1.0 + 0.1 * jax.random.normal(key_list[9], (MODEL_DIMENSION,), jnp.float32), 0.5, 1.5).astype(jnp.bfloat16)
    router_weight = draw_router_weight(jax.random.fold_in(key_list[14], 71), 0)
    expert_gate_up = normal_values(key_list[11], (SLOTS * N_EXPERT, MODEL_DIMENSION, 2 * EXPERT_HIDDEN), (MODEL_DIMENSION // 4) ** -0.5, 0.3125, ((0, 8),))
    expert_down = normal_values(key_list[12], (SLOTS * N_EXPERT, EXPERT_HIDDEN, MODEL_DIMENSION), 4 ** -0.5, 3.0, ((0, 8),))
    out_grad = normal_values(key_list[13], (TOKENS, MODEL_DIMENSION), 1.0, 6.0, ((0, 32),))
    return dict(inputs=inputs, segment_ids=segment_ids, routes=routes, expert_blocks=expert_blocks, norm1_gain=norm1_gain, q_weight=q_weight, k_weight=k_weight, value_matrix=value_matrix, o_weight=o_weight, norm2_gain=norm2_gain, router_weight=router_weight, expert_gate_up=expert_gate_up, expert_down=expert_down, out_grad=out_grad)


NORM_EPSILON = 1e-06
SCORE_SCALE = 0.015625
RESIDUAL_SCALE = 0.22
ROPE_BASE = 10000.0
MASKED_SCORE = -1e+30

def matrix_product(left, right):
    return jnp.dot(left, right, preferred_element_type=jnp.float32)

def float_product(form, left, right):
    return jnp.einsum(form, left.astype(jnp.float32), right.astype(jnp.float32), precision=lax.Precision.HIGHEST)

def rope_tables(sequence_length, head_size):
    positions = jnp.arange(sequence_length, dtype=jnp.float32)
    frequency = ROPE_BASE ** (-(jnp.arange(head_size // 2, dtype=jnp.float32) * 2.0) / head_size)
    angles = positions[:, None] * frequency[None, :]
    return (jnp.cos(angles)[:, None, :], jnp.sin(angles)[:, None, :])

def apply_rotary(tensor, cosine_lookup, sine_lookup):
    half_size = tensor.shape[-1] // 2
    front_half = tensor[..., :half_size]
    back_half = tensor[..., half_size:]
    return jnp.concatenate([front_half * cosine_lookup - back_half * sine_lookup, back_half * cosine_lookup + front_half * sine_lookup], axis=-1)

def inverse_rotary(tensor, cosine_lookup, sine_lookup):
    half_size = tensor.shape[-1] // 2
    front_half = tensor[..., :half_size]
    back_half = tensor[..., half_size:]
    return jnp.concatenate([front_half * cosine_lookup + back_half * sine_lookup, back_half * cosine_lookup - front_half * sine_lookup], axis=-1)

def norm_stats(values):
    norm_scale = lax.rsqrt(lax.optimization_barrier(jnp.mean(values * values, axis=-1, keepdims=True)) + NORM_EPSILON)
    return (values * norm_scale, norm_scale)

def norm_back(grad_out, normed, norm_scale, gain_values):
    grad_hat = grad_out * gain_values
    grad_in = norm_scale * (grad_hat - normed * lax.optimization_barrier(jnp.mean(grad_hat * normed, axis=-1, keepdims=True)))
    return (grad_in, lax.optimization_barrier(jnp.sum(grad_out * normed, axis=0)))

def masked_scores(query_rows, rows_of_keys, segments):
    scores = float_product('qhgd,khd->hgqk', query_rows, rows_of_keys) * SCORE_SCALE
    row_pos = jnp.arange(query_rows.shape[0], dtype=jnp.int32)
    col_pos = jnp.arange(rows_of_keys.shape[0], dtype=jnp.int32)
    allowed = (col_pos[None, :] <= row_pos[:, None]) & (segments[:, None] == segments[None, :])
    return jnp.where(allowed, scores, MASKED_SCORE)

def route_rows(seq_routes, expert_blocks):
    flat_routes = seq_routes.reshape(-1)
    onehot_table = (flat_routes[:, None] == jnp.arange(EXPERT_COUNT, dtype=jnp.int32)[None, :]).astype(jnp.int32)
    row_rank = lax.optimization_barrier(jnp.sum((jnp.cumsum(onehot_table, axis=0) - onehot_table) * onehot_table, axis=1))
    row_limit = lax.optimization_barrier(jnp.sum(onehot_table * expert_blocks[None, :], axis=1)) * BLK
    return (flat_routes, onehot_table, row_rank, row_rank < row_limit)

def layer_block(seq_block, weights, expert_blocks):
    gain_one, weight_q, key_projection_weight, value_projection_weight, output_projection_weight, gain_two, weight_router, gate_up_float, down_float = weights
    seq_inputs, segments, seq_routes, seq_grad = seq_block
    sequence_length = seq_inputs.shape[0]
    head_groups = QUERY_HEADS // KEY_VALUE_HEADS
    top_count = seq_routes.shape[1]
    input_float = seq_inputs.astype(jnp.float32)
    gain_first = gain_one.astype(jnp.float32)
    gain_second = gain_two.astype(jnp.float32)
    normed_one, scale_one = norm_stats(input_float)
    input_before_norm = (normed_one * gain_first).astype(jnp.bfloat16)
    cosine_lookup, sine_lookup = rope_tables(sequence_length, HEAD_DIMENSION)
    query_rows = apply_rotary(matrix_product(input_before_norm, weight_q).reshape(sequence_length, QUERY_HEADS, HEAD_DIMENSION), cosine_lookup, sine_lookup).astype(jnp.bfloat16)
    rows_of_keys = apply_rotary(matrix_product(input_before_norm, key_projection_weight).reshape(sequence_length, KEY_VALUE_HEADS, HEAD_DIMENSION), cosine_lookup, sine_lookup).astype(jnp.bfloat16)
    rows_of_values = matrix_product(input_before_norm, value_projection_weight).reshape(sequence_length, KEY_VALUE_HEADS, HEAD_DIMENSION).astype(jnp.bfloat16)
    grouped_queries = query_rows.reshape(sequence_length, KEY_VALUE_HEADS, head_groups, HEAD_DIMENSION)
    scores = masked_scores(grouped_queries, rows_of_keys, segments)
    row_max = lax.optimization_barrier(jnp.max(scores, axis=-1, keepdims=True))
    log_total = row_max + jnp.log(lax.optimization_barrier(jnp.sum(jnp.exp(scores - row_max), axis=-1, keepdims=True)))
    soft_weights = jnp.exp(scores - log_total)
    probs = soft_weights.astype(jnp.bfloat16)
    attended = float_product('hgqk,khd->qhgd', probs, rows_of_values).astype(jnp.bfloat16)
    attended_flat = attended.reshape(sequence_length, QUERY_HEADS * HEAD_DIMENSION)
    hidden = input_float + RESIDUAL_SCALE * matrix_product(attended_flat, output_projection_weight)
    normed_two, scale_two = norm_stats(hidden)
    norm_hidden = (normed_two * gain_second).astype(jnp.bfloat16)
    router_probs = jax.nn.softmax(matrix_product(norm_hidden, weight_router), axis=-1)
    flat_routes, onehot_table, row_rank, retained = route_rows(seq_routes, expert_blocks)
    table_three = onehot_table.reshape(sequence_length, top_count, EXPERT_COUNT).astype(jnp.float32)
    gate_prob = lax.optimization_barrier(jnp.sum(table_three * router_probs[:, None, :], axis=2))
    keep_three = retained.reshape(sequence_length, top_count)
    mixing = jnp.where(keep_three, gate_prob, 0.0)
    total_rows = EXPERT_COUNT * CAP
    target = jnp.where(retained, flat_routes * CAP + row_rank, total_rows)
    safe_slot = jnp.minimum(target, total_rows - 1)
    source_rows = jnp.repeat(norm_hidden, top_count, axis=0)
    buffer = jnp.zeros((total_rows, MODEL_DIMENSION), jnp.bfloat16).at[target].set(source_rows, mode='drop').reshape(EXPERT_COUNT, CAP, MODEL_DIMENSION)
    gate_up = float_product('ecd,edf->ecf', buffer, gate_up_float)
    gate_part = gate_up[..., :EXPERT_HIDDEN]
    up_part = gate_up[..., EXPERT_HIDDEN:]
    inner_act = (jax.nn.silu(gate_part) * up_part).astype(jnp.bfloat16)
    produced = float_product('ech,ehd->ecd', inner_act, down_float).astype(jnp.bfloat16)
    out_rows = produced.reshape(total_rows, MODEL_DIMENSION)[safe_slot].reshape(sequence_length, top_count, MODEL_DIMENSION).astype(jnp.float32)
    mixture = lax.optimization_barrier(jnp.sum(mixing[..., None] * out_rows, axis=1))
    output = (hidden + RESIDUAL_SCALE * mixture).astype(jnp.bfloat16)
    grad_y = seq_grad.astype(jnp.float32)
    grad_mix = RESIDUAL_SCALE * grad_y
    grad_gate = jnp.where(keep_three, lax.optimization_barrier(jnp.sum(grad_mix[:, None, :] * out_rows, axis=2)), 0.0)
    grad_rows = (mixing[..., None] * grad_mix[:, None, :]).astype(jnp.bfloat16).reshape(sequence_length * top_count, MODEL_DIMENSION)
    grad_buffer = jnp.zeros((total_rows, MODEL_DIMENSION), jnp.bfloat16).at[target].set(grad_rows, mode='drop').reshape(EXPERT_COUNT, CAP, MODEL_DIMENSION)
    grad_inner = float_product('ecd,ehd->ech', grad_buffer, down_float)
    grad_down = float_product('ech,ecd->ehd', inner_act, grad_buffer)
    squash = jax.nn.sigmoid(gate_part)
    grad_gate_part = grad_inner * up_part * squash * (1.0 + gate_part * (1.0 - squash))
    grad_up_part = grad_inner * (gate_part * squash)
    grad_gu = jnp.concatenate([grad_gate_part, grad_up_part], axis=-1).astype(jnp.bfloat16)
    grad_gate_up = float_product('ecd,ecf->edf', buffer, grad_gu)
    grad_xrows = float_product('ecf,edf->ecd', grad_gu, gate_up_float).astype(jnp.bfloat16)
    back_rows = grad_xrows.reshape(total_rows, MODEL_DIMENSION)[safe_slot].reshape(sequence_length, top_count, MODEL_DIMENSION).astype(jnp.float32)
    grad_from_rows = lax.optimization_barrier(jnp.sum(jnp.where(keep_three[..., None], back_rows, 0.0), axis=1))
    grad_probs = lax.optimization_barrier(jnp.sum(table_three * grad_gate[..., None], axis=1))
    grad_logits = router_probs * (grad_probs - lax.optimization_barrier(jnp.sum(router_probs * grad_probs, axis=1, keepdims=True)))
    router_float = weight_router.astype(jnp.float32)
    grad_norm_hidden = grad_from_rows + jnp.dot(grad_logits, router_float.T, precision=lax.Precision.HIGHEST)
    grad_router = jnp.dot(norm_hidden.astype(jnp.float32).T, grad_logits, precision=lax.Precision.HIGHEST)
    grad_hidden_part, grad_gain_two = norm_back(grad_norm_hidden, normed_two, scale_two, gain_second)
    grad_hidden = grad_y + grad_hidden_part
    branch_gradient = (RESIDUAL_SCALE * grad_hidden).astype(jnp.bfloat16)
    grad_wo = matrix_product(attended_flat.T, branch_gradient)
    attended_gradient = matrix_product(branch_gradient, output_projection_weight.T).astype(jnp.bfloat16).reshape(sequence_length, KEY_VALUE_HEADS, head_groups, HEAD_DIMENSION)
    value_gradients = float_product('hgqk,qhgd->khd', probs, attended_gradient)
    grad_weights = float_product('qhgd,khd->hgqk', attended_gradient, rows_of_values)
    row_delta = float_product('qhgd,qhgd->hgq', attended_gradient, attended)[..., None]
    grad_scores = (soft_weights * (grad_weights - row_delta) * SCORE_SCALE).astype(jnp.bfloat16)
    grad_queries = float_product('hgqk,khd->qhgd', grad_scores, rows_of_keys).reshape(sequence_length, QUERY_HEADS, HEAD_DIMENSION)
    key_gradients = float_product('hgqk,qhgd->khd', grad_scores, grouped_queries)
    grad_q_low = inverse_rotary(grad_queries, cosine_lookup, sine_lookup).astype(jnp.bfloat16).reshape(sequence_length, QUERY_HEADS * HEAD_DIMENSION)
    key_gradient_narrow = inverse_rotary(key_gradients, cosine_lookup, sine_lookup).astype(jnp.bfloat16).reshape(sequence_length, KEY_VALUE_HEADS * HEAD_DIMENSION)
    value_gradient_narrow = value_gradients.astype(jnp.bfloat16).reshape(sequence_length, KEY_VALUE_HEADS * HEAD_DIMENSION)
    grad_wq = matrix_product(input_before_norm.T, grad_q_low)
    grad_wk = matrix_product(input_before_norm.T, key_gradient_narrow)
    grad_wv = matrix_product(input_before_norm.T, value_gradient_narrow)
    grad_norm_input = matrix_product(grad_q_low, weight_q.T) + matrix_product(key_gradient_narrow, key_projection_weight.T) + matrix_product(value_gradient_narrow, value_projection_weight.T)
    grad_in_part, grad_gain_one = norm_back(grad_norm_input, normed_one, scale_one, gain_first)
    grad_inputs = grad_hidden + grad_in_part
    grads = (grad_gain_one, grad_wq, grad_wk, grad_wv, grad_wo, grad_gain_two, grad_router, grad_gate_up, grad_down)
    return ((output, grad_inputs), grads)

def reference(inputs, segment_ids, routes, expert_blocks, norm1_gain, q_weight, k_weight, value_matrix, o_weight, norm2_gain, router_weight, expert_gate_up, expert_down, out_grad):
    expert_index = jnp.arange(EXPERT_COUNT, dtype=jnp.int32)
    expert_order = expert_index % N_EXPERT * SLOTS + expert_index // N_EXPERT
    gate_up_float = expert_gate_up[expert_order].astype(jnp.float32)
    down_float = expert_down[expert_order].astype(jnp.float32)
    weights = (norm1_gain, q_weight, k_weight, value_matrix, o_weight, norm2_gain, router_weight, gate_up_float, down_float)
    seq_data = (inputs.reshape(SEQS, SEQ, MODEL_DIMENSION), segment_ids, routes.reshape(SEQS, SEQ, TOPK), out_grad.reshape(SEQS, SEQ, MODEL_DIMENSION))
    starting_state = (jnp.zeros((MODEL_DIMENSION,), jnp.float32), jnp.zeros((MODEL_DIMENSION, QUERY_HEADS * HEAD_DIMENSION), jnp.float32), jnp.zeros((MODEL_DIMENSION, KEY_VALUE_HEADS * HEAD_DIMENSION), jnp.float32), jnp.zeros((MODEL_DIMENSION, KEY_VALUE_HEADS * HEAD_DIMENSION), jnp.float32), jnp.zeros((QUERY_HEADS * HEAD_DIMENSION, MODEL_DIMENSION), jnp.float32), jnp.zeros((MODEL_DIMENSION,), jnp.float32), jnp.zeros((MODEL_DIMENSION, EXPERT_COUNT), jnp.float32), jnp.zeros((EXPERT_COUNT, MODEL_DIMENSION, 2 * EXPERT_HIDDEN), jnp.float32), jnp.zeros((EXPERT_COUNT, EXPERT_HIDDEN, MODEL_DIMENSION), jnp.float32))

    def scan_step(totals, seq_block):
        results, grads = layer_block(seq_block, weights, expert_blocks)
        return (tuple((total + grad for total, grad in zip(totals, grads))), results)
    totals, results = lax.scan(scan_step, starting_state, seq_data)
    outputs, grad_inputs = results
    grad_gate_up_full = jnp.zeros((SLOTS * N_EXPERT, MODEL_DIMENSION, 2 * EXPERT_HIDDEN), jnp.float32).at[expert_order].set(totals[7])
    grad_down_full = jnp.zeros((SLOTS * N_EXPERT, EXPERT_HIDDEN, MODEL_DIMENSION), jnp.float32).at[expert_order].set(totals[8])
    return (outputs.reshape(TOKENS, MODEL_DIMENSION), grad_inputs.reshape(TOKENS, MODEL_DIMENSION), totals[0], totals[1], totals[2], totals[3], totals[4], totals[5], totals[6], grad_gate_up_full, grad_down_full)
```

```python
import functools
import math

import jax
import jax.numpy as jnp
import numpy as np
from jax import lax
from jax.experimental import pallas as pl
from jax.experimental.pallas import tpu as pltpu
from jax.sharding import PartitionSpec as P

QUERY_HEADS = 24
KEY_VALUE_HEADS = 8
HEAD_DIMENSION = 64
EXPERT_COUNT = 40
BLK = 4
SLOT_ROWS = 32
SLOT_STRIDE = 8

NORM_EPSILON = 1e-06
SCORE_SCALE = 0.015625
RESIDUAL_SCALE = 0.22
ROPE_BASE = 10000.0
MASKED_SCORE = -1e30

MESH = pl.DeviceIdType.MESH
F32, BF16 = jnp.float32, jnp.bfloat16
MEBI = 1024 * 1024
VMEM_MOST = 67_043_328


class Grid:
    def __init__(self, axis, A, B):
        self.axis, self.A, self.B = axis, A, B
        self.me = lax.axis_index(axis)
        self.a, self.b = self.me // B, self.me % B

    def at(self, a, b):
        return a * self.B + b

    def dev(self, a, b):
        return {self.axis: self.at(a, b)}

    def here(self):
        return {self.axis: self.me}

    def near(self):
        found = []
        if self.A > 1:
            found += [
                (self.a > 0, self.dev(self.a - 1, self.b)),
                (self.a < self.A - 1, self.dev(self.a + 1, self.b)),
            ]
        if self.B > 1:
            found += [
                (self.b > 0, self.dev(self.a, self.b - 1)),
                (self.b < self.B - 1, self.dev(self.a, self.b + 1)),
            ]
        return found

    def all(self):
        n = self.A * self.B
        return [(self.me >= 0, {self.axis: (self.me + r) % n}) for r in range(1, n)]

    def next(self, kind, way):
        step = 1 if way == 0 else -1
        if kind == "a":
            return self.ahead("a", way, 1), self.dev(self.a + step, self.b)
        return self.ahead("b", way, 1), self.dev(self.a, self.b + step)

    def behind(self, kind, way, far):
        at, size = (self.a, self.A) if kind == "a" else (self.b, self.B)
        return (at - far >= 0) if way == 0 else (at + far <= size - 1)

    def ahead(self, kind, way, far):
        return self.behind(kind, 1 - way, far)


def greet(peers):
    barrier = pltpu.get_barrier_semaphore()
    for there, device in peers:

        @pl.when(there)
        def _():
            pl.semaphore_signal(barrier, inc=1, device_id=device, device_id_type=MESH)

    pl.semaphore_wait(barrier, sum(jnp.where(there, 1, 0) for there, _ in peers))


def remote(src, dst, send, recv, device):
    return pltpu.make_async_remote_copy(
        src_ref=src, dst_ref=dst, send_sem=send, recv_sem=recv, device_id=device, device_id_type=MESH
    )


def run(*steps):
    steps = list(steps)
    while steps:
        left = []
        for step in steps:
            try:
                next(step)
                left.append(step)
            except StopIteration:
                pass
        steps = left


def line_sems(A, B):
    dma = pltpu.SemaphoreType.DMA
    return [dma((2, A)), dma((2, A)), dma((2, A, B)), dma((2, A, B))]


def gather(g, own, out, sems):
    send_a, recv_a, send_b, recv_b = sems
    A, B = g.A, g.B
    row = lambda way, k: g.a - k if way == 0 else g.a + k
    col = lambda way, k: g.b - k if way == 0 else g.b + k
    rows = [(0, 0)] + [(way, k) for k in range(1, A) for way in (0, 1)]

    def along_a(way, k, src, do):
        if k < A - 1:
            there, device = g.next("a", way)
            i = g.at(row(way, k), g.b)

            @pl.when(there)
            def _():
                do(remote(src, out.at[i], send_a.at[way, k], recv_a.at[way, k + 1], device))

    def along_b(way, j, a, i, src, do):
        if j < B - 1:
            there, device = g.next("b", way)

            @pl.when(there)
            def _():
                do(remote(src, out.at[i], send_b.at[way, a, j], recv_b.at[way, a, j + 1], device))

    def start(copy):
        copy.start()

    def sent(copy):
        copy.wait_send()

    for way in (0, 1):
        along_a(way, 0, own, start)
    for way in (0, 1):
        along_b(way, 0, g.a, g.me, own, start)
    yield
    for k in range(1, A):
        for way in (0, 1):
            i = g.at(row(way, k), g.b)

            @pl.when(g.behind("a", way, k))
            def _():
                remote(out.at[i], out.at[i], send_a.at[way, k], recv_a.at[way, k], g.here()).wait_recv()
                along_a(way, k, out.at[i], start)
                for w in (0, 1):
                    along_b(w, 0, row(way, k), i, out.at[i], start)

            yield
    for j in range(1, B):
        for way, k in rows:
            for w in (0, 1):
                i = g.at(row(way, k), col(w, j))

                @pl.when(g.behind("a", way, k) & g.behind("b", w, j))
                def _():
                    a = row(way, k)
                    remote(out.at[i], out.at[i], send_b.at[w, a, j], recv_b.at[w, a, j], g.here()).wait_recv()
                    along_b(w, j, a, i, out.at[i], start)

            yield
    for way, k in rows:
        for w in (0, 1) if k == 0 else (way,):

            @pl.when(g.behind("a", w, k))
            def _():
                along_a(w, k, own, sent)

        @pl.when(g.behind("a", way, k))
        def _():
            for w in (0, 1):
                for j in range(B - 1):

                    @pl.when(g.behind("b", w, j))
                    def _():
                        along_b(w, j, row(way, k), g.me, own, sent)


def sum_slots(A, B, block, dtype=BF16):
    return [
        pltpu.VMEM((2, A) + block, dtype),
        pltpu.VMEM((2, A) + block, dtype),
        pltpu.VMEM((2, A, B - 1) + block, dtype),
        pltpu.VMEM((2, A, B - 2) + block if B > 2 else (8, 128), dtype),
    ]


def reduce(g, part, finish, sems, slots):
    send_a, recv_a, send_b, recv_b = sems
    land_a, out_a, land_b, out_b = slots
    A, B = g.A, g.B
    row = lambda way, k: g.a + k if way == 0 else g.a - k
    col = lambda way, k: g.b + k if way == 0 else g.b - k
    rows = [(way, k) for k in range(A - 1, 0, -1) for way in (0, 1)] + [(0, 0)]
    here = g.here()
    first = lambda kind, way: jnp.logical_not(g.behind(kind, way, 1))

    for way, k in rows:

        @pl.when(g.ahead("a", way, k))
        def _():
            a = row(way, k)
            for j in range(B - 1, 0, -1):
                for w in (0, 1):

                    @pl.when(g.ahead("b", w, j) & first("b", w))
                    def _():
                        remote(
                            part(g.at(a, col(w, j))),
                            land_b.at[w, a, j - 1],
                            send_b.at[w, a, j],
                            recv_b.at[w, a, j - 1],
                            g.next("b", w)[1],
                        ).start()

    yield
    for way, k in rows:

        @pl.when(g.ahead("a", way, k))
        def _():
            a = row(way, k)
            for j in range(B - 2, 0, -1):
                for w in (0, 1):

                    @pl.when(g.ahead("b", w, j) & g.behind("b", w, 1))
                    def _():
                        remote(land_b.at[w, a, j], land_b.at[w, a, j], send_b.at[w, a, j], recv_b.at[w, a, j], here).wait_recv()
                        out_b[w, a, j - 1] = (
                            part(g.at(a, col(w, j)))[...].astype(F32) + land_b[w, a, j].astype(F32)
                        ).astype(out_b.dtype)
                        remote(
                            out_b.at[w, a, j - 1],
                            land_b.at[w, a, j - 1],
                            send_b.at[w, a, j],
                            recv_b.at[w, a, j - 1],
                            g.next("b", w)[1],
                        ).start()

            for w in (0, 1):
                if B > 1:

                    @pl.when(g.behind("b", w, 1))
                    def _():
                        remote(land_b.at[w, a, 0], land_b.at[w, a, 0], send_b.at[w, a, 0], recv_b.at[w, a, 0], here).wait_recv()

            def near():
                total = part(g.at(a, g.b))[...].astype(F32)
                if B == 2:
                    return total + land_b[1 - g.b, a, 0].astype(F32)
                for w in (0, 1):
                    if B > 1:
                        total = total + jnp.where(g.behind("b", w, 1), land_b[w, a, 0].astype(F32), 0.0)
                return total

            if k > 0:

                @pl.when(g.behind("a", way, 1))
                def _():
                    if k < A - 1:
                        remote(land_a.at[way, k], land_a.at[way, k], send_a.at[way, k], recv_a.at[way, k], here).wait_recv()
                        out_a[way, k] = (near() + land_a[way, k].astype(F32)).astype(out_a.dtype)

                @pl.when(first("a", way))
                def _():
                    out_a[way, k] = near().astype(out_a.dtype)

                remote(
                    out_a.at[way, k], land_a.at[way, k - 1], send_a.at[way, k], recv_a.at[way, k - 1], g.next("a", way)[1]
                ).start()
            else:
                for w in (0, 1):
                    if A > 1:

                        @pl.when(g.behind("a", w, 1))
                        def _():
                            remote(land_a.at[w, 0], land_a.at[w, 0], send_a.at[w, 0], recv_a.at[w, 0], here).wait_recv()

                total = near()
                if A == 2:
                    total = total + land_a[1 - g.a, 0].astype(F32)
                else:
                    for w in (0, 1):
                        if A > 1:
                            total = total + jnp.where(g.behind("a", w, 1), land_a[w, 0].astype(F32), 0.0)
                finish(total)

        yield
    for way, k in rows:

        @pl.when(g.ahead("a", way, k))
        def _():
            a = row(way, k)
            for j in range(B - 1, 0, -1):
                for w in (0, 1):

                    @pl.when(g.ahead("b", w, j))
                    def _():
                        remote(part(g.me), land_b.at[w, a, j - 1], send_b.at[w, a, j], recv_b.at[w, a, j - 1], here).wait_send()

            if k > 0:
                remote(out_a.at[way, k], land_a.at[way, k - 1], send_a.at[way, k], recv_a.at[way, k - 1], here).wait_send()


def reduce_gather(g, part, out, kept, sems, slots):
    def finish(total):
        kept[...] = total.astype(kept.dtype)

    yield from reduce(g, part, finish, sems[:4], slots)
    out[g.me] = kept[...]
    yield from gather(g, kept, out, sems[4:])


def exchange_sems(n):
    return [pltpu.SemaphoreType.DMA((n,)), pltpu.SemaphoreType.DMA((n,))]


def exchange(g, part, out, sems):
    send, recv = sems
    n = g.A * g.B
    copies = []
    for r in range(1, n):
        to = (g.me + r) % n
        copies.append(remote(part.at[to], out.at[g.me], send.at[r], recv.at[r], {g.axis: to}))
        copies[-1].start()
    out[g.me] = part[g.me]
    yield
    for r in range(1, n):
        origin = (g.me + n - r) % n
        remote(part.at[origin], out.at[origin], send.at[r], recv.at[r], g.here()).wait_recv()
    yield
    for copy in copies:
        copy.wait_send()


def call(body, name, outs, ins, scratch=(), cid=None, us=10.0, **grid):
    whole = pl.BlockSpec(memory_space=pltpu.VMEM)
    params = dict(vmem_limit_bytes=VMEM_MOST)
    if cid is not None:
        params |= dict(collective_id=cid, has_side_effects=True)
    return pl.pallas_call(
        body,
        out_shape=[jax.ShapeDtypeStruct(shape, dtype) for shape, dtype in outs],
        in_specs=grid.pop("in_specs", [whole] * len(ins)),
        out_specs=grid.pop("out_specs", [whole] * len(outs)),
        scratch_shapes=list(scratch),
        compiler_params=pltpu.CompilerParams(**params),
        cost_estimate=pl.CostEstimate(flops=0, transcendentals=0, bytes_accessed=int(us * 3e6)),
        name=name,
        **grid,
    )(*ins)


def taker(refs):
    refs = list(refs)

    def take(n=None):
        if n is None:
            return refs.pop(0)
        return [refs.pop(0) for _ in range(n)]

    return take


def dot(left, right, contract=((1,), (0,))):
    return lax.dot_general(left, right, (contract, ((), ())), preferred_element_type=F32)


def halves(values):
    high = values.astype(BF16)
    return high, (values - high.astype(F32)).astype(BF16)


def norm_scale(values):
    return lax.rsqrt(jnp.mean(values * values, axis=-1, keepdims=True) + NORM_EPSILON)


def norm_back(grad, normed, scale, gain):
    grad_hat = grad * gain
    return scale * (grad_hat - normed * jnp.mean(grad_hat * normed, axis=-1, keepdims=True))


def rotary(values, cosine, sine, back=False):
    width, half = values.shape[1], HEAD_DIMENSION // 2
    later = pltpu.roll(values, width - half, 1)
    earlier = pltpu.roll(values, half, 1)
    front = lax.broadcasted_iota(jnp.int32, values.shape, 1) % HEAD_DIMENSION < half
    other = jnp.where(front, -later, earlier)
    return values * cosine - other * sine if back else values * cosine + other * sine


def allowed_pairs(segment_row):
    size = segment_row.shape[1]
    across = jnp.broadcast_to(segment_row, (size, size))
    rows = lax.broadcasted_iota(jnp.int32, (size, size), 0)
    cols = lax.broadcasted_iota(jnp.int32, (size, size), 1)
    return (cols <= rows) & (across == across.T)


def attention_weights(stacked, keys, allowed):
    scores = dot(stacked, keys, ((1,), (1,))) * SCORE_SCALE
    scores = jnp.where(allowed, scores, MASKED_SCORE)
    row_max = jnp.max(scores, axis=-1, keepdims=True)
    log_total = row_max + jnp.log(jnp.sum(jnp.exp(scores - row_max), axis=-1, keepdims=True))
    return jnp.exp(scores - log_total)


class Heads:
    def __init__(self, ranks):
        self.q, self.kv = QUERY_HEADS // ranks, KEY_VALUE_HEADS // ranks
        self.group = QUERY_HEADS // KEY_VALUE_HEADS
        self.q_cols, self.kv_cols = self.q * HEAD_DIMENSION, self.kv * HEAD_DIMENSION
        self.cols = -(-(self.q_cols + 2 * self.kv_cols) // 128) * 128

    def stack(self, rows, kv):
        first = kv * self.group
        return jnp.concatenate([self.head(rows, first + i) for i in range(self.group)], axis=0)

    def head(self, rows, i):
        return rows[:, i * HEAD_DIMENSION : (i + 1) * HEAD_DIMENSION]

    def key(self, rows, kv):
        return self.head(rows, self.q + kv)

    def value(self, rows, kv):
        return self.head(rows, self.q + self.kv + kv)


def rope_tables(length, heads):
    frequency = np.float32(ROPE_BASE) ** (-(np.arange(HEAD_DIMENSION // 2, dtype=np.float32) * 2.0) / HEAD_DIMENSION)
    angles = np.arange(length, dtype=np.float32)[:, None] * frequency.astype(np.float32)[None, :]
    cosine, sine = (np.tile(f(angles.astype(np.float64)).astype(np.float32), (1, 2)) for f in (np.cos, np.sin))
    turned = heads.q + heads.kv
    rest = heads.cols - turned * HEAD_DIMENSION
    cosine = np.concatenate([np.tile(cosine, (1, turned)), np.ones((length, rest), np.float32)], axis=1)
    sine = np.concatenate([np.tile(sine, (1, turned)), np.zeros((length, rest), np.float32)], axis=1)
    return cosine, sine


def gain_row(misc_ref, ranks, which):
    return jnp.concatenate([misc_ref[i, which : which + 1, :] for i in range(ranks)], axis=1)


def attention_forward(ranks, heads, length, x_ref, w_ref, o_ref, misc_ref, cos_ref, sin_ref, part_ref, qkv_ref, att_ref, scale_ref):
    width = x_ref.shape[2]
    gain = gain_row(misc_ref, ranks, 0)
    weights = w_ref[...].reshape(width, heads.cols)

    def one(b, carry):
        x = x_ref[b].astype(F32)
        scale = norm_scale(x)
        scale_ref[b] = jnp.broadcast_to(scale, (length, 128))
        normed = (x * scale * gain).astype(BF16)
        qkv_ref[b] = rotary(dot(normed, weights), cos_ref[...], sin_ref[...]).astype(BF16)
        qkv = qkv_ref[b]
        allowed = allowed_pairs(misc_ref[b, 8:9, :length])
        allowed = jnp.concatenate([allowed] * heads.group, axis=0)
        outs = []
        for kv in range(heads.kv):
            probs = attention_weights(heads.stack(qkv, kv), heads.key(qkv, kv), allowed).astype(BF16)
            mixed = dot(probs, heads.value(qkv, kv)).astype(BF16)
            outs += [mixed[i * length : (i + 1) * length] for i in range(heads.group)]
        att_ref[b] = jnp.concatenate(outs, axis=1)
        part_ref[b] = dot(att_ref[b], o_ref[...]).astype(BF16)
        return carry

    lax.fori_loop(0, ranks, one, 0)


def route_tables(n_expert, slots, routes, blocks):
    tokens = routes.shape[0]
    column = lax.broadcasted_iota(jnp.int32, (1, 128), 1)
    owner, slot = column // SLOT_STRIDE, column % SLOT_STRIDE
    expert = slot * n_expert + owner
    real = (owner < n_expert) & (slot < slots) & (expert < EXPERT_COUNT)
    expert = jnp.where(real, expert, -1)
    named = jnp.zeros((tokens, 128), F32)
    for k in range(routes.shape[1]):
        named = named + jnp.where(routes[:, k : k + 1] == expert, 1.0, 0.0)
    rows = lax.broadcasted_iota(jnp.int32, (tokens, tokens), 0)
    cols = lax.broadcasted_iota(jnp.int32, (tokens, tokens), 1)
    earlier = jnp.where(cols < rows, 1.0, 0.0).astype(BF16)
    rank = dot(earlier, named.astype(BF16))
    kept = (named > 0.0) & (rank < (blocks * BLK).astype(F32))
    return real, kept, jnp.where(kept, rank, -1.0)


def route_forward(ranks, n_expert, slots, x_ref, branch_ref, misc_ref, router_ref, routes_ref, blocks_ref, hidden_ref, norm_ref, scale_ref, probs_ref, meta_ref):
    gain = gain_row(misc_ref, ranks, 1)
    hidden = x_ref[...].astype(F32) + RESIDUAL_SCALE * branch_ref[...]
    hidden_ref[...] = hidden
    scale = norm_scale(hidden)
    scale_ref[...] = jnp.broadcast_to(scale, scale_ref.shape)
    norm_ref[...] = (hidden * scale * gain).astype(BF16)
    real, kept, place = route_tables(n_expert, slots, routes_ref[...], blocks_ref[0:1, :])
    router = router_ref[...].reshape(-1, 128)
    logits = jnp.where(real, dot(norm_ref[...], router), MASKED_SCORE)
    weight = jnp.exp(logits - jnp.max(logits, axis=-1, keepdims=True))
    probs = weight / jnp.sum(weight, axis=-1, keepdims=True)
    probs_ref[...] = probs
    used = n_expert * SLOT_STRIDE
    meta_ref[0] = place.T[:used]
    meta_ref[1] = jnp.where(kept, probs, 0.0).T[:used]


def experts(n_expert, slots, tokens, nh_ref, og_ref, meta_ref, up_ref, down_ref, out_ref, back_ref, gate_grad_ref, d_up_ref, d_down_ref, x_sc, og_sc, eo_sc, gx_sc, nh_in, og_in, sems):
    step = pl.program_id(0)
    mine = pl.ds(pl.multiple_of(lax.axis_index("expert") * SLOT_STRIDE, SLOT_STRIDE), SLOT_STRIDE)
    width = nh_ref.shape[2]
    hidden = down_ref.shape[1]

    def fetch(q):
        slot = q % 2
        return [
            pltpu.make_async_copy(nh_ref.at[q], nh_in.at[slot], sems.at[0, slot]),
            pltpu.make_async_copy(og_ref.at[q], og_in.at[slot], sems.at[1, slot]),
        ]

    packed = slots * SLOT_ROWS
    number = lax.broadcasted_iota(jnp.int32, (SLOT_ROWS, tokens), 0).astype(F32)

    def picks(q):
        place = meta_ref[q, 0, mine, :]
        return jnp.concatenate([jnp.where(number == place[s : s + 1], 1.0, 0.0) for s in range(slots)], axis=0)

    @pl.when(step == 0)
    def _():
        for copy in fetch(0):
            copy.start()

        def one(q, carry):
            @pl.when(q + 1 < n_expert)
            def _():
                for copy in fetch(q + 1):
                    copy.start()

            for copy in fetch(q):
                copy.wait()
            pick = picks(q).astype(BF16)
            x_sc[q] = dot(pick, nh_in[q % 2]).astype(BF16)
            og_sc[q] = dot(pick, og_in[q % 2]).astype(BF16)
            gate_grad_ref[q] = jnp.zeros((SLOT_STRIDE, tokens), F32)
            return carry

        lax.fori_loop(0, n_expert, one, 0)

    place_of = pl.ds(pl.multiple_of(step * SLOT_ROWS, SLOT_ROWS), SLOT_ROWS)
    slot_row = lax.broadcasted_iota(jnp.int32, (SLOT_STRIDE, tokens), 0) == step
    rows = n_expert * SLOT_ROWS
    x = x_sc[:, place_of, :].reshape(rows, width)
    both = dot(x, up_ref[0])
    gate, up = both[:, :hidden], both[:, hidden:]
    squash = jax.nn.sigmoid(gate)
    inner = (gate * squash * up).astype(BF16)
    produced = dot(inner, down_ref[0]).astype(BF16)
    eo_sc[:, place_of, :] = produced.reshape(n_expert, SLOT_ROWS, width)
    masks, gates = [], []
    for q in range(n_expert):
        place = jnp.sum(jnp.where(slot_row, meta_ref[q, 0, mine, :], 0.0), axis=0, keepdims=True)
        share = jnp.sum(jnp.where(slot_row, meta_ref[q, 1, mine, :], 0.0), axis=0, keepdims=True)
        masks.append(number == place)
        gates.append(jnp.sum(jnp.where(masks[q], share, 0.0), axis=1, keepdims=True))
    mix_grad = RESIDUAL_SCALE * og_sc[:, place_of, :].reshape(rows, width).astype(F32)
    grad_rows = (jnp.concatenate(gates, axis=0) * mix_grad).astype(BF16)
    gate_grad = jnp.sum(mix_grad * produced.astype(F32), axis=1, keepdims=True)
    for q in range(n_expert):
        spread = jnp.where(masks[q], gate_grad[q * SLOT_ROWS : (q + 1) * SLOT_ROWS], 0.0)
        gate_grad_ref[q] = jnp.where(slot_row, jnp.sum(spread, axis=0, keepdims=True), gate_grad_ref[q])
    grad_inner = dot(grad_rows, down_ref[0], ((1,), (1,)))
    grad_both = jnp.concatenate(
        [grad_inner * up * squash * (1.0 + gate * (1.0 - squash)), grad_inner * (gate * squash)], axis=1
    ).astype(BF16)
    gx_sc[:, place_of, :] = dot(grad_both, up_ref[0], ((1,), (1,))).astype(BF16).reshape(n_expert, SLOT_ROWS, width)
    tile = 256
    for i in range(width // tile):
        here = slice(i * tile, (i + 1) * tile)
        d_up_ref[0, here, :] = dot(x[:, here], grad_both, ((0,), (0,))).astype(d_up_ref.dtype)
    for i in range(hidden // tile):
        here = slice(i * tile, (i + 1) * tile)
        d_down_ref[0, here, :] = dot(inner[:, here], grad_rows, ((0,), (0,))).astype(d_down_ref.dtype)

    @pl.when(step == slots - 1)
    def _():
        def one(q, carry):
            pick = picks(q)
            share = meta_ref[q, 1, mine, :]
            share = jnp.concatenate([jnp.broadcast_to(share[s : s + 1], (SLOT_ROWS, tokens)) for s in range(slots)], axis=0)
            high, low = halves(pick * share)
            over = ((0,), (0,))
            out_ref[q] = (dot(high, eo_sc[q], over) + dot(low, eo_sc[q], over)).astype(BF16)
            back_ref[q] = dot(pick.astype(BF16), gx_sc[q], over).astype(BF16)
            return carry

        lax.fori_loop(0, n_expert, one, 0)


def route_backward(ranks, n_expert, shard, hidden_ref, norm_ref, scale_ref, probs_ref, misc_ref, router_ref, og_ref, mixture_ref, back_ref, gate_grad_ref, out_ref, grad_hidden_ref, branch_ref, small_ref):
    tokens, width = hidden_ref.shape
    gain = gain_row(misc_ref, ranks, 1)
    hidden = hidden_ref[...]
    out_ref[...] = (hidden + RESIDUAL_SCALE * mixture_ref[...]).astype(BF16)
    used = n_expert * SLOT_STRIDE
    spread = gate_grad_ref[...].reshape(used, tokens)
    if used < 128:
        spread = jnp.concatenate([spread, jnp.zeros((128 - used, tokens), F32)], axis=0)
    grad_probs = spread.T
    probs = probs_ref[...]
    grad_logits = probs * (grad_probs - jnp.sum(probs * grad_probs, axis=1, keepdims=True))
    high, low = halves(grad_logits)
    router = router_ref[...].reshape(width, 128)
    across = ((1,), (1,))
    grad_norm = back_ref[...] + (dot(high, router, across) + dot(low, router, across))
    scale = scale_ref[:, 0:1]
    normed = hidden * scale
    grad_hidden = og_ref[...].astype(F32) + norm_back(grad_norm, normed, scale, gain)
    grad_hidden_ref[...] = grad_hidden
    branch_ref[...] = (RESIDUAL_SCALE * grad_hidden).astype(BF16)
    over = ((0,), (0,))
    norm = norm_ref[...]
    grad_router = dot(high, norm, over) + dot(low, norm, over)
    grad_gain = jnp.sum(grad_norm * normed, axis=0, keepdims=True)
    for i in range(ranks):
        here = slice(i * shard, (i + 1) * shard)
        small_ref[i, :used, :] = grad_router[:used, here]
        small_ref[i, used:, :] = jnp.broadcast_to(grad_gain[:, here], (8, shard))


def attention_backward(ranks, heads, length, branch_ref, att_ref, qkv_ref, o_ref, misc_ref, cos_ref, sin_ref, grad_ref, d_o_ref):
    d_o_ref[...] = dot(
        att_ref[...].reshape(ranks * length, heads.q_cols), branch_ref[...].reshape(ranks * length, -1), ((0,), (0,))
    ).astype(BF16)

    def one(b, carry):
        grad_att = dot(branch_ref[b], o_ref[...], ((1,), (1,))).astype(BF16)
        att, qkv = att_ref[b], qkv_ref[b]
        allowed = allowed_pairs(misc_ref[b, 8:9, :length])
        allowed = jnp.concatenate([allowed] * heads.group, axis=0)
        d_q, d_k, d_v = [], [], []
        for kv in range(heads.kv):
            queries, keys = heads.stack(qkv, kv), heads.key(qkv, kv)
            soft = attention_weights(queries, keys, allowed)
            grads = heads.stack(grad_att, kv)
            d_v.append(dot(soft.astype(BF16), grads, ((0,), (0,))))
            delta = jnp.sum(grads.astype(F32) * heads.stack(att, kv).astype(F32), axis=1, keepdims=True)
            inner = dot(grads, heads.value(qkv, kv), ((1,), (1,)))
            d_scores = (soft * (inner - delta) * SCORE_SCALE).astype(BF16)
            rows = dot(d_scores, keys)
            d_q += [rows[i * length : (i + 1) * length] for i in range(heads.group)]
            d_k.append(dot(d_scores, queries, ((0,), (0,))))
        spare = heads.cols - heads.q_cols - 2 * heads.kv_cols
        fill = [jnp.zeros((length, spare), F32)] if spare else []
        grads = jnp.concatenate(d_q + d_k + d_v + fill, axis=1)
        grad_ref[b] = rotary(grads, cos_ref[...], sin_ref[...], back=True).astype(BF16)
        return carry

    lax.fori_loop(0, ranks, one, 0)


def projection_backward(ranks, heads, shard, x_ref, scale_ref, gain_ref, grad_ref, w_ref, small_ref, grad_x_ref, d_w_ref, sums_ref):
    normed = x_ref[...].astype(F32) * scale_ref[:, 0:1]
    norm_input = (normed * gain_ref[0:1, :]).astype(BF16)
    total = None
    for i in range(ranks):
        grads = grad_ref[i].reshape(-1, heads.cols)
        term = dot(grads, w_ref[i], ((1,), (1,)))
        total = term if total is None else total + term
        d_w_ref[:, i * heads.cols : (i + 1) * heads.cols] = dot(norm_input, grads, ((0,), (0,))).astype(BF16)
    grad_x_ref[...] = total
    small = small_ref[0]
    for i in range(1, ranks):
        small = small + small_ref[i]
    gain_grad = jnp.sum(total * normed, axis=0, keepdims=True)
    used = small.shape[0] - 8
    sums_ref[...] = jnp.zeros_like(sums_ref)
    sums_ref[:used, :] = small[:used].astype(BF16)
    second = lax.broadcasted_iota(jnp.int32, (8, shard), 0)
    sums_ref[used : used + 8, :] = jnp.where(second == 0, small[used:], jnp.where(second == 1, gain_grad, 0.0)).astype(BF16)


def last_norm(ranks, grad_ref, x_ref, misc_ref, grad_hidden_ref, out_ref):
    gain = gain_row(misc_ref, ranks, 0)
    grad = jnp.concatenate([grad_ref[i] for i in range(ranks)], axis=1)
    x = x_ref[...].astype(F32)
    scale = norm_scale(x)
    out_ref[...] = grad_hidden_ref[...] + norm_back(grad, x * scale, scale, gain)


def on_device(
    inputs,
    segment_ids,
    routes,
    expert_blocks,
    norm1_gain,
    q_weight,
    k_weight,
    value_matrix,
    o_weight,
    norm2_gain,
    router_weight,
    expert_gate_up,
    expert_down,
    out_grad,
):
    ranks, n_expert = lax.axis_size("dp"), lax.axis_size("expert")
    tokens, width = inputs.shape
    shard = q_weight.shape[0]
    slots, _, double = expert_gate_up.shape
    hidden = expert_down.shape[1]
    heads = Heads(ranks)
    group = ("dp", ranks // 2, 2)
    plane = ("expert", 4, n_expert // 4)
    used = n_expert * SLOT_STRIDE
    cosine, sine = rope_tables(tokens, heads)

    weights = jnp.concatenate(
        [w.reshape(shard, ranks, -1) for w in (q_weight, k_weight, value_matrix)], axis=2
    ).transpose(1, 0, 2)
    weights = jnp.pad(weights, ((0, 0), (0, 0), (0, heads.cols - weights.shape[2])))
    router = jnp.pad(router_weight, ((0, 0), (0, slots * n_expert - router_weight.shape[1])))
    router = router.reshape(shard, slots, n_expert).transpose(0, 2, 1)
    router = jnp.pad(router, ((0, 0), (0, 0), (0, SLOT_STRIDE - slots))).reshape(shard, used)
    router = jnp.pad(router, ((0, 0), (0, 128 - used)))
    blocks = jnp.pad(expert_blocks, (0, slots * n_expert - expert_blocks.shape[0])).reshape(slots, n_expert).T
    blocks = jnp.pad(blocks, ((0, 0), (0, SLOT_STRIDE - slots))).reshape(1, used)
    blocks = jnp.pad(blocks, ((0, 7), (0, 128 - used)))
    misc = jnp.concatenate(
        [
            jnp.stack([norm1_gain, norm2_gain]).astype(F32),
            jnp.zeros((6, shard), F32),
            jnp.pad(segment_ids.astype(F32), ((0, 7), (0, shard - tokens))),
        ]
    )

    def opening(*refs):
        take = taker(refs)
        ins, outs = take(5), take(5)
        x, w, rt, ms, og = ins
        x_all, w_all, rt_all, ms_all, og_all = outs
        dp, ex = Grid(*group), Grid(*plane)
        greet(dp.all() + ex.near())
        x_all[dp.me] = x[...]
        rt_all[dp.me] = rt[...]
        ms_all[dp.me] = ms[...]
        og_all[ex.me] = og[...]
        run(
            gather(dp, x, x_all, take(4)),
            gather(dp, ms, ms_all, take(4)),
            gather(dp, rt, rt_all, take(4)),
            exchange(dp, w, w_all, take(2)),
            gather(ex, og, og_all, take(4)),
        )

    x_all, w_all, router_all, misc_all, og_all = call(
        opening,
        "opening",
        [
            ((ranks, tokens, width), BF16),
            ((ranks, shard, heads.cols), BF16),
            ((ranks, shard, 128), BF16),
            ((ranks, 16, shard), F32),
            ((n_expert, tokens, width), BF16),
        ],
        (inputs, weights, router, misc, out_grad),
        line_sems(*group[1:]) * 3 + exchange_sems(ranks) + line_sems(*plane[1:]),
        cid=0,
        us=40,
    )

    part, qkv, att, scale_all = call(
        functools.partial(attention_forward, ranks, heads, tokens),
        "attention_forward",
        [
            ((ranks, tokens, width), BF16),
            ((ranks, tokens, heads.cols), BF16),
            ((ranks, tokens, heads.q_cols), BF16),
            ((ranks, tokens, 128), F32),
        ],
        (x_all, w_all, o_weight, misc_all, cosine, sine),
        us=15,
    )

    def branch_sum(*refs):
        take = taker(refs)
        terms, out = take(2)
        dp = Grid(*group)
        greet(dp.near())

        def finish(total):
            out[...] = total

        run(reduce(dp, lambda i: terms.at[i], finish, take(4), take(4)))

    (branch,) = call(
        branch_sum,
        "branch_sum",
        [((tokens, width), F32)],
        (part,),
        line_sems(*group[1:]) + sum_slots(*group[1:], (tokens, width)),
        cid=1,
        us=15,
    )

    hidden_rows, norm_hidden, scale_two, probs, meta = call(
        functools.partial(route_forward, ranks, n_expert, slots),
        "route_forward",
        [
            ((tokens, width), F32),
            ((tokens, width), BF16),
            ((tokens, 128), F32),
            ((tokens, 128), F32),
            ((2, used, tokens), F32),
        ],
        (inputs, branch, misc_all, router_all, routes, blocks),
        us=5,
    )

    def dispatch(*refs):
        take = taker(refs)
        (nh, mt), (nh_all, mt_all) = take(2), take(2)
        ex = Grid(*plane)
        greet(ex.near())
        nh_all[ex.me] = nh[...]
        mt_all[ex.me] = mt[...]
        run(gather(ex, nh, nh_all, take(4)), gather(ex, mt, mt_all, take(4)))

    norm_all, meta_all = call(
        dispatch,
        "dispatch",
        [((n_expert, tokens, width), BF16), ((n_expert, 2, used, tokens), F32)],
        (norm_hidden, meta),
        line_sems(*plane[1:]) * 2,
        cid=2,
        us=42,
    )

    fixed = lambda shape: pl.BlockSpec(shape, lambda s: (0,) * len(shape), pipeline_mode=pl.Buffered(1))
    moving = lambda shape: pl.BlockSpec((1,) + shape, lambda s: (s,) + (0,) * len(shape))
    packed = (n_expert, slots * SLOT_ROWS, width)
    out_part, back_part, gate_grad, d_up, d_down = call(
        functools.partial(experts, n_expert, slots, tokens),
        "experts",
        [
            ((n_expert, tokens, width), BF16),
            ((n_expert, tokens, width), BF16),
            ((n_expert, SLOT_STRIDE, tokens), F32),
            ((slots, width, double), BF16),
            ((slots, hidden, width), BF16),
        ],
        (norm_all, og_all, meta_all, expert_gate_up, expert_down),
        [pltpu.VMEM(packed, BF16)] * 4
        + [pltpu.VMEM((2, tokens, width), BF16)] * 2
        + [pltpu.SemaphoreType.DMA((2, 2))],
        us=50,
        grid=(slots,),
        in_specs=[
            pl.BlockSpec(memory_space=pl.ANY),
            pl.BlockSpec(memory_space=pl.ANY),
            fixed((n_expert, 2, used, tokens)),
            moving((width, double)),
            moving((hidden, width)),
        ],
        out_specs=[
            fixed((n_expert, tokens, width)),
            fixed((n_expert, tokens, width)),
            fixed((n_expert, SLOT_STRIDE, tokens)),
            moving((width, double)),
            moving((hidden, width)),
        ],
    )
    d_up = lax.psum_scatter(d_up, "dp", scatter_dimension=1, tiled=True).astype(F32)
    d_down = lax.psum_scatter(d_down, "dp", scatter_dimension=2, tiled=True).astype(F32)

    def combine(*refs):
        take = taker(refs)
        (terms, back_terms, gg), (out, back, gg_all) = take(3), take(3)
        ex = Grid(*plane)
        greet(ex.all())

        def finish(to):
            def store(total):
                to[...] = total

            return store

        run(
            exchange(ex, gg, gg_all, take(2)),
            reduce(ex, lambda i: back_terms.at[i], finish(back), take(4), take(4)),
            reduce(ex, lambda i: terms.at[i], finish(out), take(4), take(4)),
        )

    mixture, back, gate_grads = call(
        combine,
        "combine",
        [((tokens, width), F32), ((tokens, width), F32), ((n_expert, SLOT_STRIDE, tokens), F32)],
        (out_part, back_part, gate_grad),
        exchange_sems(n_expert) + (line_sems(*plane[1:]) + sum_slots(*plane[1:], (tokens, width))) * 2,
        cid=3,
        us=78,
    )

    output, grad_hidden, grad_branch, small = call(
        functools.partial(route_backward, ranks, n_expert, shard),
        "route_backward",
        [
            ((tokens, width), BF16),
            ((tokens, width), F32),
            ((tokens, width), BF16),
            ((ranks, used + 8, shard), F32),
        ],
        (hidden_rows, norm_hidden, scale_two, probs, misc_all, router_all, out_grad, mixture, back, gate_grads),
        us=6,
    )

    def share_branch(*refs):
        take = taker(refs)
        (br, sm), (br_all, sm_all) = take(2), take(2)
        dp = Grid(*group)
        greet(dp.all())
        br_all[dp.me] = br[...]
        run(gather(dp, br, br_all, take(4)), exchange(dp, sm, sm_all, take(2)))

    branch_all, small_all = call(
        share_branch,
        "share_branch",
        [((ranks, tokens, width), BF16), ((ranks, used + 8, shard), F32)],
        (grad_branch, small),
        line_sems(*group[1:]) + exchange_sems(ranks),
        cid=4,
        us=15,
    )

    grads, d_o = call(
        functools.partial(attention_backward, ranks, heads, tokens),
        "attention_backward",
        [((ranks, tokens, heads.cols), BF16), ((shard, width), BF16)],
        (branch_all, att, qkv, o_weight, misc_all, cosine, sine),
        us=15,
    )
    d_o = d_o.reshape(n_expert, shard // n_expert, width)

    def share_grads(*refs):
        take = taker(refs)
        (gr, do), (gr_all, do_all) = take(2), take(2)
        dp, ex = Grid(*group), Grid(*plane)
        greet(dp.near() + ex.near())
        gr_all[dp.me] = gr[...]
        run(
            gather(dp, gr, gr_all, take(4)),
            reduce_gather(ex, lambda i: do.at[i], do_all, take(), take(8), take(4)),
        )

    grads_all, d_o = call(
        share_grads,
        "share_grads",
        [((ranks, ranks, tokens, heads.cols), BF16), (d_o.shape, BF16)],
        (grads, d_o),
        line_sems(*group[1:])
        + [pltpu.VMEM(d_o.shape[1:], BF16)]
        + line_sems(*plane[1:]) * 2
        + sum_slots(*plane[1:], d_o.shape[1:]),
        cid=5,
        us=30,
    )

    x_cols = lax.dynamic_slice_in_dim(x_all.reshape(ranks * tokens, width), lax.axis_index("dp") * shard, shard, axis=1)
    sum_rows = 16 * n_expert
    grad_x, d_w, sums = call(
        functools.partial(projection_backward, ranks, heads, shard),
        "projection_backward",
        [
            ((ranks * tokens, shard), F32),
            ((shard, ranks * heads.cols), BF16),
            ((sum_rows, shard), BF16),
        ],
        (x_cols, scale_all.reshape(ranks * tokens, 128), misc, grads_all, weights, small_all),
        us=10,
    )
    grad_x = grad_x.reshape(ranks, tokens, shard)
    d_w = d_w.reshape(n_expert, shard // n_expert, ranks * heads.cols)
    sums = sums.reshape(n_expert, 16, shard)

    def closing(*refs):
        take = taker(refs)
        (gx, dw, sm), (gx_all, dw_all, sm_all) = take(3), take(3)
        dp, ex = Grid(*group), Grid(*plane)
        greet(dp.all() + ex.near())
        run(
            exchange(dp, gx, gx_all, take(2)),
            reduce_gather(ex, lambda i: sm.at[i], sm_all, take(), take(8), take(4)),
            reduce_gather(ex, lambda i: dw.at[i], dw_all, take(), take(8), take(4)),
        )

    grad_x, d_w, sums = call(
        closing,
        "closing",
        [(grad_x.shape, F32), (d_w.shape, BF16), (sums.shape, BF16)],
        (grad_x, d_w, sums),
        exchange_sems(ranks)
        + [pltpu.VMEM(sums.shape[1:], BF16)]
        + line_sems(*plane[1:]) * 2
        + sum_slots(*plane[1:], sums.shape[1:])
        + [pltpu.VMEM(d_w.shape[1:], BF16)]
        + line_sems(*plane[1:]) * 2
        + sum_slots(*plane[1:], d_w.shape[1:]),
        cid=6,
        us=55,
    )

    (grad_inputs,) = call(
        functools.partial(last_norm, ranks),
        "last_norm",
        [((tokens, width), F32)],
        (grad_x, inputs, misc_all, grad_hidden),
        us=4,
    )

    d_w = d_w.reshape(shard, ranks, heads.cols).astype(F32)
    first, second = heads.q_cols, heads.q_cols + heads.kv_cols
    d_q = d_w[:, :, :first].reshape(shard, -1)
    d_k = d_w[:, :, first:second].reshape(shard, -1)
    d_v = d_w[:, :, second : second + heads.kv_cols].reshape(shard, -1)
    d_o = d_o.reshape(shard, width).astype(F32)
    sums = sums.reshape(sum_rows, shard).astype(F32)
    d_router = sums[:used].reshape(n_expert, SLOT_STRIDE, shard)[:, :slots].transpose(2, 1, 0)
    d_router = d_router.reshape(shard, slots * n_expert)[:, : router_weight.shape[1]]
    return (output, grad_inputs, sums[used + 1], d_q, d_k, d_v, d_o, sums[used], d_router, d_up, d_down)


def solution(mesh):
    tokens = P(("dp", "expert"), None)
    rows = P("dp", None)
    return jax.shard_map(
        on_device,
        mesh=mesh,
        in_specs=(
            tokens,
            tokens,
            tokens,
            P(),
            P("dp"),
            rows,
            rows,
            rows,
            rows,
            P("dp"),
            rows,
            P("expert", None, None),
            P("expert", None, None),
            tokens,
        ),
        out_specs=(
            tokens,
            tokens,
            P("dp"),
            rows,
            rows,
            rows,
            rows,
            P("dp"),
            rows,
            P("expert", "dp", None),
            P("expert", None, "dp"),
        ),
        check_vma=False,
    )
```

```python
import functools
import math

import jax
import jax.numpy as jnp
import numpy as np
from jax import lax
from jax.experimental import pallas as pl
from jax.experimental.pallas import tpu as pltpu
from jax.sharding import PartitionSpec as P

QUERY_HEADS = 24
KEY_VALUE_HEADS = 8
HEAD_DIMENSION = 64
EXPERT_COUNT = 40
BLK = 4
SLOT_ROWS = 32
SLOT_STRIDE = 8

NORM_EPSILON = 1e-06
SCORE_SCALE = 0.015625
RESIDUAL_SCALE = 0.22
ROPE_BASE = 10000.0
MASKED_SCORE = -1e30

MESH = pl.DeviceIdType.MESH
F32, BF16 = jnp.float32, jnp.bfloat16
MEBI = 1024 * 1024
VMEM_MOST = 67_043_328


class Grid:
    def __init__(self, axis, A, B):
        self.axis, self.A, self.B = axis, A, B
        self.me = lax.axis_index(axis)
        self.a, self.b = self.me // B, self.me % B

    def at(self, a, b):
        return a * self.B + b

    def dev(self, a, b):
        return {self.axis: self.at(a, b)}

    def here(self):
        return {self.axis: self.me}

    def near(self):
        found = []
        if self.A > 1:
            found += [
                (self.a > 0, self.dev(self.a - 1, self.b)),
                (self.a < self.A - 1, self.dev(self.a + 1, self.b)),
            ]
        if self.B > 1:
            found += [
                (self.b > 0, self.dev(self.a, self.b - 1)),
                (self.b < self.B - 1, self.dev(self.a, self.b + 1)),
            ]
        return found

    def all(self):
        n = self.A * self.B
        return [(self.me >= 0, {self.axis: (self.me + r) % n}) for r in range(1, n)]

    def next(self, kind, way):
        step = 1 if way == 0 else -1
        if kind == "a":
            return self.ahead("a", way, 1), self.dev(self.a + step, self.b)
        return self.ahead("b", way, 1), self.dev(self.a, self.b + step)

    def behind(self, kind, way, far):
        at, size = (self.a, self.A) if kind == "a" else (self.b, self.B)
        return (at - far >= 0) if way == 0 else (at + far <= size - 1)

    def ahead(self, kind, way, far):
        return self.behind(kind, 1 - way, far)


def greet(peers):
    barrier = pltpu.get_barrier_semaphore()
    for there, device in peers:

        @pl.when(there)
        def _():
            pl.semaphore_signal(barrier, inc=1, device_id=device, device_id_type=MESH)

    pl.semaphore_wait(barrier, sum(jnp.where(there, 1, 0) for there, _ in peers))


def remote(src, dst, send, recv, device):
    return pltpu.make_async_remote_copy(
        src_ref=src, dst_ref=dst, send_sem=send, recv_sem=recv, device_id=device, device_id_type=MESH
    )


def begin(step):
    next(step)
    return step


def run(*steps):
    steps = list(steps)
    while steps:
        left = []
        for step in steps:
            try:
                next(step)
                left.append(step)
            except StopIteration:
                pass
        steps = left


def line_sems(A, B):
    dma = pltpu.SemaphoreType.DMA
    return [dma((2, A)), dma((2, A)), dma((2, A, B)), dma((2, A, B))]


def gather(g, own, out, sems, arrived=lambda i, block: None):
    send_a, recv_a, send_b, recv_b = sems
    A, B = g.A, g.B
    row = lambda way, k: g.a - k if way == 0 else g.a + k
    col = lambda way, k: g.b - k if way == 0 else g.b + k
    rows = [(0, 0)] + [(way, k) for k in range(1, A) for way in (0, 1)]

    def along_a(way, k, src, do):
        if k < A - 1:
            there, device = g.next("a", way)
            i = g.at(row(way, k), g.b)

            @pl.when(there)
            def _():
                do(remote(src, out.at[i], send_a.at[way, k], recv_a.at[way, k + 1], device))

    def along_b(way, j, a, i, src, do):
        if j < B - 1:
            there, device = g.next("b", way)

            @pl.when(there)
            def _():
                do(remote(src, out.at[i], send_b.at[way, a, j], recv_b.at[way, a, j + 1], device))

    def start(copy):
        copy.start()

    def sent(copy):
        copy.wait_send()

    for way in (0, 1):
        along_a(way, 0, own, start)
    for way in (0, 1):
        along_b(way, 0, g.a, g.me, own, start)
    arrived(g.me, own)
    yield
    for k in range(1, A):
        for way in (0, 1):
            i = g.at(row(way, k), g.b)

            @pl.when(g.behind("a", way, k))
            def _():
                remote(out.at[i], out.at[i], send_a.at[way, k], recv_a.at[way, k], g.here()).wait_recv()
                along_a(way, k, out.at[i], start)
                for w in (0, 1):
                    along_b(w, 0, row(way, k), i, out.at[i], start)
                arrived(i, out.at[i])

            yield
    for j in range(1, B):
        for way, k in rows:
            for w in (0, 1):
                i = g.at(row(way, k), col(w, j))

                @pl.when(g.behind("a", way, k) & g.behind("b", w, j))
                def _():
                    a = row(way, k)
                    remote(out.at[i], out.at[i], send_b.at[w, a, j], recv_b.at[w, a, j], g.here()).wait_recv()
                    along_b(w, j, a, i, out.at[i], start)
                    arrived(i, out.at[i])

            yield
    for way, k in rows:
        for w in (0, 1) if k == 0 else (way,):

            @pl.when(g.behind("a", w, k))
            def _():
                along_a(w, k, own, sent)

        @pl.when(g.behind("a", way, k))
        def _():
            for w in (0, 1):
                for j in range(B - 1):

                    @pl.when(g.behind("b", w, j))
                    def _():
                        along_b(w, j, row(way, k), g.me, own, sent)


def sum_slots(A, B, block, dtype=BF16):
    return [
        pltpu.VMEM((2, A) + block, dtype),
        pltpu.VMEM((2, A) + block, dtype),
        pltpu.VMEM((2, A, B - 1) + block, dtype),
        pltpu.VMEM((2, A, B - 2) + block if B > 2 else (8, 128), dtype),
    ]


def reduce(g, part, finish, sems, slots):
    send_a, recv_a, send_b, recv_b = sems
    land_a, out_a, land_b, out_b = slots
    A, B = g.A, g.B
    row = lambda way, k: g.a + k if way == 0 else g.a - k
    col = lambda way, k: g.b + k if way == 0 else g.b - k
    rows = [(way, k) for k in range(A - 1, 0, -1) for way in (0, 1)] + [(0, 0)]
    here = g.here()
    first = lambda kind, way: jnp.logical_not(g.behind(kind, way, 1))

    for way, k in rows:

        @pl.when(g.ahead("a", way, k))
        def _():
            a = row(way, k)
            for j in range(B - 1, 0, -1):
                for w in (0, 1):

                    @pl.when(g.ahead("b", w, j) & first("b", w))
                    def _():
                        remote(
                            part(g.at(a, col(w, j))),
                            land_b.at[w, a, j - 1],
                            send_b.at[w, a, j],
                            recv_b.at[w, a, j - 1],
                            g.next("b", w)[1],
                        ).start()

    yield
    for way, k in rows:

        @pl.when(g.ahead("a", way, k))
        def _():
            a = row(way, k)
            for j in range(B - 2, 0, -1):
                for w in (0, 1):

                    @pl.when(g.ahead("b", w, j) & g.behind("b", w, 1))
                    def _():
                        remote(land_b.at[w, a, j], land_b.at[w, a, j], send_b.at[w, a, j], recv_b.at[w, a, j], here).wait_recv()
                        out_b[w, a, j - 1] = (
                            part(g.at(a, col(w, j)))[...].astype(F32) + land_b[w, a, j].astype(F32)
                        ).astype(out_b.dtype)
                        remote(
                            out_b.at[w, a, j - 1],
                            land_b.at[w, a, j - 1],
                            send_b.at[w, a, j],
                            recv_b.at[w, a, j - 1],
                            g.next("b", w)[1],
                        ).start()

            for w in (0, 1):
                if B > 1:

                    @pl.when(g.behind("b", w, 1))
                    def _():
                        remote(land_b.at[w, a, 0], land_b.at[w, a, 0], send_b.at[w, a, 0], recv_b.at[w, a, 0], here).wait_recv()

            def near():
                total = part(g.at(a, g.b))[...].astype(F32)
                if B == 2:
                    return total + land_b[1 - g.b, a, 0].astype(F32)
                for w in (0, 1):
                    if B > 1:
                        total = total + jnp.where(g.behind("b", w, 1), land_b[w, a, 0].astype(F32), 0.0)
                return total

            if k > 0:

                @pl.when(g.behind("a", way, 1))
                def _():
                    if k < A - 1:
                        remote(land_a.at[way, k], land_a.at[way, k], send_a.at[way, k], recv_a.at[way, k], here).wait_recv()
                        out_a[way, k] = (near() + land_a[way, k].astype(F32)).astype(out_a.dtype)

                @pl.when(first("a", way))
                def _():
                    out_a[way, k] = near().astype(out_a.dtype)

                remote(
                    out_a.at[way, k], land_a.at[way, k - 1], send_a.at[way, k], recv_a.at[way, k - 1], g.next("a", way)[1]
                ).start()
            else:
                for w in (0, 1):
                    if A > 1:

                        @pl.when(g.behind("a", w, 1))
                        def _():
                            remote(land_a.at[w, 0], land_a.at[w, 0], send_a.at[w, 0], recv_a.at[w, 0], here).wait_recv()

                total = near()
                if A == 2:
                    total = total + land_a[1 - g.a, 0].astype(F32)
                else:
                    for w in (0, 1):
                        if A > 1:
                            total = total + jnp.where(g.behind("a", w, 1), land_a[w, 0].astype(F32), 0.0)
                finish(total)

        yield
    for way, k in rows:

        @pl.when(g.ahead("a", way, k))
        def _():
            a = row(way, k)
            for j in range(B - 1, 0, -1):
                for w in (0, 1):

                    @pl.when(g.ahead("b", w, j))
                    def _():
                        remote(part(g.me), land_b.at[w, a, j - 1], send_b.at[w, a, j], recv_b.at[w, a, j - 1], here).wait_send()

            if k > 0:
                remote(out_a.at[way, k], land_a.at[way, k - 1], send_a.at[way, k], recv_a.at[way, k - 1], here).wait_send()


def reduce_gather(g, part, out, kept, sems, slots):
    def finish(total):
        kept[...] = total.astype(kept.dtype)

    yield from reduce(g, part, finish, sems[:4], slots)
    out[g.me] = kept[...]
    yield from gather(g, kept, out, sems[4:])


def exchange_sems(n):
    return [pltpu.SemaphoreType.DMA((n,)), pltpu.SemaphoreType.DMA((n,))]


def pass_slices(g, out, sems):
    send, recv = sems
    n = g.A * g.B

    def copies(i, block):
        for r in range(1, n):
            to = (g.me + r) % n
            yield remote(block.at[to], out.at[g.me, i], send.at[i, r], recv.at[i, r], {g.axis: to})

    def arrived(i, block):
        for copy in copies(i, block):
            copy.start()

    def end(blocks, block):
        for i in blocks:
            for r in range(1, n):
                mine = out.at[(g.me + n - r) % n, i]
                remote(mine, mine, send.at[i, r], recv.at[i, r], g.here()).wait_recv()
            for copy in copies(i, block):
                copy.wait_send()

    return arrived, end


def exchange(g, part, out, sems):
    send, recv = sems
    n = g.A * g.B
    copies = []
    for r in range(1, n):
        to = (g.me + r) % n
        copies.append(remote(part.at[to], out.at[g.me], send.at[r], recv.at[r], {g.axis: to}))
        copies[-1].start()
    out[g.me] = part[g.me]
    yield
    for r in range(1, n):
        origin = (g.me + n - r) % n
        remote(part.at[origin], out.at[origin], send.at[r], recv.at[r], g.here()).wait_recv()
    yield
    for copy in copies:
        copy.wait_send()


VMEM = pl.BlockSpec(memory_space=pltpu.VMEM)
ANY = pl.BlockSpec(memory_space=pl.ANY)


def call(body, name, outs, ins, scratch=(), cid=None, us=10.0, **grid):
    whole = VMEM
    params = dict(vmem_limit_bytes=VMEM_MOST)
    if cid is not None:
        params |= dict(collective_id=cid, has_side_effects=True)
    return pl.pallas_call(
        body,
        out_shape=[jax.ShapeDtypeStruct(shape, dtype) for shape, dtype in outs],
        in_specs=grid.pop("in_specs", [whole] * len(ins)),
        out_specs=grid.pop("out_specs", [whole] * len(outs)),
        scratch_shapes=list(scratch),
        compiler_params=pltpu.CompilerParams(**params),
        cost_estimate=pl.CostEstimate(flops=0, transcendentals=0, bytes_accessed=int(us * 3e6)),
        name=name,
        **grid,
    )(*ins)


def taker(refs):
    refs = list(refs)

    def take(n=None):
        if n is None:
            return refs.pop(0)
        return [refs.pop(0) for _ in range(n)]

    return take


def dot(left, right, contract=((1,), (0,))):
    return lax.dot_general(left, right, (contract, ((), ())), preferred_element_type=F32)


def halves(values):
    high = values.astype(BF16)
    return high, (values - high.astype(F32)).astype(BF16)


def norm_scale(values):
    return lax.rsqrt(jnp.mean(values * values, axis=-1, keepdims=True) + NORM_EPSILON)


def norm_back(grad, normed, scale, gain):
    grad_hat = grad * gain
    return scale * (grad_hat - normed * jnp.mean(grad_hat * normed, axis=-1, keepdims=True))


def rotary(values, cosine, sine, back=False):
    width, half = values.shape[1], HEAD_DIMENSION // 2
    later = pltpu.roll(values, width - half, 1)
    earlier = pltpu.roll(values, half, 1)
    front = lax.broadcasted_iota(jnp.int32, values.shape, 1) % HEAD_DIMENSION < half
    other = jnp.where(front, -later, earlier)
    return values * cosine - other * sine if back else values * cosine + other * sine


def allowed_pairs(segment_row):
    size = segment_row.shape[1]
    across = jnp.broadcast_to(segment_row, (size, size))
    rows = lax.broadcasted_iota(jnp.int32, (size, size), 0)
    cols = lax.broadcasted_iota(jnp.int32, (size, size), 1)
    return (cols <= rows) & (across == across.T)


def attention_weights(stacked, keys, allowed):
    scores = dot(stacked, keys, ((1,), (1,))) * SCORE_SCALE
    scores = jnp.where(allowed, scores, MASKED_SCORE)
    row_max = jnp.max(scores, axis=-1, keepdims=True)
    log_total = row_max + jnp.log(jnp.sum(jnp.exp(scores - row_max), axis=-1, keepdims=True))
    return jnp.exp(scores - log_total)


class Heads:
    def __init__(self, ranks):
        self.q, self.kv = QUERY_HEADS // ranks, KEY_VALUE_HEADS // ranks
        self.group = QUERY_HEADS // KEY_VALUE_HEADS
        self.q_cols, self.kv_cols = self.q * HEAD_DIMENSION, self.kv * HEAD_DIMENSION
        self.cols = -(-(self.q_cols + 2 * self.kv_cols) // 128) * 128

    def stack(self, rows, kv):
        first = kv * self.group
        return jnp.concatenate([self.head(rows, first + i) for i in range(self.group)], axis=0)

    def head(self, rows, i):
        return rows[:, i * HEAD_DIMENSION : (i + 1) * HEAD_DIMENSION]

    def key(self, rows, kv):
        return self.head(rows, self.q + kv)

    def value(self, rows, kv):
        return self.head(rows, self.q + self.kv + kv)


def rope_tables(length, heads):
    frequency = np.float32(ROPE_BASE) ** (-(np.arange(HEAD_DIMENSION // 2, dtype=np.float32) * 2.0) / HEAD_DIMENSION)
    angles = np.arange(length, dtype=np.float32)[:, None] * frequency.astype(np.float32)[None, :]
    cosine, sine = (np.tile(f(angles.astype(np.float64)).astype(np.float32), (1, 2)) for f in (np.cos, np.sin))
    turned = heads.q + heads.kv
    rest = heads.cols - turned * HEAD_DIMENSION
    cosine = np.concatenate([np.tile(cosine, (1, turned)), np.ones((length, rest), np.float32)], axis=1)
    sine = np.concatenate([np.tile(sine, (1, turned)), np.zeros((length, rest), np.float32)], axis=1)
    return cosine, sine


def gain_row(misc_ref, ranks, which):
    return jnp.concatenate([misc_ref[i, which : which + 1, :] for i in range(ranks)], axis=1)


def attention_forward(ranks, heads, length, x_ref, w_ref, o_ref, misc_ref, cos_ref, sin_ref, part_ref, qkv_ref, att_ref, scale_ref):
    width = x_ref.shape[2]
    gain = gain_row(misc_ref, ranks, 0)
    weights = w_ref[...].reshape(width, heads.cols)

    def one(b, carry):
        x = x_ref[b].astype(F32)
        scale = norm_scale(x)
        scale_ref[b] = jnp.broadcast_to(scale, (length, 128))
        normed = (x * scale * gain).astype(BF16)
        qkv_ref[b] = rotary(dot(normed, weights), cos_ref[...], sin_ref[...]).astype(BF16)
        qkv = qkv_ref[b]
        allowed = allowed_pairs(misc_ref[b, 8:9, :length])
        allowed = jnp.concatenate([allowed] * heads.group, axis=0)
        outs = []
        for kv in range(heads.kv):
            probs = attention_weights(heads.stack(qkv, kv), heads.key(qkv, kv), allowed).astype(BF16)
            mixed = dot(probs, heads.value(qkv, kv)).astype(BF16)
            outs += [mixed[i * length : (i + 1) * length] for i in range(heads.group)]
        att_ref[b] = jnp.concatenate(outs, axis=1)
        part_ref[b] = dot(att_ref[b], o_ref[...]).astype(BF16)
        return carry

    lax.fori_loop(0, ranks, one, 0)


def column_experts(n_expert, slots):
    column = lax.broadcasted_iota(jnp.int32, (1, 128), 1)
    owner, slot = column // SLOT_STRIDE, column % SLOT_STRIDE
    expert = slot * n_expert + owner
    real = (owner < n_expert) & (slot < slots) & (expert < EXPERT_COUNT)
    return real, jnp.where(real, expert, -1)


def column_picks(n_expert, slots):
    _, expert = column_experts(n_expert, slots)
    return jnp.where(lax.broadcasted_iota(jnp.int32, (EXPERT_COUNT, 128), 0) == expert, 1.0, 0.0)


def route_tables(expert, routes, blocks_ref):
    tokens = routes.shape[0]
    named = jnp.zeros((tokens, 128), F32)
    for k in range(routes.shape[1]):
        named = named + jnp.where(routes[:, k : k + 1] == expert, 1.0, 0.0)
    limit = jnp.zeros((1, 128), jnp.int32)
    for e in range(EXPERT_COUNT):
        limit = jnp.where(expert == e, blocks_ref[e] * BLK, limit)
    rows = lax.broadcasted_iota(jnp.int32, (tokens, tokens), 0)
    cols = lax.broadcasted_iota(jnp.int32, (tokens, tokens), 1)
    earlier = jnp.where(cols < rows, 1.0, 0.0).astype(BF16)
    rank = dot(earlier, named.astype(BF16))
    kept = (named > 0.0) & (rank < limit.astype(F32))
    return kept, jnp.where(kept, rank, -1.0)


def route_forward(ranks, n_expert, slots, x_ref, branch_ref, misc_ref, router_ref, routes_ref, blocks_ref, hidden_ref, norm_ref, scale_ref, probs_ref, meta_ref, table_ref):
    gain = gain_row(misc_ref, ranks, 1)
    width = x_ref.shape[1]
    shard = width // ranks
    hidden = x_ref[...].astype(F32) + RESIDUAL_SCALE * branch_ref[...]
    hidden_ref[...] = hidden
    scale = norm_scale(hidden)
    scale_ref[...] = jnp.broadcast_to(scale, scale_ref.shape)
    norm = (hidden * scale * gain).astype(BF16)
    for i in range(ranks):
        norm_ref[i] = norm[:, i * shard : (i + 1) * shard]
    real, expert = column_experts(n_expert, slots)
    kept, place = route_tables(expert, routes_ref[...], blocks_ref)
    router = router_ref[...].reshape(width, -1)
    table_ref[...] = dot(router, column_picks(n_expert, slots).astype(BF16)).astype(BF16)
    logits = jnp.where(real, dot(norm, table_ref[...]), MASKED_SCORE)
    weight = jnp.exp(logits - jnp.max(logits, axis=-1, keepdims=True))
    probs = weight / jnp.sum(weight, axis=-1, keepdims=True)
    probs_ref[...] = probs
    used = n_expert * SLOT_STRIDE
    meta_ref[0] = place.T[:used]
    meta_ref[1] = jnp.where(kept, probs, 0.0).T[:used]


def row_picks(slots, place):
    number = lax.broadcasted_iota(jnp.int32, (SLOT_ROWS, place.shape[1]), 0).astype(F32)
    return jnp.concatenate([jnp.where(number == place[s : s + 1], 1.0, 0.0) for s in range(slots)], axis=0)


def row_shares(slots, share):
    return jnp.concatenate(
        [jnp.broadcast_to(share[s : s + 1], (SLOT_ROWS, share.shape[1])) for s in range(slots)], axis=0
    )


def experts(n_expert, slots, tokens, nh_ref, og_ref, meta_ref, up_ref, down_ref, out_ref, back_ref, gate_grad_ref, inner_ref, both_ref, x_sc, og_sc, eo_sc, gx_sc, nh_in, og_in, sems):
    step = pl.program_id(0)
    mine = pl.ds(pl.multiple_of(lax.axis_index("expert") * SLOT_STRIDE, SLOT_STRIDE), SLOT_STRIDE)
    ranks, _, shard = nh_ref.shape[1:]
    width = ranks * shard
    hidden = down_ref.shape[1]

    def fetch(q):
        slot = q % 2
        return [
            pltpu.make_async_copy(nh_ref.at[q], nh_in.at[slot], sems.at[0, slot]),
            pltpu.make_async_copy(og_ref.at[q], og_in.at[slot], sems.at[1, slot]),
        ]

    @pl.when(step == 0)
    def _():
        for copy in fetch(0):
            copy.start()

        def one(q, carry):
            @pl.when(q + 1 < n_expert)
            def _():
                for copy in fetch(q + 1):
                    copy.start()

            for copy in fetch(q):
                copy.wait()
            pick = row_picks(slots, meta_ref[q, 0, mine, :]).astype(BF16)
            for i in range(ranks):
                here = slice(i * shard, (i + 1) * shard)
                x_sc[q, :, here] = dot(pick, nh_in[q % 2, i]).astype(BF16)
                og_sc[q, :, here] = dot(pick, og_in[q % 2, i]).astype(BF16)
            gate_grad_ref[q] = jnp.zeros((SLOT_STRIDE, tokens), F32)
            return carry

        lax.fori_loop(0, n_expert, one, 0)

    place_of = pl.ds(pl.multiple_of(step * SLOT_ROWS, SLOT_ROWS), SLOT_ROWS)
    slot_row = lax.broadcasted_iota(jnp.int32, (SLOT_STRIDE, tokens), 0) == step
    number = lax.broadcasted_iota(jnp.int32, (SLOT_ROWS, tokens), 0).astype(F32)
    rows = n_expert * SLOT_ROWS
    x = x_sc[:, place_of, :].reshape(rows, width)
    both = dot(x, up_ref[0])
    gate, up = both[:, :hidden], both[:, hidden:]
    squash = jax.nn.sigmoid(gate)
    inner = (gate * squash * up).astype(BF16)
    inner_ref[0] = inner
    produced = dot(inner, down_ref[0]).astype(BF16)
    eo_sc[:, place_of, :] = produced.reshape(n_expert, SLOT_ROWS, width)
    masks, gates = [], []
    for q in range(n_expert):
        place = jnp.sum(jnp.where(slot_row, meta_ref[q, 0, mine, :], 0.0), axis=0, keepdims=True)
        share = jnp.sum(jnp.where(slot_row, meta_ref[q, 1, mine, :], 0.0), axis=0, keepdims=True)
        masks.append(number == place)
        gates.append(jnp.sum(jnp.where(masks[q], share, 0.0), axis=1, keepdims=True))
    mix_grad = RESIDUAL_SCALE * og_sc[:, place_of, :].reshape(rows, width).astype(F32)
    grad_rows = (jnp.concatenate(gates, axis=0) * mix_grad).astype(BF16)
    gate_grad = jnp.sum(mix_grad * produced.astype(F32), axis=1, keepdims=True)
    for q in range(n_expert):
        spread = jnp.where(masks[q], gate_grad[q * SLOT_ROWS : (q + 1) * SLOT_ROWS], 0.0)
        gate_grad_ref[q] = jnp.where(slot_row, jnp.sum(spread, axis=0, keepdims=True), gate_grad_ref[q])
    grad_inner = dot(grad_rows, down_ref[0], ((1,), (1,)))
    grad_both = jnp.concatenate(
        [grad_inner * up * squash * (1.0 + gate * (1.0 - squash)), grad_inner * (gate * squash)], axis=1
    ).astype(BF16)
    both_ref[0] = grad_both
    gx_sc[:, place_of, :] = dot(grad_both, up_ref[0], ((1,), (1,))).astype(BF16).reshape(n_expert, SLOT_ROWS, width)

    @pl.when(step == slots - 1)
    def _():
        def one(q, carry):
            pick = row_picks(slots, meta_ref[q, 0, mine, :])
            high, low = halves(pick * row_shares(slots, meta_ref[q, 1, mine, :]))
            over = ((0,), (0,))
            out_ref[q] = (dot(high, eo_sc[q], over) + dot(low, eo_sc[q], over)).astype(BF16)
            back_ref[q] = dot(pick.astype(BF16), gx_sc[q], over).astype(BF16)
            return carry

        lax.fori_loop(0, n_expert, one, 0)


def route_backward(ranks, n_expert, shard, hidden_ref, norm_ref, scale_ref, probs_ref, misc_ref, router_ref, og_ref, mixture_ref, back_ref, gate_grad_ref, out_ref, grad_hidden_ref, branch_ref, small_ref):
    tokens, width = hidden_ref.shape
    gain = gain_row(misc_ref, ranks, 1)
    hidden = hidden_ref[...]
    out_ref[...] = (hidden + RESIDUAL_SCALE * mixture_ref[...]).astype(BF16)
    used = n_expert * SLOT_STRIDE
    spread = gate_grad_ref[...].reshape(used, tokens)
    if used < 128:
        spread = jnp.concatenate([spread, jnp.zeros((128 - used, tokens), F32)], axis=0)
    grad_probs = spread.T
    probs = probs_ref[...]
    grad_logits = probs * (grad_probs - jnp.sum(probs * grad_probs, axis=1, keepdims=True))
    high, low = halves(grad_logits)
    router = router_ref[...]
    across = ((1,), (1,))
    grad_norm = back_ref[...] + (dot(high, router, across) + dot(low, router, across))
    scale = scale_ref[:, 0:1]
    normed = hidden * scale
    grad_hidden = og_ref[...].astype(F32) + norm_back(grad_norm, normed, scale, gain)
    grad_hidden_ref[...] = grad_hidden
    branch_ref[...] = (RESIDUAL_SCALE * grad_hidden).astype(BF16)
    over = ((0,), (0,))
    grad_gain = jnp.sum(grad_norm * normed, axis=0, keepdims=True)
    for i in range(ranks):
        here = slice(i * shard, (i + 1) * shard)
        grad_router = dot(high, norm_ref[i], over) + dot(low, norm_ref[i], over)
        small_ref[i, :used, :] = grad_router[:used]
        small_ref[i, used:, :] = jnp.broadcast_to(grad_gain[:, here], (8, shard))


def attention_backward(ranks, heads, length, branch_ref, att_ref, qkv_ref, o_ref, misc_ref, cos_ref, sin_ref, grad_ref, d_o_ref):
    d_o_ref[...] = dot(
        att_ref[...].reshape(ranks * length, heads.q_cols), branch_ref[...].reshape(ranks * length, -1), ((0,), (0,))
    ).astype(BF16)

    def one(b, carry):
        grad_att = dot(branch_ref[b], o_ref[...], ((1,), (1,))).astype(BF16)
        att, qkv = att_ref[b], qkv_ref[b]
        allowed = allowed_pairs(misc_ref[b, 8:9, :length])
        allowed = jnp.concatenate([allowed] * heads.group, axis=0)
        d_q, d_k, d_v = [], [], []
        for kv in range(heads.kv):
            queries, keys = heads.stack(qkv, kv), heads.key(qkv, kv)
            soft = attention_weights(queries, keys, allowed)
            grads = heads.stack(grad_att, kv)
            d_v.append(dot(soft.astype(BF16), grads, ((0,), (0,))))
            delta = jnp.sum(grads.astype(F32) * heads.stack(att, kv).astype(F32), axis=1, keepdims=True)
            inner = dot(grads, heads.value(qkv, kv), ((1,), (1,)))
            d_scores = (soft * (inner - delta) * SCORE_SCALE).astype(BF16)
            rows = dot(d_scores, keys)
            d_q += [rows[i * length : (i + 1) * length] for i in range(heads.group)]
            d_k.append(dot(d_scores, queries, ((0,), (0,))))
        spare = heads.cols - heads.q_cols - 2 * heads.kv_cols
        fill = [jnp.zeros((length, spare), F32)] if spare else []
        grads = jnp.concatenate(d_q + d_k + d_v + fill, axis=1)
        grad_ref[b] = rotary(grads, cos_ref[...], sin_ref[...], back=True).astype(BF16)
        return carry

    lax.fori_loop(0, ranks, one, 0)


def projection_backward(ranks, heads, shard, x_ref, scale_ref, gain_ref, grad_ref, w_ref, small_ref, grad_x_ref, d_w_ref, sums_ref):
    normed = x_ref[...].astype(F32) * scale_ref[:, 0:1]
    norm_input = (normed * gain_ref[0:1, :]).astype(BF16)
    total = None
    for i in range(ranks):
        grads = grad_ref[i].reshape(-1, heads.cols)
        term = dot(grads, w_ref[i], ((1,), (1,)))
        total = term if total is None else total + term
        d_w_ref[:, i * heads.cols : (i + 1) * heads.cols] = dot(norm_input, grads, ((0,), (0,))).astype(BF16)
    grad_x_ref[...] = total
    small = small_ref[0]
    for i in range(1, ranks):
        small = small + small_ref[i]
    gain_grad = jnp.sum(total * normed, axis=0, keepdims=True)
    used = small.shape[0] - 8
    sums_ref[...] = jnp.zeros_like(sums_ref)
    sums_ref[:used, :] = small[:used].astype(BF16)
    second = lax.broadcasted_iota(jnp.int32, (8, shard), 0)
    sums_ref[used : used + 8, :] = jnp.where(second == 0, small[used:], jnp.where(second == 1, gain_grad, 0.0)).astype(BF16)


def finish(ranks, n_expert, slots, heads, tokens, nh_ref, og_ref, xd_ref, ogd_ref, meta_ref, own_both_ref, both_ref, own_inner_ref, inner_ref, grad_ref, x_ref, misc_ref, grad_hidden_ref, d_w_ref, d_o_ref, sums_ref, d_up_ref, d_down_ref, grad_inputs_ref, q_ref, k_ref, v_ref, o_ref, router_ref, gain_one_ref, gain_two_ref, x_sc, og_sc, x_in, og_in, sems):
    step = pl.program_id(0)
    me = lax.axis_index("dp")
    rows = n_expert * SLOT_ROWS
    shard = x_in.shape[2]

    @pl.when(step == 0)
    def _():
        def fetch(j, q, do):
            at, slot = (me + j) % ranks, q % 2

            def both(x, og):
                do(pltpu.make_async_copy(x, x_in.at[slot], sems.at[0, slot]))
                do(pltpu.make_async_copy(og, og_in.at[slot], sems.at[1, slot]))

            if j == 0:
                both(nh_ref.at[q, me], og_ref.at[q, me])
            else:
                both(xd_ref.at[at, q], ogd_ref.at[at, q])

        for j in range(ranks):
            fetch(j, 0, lambda copy: copy.start())

            def one(q, carry):
                @pl.when(q + 1 < n_expert)
                def _():
                    fetch(j, q + 1, lambda copy: copy.start())

                fetch(j, q, lambda copy: copy.wait())
                at = (me + j) % ranks
                pick = row_picks(slots, meta_ref[at, q, 0])
                share = jnp.sum(pick * row_shares(slots, meta_ref[at, q, 1]), axis=1, keepdims=True)
                pick = pick.astype(BF16)
                x_sc[j, q] = dot(pick, x_in[q % 2]).astype(BF16)
                og_sc[j, q] = (share * (RESIDUAL_SCALE * dot(pick, og_in[q % 2]))).astype(BF16)
                return carry

            lax.fori_loop(0, n_expert, one, 0)
        gain = gain_row(misc_ref, ranks, 0)
        grad = jnp.concatenate([grad_ref[i] for i in range(ranks)], axis=1)
        x = x_ref[...].astype(F32)
        scale = norm_scale(x)
        grad_inputs_ref[...] = grad_hidden_ref[...] + norm_back(grad, x * scale, scale, gain)
        first, second = heads.q_cols, heads.q_cols + heads.kv_cols
        for i in range(ranks):
            start = i * heads.cols
            q_ref[:, i * heads.q_cols : (i + 1) * heads.q_cols] = d_w_ref[:, start : start + first].astype(F32)
            here = slice(i * heads.kv_cols, (i + 1) * heads.kv_cols)
            k_ref[:, here] = d_w_ref[:, start + first : start + second].astype(F32)
            v_ref[:, here] = d_w_ref[:, start + second : start + second + heads.kv_cols].astype(F32)
        o_ref[...] = d_o_ref[...].astype(F32)
        used = n_expert * SLOT_STRIDE
        picks = column_picks(n_expert, slots).astype(BF16)
        router_ref[...] = lax.dot_general(
            sums_ref[:128], picks, (((0,), (1,)), ((), ())), preferred_element_type=F32
        )
        ends = sums_ref[used : used + 16, :].astype(F32)
        gain_two_ref[...] = ends[0:1]
        gain_one_ref[...] = ends[1:2]

    place_of = pl.ds(pl.multiple_of(step * SLOT_ROWS, SLOT_ROWS), SLOT_ROWS)
    over = ((0,), (0,))
    d_up = d_down = None
    for j in range(ranks):
        at = (me + j) % ranks
        x = x_sc[j, :, place_of, :].reshape(rows, shard)
        og = og_sc[j, :, place_of, :].reshape(rows, shard)
        up = dot(x, own_both_ref[0] if j == 0 else both_ref[at, 0], over)
        down = dot(own_inner_ref[0] if j == 0 else inner_ref[at, 0], og, over)
        d_up, d_down = (up, down) if j == 0 else (d_up + up, d_down + down)
    d_up_ref[0] = d_up
    d_down_ref[0] = d_down


def on_device(
    inputs,
    segment_ids,
    routes,
    expert_blocks,
    norm1_gain,
    q_weight,
    k_weight,
    value_matrix,
    o_weight,
    norm2_gain,
    router_weight,
    expert_gate_up,
    expert_down,
    out_grad,
):
    ranks, n_expert = lax.axis_size("dp"), lax.axis_size("expert")
    tokens, width = inputs.shape
    shard = q_weight.shape[0]
    slots, _, double = expert_gate_up.shape
    hidden = expert_down.shape[1]
    heads = Heads(ranks)
    group = ("dp", ranks // 2, 2)
    plane = ("expert", 4, n_expert // 4)
    used = n_expert * SLOT_STRIDE
    cosine, sine = rope_tables(tokens, heads)

    gains = jnp.stack([norm1_gain, norm2_gain]).astype(F32)

    def opening(*refs):
        take = taker(refs)
        x, wq, wk, wv, rt, gn, sg, og = take(8)
        x_all, w, w_all, rt_all, ms_all, og_all, ms, og_own = take(8)
        dp, ex = Grid(*group), Grid(*plane)
        for i in range(ranks):
            at = 0
            for ref, cols in ((wq, heads.q_cols), (wk, heads.kv_cols), (wv, heads.kv_cols)):
                w[i, :, at : at + cols] = ref[:, i * cols : (i + 1) * cols]
                at += cols
            if at < heads.cols:
                w[i, :, at:] = jnp.zeros((shard, heads.cols - at), BF16)
            og_own[i] = og[:, i * shard : (i + 1) * shard]
        ms[...] = jnp.zeros_like(ms)
        ms[0:2, :] = gn[...]
        ms[8:9, :tokens] = sg[...].astype(F32)
        x_all[dp.me] = x[...]
        rt_all[dp.me] = rt[...]
        ms_all[dp.me] = ms[...]
        og_all[ex.me] = og_own[...]
        greet(dp.all() + ex.near())
        small = [begin(gather(dp, ms, ms_all, take(4))), begin(gather(dp, rt, rt_all, take(4)))]
        xs = begin(gather(dp, x, x_all, take(4)))
        ogs = begin(gather(ex, og_own, og_all, take(4)))
        ws = begin(exchange(dp, w, w_all, take(2)))
        run(*small, xs, ogs)
        run(ws)

    x_all, weights, w_all, router_all, misc_all, og_all = call(
        opening,
        "opening",
        [
            ((ranks, tokens, width), BF16),
            ((ranks, shard, heads.cols), BF16),
            ((ranks, shard, heads.cols), BF16),
            ((ranks, shard, router_weight.shape[1]), BF16),
            ((ranks, 16, shard), F32),
            ((n_expert, ranks, tokens, shard), BF16),
        ],
        (inputs, q_weight, k_weight, value_matrix, router_weight, gains, segment_ids, out_grad),
        [pltpu.VMEM((16, shard), F32), pltpu.VMEM((ranks, tokens, shard), BF16)]
        + line_sems(*group[1:]) * 3
        + line_sems(*plane[1:])
        + exchange_sems(ranks),
        cid=0,
        us=40,
    )

    part, qkv, att, scale_all = call(
        functools.partial(attention_forward, ranks, heads, tokens),
        "attention_forward",
        [
            ((ranks, tokens, width), BF16),
            ((ranks, tokens, heads.cols), BF16),
            ((ranks, tokens, heads.q_cols), BF16),
            ((ranks, tokens, 128), F32),
        ],
        (x_all, w_all, o_weight, misc_all, cosine, sine),
        us=15,
    )

    def branch_sum(*refs):
        take = taker(refs)
        terms, out = take(2)
        dp = Grid(*group)
        greet(dp.near())

        def finish(total):
            out[...] = total

        run(reduce(dp, lambda i: terms.at[i], finish, take(4), take(4)))

    (branch,) = call(
        branch_sum,
        "branch_sum",
        [((tokens, width), F32)],
        (part,),
        line_sems(*group[1:]) + sum_slots(*group[1:], (tokens, width)),
        cid=1,
        us=15,
    )

    hidden_rows, norm_hidden, scale_two, probs, meta, router = call(
        functools.partial(route_forward, ranks, n_expert, slots),
        "route_forward",
        [
            ((tokens, width), F32),
            ((ranks, tokens, shard), BF16),
            ((tokens, 128), F32),
            ((tokens, 128), F32),
            ((2, used, tokens), F32),
            ((width, 128), BF16),
        ],
        (inputs, branch, misc_all, router_all, routes, expert_blocks),
        us=5,
        in_specs=[VMEM] * 5 + [pl.BlockSpec(memory_space=pltpu.SMEM)],
    )

    def dispatch(*refs):
        take = taker(refs)
        (nh, mt), (nh_all, mt_all, xd) = take(2), take(3)
        dp, ex = Grid(*group), Grid(*plane)
        nh_all[ex.me] = nh[...]
        mt_all[ex.me] = mt[...]
        greet(dp.all() + ex.near())
        arrived, end = pass_slices(dp, xd, take(2))
        run(gather(ex, nh, nh_all, take(4), arrived), gather(ex, mt, mt_all, take(4)))
        end(range(n_expert), nh)

    norm_all, meta_all, norm_slices = call(
        dispatch,
        "dispatch",
        [
            ((n_expert, ranks, tokens, shard), BF16),
            ((n_expert, 2, used, tokens), F32),
            ((ranks, n_expert, tokens, shard), BF16),
        ],
        (norm_hidden, meta),
        [pltpu.SemaphoreType.DMA((n_expert, ranks))] * 2 + line_sems(*plane[1:]) * 2,
        cid=2,
        us=42,
        out_specs=[VMEM, VMEM, ANY],
    )

    fixed = lambda shape: pl.BlockSpec(shape, lambda s: (0,) * len(shape), pipeline_mode=pl.Buffered(1))
    moving = lambda shape: pl.BlockSpec((1,) + shape, lambda s: (s,) + (0,) * len(shape))
    packed = (n_expert, slots * SLOT_ROWS, width)
    rows = n_expert * SLOT_ROWS
    out_part, back_part, gate_grad, inner, grad_both = call(
        functools.partial(experts, n_expert, slots, tokens),
        "experts",
        [
            ((n_expert, tokens, width), BF16),
            ((n_expert, tokens, width), BF16),
            ((n_expert, SLOT_STRIDE, tokens), F32),
            ((slots, rows, hidden), BF16),
            ((slots, rows, double), BF16),
        ],
        (norm_all, og_all, meta_all, expert_gate_up, expert_down),
        [pltpu.VMEM(packed, BF16)] * 4
        + [pltpu.VMEM((2, ranks, tokens, shard), BF16)] * 2
        + [pltpu.SemaphoreType.DMA((2, 2))],
        us=40,
        grid=(slots,),
        in_specs=[ANY, ANY, fixed((n_expert, 2, used, tokens)), moving((width, double)), moving((hidden, width))],
        out_specs=[
            fixed((n_expert, tokens, width)),
            fixed((n_expert, tokens, width)),
            fixed((n_expert, SLOT_STRIDE, tokens)),
            moving((rows, hidden)),
            moving((rows, double)),
        ],
    )

    def combine(*refs):
        take = taker(refs)
        (terms, back_terms, gg, mt, gb, og), (out, back, gg_all, mt_all, gb_all, ogd) = take(6), take(6)
        mt_own = take()
        dp, ex = Grid(*group), Grid(*plane)
        mine = pl.ds(pl.multiple_of(ex.me * SLOT_STRIDE, SLOT_STRIDE), SLOT_STRIDE)
        mt_own[...] = mt[:, :, mine, :]
        mt_all[dp.me] = mt_own[...]
        greet(dp.all() + ex.all())

        def finish(to):
            def store(total):
                to[...] = total

            return store

        ggs = begin(exchange(ex, gg, gg_all, take(2)))
        mts = begin(gather(dp, mt_own, mt_all, take(4)))
        backs = begin(reduce(ex, lambda i: back_terms.at[i], finish(back), take(4), take(4)))
        gbs = begin(gather(dp, gb, gb_all, take(4)))
        arrived, end = pass_slices(dp, ogd, take(2))
        for i in range(n_expert):
            arrived(i, og.at[i])
        outs = begin(reduce(ex, lambda i: terms.at[i], finish(out), take(4), take(4)))
        run(ggs, mts)
        run(backs)
        run(gbs)
        run(outs)
        end(range(n_expert), og.at[0])

    mixture, back, gate_grads, meta_group, both_all, og_slices = call(
        combine,
        "combine",
        [
            ((tokens, width), F32),
            ((tokens, width), F32),
            ((n_expert, SLOT_STRIDE, tokens), F32),
            ((ranks, n_expert, 2, SLOT_STRIDE, tokens), F32),
            ((ranks, slots, rows, double), BF16),
            ((ranks, n_expert, tokens, shard), BF16),
        ],
        (out_part, back_part, gate_grad, meta_all, grad_both, og_all),
        [pltpu.VMEM((n_expert, 2, SLOT_STRIDE, tokens), F32)]
        + exchange_sems(n_expert)
        + line_sems(*group[1:])
        + line_sems(*plane[1:])
        + sum_slots(*plane[1:], (tokens, width))
        + line_sems(*group[1:])
        + [pltpu.SemaphoreType.DMA((n_expert, ranks))] * 2
        + line_sems(*plane[1:])
        + sum_slots(*plane[1:], (tokens, width)),
        cid=3,
        us=78,
        in_specs=[VMEM] * 4 + [ANY] * 2,
        out_specs=[VMEM] * 4 + [ANY] * 2,
    )

    output, grad_hidden, grad_branch, small = call(
        functools.partial(route_backward, ranks, n_expert, shard),
        "route_backward",
        [
            ((tokens, width), BF16),
            ((tokens, width), F32),
            ((tokens, width), BF16),
            ((ranks, used + 8, shard), F32),
        ],
        (hidden_rows, norm_hidden, scale_two, probs, misc_all, router, out_grad, mixture, back, gate_grads),
        us=6,
    )

    def share_branch(*refs):
        take = taker(refs)
        (br, sm), (br_all, sm_all) = take(2), take(2)
        dp = Grid(*group)
        greet(dp.all())
        br_all[dp.me] = br[...]
        brs = begin(gather(dp, br, br_all, take(4)))
        sms = begin(exchange(dp, sm, sm_all, take(2)))
        run(brs)
        run(sms)

    branch_all, small_all = call(
        share_branch,
        "share_branch",
        [((ranks, tokens, width), BF16), ((ranks, used + 8, shard), F32)],
        (grad_branch, small),
        line_sems(*group[1:]) + exchange_sems(ranks),
        cid=4,
        us=15,
    )

    grads, d_o = call(
        functools.partial(attention_backward, ranks, heads, tokens),
        "attention_backward",
        [((ranks, tokens, heads.cols), BF16), ((shard, width), BF16)],
        (branch_all, att, qkv, o_weight, misc_all, cosine, sine),
        us=15,
    )
    d_o = d_o.reshape(n_expert, shard // n_expert, width)

    def share_grads(*refs):
        take = taker(refs)
        (gr, do), (gr_all, do_all) = take(2), take(2)
        dp, ex = Grid(*group), Grid(*plane)
        greet(dp.near() + ex.near())
        gr_all[dp.me] = gr[...]
        run(
            gather(dp, gr, gr_all, take(4)),
            reduce_gather(ex, lambda i: do.at[i], do_all, take(), take(8), take(4)),
        )

    grads_all, d_o = call(
        share_grads,
        "share_grads",
        [((ranks, ranks, tokens, heads.cols), BF16), (d_o.shape, BF16)],
        (grads, d_o),
        line_sems(*group[1:])
        + [pltpu.VMEM(d_o.shape[1:], BF16)]
        + line_sems(*plane[1:]) * 2
        + sum_slots(*plane[1:], d_o.shape[1:]),
        cid=5,
        us=30,
    )

    x_cols = lax.dynamic_slice_in_dim(x_all.reshape(ranks * tokens, width), lax.axis_index("dp") * shard, shard, axis=1)
    sum_rows = 16 * n_expert
    grad_x, d_w, sums = call(
        functools.partial(projection_backward, ranks, heads, shard),
        "projection_backward",
        [
            ((ranks * tokens, shard), F32),
            ((shard, ranks * heads.cols), BF16),
            ((sum_rows, shard), BF16),
        ],
        (x_cols, scale_all.reshape(ranks * tokens, 128), gains, grads_all, weights, small_all),
        us=10,
    )
    grad_x = grad_x.reshape(ranks, tokens, shard)
    d_w = d_w.reshape(n_expert, shard // n_expert, ranks * heads.cols)
    sums = sums.reshape(n_expert, 16, shard)

    def closing(*refs):
        take = taker(refs)
        (gx, dw, sm, inr), (gx_all, dw_all, sm_all, inr_all) = take(4), take(4)
        dp, ex = Grid(*group), Grid(*plane)
        greet(dp.all() + ex.near())
        gxs = begin(exchange(dp, gx, gx_all, take(2)))
        sms = begin(reduce_gather(ex, lambda i: sm.at[i], sm_all, take(), take(8), take(4)))
        dws = begin(reduce_gather(ex, lambda i: dw.at[i], dw_all, take(), take(8), take(4)))
        inrs = begin(gather(dp, inr, inr_all, take(4)))
        run(sms, dws)
        run(gxs)
        run(inrs)

    grad_x, d_w, sums, inner_all = call(
        closing,
        "closing",
        [(grad_x.shape, F32), (d_w.shape, BF16), (sums.shape, BF16), ((ranks, slots, rows, hidden), BF16)],
        (grad_x, d_w, sums, inner),
        exchange_sems(ranks)
        + [pltpu.VMEM(sums.shape[1:], BF16)]
        + line_sems(*plane[1:]) * 2
        + sum_slots(*plane[1:], sums.shape[1:])
        + [pltpu.VMEM(d_w.shape[1:], BF16)]
        + line_sems(*plane[1:]) * 2
        + sum_slots(*plane[1:], d_w.shape[1:])
        + line_sems(*group[1:]),
        cid=6,
        us=55,
        in_specs=[VMEM] * 3 + [ANY],
        out_specs=[VMEM] * 3 + [ANY],
    )

    gathered = lambda shape: pl.BlockSpec((ranks, 1) + shape, lambda s: (0, s) + (0,) * len(shape))
    d_w = d_w.reshape(shard, ranks * heads.cols)
    d_o = d_o.reshape(shard, width)
    sums = sums.reshape(sum_rows, shard)
    ins = (grad_x, inputs, misc_all, grad_hidden, d_w, d_o, sums)
    outs = [
        ((slots, shard, double), F32),
        ((slots, hidden, shard), F32),
        ((tokens, width), F32),
        ((shard, QUERY_HEADS * HEAD_DIMENSION), F32),
        ((shard, KEY_VALUE_HEADS * HEAD_DIMENSION), F32),
        ((shard, KEY_VALUE_HEADS * HEAD_DIMENSION), F32),
        ((shard, width), F32),
        (router_weight.shape, F32),
        ((1, shard), F32),
        ((1, shard), F32),
    ]
    d_up, d_down, grad_inputs, d_q, d_k, d_v, d_o, d_router, gain_one, gain_two = call(
        functools.partial(finish, ranks, n_expert, slots, heads, tokens),
        "finish",
        outs,
        (norm_all, og_all, norm_slices, og_slices, meta_group, grad_both, both_all, inner, inner_all) + ins,
        [pltpu.VMEM((ranks, n_expert, slots * SLOT_ROWS, shard), BF16)] * 2
        + [pltpu.VMEM((2, tokens, shard), BF16)] * 2
        + [pltpu.SemaphoreType.DMA((2, 2))],
        us=20,
        grid=(slots,),
        in_specs=[ANY] * 4
        + [
            fixed(meta_group.shape),
            moving((rows, double)),
            gathered((rows, double)),
            moving((rows, hidden)),
            gathered((rows, hidden)),
        ]
        + [fixed(array.shape) for array in ins],
        out_specs=[moving((shard, double)), moving((hidden, shard))] + [fixed(shape) for shape, _ in outs[2:]],
    )
    return (
        output,
        grad_inputs,
        gain_one.reshape(shard),
        d_q,
        d_k,
        d_v,
        d_o,
        gain_two.reshape(shard),
        d_router,
        d_up,
        d_down,
    )


def solution(mesh):
    tokens = P(("dp", "expert"), None)
    rows = P("dp", None)
    return jax.shard_map(
        on_device,
        mesh=mesh,
        in_specs=(
            tokens,
            tokens,
            tokens,
            P(),
            P("dp"),
            rows,
            rows,
            rows,
            rows,
            P("dp"),
            rows,
            P("expert", None, None),
            P("expert", None, None),
            tokens,
        ),
        out_specs=(
            tokens,
            tokens,
            P("dp"),
            rows,
            rows,
            rows,
            rows,
            P("dp"),
            rows,
            P("expert", "dp", None),
            P("expert", None, "dp"),
        ),
        check_vma=False,
    )
```

```python
import functools
import math

import jax
import jax.numpy as jnp
import numpy as np
from jax import lax
from jax.experimental import pallas as pl
from jax.experimental.pallas import tpu as pltpu
from jax.sharding import PartitionSpec as P

QUERY_HEADS = 24
KEY_VALUE_HEADS = 8
HEAD_DIMENSION = 64
EXPERT_COUNT = 40
BLK = 4
SLOT_ROWS = 32
SLOT_STRIDE = 8

NORM_EPSILON = 1e-06
SCORE_SCALE = 0.015625
RESIDUAL_SCALE = 0.22
ROPE_BASE = 10000.0
MASKED_SCORE = -1e30

MESH = pl.DeviceIdType.MESH
F32, BF16 = jnp.float32, jnp.bfloat16
MEBI = 1024 * 1024
VMEM_MOST = 67_043_328


class Grid:
    def __init__(self, axis, A, B):
        self.axis, self.A, self.B = axis, A, B
        self.me = lax.axis_index(axis)
        self.a, self.b = self.me // B, self.me % B

    def at(self, a, b):
        return a * self.B + b

    def dev(self, a, b):
        return {self.axis: self.at(a, b)}

    def here(self):
        return {self.axis: self.me}

    def near(self):
        found = []
        if self.A > 1:
            found += [
                (self.a > 0, self.dev(self.a - 1, self.b)),
                (self.a < self.A - 1, self.dev(self.a + 1, self.b)),
            ]
        if self.B > 1:
            found += [
                (self.b > 0, self.dev(self.a, self.b - 1)),
                (self.b < self.B - 1, self.dev(self.a, self.b + 1)),
            ]
        return found

    def all(self):
        n = self.A * self.B
        return [(self.me >= 0, {self.axis: (self.me + r) % n}) for r in range(1, n)]

    def next(self, kind, way):
        step = 1 if way == 0 else -1
        if kind == "a":
            return self.ahead("a", way, 1), self.dev(self.a + step, self.b)
        return self.ahead("b", way, 1), self.dev(self.a, self.b + step)

    def behind(self, kind, way, far):
        at, size = (self.a, self.A) if kind == "a" else (self.b, self.B)
        return (at - far >= 0) if way == 0 else (at + far <= size - 1)

    def ahead(self, kind, way, far):
        return self.behind(kind, 1 - way, far)


def greet(peers):
    barrier = pltpu.get_barrier_semaphore()
    for there, device in peers:

        @pl.when(there)
        def _():
            pl.semaphore_signal(barrier, inc=1, device_id=device, device_id_type=MESH)

    pl.semaphore_wait(barrier, sum(jnp.where(there, 1, 0) for there, _ in peers))


def remote(src, dst, send, recv, device):
    return pltpu.make_async_remote_copy(
        src_ref=src, dst_ref=dst, send_sem=send, recv_sem=recv, device_id=device, device_id_type=MESH
    )


class Part:
    def __init__(self, ref, *rest):
        self.ref, self.rest, self.at = ref, rest, self

    def __getitem__(self, i):
        return self.ref.at[(i,) + self.rest]


def begin(step):
    next(step)
    return step


def run(*steps):
    steps = list(steps)
    while steps:
        left = []
        for step in steps:
            try:
                next(step)
                left.append(step)
            except StopIteration:
                pass
        steps = left


def line_sems(A, B):
    dma = pltpu.SemaphoreType.DMA
    return [dma((2, A)), dma((2, A)), dma((2, A, B)), dma((2, A, B))]


def gather(g, own, out, sems, arrived=lambda i, block: None):
    send_a, recv_a, send_b, recv_b = sems
    A, B = g.A, g.B
    row = lambda way, k: g.a - k if way == 0 else g.a + k
    col = lambda way, k: g.b - k if way == 0 else g.b + k
    rows = [(0, 0)] + [(way, k) for k in range(1, A) for way in (0, 1)]

    def along_a(way, k, src, do):
        if k < A - 1:
            there, device = g.next("a", way)
            i = g.at(row(way, k), g.b)

            @pl.when(there)
            def _():
                do(remote(src, out.at[i], send_a.at[way, k], recv_a.at[way, k + 1], device))

    def along_b(way, j, a, i, src, do):
        if j < B - 1:
            there, device = g.next("b", way)

            @pl.when(there)
            def _():
                do(remote(src, out.at[i], send_b.at[way, a, j], recv_b.at[way, a, j + 1], device))

    def start(copy):
        copy.start()

    def sent(copy):
        copy.wait_send()

    for way in (0, 1):
        along_a(way, 0, own, start)
    for way in (0, 1):
        along_b(way, 0, g.a, g.me, own, start)
    arrived(g.me, own)
    yield
    for k in range(1, A):
        for way in (0, 1):
            i = g.at(row(way, k), g.b)

            @pl.when(g.behind("a", way, k))
            def _():
                remote(out.at[i], out.at[i], send_a.at[way, k], recv_a.at[way, k], g.here()).wait_recv()
                along_a(way, k, out.at[i], start)
                for w in (0, 1):
                    along_b(w, 0, row(way, k), i, out.at[i], start)
                arrived(i, out.at[i])

            yield
    for j in range(1, B):
        for way, k in rows:
            for w in (0, 1):
                i = g.at(row(way, k), col(w, j))

                @pl.when(g.behind("a", way, k) & g.behind("b", w, j))
                def _():
                    a = row(way, k)
                    remote(out.at[i], out.at[i], send_b.at[w, a, j], recv_b.at[w, a, j], g.here()).wait_recv()
                    along_b(w, j, a, i, out.at[i], start)
                    arrived(i, out.at[i])

            yield
    for way, k in rows:
        for w in (0, 1) if k == 0 else (way,):

            @pl.when(g.behind("a", w, k))
            def _():
                along_a(w, k, own, sent)

        @pl.when(g.behind("a", way, k))
        def _():
            for w in (0, 1):
                for j in range(B - 1):

                    @pl.when(g.behind("b", w, j))
                    def _():
                        along_b(w, j, row(way, k), g.me, own, sent)


def sum_slots(A, B, block, dtype=BF16):
    return [
        pltpu.VMEM((2, A - 1) + block, dtype),
        pltpu.VMEM((2, A - 1) + block, dtype),
        pltpu.VMEM((2, A, B - 1) + block, dtype),
        pltpu.VMEM((2, A, B - 2) + block if B > 2 else (8, 128), dtype),
    ]


def reduce(g, part, finish, sems, slots):
    send_a, recv_a, send_b, recv_b = sems
    land_a, out_a, land_b, out_b = slots
    A, B = g.A, g.B
    row = lambda way, k: g.a + k if way == 0 else g.a - k
    col = lambda way, k: g.b + k if way == 0 else g.b - k
    rows = [(way, k) for k in range(A - 1, 0, -1) for way in (0, 1)] + [(0, 0)]
    here = g.here()
    first = lambda kind, way: jnp.logical_not(g.behind(kind, way, 1))

    for way, k in rows:

        @pl.when(g.ahead("a", way, k))
        def _():
            a = row(way, k)
            for j in range(B - 1, 0, -1):
                for w in (0, 1):

                    @pl.when(g.ahead("b", w, j) & first("b", w))
                    def _():
                        remote(
                            part(g.at(a, col(w, j))),
                            land_b.at[w, a, j - 1],
                            send_b.at[w, a, j],
                            recv_b.at[w, a, j - 1],
                            g.next("b", w)[1],
                        ).start()

    yield
    for way, k in rows:

        @pl.when(g.ahead("a", way, k))
        def _():
            a = row(way, k)
            for j in range(B - 2, 0, -1):
                for w in (0, 1):

                    @pl.when(g.ahead("b", w, j) & g.behind("b", w, 1))
                    def _():
                        remote(land_b.at[w, a, j], land_b.at[w, a, j], send_b.at[w, a, j], recv_b.at[w, a, j], here).wait_recv()
                        out_b[w, a, j - 1] = (
                            part(g.at(a, col(w, j)))[...].astype(F32) + land_b[w, a, j].astype(F32)
                        ).astype(out_b.dtype)
                        remote(
                            out_b.at[w, a, j - 1],
                            land_b.at[w, a, j - 1],
                            send_b.at[w, a, j],
                            recv_b.at[w, a, j - 1],
                            g.next("b", w)[1],
                        ).start()

            for w in (0, 1):
                if B > 1:

                    @pl.when(g.behind("b", w, 1))
                    def _():
                        remote(land_b.at[w, a, 0], land_b.at[w, a, 0], send_b.at[w, a, 0], recv_b.at[w, a, 0], here).wait_recv()

            def near():
                total = part(g.at(a, g.b))[...].astype(F32)
                if B == 2:
                    return total + land_b[1 - g.b, a, 0].astype(F32)
                for w in (0, 1):
                    if B > 1:
                        total = total + jnp.where(g.behind("b", w, 1), land_b[w, a, 0].astype(F32), 0.0)
                return total

            if k > 0:

                @pl.when(g.behind("a", way, 1))
                def _():
                    if k < A - 1:
                        remote(land_a.at[way, k], land_a.at[way, k], send_a.at[way, k], recv_a.at[way, k], here).wait_recv()
                        out_a[way, k - 1] = (near() + land_a[way, k].astype(F32)).astype(out_a.dtype)

                @pl.when(first("a", way))
                def _():
                    out_a[way, k - 1] = near().astype(out_a.dtype)

                remote(
                    out_a.at[way, k - 1], land_a.at[way, k - 1], send_a.at[way, k], recv_a.at[way, k - 1], g.next("a", way)[1]
                ).start()
            else:
                for w in (0, 1):
                    if A > 1:

                        @pl.when(g.behind("a", w, 1))
                        def _():
                            remote(land_a.at[w, 0], land_a.at[w, 0], send_a.at[w, 0], recv_a.at[w, 0], here).wait_recv()

                total = near()
                if A == 2:
                    total = total + land_a[1 - g.a, 0].astype(F32)
                else:
                    for w in (0, 1):
                        if A > 1:
                            total = total + jnp.where(g.behind("a", w, 1), land_a[w, 0].astype(F32), 0.0)
                finish(total)

        yield
    for way, k in rows:

        @pl.when(g.ahead("a", way, k))
        def _():
            a = row(way, k)
            for j in range(B - 1, 0, -1):
                for w in (0, 1):

                    @pl.when(g.ahead("b", w, j))
                    def _():
                        remote(part(g.me), land_b.at[w, a, j - 1], send_b.at[w, a, j], recv_b.at[w, a, j - 1], here).wait_send()

            if k > 0:
                remote(out_a.at[way, k - 1], land_a.at[way, k - 1], send_a.at[way, k], recv_a.at[way, k - 1], here).wait_send()


def reduce_gather(g, part, out, kept, sems, slots):
    def finish(total):
        kept[...] = total.astype(kept.dtype)

    yield from reduce(g, part, finish, sems[:4], slots)
    out[g.me] = kept[...]
    yield from gather(g, kept, out, sems[4:])


def exchange_sems(n):
    return [pltpu.SemaphoreType.DMA((n,)), pltpu.SemaphoreType.DMA((n,))]


def pass_slices(g, out, sems):
    send, recv = sems
    n = g.A * g.B

    def copies(i, block):
        for r in range(1, n):
            to = (g.me + r) % n
            yield remote(block.at[to], out.at[g.me, i], send.at[i, r], recv.at[i, r], {g.axis: to})

    def arrived(i, block):
        for copy in copies(i, block):
            copy.start()

    def end(blocks, block):
        for i in blocks:
            for r in range(1, n):
                mine = out.at[(g.me + n - r) % n, i]
                remote(mine, mine, send.at[i, r], recv.at[i, r], g.here()).wait_recv()
            for copy in copies(i, block):
                copy.wait_send()

    return arrived, end


def exchange(g, part, out, sems):
    send, recv = sems
    n = g.A * g.B
    copies = []
    for r in range(1, n):
        to = (g.me + r) % n
        copies.append(remote(part.at[to], out.at[g.me], send.at[r], recv.at[r], {g.axis: to}))
        copies[-1].start()
    out[g.me] = part[g.me]
    yield
    for r in range(1, n):
        origin = (g.me + n - r) % n
        remote(part.at[origin], out.at[origin], send.at[r], recv.at[r], g.here()).wait_recv()
    yield
    for copy in copies:
        copy.wait_send()


VMEM = pl.BlockSpec(memory_space=pltpu.VMEM)
ANY = pl.BlockSpec(memory_space=pl.ANY)


def call(body, name, outs, ins, scratch=(), cid=None, us=10.0, **grid):
    whole = VMEM
    params = dict(vmem_limit_bytes=VMEM_MOST)
    if cid is not None:
        params |= dict(collective_id=cid, has_side_effects=True)
    return pl.pallas_call(
        body,
        out_shape=[jax.ShapeDtypeStruct(shape, dtype) for shape, dtype in outs],
        in_specs=grid.pop("in_specs", [whole] * len(ins)),
        out_specs=grid.pop("out_specs", [whole] * len(outs)),
        scratch_shapes=list(scratch),
        compiler_params=pltpu.CompilerParams(**params),
        cost_estimate=pl.CostEstimate(flops=0, transcendentals=0, bytes_accessed=int(us * 3e6)),
        name=name,
        **grid,
    )(*ins)


def taker(refs):
    refs = list(refs)

    def take(n=None):
        if n is None:
            return refs.pop(0)
        return [refs.pop(0) for _ in range(n)]

    return take


def dot(left, right, contract=((1,), (0,))):
    return lax.dot_general(left, right, (contract, ((), ())), preferred_element_type=F32)


def halves(values):
    high = values.astype(BF16)
    return high, (values - high.astype(F32)).astype(BF16)


def norm_scale(values):
    return lax.rsqrt(jnp.mean(values * values, axis=-1, keepdims=True) + NORM_EPSILON)


def norm_back(grad, normed, scale, gain):
    grad_hat = grad * gain
    return scale * (grad_hat - normed * jnp.mean(grad_hat * normed, axis=-1, keepdims=True))


def rotary(values, cosine, sine, back=False):
    width, half = values.shape[1], HEAD_DIMENSION // 2
    later = pltpu.roll(values, width - half, 1)
    earlier = pltpu.roll(values, half, 1)
    front = lax.broadcasted_iota(jnp.int32, values.shape, 1) % HEAD_DIMENSION < half
    other = jnp.where(front, -later, earlier)
    return values * cosine - other * sine if back else values * cosine + other * sine


def allowed_pairs(segment_row):
    size = segment_row.shape[1]
    across = jnp.broadcast_to(segment_row, (size, size))
    rows = lax.broadcasted_iota(jnp.int32, (size, size), 0)
    cols = lax.broadcasted_iota(jnp.int32, (size, size), 1)
    return (cols <= rows) & (across == across.T)


def attention_weights(stacked, keys, allowed):
    scores = dot(stacked, keys, ((1,), (1,))) * SCORE_SCALE
    scores = jnp.where(allowed, scores, MASKED_SCORE)
    row_max = jnp.max(scores, axis=-1, keepdims=True)
    log_total = row_max + jnp.log(jnp.sum(jnp.exp(scores - row_max), axis=-1, keepdims=True))
    return jnp.exp(scores - log_total)


class Heads:
    def __init__(self, ranks):
        self.q, self.kv = QUERY_HEADS // ranks, KEY_VALUE_HEADS // ranks
        self.group = QUERY_HEADS // KEY_VALUE_HEADS
        self.q_cols, self.kv_cols = self.q * HEAD_DIMENSION, self.kv * HEAD_DIMENSION
        self.cols = -(-(self.q_cols + 2 * self.kv_cols) // 128) * 128

    def stack(self, rows, kv):
        first = kv * self.group
        return jnp.concatenate([self.head(rows, first + i) for i in range(self.group)], axis=0)

    def head(self, rows, i):
        return rows[:, i * HEAD_DIMENSION : (i + 1) * HEAD_DIMENSION]

    def key(self, rows, kv):
        return self.head(rows, self.q + kv)

    def value(self, rows, kv):
        return self.head(rows, self.q + self.kv + kv)


def rope_tables(length, heads):
    frequency = np.float32(ROPE_BASE) ** (-(np.arange(HEAD_DIMENSION // 2, dtype=np.float32) * 2.0) / HEAD_DIMENSION)
    angles = np.arange(length, dtype=np.float32)[:, None] * frequency.astype(np.float32)[None, :]
    cosine, sine = (np.tile(f(angles.astype(np.float64)).astype(np.float32), (1, 2)) for f in (np.cos, np.sin))
    turned = heads.q + heads.kv
    rest = heads.cols - turned * HEAD_DIMENSION
    cosine = np.concatenate([np.tile(cosine, (1, turned)), np.ones((length, rest), np.float32)], axis=1)
    sine = np.concatenate([np.tile(sine, (1, turned)), np.zeros((length, rest), np.float32)], axis=1)
    return cosine, sine


def gain_row(misc_ref, ranks, which):
    return jnp.concatenate([misc_ref[i, which : which + 1, :] for i in range(ranks)], axis=1)


def attention_forward(ranks, heads, length, x_ref, w_ref, o_ref, misc_ref, cos_ref, sin_ref, part_ref, qkv_ref, att_ref, scale_ref):
    width = x_ref.shape[2]
    gain = gain_row(misc_ref, ranks, 0)
    weights = w_ref[...].reshape(width, heads.cols)

    def one(b, carry):
        x = x_ref[b].astype(F32)
        scale = norm_scale(x)
        scale_ref[b] = jnp.broadcast_to(scale, (length, 128))
        normed = (x * scale * gain).astype(BF16)
        qkv_ref[b] = rotary(dot(normed, weights), cos_ref[...], sin_ref[...]).astype(BF16)
        qkv = qkv_ref[b]
        allowed = allowed_pairs(misc_ref[b, 8:9, :length])
        allowed = jnp.concatenate([allowed] * heads.group, axis=0)
        outs = []
        for kv in range(heads.kv):
            probs = attention_weights(heads.stack(qkv, kv), heads.key(qkv, kv), allowed).astype(BF16)
            mixed = dot(probs, heads.value(qkv, kv)).astype(BF16)
            outs += [mixed[i * length : (i + 1) * length] for i in range(heads.group)]
        att_ref[b] = jnp.concatenate(outs, axis=1)
        part_ref[b] = dot(att_ref[b], o_ref[...]).astype(BF16)
        return carry

    lax.fori_loop(0, ranks, one, 0)


def column_experts(n_expert, slots, axis):
    column = lax.broadcasted_iota(jnp.int32, (1, 128) if axis else (128, 1), axis)
    owner, slot = column // SLOT_STRIDE, column % SLOT_STRIDE
    expert = slot * n_expert + owner
    real = (owner < n_expert) & (slot < slots) & (expert < EXPERT_COUNT)
    return real, jnp.where(real, expert, -1)


def column_picks(n_expert, slots):
    _, expert = column_experts(n_expert, slots, 1)
    return jnp.where(lax.broadcasted_iota(jnp.int32, (EXPERT_COUNT, 128), 0) == expert, 1.0, 0.0)


def route_tables(n_expert, slots, routes, blocks_ref):
    tokens = routes.shape[1]
    _, expert = column_experts(n_expert, slots, 0)
    named = jnp.zeros((128, tokens), F32)
    for k in range(routes.shape[0]):
        named = named + jnp.where(routes[k : k + 1, :] == expert, 1.0, 0.0)
    limit = jnp.zeros((128, 1), jnp.int32)
    for e in range(EXPERT_COUNT):
        limit = jnp.where(expert == e, blocks_ref[e] * BLK, limit)
    rows = lax.broadcasted_iota(jnp.int32, (tokens, tokens), 0)
    cols = lax.broadcasted_iota(jnp.int32, (tokens, tokens), 1)
    earlier = jnp.where(rows < cols, 1.0, 0.0).astype(BF16)
    rank = dot(named.astype(BF16), earlier)
    kept = (named > 0.0) & (rank < limit.astype(F32))
    return kept, jnp.where(kept, rank, -1.0)


def route_forward(ranks, n_expert, slots, x_ref, branch_ref, misc_ref, router_ref, routes_ref, blocks_ref, hidden_ref, norm_ref, scale_ref, probs_ref, meta_ref, table_ref):
    gain = gain_row(misc_ref, ranks, 1)
    width = x_ref.shape[1]
    shard = width // ranks
    hidden = x_ref[...].astype(F32) + RESIDUAL_SCALE * branch_ref[...]
    hidden_ref[...] = hidden
    scale = norm_scale(hidden)
    scale_ref[...] = jnp.broadcast_to(scale, scale_ref.shape)
    norm = (hidden * scale * gain).astype(BF16)
    picks = column_picks(n_expert, slots).astype(BF16)
    for i in range(ranks):
        here = slice(i * shard, (i + 1) * shard)
        norm_ref[i] = norm[:, here]
        table_ref[here, :] = dot(router_ref[i], picks, ((0,), (0,))).astype(BF16)
    kept, place = route_tables(n_expert, slots, routes_ref[...], blocks_ref)
    real, _ = column_experts(n_expert, slots, 1)
    logits = jnp.where(real, dot(norm, table_ref[...]), MASKED_SCORE)
    weight = jnp.exp(logits - jnp.max(logits, axis=-1, keepdims=True))
    probs = weight / jnp.sum(weight, axis=-1, keepdims=True)
    probs_ref[...] = probs
    used = n_expert * SLOT_STRIDE
    meta_ref[0] = place[:used]
    meta_ref[1] = jnp.where(kept, probs.T, 0.0)[:used]


def row_picks(slots, place):
    number = lax.broadcasted_iota(jnp.int32, (SLOT_ROWS, place.shape[1]), 0).astype(F32)
    return jnp.concatenate([jnp.where(number == place[s : s + 1], 1.0, 0.0) for s in range(slots)], axis=0)


def row_shares(slots, share):
    return jnp.concatenate(
        [jnp.broadcast_to(share[s : s + 1], (SLOT_ROWS, share.shape[1])) for s in range(slots)], axis=0
    )


def experts(n_expert, slots, tokens, nh_ref, og_ref, meta_ref, up_ref, down_ref, out_ref, back_ref, gate_grad_ref, inner_ref, both_ref, x_sc, og_sc, eo_sc, gx_sc, nh_in, og_in, sems):
    step = pl.program_id(0)
    mine = pl.ds(pl.multiple_of(lax.axis_index("expert") * SLOT_STRIDE, SLOT_STRIDE), SLOT_STRIDE)
    ranks, _, shard = nh_ref.shape[1:]
    width = ranks * shard
    hidden = down_ref.shape[1]

    def fetch(q):
        slot = q % 2
        return [
            pltpu.make_async_copy(nh_ref.at[q], nh_in.at[slot], sems.at[0, slot]),
            pltpu.make_async_copy(og_ref.at[q], og_in.at[slot], sems.at[1, slot]),
        ]

    @pl.when(step == 0)
    def _():
        for copy in fetch(0):
            copy.start()

        def one(q, carry):
            @pl.when(q + 1 < n_expert)
            def _():
                for copy in fetch(q + 1):
                    copy.start()

            for copy in fetch(q):
                copy.wait()
            pick = row_picks(slots, meta_ref[q, 0, mine, :]).astype(BF16)
            for i in range(ranks):
                here = slice(i * shard, (i + 1) * shard)
                x_sc[q, :, here] = dot(pick, nh_in[q % 2, i]).astype(BF16)
                og_sc[q, :, here] = dot(pick, og_in[q % 2, i]).astype(BF16)
            gate_grad_ref[q] = jnp.zeros((SLOT_STRIDE, tokens), F32)
            return carry

        lax.fori_loop(0, n_expert, one, 0)

    place_of = pl.ds(pl.multiple_of(step * SLOT_ROWS, SLOT_ROWS), SLOT_ROWS)
    slot_row = lax.broadcasted_iota(jnp.int32, (SLOT_STRIDE, tokens), 0) == step
    number = lax.broadcasted_iota(jnp.int32, (SLOT_ROWS, tokens), 0).astype(F32)
    rows = n_expert * SLOT_ROWS
    x = x_sc[:, place_of, :].reshape(rows, width)
    both = dot(x, up_ref[0])
    gate, up = both[:, :hidden], both[:, hidden:]
    squash = jax.nn.sigmoid(gate)
    inner = (gate * squash * up).astype(BF16)
    inner_ref[0] = inner
    produced = dot(inner, down_ref[0]).astype(BF16)
    eo_sc[:, place_of, :] = produced.reshape(n_expert, SLOT_ROWS, width)
    masks, gates = [], []
    for q in range(n_expert):
        place = jnp.sum(jnp.where(slot_row, meta_ref[q, 0, mine, :], 0.0), axis=0, keepdims=True)
        share = jnp.sum(jnp.where(slot_row, meta_ref[q, 1, mine, :], 0.0), axis=0, keepdims=True)
        masks.append(number == place)
        gates.append(jnp.sum(jnp.where(masks[q], share, 0.0), axis=1, keepdims=True))
    mix_grad = RESIDUAL_SCALE * og_sc[:, place_of, :].reshape(rows, width).astype(F32)
    grad_rows = (jnp.concatenate(gates, axis=0) * mix_grad).astype(BF16)
    gate_grad = jnp.sum(mix_grad * produced.astype(F32), axis=1, keepdims=True)
    for q in range(n_expert):
        spread = jnp.where(masks[q], gate_grad[q * SLOT_ROWS : (q + 1) * SLOT_ROWS], 0.0)
        gate_grad_ref[q] = jnp.where(slot_row, jnp.sum(spread, axis=0, keepdims=True), gate_grad_ref[q])
    grad_inner = dot(grad_rows, down_ref[0], ((1,), (1,)))
    grad_both = jnp.concatenate(
        [grad_inner * up * squash * (1.0 + gate * (1.0 - squash)), grad_inner * (gate * squash)], axis=1
    ).astype(BF16)
    both_ref[0] = grad_both
    gx_sc[:, place_of, :] = dot(grad_both, up_ref[0], ((1,), (1,))).astype(BF16).reshape(n_expert, SLOT_ROWS, width)

    @pl.when(step == slots - 1)
    def _():
        def one(q, carry):
            pick = row_picks(slots, meta_ref[q, 0, mine, :])
            high, low = halves(pick * row_shares(slots, meta_ref[q, 1, mine, :]))
            over = ((0,), (0,))
            out_ref[q] = (dot(high, eo_sc[q], over) + dot(low, eo_sc[q], over)).astype(BF16)
            back_ref[q] = dot(pick.astype(BF16), gx_sc[q], over).astype(BF16)
            return carry

        lax.fori_loop(0, n_expert, one, 0)


def route_backward(ranks, n_expert, shard, hidden_ref, norm_ref, scale_ref, probs_ref, misc_ref, router_ref, og_ref, back_ref, gate_grad_ref, grad_hidden_ref, branch_ref, small_ref):
    tokens, width = hidden_ref.shape
    gain = gain_row(misc_ref, ranks, 1)
    hidden = hidden_ref[...]
    used = n_expert * SLOT_STRIDE
    spread = gate_grad_ref[...].reshape(used, tokens)
    if used < 128:
        spread = jnp.concatenate([spread, jnp.zeros((128 - used, tokens), F32)], axis=0)
    grad_probs = spread.T
    probs = probs_ref[...]
    grad_logits = probs * (grad_probs - jnp.sum(probs * grad_probs, axis=1, keepdims=True))
    high, low = halves(grad_logits)
    router = router_ref[...]
    across = ((1,), (1,))
    grad_norm = back_ref[...] + (dot(high, router, across) + dot(low, router, across))
    scale = scale_ref[:, 0:1]
    normed = hidden * scale
    grad_hidden = og_ref[...].astype(F32) + norm_back(grad_norm, normed, scale, gain)
    grad_hidden_ref[...] = grad_hidden
    branch_ref[...] = (RESIDUAL_SCALE * grad_hidden).astype(BF16)
    over = ((0,), (0,))
    grad_gain = jnp.sum(grad_norm * normed, axis=0, keepdims=True)
    for i in range(ranks):
        here = slice(i * shard, (i + 1) * shard)
        grad_router = dot(high, norm_ref[i], over) + dot(low, norm_ref[i], over)
        small_ref[i, :used, :] = grad_router[:used]
        small_ref[i, used:, :] = jnp.broadcast_to(grad_gain[:, here], (8, shard))


def store_blocks(ref, cols, values):
    count, rows = ref.shape[0], ref.shape[1]
    for i in range(count):
        ref[i, :, cols] = values[i * rows : (i + 1) * rows]


def attention_backward(ranks, heads, length, branch_ref, att_ref, qkv_ref, o_ref, misc_ref, cos_ref, sin_ref, grad_ref, d_o_ref):
    d_o = dot(att_ref[...].reshape(ranks * length, heads.q_cols), branch_ref[...].reshape(ranks * length, -1), ((0,), (0,)))
    store_blocks(d_o_ref, slice(None), d_o.astype(BF16))

    def one(b, carry):
        grad_att = dot(branch_ref[b], o_ref[...], ((1,), (1,))).astype(BF16)
        att, qkv = att_ref[b], qkv_ref[b]
        allowed = allowed_pairs(misc_ref[b, 8:9, :length])
        allowed = jnp.concatenate([allowed] * heads.group, axis=0)
        d_q, d_k, d_v = [], [], []
        for kv in range(heads.kv):
            queries, keys = heads.stack(qkv, kv), heads.key(qkv, kv)
            soft = attention_weights(queries, keys, allowed)
            grads = heads.stack(grad_att, kv)
            d_v.append(dot(soft.astype(BF16), grads, ((0,), (0,))))
            delta = jnp.sum(grads.astype(F32) * heads.stack(att, kv).astype(F32), axis=1, keepdims=True)
            inner = dot(grads, heads.value(qkv, kv), ((1,), (1,)))
            d_scores = (soft * (inner - delta) * SCORE_SCALE).astype(BF16)
            rows = dot(d_scores, keys)
            d_q += [rows[i * length : (i + 1) * length] for i in range(heads.group)]
            d_k.append(dot(d_scores, queries, ((0,), (0,))))
        spare = heads.cols - heads.q_cols - 2 * heads.kv_cols
        fill = [jnp.zeros((length, spare), F32)] if spare else []
        grads = jnp.concatenate(d_q + d_k + d_v + fill, axis=1)
        grad_ref[b] = rotary(grads, cos_ref[...], sin_ref[...], back=True).astype(BF16)
        return carry

    lax.fori_loop(0, ranks, one, 0)


def projection_backward(ranks, heads, shard, x_ref, scale_ref, gain_ref, grad_ref, w_ref, small_ref, grad_x_ref, d_w_ref, sums_ref):
    normed = x_ref[...].astype(F32) * scale_ref[:, 0:1]
    norm_input = (normed * gain_ref[0:1, :]).astype(BF16)
    total = None
    for i in range(ranks):
        grads = grad_ref[i].reshape(-1, heads.cols)
        term = dot(grads, w_ref[i], ((1,), (1,)))
        total = term if total is None else total + term
        store_blocks(d_w_ref, slice(i * heads.cols, (i + 1) * heads.cols), dot(norm_input, grads, ((0,), (0,))).astype(BF16))
    grad_x_ref[...] = total.reshape(grad_x_ref.shape)
    small = small_ref[0]
    for i in range(1, ranks):
        small = small + small_ref[i]
    gain_grad = jnp.sum(total * normed, axis=0, keepdims=True)
    used = small.shape[0] - 8
    sums_ref[...] = jnp.zeros_like(sums_ref)
    sums_ref[:used, :] = small[:used].astype(BF16)
    second = lax.broadcasted_iota(jnp.int32, (8, shard), 0)
    sums_ref[used : used + 8, :] = jnp.where(second == 0, small[used:], jnp.where(second == 1, gain_grad, 0.0)).astype(BF16)


def finish(ranks, n_expert, slots, early, heads, tokens, nh_ref, og_ref, xd_ref, ogd_ref, meta_ref, own_both_ref, both_ref, late_both_ref, own_inner_ref, inner_ref, grad_ref, x_ref, misc_ref, grad_hidden_ref, hidden_ref, mixture_ref, d_w_ref, d_o_ref, sums_ref, d_up_ref, d_down_ref, output_ref, grad_inputs_ref, q_ref, k_ref, v_ref, o_ref, router_ref, gain_one_ref, gain_two_ref, x_sc, og_sc, x_in, og_in, sems):
    step = pl.program_id(0)
    me = lax.axis_index("dp")
    rows = n_expert * SLOT_ROWS
    shard = x_in.shape[3]

    @pl.when(step == 0)
    def _():
        def fetch(j, do):
            at, slot = (me + j) % ranks, j % 2
            x, og = (nh_ref.at[:, me], og_ref.at[:, me]) if j == 0 else (xd_ref.at[at], ogd_ref.at[at])
            do(pltpu.make_async_copy(x, x_in.at[slot], sems.at[0, slot]))
            do(pltpu.make_async_copy(og, og_in.at[slot], sems.at[1, slot]))

        fetch(0, lambda copy: copy.start())
        for j in range(ranks):
            if j + 1 < ranks:
                fetch(j + 1, lambda copy: copy.start())
            fetch(j, lambda copy: copy.wait())

            def one(q, carry):
                at = (me + j) % ranks
                pick = row_picks(slots, meta_ref[at, q, 0])
                share = jnp.sum(pick * row_shares(slots, meta_ref[at, q, 1]), axis=1, keepdims=True)
                pick = pick.astype(BF16)
                x_sc[j, q] = dot(pick, x_in[j % 2, q]).astype(BF16)
                og_sc[j, q] = (share * (RESIDUAL_SCALE * dot(pick, og_in[j % 2, q]))).astype(BF16)
                return carry

            lax.fori_loop(0, n_expert, one, 0)

    @pl.when(step == slots - 1)
    def _():
        output_ref[...] = (hidden_ref[...] + RESIDUAL_SCALE * mixture_ref[...]).astype(BF16)
        gain = gain_row(misc_ref, ranks, 0)
        grad = jnp.concatenate([grad_ref[i] for i in range(ranks)], axis=1)
        x = x_ref[...].astype(F32)
        scale = norm_scale(x)
        grad_inputs_ref[...] = grad_hidden_ref[...] + norm_back(grad, x * scale, scale, gain)
        first, second = heads.q_cols, heads.q_cols + heads.kv_cols
        for i in range(ranks):
            start = i * heads.cols
            q_ref[:, i * heads.q_cols : (i + 1) * heads.q_cols] = d_w_ref[:, start : start + first].astype(F32)
            here = slice(i * heads.kv_cols, (i + 1) * heads.kv_cols)
            k_ref[:, here] = d_w_ref[:, start + first : start + second].astype(F32)
            v_ref[:, here] = d_w_ref[:, start + second : start + second + heads.kv_cols].astype(F32)
        o_ref[...] = d_o_ref[...].astype(F32)
        used = n_expert * SLOT_STRIDE
        router_ref[...] = dot(column_picks(n_expert, slots).astype(BF16), sums_ref[:128])
        ends = sums_ref[used : used + 16, :].astype(F32)
        gain_two_ref[...] = ends[0:1]
        gain_one_ref[...] = ends[1:2]

    place_of = pl.ds(pl.multiple_of(step * SLOT_ROWS, SLOT_ROWS), SLOT_ROWS)
    over = ((0,), (0,))

    def form(their_both):
        d_up = d_down = None
        for j in range(ranks):
            at = (me + j) % ranks
            x = x_sc[j, :, place_of, :].reshape(rows, shard)
            og = og_sc[j, :, place_of, :].reshape(rows, shard)
            up = dot(x, own_both_ref[0] if j == 0 else their_both[at, 0], over)
            down = dot(own_inner_ref[0] if j == 0 else inner_ref[at, 0], og, over)
            d_up, d_down = (up, down) if j == 0 else (d_up + up, d_down + down)
        d_up_ref[0] = d_up
        d_down_ref[0] = d_down

    @pl.when(step < early)
    def _():
        form(both_ref)

    @pl.when(step >= early)
    def _():
        form(late_both_ref)


def on_device(
    inputs,
    segment_ids,
    routes,
    expert_blocks,
    norm1_gain,
    q_weight,
    k_weight,
    value_matrix,
    o_weight,
    norm2_gain,
    router_weight,
    expert_gate_up,
    expert_down,
    out_grad,
):
    ranks, n_expert = lax.axis_size("dp"), lax.axis_size("expert")
    tokens, width = inputs.shape
    shard = q_weight.shape[0]
    slots, _, double = expert_gate_up.shape
    hidden = expert_down.shape[1]
    heads = Heads(ranks)
    group = ("dp", ranks // 2, 2)
    plane = ("expert", 4, n_expert // 4)
    used = n_expert * SLOT_STRIDE
    cosine, sine = rope_tables(tokens, heads)

    gains = jnp.stack([norm1_gain, norm2_gain]).astype(F32)

    def opening(*refs):
        take = taker(refs)
        x, wq, wk, wv, rt, gn, sg, og = take(8)
        x_all, w, w_all, rt_all, ms_all, og_all, ms, og_own = take(8)
        dp, ex = Grid(*group), Grid(*plane)
        for i in range(ranks):
            at = 0
            for ref, cols in ((wq, heads.q_cols), (wk, heads.kv_cols), (wv, heads.kv_cols)):
                w[i, :, at : at + cols] = ref[:, i * cols : (i + 1) * cols]
                at += cols
            if at < heads.cols:
                w[i, :, at:] = jnp.zeros((shard, heads.cols - at), BF16)
            og_own[i] = og[:, i * shard : (i + 1) * shard]
        ms[...] = jnp.zeros_like(ms)
        ms[0:2, :] = gn[...]
        ms[8:9, :tokens] = sg[...].astype(F32)
        x_all[dp.me] = x[...]
        rt_all[dp.me] = rt[...]
        ms_all[dp.me] = ms[...]
        og_all[ex.me] = og_own[...]
        greet(dp.all() + ex.near())
        small = [begin(gather(dp, ms, ms_all, take(4))), begin(gather(dp, rt, rt_all, take(4)))]
        xs = begin(gather(dp, x, x_all, take(4)))
        ogs = begin(gather(ex, og_own, og_all, take(4)))
        ws = begin(exchange(dp, w, w_all, take(2)))
        run(*small, xs, ogs)
        run(ws)

    x_all, weights, w_all, router_all, misc_all, og_all = call(
        opening,
        "opening",
        [
            ((ranks, tokens, width), BF16),
            ((ranks, shard, heads.cols), BF16),
            ((ranks, shard, heads.cols), BF16),
            ((ranks, router_weight.shape[1], shard), BF16),
            ((ranks, 16, shard), F32),
            ((n_expert, ranks, tokens, shard), BF16),
        ],
        (inputs, q_weight, k_weight, value_matrix, router_weight.T, gains, segment_ids, out_grad),
        [pltpu.VMEM((16, shard), F32), pltpu.VMEM((ranks, tokens, shard), BF16)]
        + line_sems(*group[1:]) * 3
        + line_sems(*plane[1:])
        + exchange_sems(ranks),
        cid=0,
        us=40,
    )

    part, qkv, att, scale_all = call(
        functools.partial(attention_forward, ranks, heads, tokens),
        "attention_forward",
        [
            ((ranks, tokens, width), BF16),
            ((ranks, tokens, heads.cols), BF16),
            ((ranks, tokens, heads.q_cols), BF16),
            ((ranks, tokens, 128), F32),
        ],
        (x_all, w_all, o_weight, misc_all, cosine, sine),
        us=15,
    )

    def branch_sum(*refs):
        take = taker(refs)
        terms, out = take(2)
        dp = Grid(*group)
        greet(dp.near())

        def finish(total):
            out[...] = total

        run(reduce(dp, lambda i: terms.at[i], finish, take(4), take(4)))

    (branch,) = call(
        branch_sum,
        "branch_sum",
        [((tokens, width), F32)],
        (part,),
        line_sems(*group[1:]) + sum_slots(*group[1:], (tokens, width)),
        cid=1,
        us=15,
    )

    hidden_rows, norm_hidden, scale_two, probs, meta, router = call(
        functools.partial(route_forward, ranks, n_expert, slots),
        "route_forward",
        [
            ((tokens, width), F32),
            ((ranks, tokens, shard), BF16),
            ((tokens, 128), F32),
            ((tokens, 128), F32),
            ((2, used, tokens), F32),
            ((width, 128), BF16),
        ],
        (inputs, branch, misc_all, router_all, routes.T, expert_blocks),
        us=5,
        in_specs=[VMEM] * 5 + [pl.BlockSpec(memory_space=pltpu.SMEM)],
    )

    def dispatch(*refs):
        take = taker(refs)
        (nh, mt), (nh_all, mt_all, xd) = take(2), take(3)
        dp, ex = Grid(*group), Grid(*plane)
        nh_all[ex.me] = nh[...]
        mt_all[ex.me] = mt[...]
        greet(dp.all() + ex.near())
        arrived, end = pass_slices(dp, xd, take(2))
        run(gather(ex, nh, nh_all, take(4), arrived), gather(ex, mt, mt_all, take(4)))
        end(range(n_expert), nh)

    norm_all, meta_all, norm_slices = call(
        dispatch,
        "dispatch",
        [
            ((n_expert, ranks, tokens, shard), BF16),
            ((n_expert, 2, used, tokens), F32),
            ((ranks, n_expert, tokens, shard), BF16),
        ],
        (norm_hidden, meta),
        [pltpu.SemaphoreType.DMA((n_expert, ranks))] * 2 + line_sems(*plane[1:]) * 2,
        cid=2,
        us=42,
        out_specs=[VMEM, VMEM, ANY],
    )

    fixed = lambda shape: pl.BlockSpec(shape, lambda s: (0,) * len(shape), pipeline_mode=pl.Buffered(1))
    moving = lambda shape: pl.BlockSpec((1,) + shape, lambda s: (s,) + (0,) * len(shape))
    packed = (n_expert, slots * SLOT_ROWS, width)
    rows = n_expert * SLOT_ROWS
    out_part, back_part, gate_grad, inner, grad_both = call(
        functools.partial(experts, n_expert, slots, tokens),
        "experts",
        [
            ((n_expert, tokens, width), BF16),
            ((n_expert, tokens, width), BF16),
            ((n_expert, SLOT_STRIDE, tokens), F32),
            ((slots, rows, hidden), BF16),
            ((slots, rows, double), BF16),
        ],
        (norm_all, og_all, meta_all, expert_gate_up, expert_down),
        [pltpu.VMEM(packed, BF16)] * 4
        + [pltpu.VMEM((2, ranks, tokens, shard), BF16)] * 2
        + [pltpu.SemaphoreType.DMA((2, 2))],
        us=40,
        grid=(slots,),
        in_specs=[ANY, ANY, fixed((n_expert, 2, used, tokens)), moving((width, double)), moving((hidden, width))],
        out_specs=[
            fixed((n_expert, tokens, width)),
            fixed((n_expert, tokens, width)),
            fixed((n_expert, SLOT_STRIDE, tokens)),
            moving((rows, hidden)),
            moving((rows, double)),
        ],
    )

    early = slots * 3 // 5

    def combine(*refs):
        take = taker(refs)
        (back_terms, gg, mt, gb), (back, gg_all, mt_all, gb_all) = take(4), take(4)
        mt_own = take()
        dp, ex = Grid(*group), Grid(*plane)
        mine = pl.ds(pl.multiple_of(ex.me * SLOT_STRIDE, SLOT_STRIDE), SLOT_STRIDE)
        mt_own[...] = mt[:, :, mine, :]
        mt_all[dp.me] = mt_own[...]
        greet(dp.all() + ex.all())

        def store(total):
            back[...] = total

        ggs = begin(exchange(ex, gg, gg_all, take(2)))
        mts = begin(gather(dp, mt_own, mt_all, take(4)))
        backs = begin(reduce(ex, lambda i: back_terms.at[i], store, take(4), take(4)))
        gbs = begin(gather(dp, gb.at[pl.ds(0, early)], gb_all, take(4)))
        run(ggs, mts)
        run(backs)
        run(gbs)

    back, gate_grads, meta_group, both_all = call(
        combine,
        "combine",
        [
            ((tokens, width), F32),
            ((n_expert, SLOT_STRIDE, tokens), F32),
            ((ranks, n_expert, 2, SLOT_STRIDE, tokens), F32),
            ((ranks, early, rows, double), BF16),
        ],
        (back_part, gate_grad, meta_all, grad_both),
        [pltpu.VMEM((n_expert, 2, SLOT_STRIDE, tokens), F32)]
        + exchange_sems(n_expert)
        + line_sems(*group[1:])
        + line_sems(*plane[1:])
        + sum_slots(*plane[1:], (tokens, width))
        + line_sems(*group[1:]),
        cid=3,
        us=42,
        in_specs=[VMEM] * 3 + [ANY],
        out_specs=[VMEM] * 3 + [ANY],
    )

    grad_hidden, grad_branch, small = call(
        functools.partial(route_backward, ranks, n_expert, shard),
        "route_backward",
        [
            ((tokens, width), F32),
            ((tokens, width), BF16),
            ((ranks, used + 8, shard), F32),
        ],
        (hidden_rows, norm_hidden, scale_two, probs, misc_all, router, out_grad, back, gate_grads),
        us=6,
    )

    sum_rows = 16 * n_expert
    part_rows = shard // n_expert
    o_block, w_block, s_block = (part_rows, width), (part_rows, ranks * heads.cols), (16, shard)

    def backward(*refs):
        take = taker(refs)
        br, sm, at, qkv, wo, ms, cs, sn, xa, sc, gn, w, terms, og, gb, inr = take(16)
        mix, gx_all, do_all, dw_all, su_all, ogd, gb_all, inr_all = take(8)
        br_all, sm_all, gr, gr_all, do, dw, su, gx, xc = take(9)
        dp, ex = Grid(*group), Grid(*plane)
        br_all[dp.me] = br[...]
        greet(dp.all() + ex.near())

        def store(total):
            mix[...] = total

        brs = begin(gather(dp, br, br_all, take(4)))
        sms = begin(exchange(dp, sm, sm_all, take(2)))
        outs = begin(reduce(ex, lambda i: terms.at[i], store, take(4), take(4)))
        run(brs)
        arrived, end = pass_slices(dp, ogd, take(2))
        for i in range(n_expert // 3):
            arrived(i, og.at[i])
        for i in range(ranks):

            @pl.when(dp.me == i)
            def _():
                for b in range(ranks):
                    xc[b * tokens : (b + 1) * tokens, :] = xa[b, :, i * shard : (i + 1) * shard]

        attention_backward(ranks, heads, tokens, br_all, at, qkv, wo, ms, cs, sn, gr, do)
        gr_all[dp.me] = gr[...]
        grs = begin(gather(dp, gr, gr_all, take(4)))
        dos = begin(reduce_gather(ex, lambda i: do.at[i], do_all, take(), take(8), take(4)))
        run(sms)
        run(outs)
        run(grs)
        for i in range(n_expert // 3, n_expert):
            arrived(i, og.at[i])
        inrs = begin(gather(dp, inr, inr_all, take(4)))
        gbs = begin(gather(dp, gb.at[pl.ds(early, slots - early)], gb_all, take(4)))
        projection_backward(ranks, heads, shard, xc, sc, gn, gr_all, w, sm_all, gx, dw, su)
        gxs = begin(exchange(dp, gx, gx_all, take(2)))
        sus = begin(reduce_gather(ex, lambda i: su.at[pl.ds(pl.multiple_of(i * 16, 16), 16)], su_all, take(), take(8), take(4)))
        dws = begin(reduce_gather(ex, lambda i: dw.at[i], dw_all, take(), take(8), take(4)))
        run(dos)
        run(sus)
        run(dws)
        run(gxs)
        run(inrs)
        run(gbs)
        end(range(n_expert), og.at[0])

    summed = lambda block: [pltpu.VMEM(block, BF16)] + line_sems(*plane[1:]) * 2 + sum_slots(*plane[1:], block)
    mixture, grad_x, d_o, d_w, sums, og_slices, both_late, inner_all = call(
        backward,
        "backward",
        [
            ((tokens, width), F32),
            ((ranks, tokens, shard), F32),
            ((n_expert,) + o_block, BF16),
            ((n_expert,) + w_block, BF16),
            ((n_expert,) + s_block, BF16),
            ((ranks, n_expert, tokens, shard), BF16),
            ((ranks, slots - early, rows, double), BF16),
            ((ranks, slots, rows, hidden), BF16),
        ],
        (
            grad_branch,
            small,
            att,
            qkv,
            o_weight,
            misc_all,
            cosine,
            sine,
            x_all,
            scale_all.reshape(ranks * tokens, 128),
            gains,
            weights,
            out_part,
            og_all,
            grad_both,
            inner,
        ),
        [
            pltpu.VMEM((ranks, tokens, width), BF16),
            pltpu.VMEM((ranks, used + 8, shard), F32),
            pltpu.VMEM((ranks, tokens, heads.cols), BF16),
            pltpu.VMEM((ranks, ranks, tokens, heads.cols), BF16),
            pltpu.VMEM((n_expert,) + o_block, BF16),
            pltpu.VMEM((n_expert,) + w_block, BF16),
            pltpu.VMEM((sum_rows, shard), BF16),
            pltpu.VMEM((ranks, tokens, shard), F32),
            pltpu.VMEM((ranks * tokens, shard), BF16),
        ]
        + line_sems(*group[1:])
        + exchange_sems(ranks)
        + line_sems(*plane[1:])
        + sum_slots(*plane[1:], (tokens, width))
        + [pltpu.SemaphoreType.DMA((n_expert, ranks))] * 2
        + line_sems(*group[1:])
        + summed(o_block)
        + line_sems(*group[1:]) * 2
        + exchange_sems(ranks)
        + summed(s_block)
        + summed(w_block),
        cid=4,
        us=130,
        in_specs=[VMEM] * 13 + [ANY] * 3,
        out_specs=[VMEM] * 5 + [ANY] * 3,
    )

    held = pl.Buffered(2 if ranks * rows <= 1024 else 1)
    gathered = lambda shape, at: pl.BlockSpec(
        (ranks, 1) + shape, lambda s: (0, at(s)) + (0,) * len(shape), pipeline_mode=held
    )
    d_w = d_w.reshape(shard, ranks * heads.cols)
    d_o = d_o.reshape(shard, width)
    sums = sums.reshape(sum_rows, shard)
    ins = (grad_x, inputs, misc_all, grad_hidden, hidden_rows, mixture, d_w, d_o, sums)
    outs = [
        ((slots, shard, double), F32),
        ((slots, hidden, shard), F32),
        ((tokens, width), BF16),
        ((tokens, width), F32),
        ((shard, QUERY_HEADS * HEAD_DIMENSION), F32),
        ((shard, KEY_VALUE_HEADS * HEAD_DIMENSION), F32),
        ((shard, KEY_VALUE_HEADS * HEAD_DIMENSION), F32),
        ((shard, width), F32),
        ((router_weight.shape[1], shard), F32),
        ((1, shard), F32),
        ((1, shard), F32),
    ]
    d_up, d_down, output, grad_inputs, d_q, d_k, d_v, d_o, d_router, gain_one, gain_two = call(
        functools.partial(finish, ranks, n_expert, slots, early, heads, tokens),
        "finish",
        outs,
        (norm_all, og_all, norm_slices, og_slices, meta_group, grad_both, both_all, both_late, inner, inner_all) + ins,
        [pltpu.VMEM((ranks, n_expert, slots * SLOT_ROWS, shard), BF16)] * 2
        + [pltpu.VMEM((2, n_expert, tokens, shard), BF16)] * 2
        + [pltpu.SemaphoreType.DMA((2, 2))],
        us=20,
        grid=(slots,),
        in_specs=[ANY] * 4
        + [
            fixed(meta_group.shape),
            moving((rows, double)),
            gathered((rows, double), lambda s: jnp.minimum(s, early - 1)),
            gathered((rows, double), lambda s: jnp.maximum(s - early, 0)),
            moving((rows, hidden)),
            gathered((rows, hidden), lambda s: s),
        ]
        + [fixed(array.shape) for array in ins],
        out_specs=[moving((shard, double)), moving((hidden, shard))] + [fixed(shape) for shape, _ in outs[2:]],
    )
    return (
        output,
        grad_inputs,
        gain_one.reshape(shard),
        d_q,
        d_k,
        d_v,
        d_o,
        gain_two.reshape(shard),
        d_router.T,
        d_up,
        d_down,
    )


def solution(mesh):
    tokens = P(("dp", "expert"), None)
    rows = P("dp", None)
    return jax.shard_map(
        on_device,
        mesh=mesh,
        in_specs=(
            tokens,
            tokens,
            tokens,
            P(),
            P("dp"),
            rows,
            rows,
            rows,
            rows,
            P("dp"),
            rows,
            P("expert", None, None),
            P("expert", None, None),
            tokens,
        ),
        out_specs=(
            tokens,
            tokens,
            P("dp"),
            rows,
            rows,
            rows,
            rows,
            P("dp"),
            rows,
            P("expert", "dp", None),
            P("expert", None, "dp"),
        ),
        check_vma=False,
    )
```

```python
import functools
import math

import jax
import jax.numpy as jnp
import numpy as np
from jax import lax
from jax.experimental import pallas as pl
from jax.experimental.pallas import tpu as pltpu
from jax.sharding import PartitionSpec as P

QUERY_HEADS = 24
KEY_VALUE_HEADS = 8
HEAD_DIMENSION = 64
EXPERT_COUNT = 40
BLK = 4
SLOT_ROWS = 32
SLOT_STRIDE = 8

NORM_EPSILON = 1e-06
SCORE_SCALE = 0.015625
RESIDUAL_SCALE = 0.22
ROPE_BASE = 10000.0
MASKED_SCORE = -1e30

MESH = pl.DeviceIdType.MESH
F32, BF16 = jnp.float32, jnp.bfloat16
MEBI = 1024 * 1024
VMEM_MOST = 67_043_328


class Grid:
    def __init__(self, axis, A, B, step_a=None, step_b=1):
        self.axis, self.A, self.B = axis, A, B
        self.step_a, self.step_b = B if step_a is None else step_a, step_b
        self.me = lax.axis_index(axis)
        self.a, self.b = self.me // self.step_a % A, self.me // self.step_b % B

    def at(self, a, b):
        return a * self.step_a + b * self.step_b

    def dev(self, a, b):
        return {self.axis: self.at(a, b)}

    def here(self):
        return {self.axis: self.me}

    def near(self):
        found = []
        if self.A > 1:
            found += [
                (self.a > 0, self.dev(self.a - 1, self.b)),
                (self.a < self.A - 1, self.dev(self.a + 1, self.b)),
            ]
        found += [(self.me >= 0, self.dev(self.a, (self.b + r) % self.B)) for r in range(1, self.B)]
        return found

    def all(self):
        n = self.A * self.B
        return [(self.me >= 0, {self.axis: (self.me + r) % n}) for r in range(1, n)]

    def next(self, kind, way):
        step = 1 if way == 0 else -1
        if kind == "a":
            return self.ahead("a", way, 1), self.dev(self.a + step, self.b)
        return self.ahead("b", way, 1), self.dev(self.a, self.b + step)

    def behind(self, kind, way, far):
        at, size = (self.a, self.A) if kind == "a" else (self.b, self.B)
        return (at - far >= 0) if way == 0 else (at + far <= size - 1)

    def ahead(self, kind, way, far):
        return self.behind(kind, 1 - way, far)


def greet(peers):
    barrier = pltpu.get_barrier_semaphore()
    for there, device in peers:

        @pl.when(there)
        def _():
            pl.semaphore_signal(barrier, inc=1, device_id=device, device_id_type=MESH)

    pl.semaphore_wait(barrier, sum(jnp.where(there, 1, 0) for there, _ in peers))


def remote(src, dst, send, recv, device):
    return pltpu.make_async_remote_copy(
        src_ref=src, dst_ref=dst, send_sem=send, recv_sem=recv, device_id=device, device_id_type=MESH
    )


class Part:
    def __init__(self, ref, *rest):
        self.ref, self.rest, self.at = ref, rest, self

    def __getitem__(self, i):
        return self.ref.at[(i,) + self.rest]


def begin(step):
    next(step)
    return step


def advance(step, count):
    for _ in range(count):
        next(step)


def run(*steps):
    steps = list(steps)
    while steps:
        left = []
        for step in steps:
            try:
                next(step)
                left.append(step)
            except StopIteration:
                pass
        steps = left


def line_sems(A, B):
    dma = pltpu.SemaphoreType.DMA
    return [dma((2, A)), dma((2, A)), dma((2, A, B)), dma((2, A, B))]


def gather(g, own, out, sems, arrived=lambda i, block: None):
    send_a, recv_a, send_b, recv_b = sems
    A, B = g.A, g.B
    row = lambda way, k: g.a - k if way == 0 else g.a + k
    col = lambda way, k: g.b - k if way == 0 else g.b + k
    rows = [(0, 0)] + [(way, k) for k in range(1, A) for way in (0, 1)]

    def along_a(way, k, src, do):
        if k < A - 1:
            there, device = g.next("a", way)
            i = g.at(row(way, k), g.b)

            @pl.when(there)
            def _():
                do(remote(src, out.at[i], send_a.at[way, k], recv_a.at[way, k + 1], device))

    def along_b(way, j, a, i, src, do):
        if j < B - 1:
            there, device = g.next("b", way)

            @pl.when(there)
            def _():
                do(remote(src, out.at[i], send_b.at[way, a, j], recv_b.at[way, a, j + 1], device))

    def start(copy):
        copy.start()

    def sent(copy):
        copy.wait_send()

    for way in (0, 1):
        along_a(way, 0, own, start)
    for way in (0, 1):
        along_b(way, 0, g.a, g.me, own, start)
    arrived(g.me, own)
    yield
    for k in range(1, A):
        for way in (0, 1):
            i = g.at(row(way, k), g.b)

            @pl.when(g.behind("a", way, k))
            def _():
                remote(out.at[i], out.at[i], send_a.at[way, k], recv_a.at[way, k], g.here()).wait_recv()
                along_a(way, k, out.at[i], start)
                for w in (0, 1):
                    along_b(w, 0, row(way, k), i, out.at[i], start)
                arrived(i, out.at[i])

            yield
    for j in range(1, B):
        for way, k in rows:
            for w in (0, 1):
                i = g.at(row(way, k), col(w, j))

                @pl.when(g.behind("a", way, k) & g.behind("b", w, j))
                def _():
                    a = row(way, k)
                    remote(out.at[i], out.at[i], send_b.at[w, a, j], recv_b.at[w, a, j], g.here()).wait_recv()
                    along_b(w, j, a, i, out.at[i], start)
                    arrived(i, out.at[i])

            yield
    for way, k in rows:
        for w in (0, 1) if k == 0 else (way,):

            @pl.when(g.behind("a", w, k))
            def _():
                along_a(w, k, own, sent)

        @pl.when(g.behind("a", way, k))
        def _():
            for w in (0, 1):
                for j in range(B - 1):

                    @pl.when(g.behind("b", w, j))
                    def _():
                        along_b(w, j, row(way, k), g.me, own, sent)


def sum_slots(A, B, block, dtype=BF16):
    return [
        pltpu.VMEM((A + 1,) + block, dtype),
        pltpu.VMEM((A,) + block, dtype),
        pltpu.VMEM((A, B - 1) + block, dtype),
    ]


def reduce(g, part, finish, sems, slots):
    send_a, recv_a, send_b, recv_b = sems
    land_a, out_a, land_b = slots
    A, B = g.A, g.B
    row = lambda way, k: g.a + k if way == 0 else g.a - k
    rows = [(way, k) for k in range(A - 1, 0, -1) for way in (0, 1)] + [(0, 0)]
    here = g.here()

    def across(a, r):
        to = (g.b + r) % B
        return remote(part(g.at(a, to)), land_b.at[a, r - 1], send_b.at[0, a, r], recv_b.at[0, a, r], g.dev(g.a, to))

    def landing(way, k):
        return land_a.at[A if k == 0 and way == 1 else row(way, k)]

    def along(way, k):
        to = A if k == 1 and way == 1 else row(way, k)
        return remote(
            out_a.at[row(way, k)], land_a.at[to], send_a.at[way, k], recv_a.at[way, k - 1], g.next("a", way)[1]
        )

    def landed(way, k):
        remote(landing(way, k), landing(way, k), send_a.at[way, k], recv_a.at[way, k], here).wait_recv()

    for way, k in rows:

        @pl.when(g.ahead("a", way, k))
        def _():
            for r in range(1, B):
                across(row(way, k), r).start()

    yield
    for way, k in rows:

        @pl.when(g.ahead("a", way, k))
        def _():
            a = row(way, k)
            for r in range(1, B):
                mine = land_b.at[a, r - 1]
                remote(mine, mine, send_b.at[0, a, r], recv_b.at[0, a, r], here).wait_recv()

            def near():
                total = part(g.at(a, g.b))[...].astype(F32)
                for r in range(1, B):
                    total = total + land_b[a, r - 1].astype(F32)
                return total

            if k > 0:
                if k < A - 1:

                    @pl.when(g.behind("a", way, 1))
                    def _():
                        landed(way, k)
                        out_a[a] = (near() + landing(way, k)[...].astype(F32)).astype(out_a.dtype)

                @pl.when(jnp.logical_not(g.behind("a", way, 1)))
                def _():
                    out_a[a] = near().astype(out_a.dtype)

                along(way, k).start()
            else:
                for w in (0, 1):
                    if A > 1:

                        @pl.when(g.behind("a", w, 1))
                        def _():
                            landed(w, 0)

                total = near()
                if A == 2:
                    total = total + land_a[jnp.where(g.a == 1, 1, A)].astype(F32)
                else:
                    for w in (0, 1):
                        if A > 1:
                            total = total + jnp.where(g.behind("a", w, 1), landing(w, 0)[...].astype(F32), 0.0)
                finish(total)

        yield
    for way, k in rows:

        @pl.when(g.ahead("a", way, k))
        def _():
            for r in range(1, B):
                across(row(way, k), r).wait_send()
            if k > 0:
                along(way, k).wait_send()


def reduce_gather(g, part, out, kept, sems, slots):
    def finish(total):
        kept[...] = total.astype(kept.dtype)

    yield from reduce(g, part, finish, sems[:4], slots)
    out[g.me] = kept[...]
    yield from gather(g, kept, out, sems[4:])


def exchange_sems(n):
    return [pltpu.SemaphoreType.DMA((n,)), pltpu.SemaphoreType.DMA((n,))]


def pass_slices(g, out, sems):
    send, recv = sems
    n = g.A * g.B

    def copies(i, block):
        for r in range(1, n):
            to = (g.me + r) % n
            yield remote(block.at[to], out.at[g.me, i], send.at[i, r], recv.at[i, r], {g.axis: to})

    def arrived(i, block):
        for copy in copies(i, block):
            copy.start()

    def end(blocks, block):
        for i in blocks:
            for r in range(1, n):
                mine = out.at[(g.me + n - r) % n, i]
                remote(mine, mine, send.at[i, r], recv.at[i, r], g.here()).wait_recv()
            for copy in copies(i, block):
                copy.wait_send()

    return arrived, end


def exchange(g, part, out, sems):
    send, recv = sems
    n = g.A * g.B
    copies = []
    for r in range(1, n):
        to = (g.me + r) % n
        copies.append(remote(part.at[to], out.at[g.me], send.at[r], recv.at[r], {g.axis: to}))
        copies[-1].start()
    out[g.me] = part[g.me]
    yield
    for r in range(1, n):
        origin = (g.me + n - r) % n
        remote(part.at[origin], out.at[origin], send.at[r], recv.at[r], g.here()).wait_recv()
    yield
    for copy in copies:
        copy.wait_send()


VMEM = pl.BlockSpec(memory_space=pltpu.VMEM)
ANY = pl.BlockSpec(memory_space=pl.ANY)


def call(body, name, outs, ins, scratch=(), cid=None, us=10.0, **grid):
    whole = VMEM
    params = dict(vmem_limit_bytes=VMEM_MOST)
    if cid is not None:
        params |= dict(collective_id=cid, has_side_effects=True)
    return pl.pallas_call(
        body,
        out_shape=[jax.ShapeDtypeStruct(shape, dtype) for shape, dtype in outs],
        in_specs=grid.pop("in_specs", [whole] * len(ins)),
        out_specs=grid.pop("out_specs", [whole] * len(outs)),
        scratch_shapes=list(scratch),
        compiler_params=pltpu.CompilerParams(**params),
        cost_estimate=pl.CostEstimate(flops=0, transcendentals=0, bytes_accessed=int(us * 3e6)),
        name=name,
        **grid,
    )(*ins)


def taker(refs):
    refs = list(refs)

    def take(n=None):
        if n is None:
            return refs.pop(0)
        return [refs.pop(0) for _ in range(n)]

    return take


def dot(left, right, contract=((1,), (0,))):
    return lax.dot_general(left, right, (contract, ((), ())), preferred_element_type=F32)


def halves(values):
    high = values.astype(BF16)
    return high, (values - high.astype(F32)).astype(BF16)


def norm_scale(values):
    return lax.rsqrt(jnp.mean(values * values, axis=-1, keepdims=True) + NORM_EPSILON)


def norm_back(grad, normed, scale, gain):
    grad_hat = grad * gain
    return scale * (grad_hat - normed * jnp.mean(grad_hat * normed, axis=-1, keepdims=True))


def rotary(values, cosine, sine, back=False):
    width, half = values.shape[1], HEAD_DIMENSION // 2
    later = pltpu.roll(values, width - half, 1)
    earlier = pltpu.roll(values, half, 1)
    front = lax.broadcasted_iota(jnp.int32, values.shape, 1) % HEAD_DIMENSION < half
    other = jnp.where(front, -later, earlier)
    return values * cosine - other * sine if back else values * cosine + other * sine


def allowed_pairs(segment_row):
    size = segment_row.shape[1]
    across = jnp.broadcast_to(segment_row, (size, size))
    rows = lax.broadcasted_iota(jnp.int32, (size, size), 0)
    cols = lax.broadcasted_iota(jnp.int32, (size, size), 1)
    return (cols <= rows) & (across == across.T)


def attention_weights(stacked, keys, allowed):
    scores = dot(stacked, keys, ((1,), (1,))) * SCORE_SCALE
    scores = jnp.where(allowed, scores, MASKED_SCORE)
    row_max = jnp.max(scores, axis=-1, keepdims=True)
    log_total = row_max + jnp.log(jnp.sum(jnp.exp(scores - row_max), axis=-1, keepdims=True))
    return jnp.exp(scores - log_total)


class Heads:
    def __init__(self, ranks):
        self.q, self.kv = QUERY_HEADS // ranks, KEY_VALUE_HEADS // ranks
        self.group = QUERY_HEADS // KEY_VALUE_HEADS
        self.q_cols, self.kv_cols = self.q * HEAD_DIMENSION, self.kv * HEAD_DIMENSION
        self.cols = -(-(self.q_cols + 2 * self.kv_cols) // 128) * 128

    def stack(self, rows, kv):
        first = kv * self.group
        return jnp.concatenate([self.head(rows, first + i) for i in range(self.group)], axis=0)

    def head(self, rows, i):
        return rows[:, i * HEAD_DIMENSION : (i + 1) * HEAD_DIMENSION]

    def key(self, rows, kv):
        return self.head(rows, self.q + kv)

    def value(self, rows, kv):
        return self.head(rows, self.q + self.kv + kv)


def rope_tables(length, heads):
    frequency = np.float32(ROPE_BASE) ** (-(np.arange(HEAD_DIMENSION // 2, dtype=np.float32) * 2.0) / HEAD_DIMENSION)
    angles = np.arange(length, dtype=np.float32)[:, None] * frequency.astype(np.float32)[None, :]
    cosine, sine = (np.tile(f(angles.astype(np.float64)).astype(np.float32), (1, 2)) for f in (np.cos, np.sin))
    turned = heads.q + heads.kv
    rest = heads.cols - turned * HEAD_DIMENSION
    cosine = np.concatenate([np.tile(cosine, (1, turned)), np.ones((length, rest), np.float32)], axis=1)
    sine = np.concatenate([np.tile(sine, (1, turned)), np.zeros((length, rest), np.float32)], axis=1)
    return cosine, sine


def gain_row(misc_ref, ranks, which):
    return jnp.concatenate([misc_ref[i, which : which + 1, :] for i in range(ranks)], axis=1)


def attention_forward(ranks, heads, length, x_ref, w_ref, o_ref, misc_ref, cos_ref, sin_ref, part_ref, qkv_ref, att_ref, scale_ref):
    width = x_ref.shape[2]
    gain = gain_row(misc_ref, ranks, 0)
    weights = w_ref[...].reshape(width, heads.cols)

    def one(b, carry):
        x = x_ref[b].astype(F32)
        scale = norm_scale(x)
        scale_ref[b] = jnp.broadcast_to(scale, (length, 128))
        normed = (x * scale * gain).astype(BF16)
        qkv_ref[b] = rotary(dot(normed, weights), cos_ref[...], sin_ref[...]).astype(BF16)
        qkv = qkv_ref[b]
        allowed = allowed_pairs(misc_ref[b, 8:9, :length])
        allowed = jnp.concatenate([allowed] * heads.group, axis=0)
        outs = []
        for kv in range(heads.kv):
            probs = attention_weights(heads.stack(qkv, kv), heads.key(qkv, kv), allowed).astype(BF16)
            mixed = dot(probs, heads.value(qkv, kv)).astype(BF16)
            outs += [mixed[i * length : (i + 1) * length] for i in range(heads.group)]
        att_ref[b] = jnp.concatenate(outs, axis=1)
        part_ref[b] = dot(att_ref[b], o_ref[...]).astype(BF16)
        return carry

    lax.fori_loop(0, ranks, one, 0)


def column_experts(n_expert, slots, axis):
    column = lax.broadcasted_iota(jnp.int32, (1, 128) if axis else (128, 1), axis)
    owner, slot = column // SLOT_STRIDE, column % SLOT_STRIDE
    expert = slot * n_expert + owner
    real = (owner < n_expert) & (slot < slots) & (expert < EXPERT_COUNT)
    return real, jnp.where(real, expert, -1)


def column_picks(n_expert, slots):
    _, expert = column_experts(n_expert, slots, 1)
    return jnp.where(lax.broadcasted_iota(jnp.int32, (EXPERT_COUNT, 128), 0) == expert, 1.0, 0.0)


def route_tables(n_expert, slots, routes, blocks_ref):
    tokens = routes.shape[1]
    _, expert = column_experts(n_expert, slots, 0)
    named = jnp.zeros((128, tokens), F32)
    for k in range(routes.shape[0]):
        named = named + jnp.where(routes[k : k + 1, :] == expert, 1.0, 0.0)
    limit = jnp.zeros((128, 1), jnp.int32)
    for e in range(EXPERT_COUNT):
        limit = jnp.where(expert == e, blocks_ref[e] * BLK, limit)
    rows = lax.broadcasted_iota(jnp.int32, (tokens, tokens), 0)
    cols = lax.broadcasted_iota(jnp.int32, (tokens, tokens), 1)
    earlier = jnp.where(rows < cols, 1.0, 0.0).astype(BF16)
    rank = dot(named.astype(BF16), earlier)
    kept = (named > 0.0) & (rank < limit.astype(F32))
    return kept, jnp.where(kept, rank, -1.0)


def route_forward(ranks, n_expert, slots, x_ref, branch_ref, misc_ref, router_ref, routes_ref, blocks_ref, hidden_ref, norm_ref, scale_ref, probs_ref, meta_ref, table_ref):
    gain = gain_row(misc_ref, ranks, 1)
    width = x_ref.shape[1]
    shard = width // ranks
    hidden = x_ref[...].astype(F32) + RESIDUAL_SCALE * branch_ref[...]
    hidden_ref[...] = hidden
    scale = norm_scale(hidden)
    scale_ref[...] = jnp.broadcast_to(scale, scale_ref.shape)
    norm = (hidden * scale * gain).astype(BF16)
    picks = column_picks(n_expert, slots).astype(BF16)
    for i in range(ranks):
        here = slice(i * shard, (i + 1) * shard)
        norm_ref[i] = norm[:, here]
        table_ref[here, :] = dot(router_ref[i], picks, ((0,), (0,))).astype(BF16)
    kept, place = route_tables(n_expert, slots, routes_ref[...], blocks_ref)
    real, _ = column_experts(n_expert, slots, 1)
    logits = jnp.where(real, dot(norm, table_ref[...]), MASKED_SCORE)
    weight = jnp.exp(logits - jnp.max(logits, axis=-1, keepdims=True))
    probs = weight / jnp.sum(weight, axis=-1, keepdims=True)
    probs_ref[...] = probs
    used = n_expert * SLOT_STRIDE
    meta_ref[0] = place[:used]
    meta_ref[1] = jnp.where(kept, probs.T, 0.0)[:used]


def row_picks(slots, place):
    number = lax.broadcasted_iota(jnp.int32, (SLOT_ROWS, place.shape[1]), 0).astype(F32)
    return jnp.concatenate([jnp.where(number == place[s : s + 1], 1.0, 0.0) for s in range(slots)], axis=0)


def row_shares(slots, share):
    return jnp.concatenate(
        [jnp.broadcast_to(share[s : s + 1], (SLOT_ROWS, share.shape[1])) for s in range(slots)], axis=0
    )


def pick_rows(slots, n_expert, mine, meta_ref, block, to_sc):
    def one(q, carry):
        pick = row_picks(slots, meta_ref[q, 0, mine, :]).astype(BF16)
        ranks, _, shard = block(q).shape
        for i in range(ranks):
            to_sc[q, :, i * shard : (i + 1) * shard] = dot(pick, block(q)[i]).astype(BF16)
        return carry

    lax.fori_loop(0, n_expert, one, 0)


def expert_slot(n_expert, tokens, s, mine, meta_ref, up_ref, down_ref, gate_grad_ref, inner_ref, both_ref, x_sc, og_sc):
    width = x_sc.shape[2]
    hidden = down_ref.shape[0]
    place_of = pl.ds(pl.multiple_of(s * SLOT_ROWS, SLOT_ROWS), SLOT_ROWS)
    slot_row = lax.broadcasted_iota(jnp.int32, (SLOT_STRIDE, tokens), 0) == s
    number = lax.broadcasted_iota(jnp.int32, (SLOT_ROWS, tokens), 0).astype(F32)
    rows = n_expert * SLOT_ROWS
    both = dot(x_sc[:, place_of, :].reshape(rows, width), up_ref[...])
    gate, up = both[:, :hidden], both[:, hidden:]
    squash = jax.nn.sigmoid(gate)
    inner = (gate * squash * up).astype(BF16)
    inner_ref[s] = inner
    produced = dot(inner, down_ref[...]).astype(BF16)
    masks, gates = [], []
    for q in range(n_expert):
        place = jnp.sum(jnp.where(slot_row, meta_ref[q, 0, mine, :], 0.0), axis=0, keepdims=True)
        share = jnp.sum(jnp.where(slot_row, meta_ref[q, 1, mine, :], 0.0), axis=0, keepdims=True)
        masks.append(number == place)
        gates.append(jnp.sum(jnp.where(masks[q], share, 0.0), axis=1, keepdims=True))
    mix_grad = RESIDUAL_SCALE * og_sc[:, place_of, :].reshape(rows, width).astype(F32)
    grad_rows = (jnp.concatenate(gates, axis=0) * mix_grad).astype(BF16)
    gate_grad = jnp.sum(mix_grad * produced.astype(F32), axis=1, keepdims=True)
    og_sc[:, place_of, :] = produced.reshape(n_expert, SLOT_ROWS, width)
    for q in range(n_expert):
        spread = jnp.where(masks[q], gate_grad[q * SLOT_ROWS : (q + 1) * SLOT_ROWS], 0.0)
        gate_grad_ref[q] = jnp.where(slot_row, jnp.sum(spread, axis=0, keepdims=True), gate_grad_ref[q])
    grad_inner = dot(grad_rows, down_ref[...], ((1,), (1,)))
    grad_both = jnp.concatenate(
        [grad_inner * up * squash * (1.0 + gate * (1.0 - squash)), grad_inner * (gate * squash)], axis=1
    ).astype(BF16)
    both_ref[s] = grad_both
    x_sc[:, place_of, :] = dot(grad_both, up_ref[...], ((1,), (1,))).astype(BF16).reshape(n_expert, SLOT_ROWS, width)


def sum_rows_back(slots, n_expert, mine, meta_ref, out_ref, back_ref, eo_sc, gx_sc):
    def one(q, carry):
        pick = row_picks(slots, meta_ref[q, 0, mine, :])
        high, low = halves(pick * row_shares(slots, meta_ref[q, 1, mine, :]))
        over = ((0,), (0,))
        back_ref[q] = dot(pick.astype(BF16), gx_sc[q], over).astype(BF16)
        out_ref[q] = (dot(high, eo_sc[q], over) + dot(low, eo_sc[q], over)).astype(BF16)
        return carry

    lax.fori_loop(0, n_expert, one, 0)


def route_backward(ranks, n_expert, shard, hidden_ref, norm_ref, scale_ref, probs_ref, misc_ref, router_ref, og_ref, back_ref, gate_grad_ref, grad_hidden_ref, branch_ref, small_ref):
    tokens, width = hidden_ref.shape
    gain = gain_row(misc_ref, ranks, 1)
    hidden = hidden_ref[...]
    used = n_expert * SLOT_STRIDE
    spread = gate_grad_ref[...].reshape(used, tokens)
    if used < 128:
        spread = jnp.concatenate([spread, jnp.zeros((128 - used, tokens), F32)], axis=0)
    grad_probs = spread.T
    probs = probs_ref[...]
    grad_logits = probs * (grad_probs - jnp.sum(probs * grad_probs, axis=1, keepdims=True))
    high, low = halves(grad_logits)
    router = router_ref[...]
    across = ((1,), (1,))
    grad_norm = back_ref[...] + (dot(high, router, across) + dot(low, router, across))
    scale = scale_ref[:, 0:1]
    normed = hidden * scale
    grad_hidden = og_ref[...].astype(F32) + norm_back(grad_norm, normed, scale, gain)
    grad_hidden_ref[...] = grad_hidden
    branch_ref[...] = (RESIDUAL_SCALE * grad_hidden).astype(BF16)
    over = ((0,), (0,))
    grad_gain = jnp.sum(grad_norm * normed, axis=0, keepdims=True)
    for i in range(ranks):
        here = slice(i * shard, (i + 1) * shard)
        grad_router = dot(high, norm_ref[i], over) + dot(low, norm_ref[i], over)
        small_ref[i, :used, :] = grad_router[:used]
        small_ref[i, used:, :] = jnp.broadcast_to(grad_gain[:, here], (8, shard))


def store_blocks(ref, cols, values):
    count, rows = ref.shape[0], ref.shape[1]
    for i in range(count):
        ref[i, :, cols] = values[i * rows : (i + 1) * rows]


def attention_backward(ranks, heads, length, branch_ref, att_ref, qkv_ref, o_ref, misc_ref, cos_ref, sin_ref, grad_ref, d_o_ref):
    d_o = dot(att_ref[...].reshape(ranks * length, heads.q_cols), branch_ref[...].reshape(ranks * length, -1), ((0,), (0,)))
    store_blocks(d_o_ref, slice(None), d_o.astype(BF16))

    def one(b, carry):
        grad_att = dot(branch_ref[b], o_ref[...], ((1,), (1,))).astype(BF16)
        att, qkv = att_ref[b], qkv_ref[b]
        allowed = allowed_pairs(misc_ref[b, 8:9, :length])
        allowed = jnp.concatenate([allowed] * heads.group, axis=0)
        d_q, d_k, d_v = [], [], []
        for kv in range(heads.kv):
            queries, keys = heads.stack(qkv, kv), heads.key(qkv, kv)
            soft = attention_weights(queries, keys, allowed)
            grads = heads.stack(grad_att, kv)
            d_v.append(dot(soft.astype(BF16), grads, ((0,), (0,))))
            delta = jnp.sum(grads.astype(F32) * heads.stack(att, kv).astype(F32), axis=1, keepdims=True)
            inner = dot(grads, heads.value(qkv, kv), ((1,), (1,)))
            d_scores = (soft * (inner - delta) * SCORE_SCALE).astype(BF16)
            rows = dot(d_scores, keys)
            d_q += [rows[i * length : (i + 1) * length] for i in range(heads.group)]
            d_k.append(dot(d_scores, queries, ((0,), (0,))))
        spare = heads.cols - heads.q_cols - 2 * heads.kv_cols
        fill = [jnp.zeros((length, spare), F32)] if spare else []
        grads = jnp.concatenate(d_q + d_k + d_v + fill, axis=1)
        grad_ref[b] = rotary(grads, cos_ref[...], sin_ref[...], back=True).astype(BF16)
        return carry

    lax.fori_loop(0, ranks, one, 0)


def projection_backward(ranks, heads, shard, x_ref, scale_ref, gain_ref, grad_ref, w_ref, small_ref, grad_x_ref, d_w_ref, sums_ref):
    normed = x_ref[...].astype(F32) * scale_ref[:, 0:1]
    norm_input = (normed * gain_ref[0:1, :]).astype(BF16)
    total = None
    for i in range(ranks):
        grads = grad_ref[i].reshape(-1, heads.cols)
        term = dot(grads, w_ref[i], ((1,), (1,)))
        total = term if total is None else total + term
        store_blocks(d_w_ref, slice(i * heads.cols, (i + 1) * heads.cols), dot(norm_input, grads, ((0,), (0,))).astype(BF16))
    grad_x_ref[...] = total.reshape(grad_x_ref.shape)
    small = small_ref[0]
    for i in range(1, ranks):
        small = small + small_ref[i]
    gain_grad = jnp.sum(total * normed, axis=0, keepdims=True)
    used = small.shape[0] - 8
    sums_ref[...] = jnp.zeros_like(sums_ref)
    sums_ref[:used, :] = small[:used].astype(BF16)
    second = lax.broadcasted_iota(jnp.int32, (8, shard), 0)
    sums_ref[used : used + 8, :] = jnp.where(second == 0, small[used:], jnp.where(second == 1, gain_grad, 0.0)).astype(BF16)


def finish(ranks, n_expert, slots, early, heads, tokens, og_ref, xd_ref, ogd_ref, meta_ref, own_both_ref, both_ref, late_both_ref, own_inner_ref, inner_ref, grad_ref, x_ref, misc_ref, grad_hidden_ref, hidden_ref, mixture_ref, d_w_ref, d_o_ref, sums_ref, d_up_ref, d_down_ref, output_ref, grad_inputs_ref, q_ref, k_ref, v_ref, o_ref, router_ref, gain_one_ref, gain_two_ref, x_sc, og_sc, x_in, og_in, sems):
    step = pl.program_id(0)
    me = lax.axis_index("dp")
    rows = n_expert * SLOT_ROWS
    shard = x_in.shape[3]

    @pl.when(step == 0)
    def _():
        def fetch(j, do):
            at, slot = (me + j) % ranks, j % 2
            og = og_ref.at[:, me] if j == 0 else ogd_ref.at[at]
            do(pltpu.make_async_copy(xd_ref.at[at], x_in.at[slot], sems.at[0, slot]))
            do(pltpu.make_async_copy(og, og_in.at[slot], sems.at[1, slot]))

        fetch(0, lambda copy: copy.start())
        for j in range(ranks):
            if j + 1 < ranks:
                fetch(j + 1, lambda copy: copy.start())
            fetch(j, lambda copy: copy.wait())

            def one(q, carry):
                at = (me + j) % ranks
                pick = row_picks(slots, meta_ref[at, q, 0])
                share = jnp.sum(pick * row_shares(slots, meta_ref[at, q, 1]), axis=1, keepdims=True)
                pick = pick.astype(BF16)
                x_sc[j, q] = dot(pick, x_in[j % 2, q]).astype(BF16)
                og_sc[j, q] = (share * (RESIDUAL_SCALE * dot(pick, og_in[j % 2, q]))).astype(BF16)
                return carry

            lax.fori_loop(0, n_expert, one, 0)

    @pl.when(step == slots - 1)
    def _():
        output_ref[...] = (hidden_ref[...] + RESIDUAL_SCALE * mixture_ref[...]).astype(BF16)
        gain = gain_row(misc_ref, ranks, 0)
        grad = jnp.concatenate([grad_ref[i] for i in range(ranks)], axis=1)
        x = x_ref[...].astype(F32)
        scale = norm_scale(x)
        grad_inputs_ref[...] = grad_hidden_ref[...] + norm_back(grad, x * scale, scale, gain)
        first, second = heads.q_cols, heads.q_cols + heads.kv_cols
        for i in range(ranks):
            start = i * heads.cols
            q_ref[:, i * heads.q_cols : (i + 1) * heads.q_cols] = d_w_ref[:, start : start + first].astype(F32)
            here = slice(i * heads.kv_cols, (i + 1) * heads.kv_cols)
            k_ref[:, here] = d_w_ref[:, start + first : start + second].astype(F32)
            v_ref[:, here] = d_w_ref[:, start + second : start + second + heads.kv_cols].astype(F32)
        o_ref[...] = d_o_ref[...].astype(F32)
        used = n_expert * SLOT_STRIDE
        router_ref[...] = dot(column_picks(n_expert, slots).astype(BF16), sums_ref[:128])
        ends = sums_ref[used : used + 16, :].astype(F32)
        gain_two_ref[...] = ends[0:1]
        gain_one_ref[...] = ends[1:2]

    place_of = pl.ds(pl.multiple_of(step * SLOT_ROWS, SLOT_ROWS), SLOT_ROWS)
    over = ((0,), (0,))

    def form(their_both):
        d_up = d_down = None
        for j in range(ranks):
            at = (me + j) % ranks
            x = x_sc[j, :, place_of, :].reshape(rows, shard)
            og = og_sc[j, :, place_of, :].reshape(rows, shard)
            up = dot(x, own_both_ref[0] if j == 0 else their_both[at, 0], over)
            down = dot(own_inner_ref[0] if j == 0 else inner_ref[at, 0], og, over)
            d_up, d_down = (up, down) if j == 0 else (d_up + up, d_down + down)
        d_up_ref[0] = d_up
        d_down_ref[0] = d_down

    @pl.when(step < early)
    def _():
        form(both_ref)

    @pl.when(step >= early)
    def _():
        form(late_both_ref)


def on_device(
    inputs,
    segment_ids,
    routes,
    expert_blocks,
    norm1_gain,
    q_weight,
    k_weight,
    value_matrix,
    o_weight,
    norm2_gain,
    router_weight,
    expert_gate_up,
    expert_down,
    out_grad,
):
    ranks, n_expert = lax.axis_size("dp"), lax.axis_size("expert")
    tokens, width = inputs.shape
    shard = q_weight.shape[0]
    slots, _, double = expert_gate_up.shape
    hidden = expert_down.shape[1]
    heads = Heads(ranks)
    group = ("dp", ranks // 2, 2)
    plane = ("expert", 4, n_expert // 4)
    used = n_expert * SLOT_STRIDE
    cosine, sine = rope_tables(tokens, heads)

    gains = jnp.stack([norm1_gain, norm2_gain]).astype(F32)
    dma = pltpu.SemaphoreType.DMA

    def forward(*refs):
        take = taker(refs)
        x, wq, wk, wv, rt, gn, sg, og, wo, cs, sn, routes_ref, blocks_ref = take(13)
        w, ms_all, og_all, qkv, att, scale_one, xc, hidden_ref, norm, scale_two, probs, meta, table = take(13)
        x_all, w_all, rt_all, ms, og_own, part, branch, own_sem = take(8)
        dp, ex = Grid(*group), Grid(*plane)
        for i in range(ranks):
            at = 0
            for ref, cols in ((wq, heads.q_cols), (wk, heads.kv_cols), (wv, heads.kv_cols)):
                w[i, :, at : at + cols] = ref[:, i * cols : (i + 1) * cols]
                at += cols
            if at < heads.cols:
                w[i, :, at:] = jnp.zeros((shard, heads.cols - at), BF16)
            og_own[i] = og[:, i * shard : (i + 1) * shard]
        ms[...] = jnp.zeros_like(ms)
        ms[0:2, :] = gn[...]
        ms[8:9, :tokens] = sg[...].astype(F32)
        x_all[dp.me] = x[...]
        rt_all[dp.me] = rt[...]
        ms_all[dp.me] = ms[...]
        greet(dp.all() + ex.near())
        keep = pltpu.make_async_copy(og_own, og_all.at[ex.me], own_sem)
        keep.start()
        small = [begin(gather(dp, ms, ms_all, take(4))), begin(gather(dp, rt, rt_all, take(4)))]
        xs = begin(gather(dp, x, x_all, take(4)))
        ws = begin(exchange(dp, w, w_all, take(2)))
        ogs = begin(gather(ex, og_own, og_all, take(4)))
        run(*small, xs)
        for i in range(ranks):

            @pl.when(dp.me == i)
            def _():
                for b in range(ranks):
                    xc[b * tokens : (b + 1) * tokens, :] = x_all[b, :, i * shard : (i + 1) * shard]

        advance(ogs, 2 * (plane[1] - 1))
        run(ws)
        attention_forward(ranks, heads, tokens, x_all, w_all, wo, ms_all, cs, sn, part, qkv, att, scale_one)

        def store(total):
            branch[...] = total

        run(reduce(dp, lambda i: part.at[i], store, take(4), take(3)))
        route_forward(ranks, n_expert, slots, x, branch, ms_all, rt_all, routes_ref, blocks_ref, hidden_ref, norm, scale_two, probs, meta, table)
        run(ogs)
        keep.wait()

    (
        weights,
        misc_all,
        og_all,
        qkv,
        att,
        scale_one,
        x_cols,
        hidden_rows,
        norm_hidden,
        scale_two,
        probs,
        meta,
        router,
    ) = call(
        forward,
        "forward",
        [
            ((ranks, shard, heads.cols), BF16),
            ((ranks, 16, shard), F32),
            ((n_expert, ranks, tokens, shard), BF16),
            ((ranks, tokens, heads.cols), BF16),
            ((ranks, tokens, heads.q_cols), BF16),
            ((ranks, tokens, 128), F32),
            ((ranks * tokens, shard), BF16),
            ((tokens, width), F32),
            ((ranks, tokens, shard), BF16),
            ((tokens, 128), F32),
            ((tokens, 128), F32),
            ((2, used, tokens), F32),
            ((width, 128), BF16),
        ],
        (
            inputs,
            q_weight,
            k_weight,
            value_matrix,
            router_weight.T,
            gains,
            segment_ids,
            out_grad,
            o_weight,
            cosine,
            sine,
            routes.T,
            expert_blocks,
        ),
        [
            pltpu.VMEM((ranks, tokens, width), BF16),
            pltpu.VMEM((ranks, shard, heads.cols), BF16),
            pltpu.VMEM((ranks, router_weight.shape[1], shard), BF16),
            pltpu.VMEM((16, shard), F32),
            pltpu.VMEM((ranks, tokens, shard), BF16),
            pltpu.VMEM((ranks, tokens, width), BF16),
            pltpu.VMEM((tokens, width), F32),
            dma(()),
        ]
        + line_sems(*group[1:]) * 3
        + exchange_sems(ranks)
        + line_sems(*plane[1:])
        + line_sems(*group[1:])
        + sum_slots(*group[1:], (tokens, width)),
        cid=0,
        us=70,
        in_specs=[VMEM] * 12 + [pl.BlockSpec(memory_space=pltpu.SMEM)],
        out_specs=[VMEM] * 2 + [ANY] + [VMEM] * 10,
    )

    fixed = lambda shape: pl.BlockSpec(shape, lambda s: (0,) * len(shape), pipeline_mode=pl.Buffered(1))
    moving = lambda shape: pl.BlockSpec((1,) + shape, lambda s: (s,) + (0,) * len(shape))
    rows = n_expert * SLOT_ROWS
    deep = 2 if ranks * rows <= 1024 else 1
    early = slots * 3 // 5

    def mixture_of_experts(*refs):
        take = taker(refs)
        nh, mt, hid, sc, pb, ms, tb, og_mine, og, up, down = take(11)
        out_part, inr, gb, grad_hidden_ref, branch_ref, small_ref, mt_group, xd, gb_all = take(9)
        nh_all, mt_all, gg, gg_all, back_part, mt_own, x_sc, og_sc, og_in, up_in, down_in = take(11)
        og_sems, up_sems, own_sems = take(3)
        dp, ex = Grid(*group), Grid(*plane)
        mine = pl.ds(pl.multiple_of(ex.me * SLOT_STRIDE, SLOT_STRIDE), SLOT_STRIDE)
        nh_all[ex.me] = nh[...]
        mt_all[ex.me] = mt[...]
        gg[...] = jnp.zeros_like(gg)

        def fetch(s, do):
            do(pltpu.make_async_copy(up.at[s], up_in.at[s % deep], up_sems.at[0, s % deep]))
            do(pltpu.make_async_copy(down.at[s], down_in.at[s % deep], up_sems.at[1, s % deep]))

        for s in range(deep):
            fetch(s, lambda copy: copy.start())
        greet(dp.all() + ex.all())
        mts = begin(gather(ex, mt, mt_all, take(4)))
        passed, end = pass_slices(dp, xd, take(2))

        def keep(i, block):
            return pltpu.make_async_copy(block.at[dp.me], xd.at[dp.me, i], own_sems.at[i])

        def arrived(i, block):
            passed(i, block)
            keep(i, block).start()

        nhs = begin(gather(ex, nh, nh_all, take(4), arrived))
        run(mts)

        def fetch_og(q):
            return pltpu.make_async_copy(og.at[q], og_in.at[q % 2], og_sems.at[q % 2])

        fetch_og(0).start()

        def pick_og(q, carry):
            @pl.when(q + 1 < n_expert)
            def _():
                fetch_og(q + 1).start()

            fetch_og(q).wait()
            pick = row_picks(slots, mt_all[q, 0, mine, :]).astype(BF16)
            for i in range(ranks):
                og_sc[q, :, i * shard : (i + 1) * shard] = dot(pick, og_in[q % 2, i]).astype(BF16)
            return carry

        lax.fori_loop(0, n_expert, pick_og, 0)
        mt_own[...] = mt_all[:, :, mine, :]
        mt_group[dp.me] = mt_own[...]
        mgs = begin(gather(dp, mt_own, mt_group, take(4)))
        run(nhs)
        pick_rows(slots, n_expert, mine, mt_all, lambda q: nh_all.at[q], x_sc)

        def one(s, carry):
            fetch(s, lambda copy: copy.wait())
            expert_slot(n_expert, tokens, s, mine, mt_all, up_in.at[s % deep], down_in.at[s % deep], gg, inr, gb, x_sc, og_sc)

            @pl.when(s + deep < slots)
            def _():
                fetch(s + deep, lambda copy: copy.start())

            return carry

        lax.fori_loop(0, slots, one, 0)
        run(mgs)
        gbs = begin(gather(dp, gb.at[pl.ds(0, early)], gb_all, take(4)))
        sum_rows_back(slots, n_expert, mine, mt_all, out_part, back_part, og_sc, x_sc)

        def store(total):
            grad_hidden_ref[...] = total

        ggs = begin(exchange(ex, gg, gg_all, take(2)))
        run(reduce(ex, lambda i: back_part.at[i], store, take(4), take(3)))
        run(ggs)
        route_backward(ranks, n_expert, shard, hid, nh, sc, pb, ms, tb, og_mine, grad_hidden_ref, gg_all, grad_hidden_ref, branch_ref, small_ref)
        run(gbs)
        end(range(n_expert), nh)
        for i in range(n_expert):
            keep(i, nh).wait()

    out_part, inner, grad_both, grad_hidden, grad_branch, small, meta_group, norm_slices, both_all = call(
        mixture_of_experts,
        "mixture_of_experts",
        [
            ((n_expert, tokens, width), BF16),
            ((slots, rows, hidden), BF16),
            ((slots, rows, double), BF16),
            ((tokens, width), F32),
            ((tokens, width), BF16),
            ((ranks, used + 8, shard), F32),
            ((ranks, n_expert, 2, SLOT_STRIDE, tokens), F32),
            ((ranks, n_expert, tokens, shard), BF16),
            ((ranks, early, rows, double), BF16),
        ],
        (
            norm_hidden,
            meta,
            hidden_rows,
            scale_two,
            probs,
            misc_all,
            router,
            out_grad,
            og_all,
            expert_gate_up,
            expert_down,
        ),
        [
            pltpu.VMEM((n_expert, ranks, tokens, shard), BF16),
            pltpu.VMEM((n_expert, 2, used, tokens), F32),
            pltpu.VMEM((n_expert, SLOT_STRIDE, tokens), F32),
            pltpu.VMEM((n_expert, SLOT_STRIDE, tokens), F32),
            pltpu.VMEM((n_expert, tokens, width), BF16),
            pltpu.VMEM((n_expert, 2, SLOT_STRIDE, tokens), F32),
            pltpu.VMEM((n_expert, slots * SLOT_ROWS, width), BF16),
            pltpu.VMEM((n_expert, slots * SLOT_ROWS, width), BF16),
            pltpu.VMEM((2, ranks, tokens, shard), BF16),
            pltpu.VMEM((deep, width, double), BF16),
            pltpu.VMEM((deep, hidden, width), BF16),
            dma((2,)),
            dma((2, deep)),
            dma((n_expert,)),
        ]
        + line_sems(*plane[1:])
        + [dma((n_expert, ranks))] * 2
        + line_sems(*plane[1:])
        + line_sems(*group[1:]) * 2
        + exchange_sems(n_expert)
        + line_sems(*plane[1:])
        + sum_slots(*plane[1:], (tokens, width)),
        cid=1,
        us=115,
        in_specs=[VMEM] * 8 + [ANY] * 3,
        out_specs=[VMEM] * 7 + [ANY] * 2,
    )

    sum_rows = 16 * n_expert
    part_rows = shard // n_expert
    o_block, w_block, s_block = (part_rows, width), (part_rows, ranks * heads.cols), (16, shard)

    def backward(*refs):
        take = taker(refs)
        br, sm, at, qkv, wo, ms, cs, sn, xc, sc, gn, w, terms, og, gb, inr = take(16)
        mix, gx_all, do_all, dw_all, su_all, ogd, gb_all, inr_all = take(8)
        br_all, sm_all, gr, gr_all, do, dw, su, gx = take(8)
        dp, ex = Grid(*group), Grid(*plane)
        br_all[dp.me] = br[...]
        greet(dp.all() + ex.near())

        def store(total):
            mix[...] = total

        brs = begin(gather(dp, br, br_all, take(4)))
        sms = begin(exchange(dp, sm, sm_all, take(2)))
        outs = begin(reduce(ex, lambda i: terms.at[i], store, take(4), take(3)))
        run(brs)
        passed, end = pass_slices(dp, ogd, take(2))
        for i in range(n_expert // 3):
            passed(i, og.at[i])
        advance(outs, 2)
        attention_backward(ranks, heads, tokens, br_all, at, qkv, wo, ms, cs, sn, gr, do)
        gr_all[dp.me] = gr[...]
        grs = begin(gather(dp, gr, gr_all, take(4)))
        dos = begin(reduce_gather(ex, lambda i: do.at[i], do_all, take(), take(8), take(3)))
        advance(outs, 2)
        run(sms)
        run(grs)
        for i in range(n_expert // 3, n_expert):
            passed(i, og.at[i])
        inrs = begin(gather(dp, inr, inr_all, take(4)))
        gbs = begin(gather(dp, gb.at[pl.ds(early, slots - early)], gb_all, take(4)))
        advance(outs, 2)
        projection_backward(ranks, heads, shard, xc, sc, gn, gr_all, w, sm_all, gx, dw, su)
        gxs = begin(exchange(dp, gx, gx_all, take(2)))
        dws = begin(reduce_gather(ex, lambda i: dw.at[i], dw_all, take(), take(8), take(3)))
        sus = begin(reduce_gather(ex, lambda i: su.at[pl.ds(pl.multiple_of(i * 16, 16), 16)], su_all, take(), take(8), take(3)))
        run(outs)
        run(dos, dws, sus)
        run(gxs)
        run(inrs)
        run(gbs)
        end(range(n_expert), og.at[0])

    summed = lambda block: [pltpu.VMEM(block, BF16)] + line_sems(*plane[1:]) * 2 + sum_slots(*plane[1:], block)
    mixture, grad_x, d_o, d_w, sums, og_slices, both_late, inner_all = call(
        backward,
        "backward",
        [
            ((tokens, width), F32),
            ((ranks, tokens, shard), F32),
            ((n_expert,) + o_block, BF16),
            ((n_expert,) + w_block, BF16),
            ((n_expert,) + s_block, BF16),
            ((ranks, n_expert, tokens, shard), BF16),
            ((ranks, slots - early, rows, double), BF16),
            ((ranks, slots, rows, hidden), BF16),
        ],
        (
            grad_branch,
            small,
            att,
            qkv,
            o_weight,
            misc_all,
            cosine,
            sine,
            x_cols,
            scale_one.reshape(ranks * tokens, 128),
            gains,
            weights,
            out_part,
            og_all,
            grad_both,
            inner,
        ),
        [
            pltpu.VMEM((ranks, tokens, width), BF16),
            pltpu.VMEM((ranks, used + 8, shard), F32),
            pltpu.VMEM((ranks, tokens, heads.cols), BF16),
            pltpu.VMEM((ranks, ranks, tokens, heads.cols), BF16),
            pltpu.VMEM((n_expert,) + o_block, BF16),
            pltpu.VMEM((n_expert,) + w_block, BF16),
            pltpu.VMEM((sum_rows, shard), BF16),
            pltpu.VMEM((ranks, tokens, shard), F32),
        ]
        + line_sems(*group[1:])
        + exchange_sems(ranks)
        + line_sems(*plane[1:])
        + sum_slots(*plane[1:], (tokens, width))
        + [pltpu.SemaphoreType.DMA((n_expert, ranks))] * 2
        + line_sems(*group[1:])
        + summed(o_block)
        + line_sems(*group[1:]) * 2
        + exchange_sems(ranks)
        + summed(w_block)
        + summed(s_block),
        cid=2,
        us=130,
        in_specs=[VMEM] * 13 + [ANY] * 3,
        out_specs=[VMEM] * 5 + [ANY] * 3,
    )

    held = pl.Buffered(deep)
    gathered = lambda shape, at: pl.BlockSpec(
        (ranks, 1) + shape, lambda s: (0, at(s)) + (0,) * len(shape), pipeline_mode=held
    )
    d_w = d_w.reshape(shard, ranks * heads.cols)
    d_o = d_o.reshape(shard, width)
    sums = sums.reshape(sum_rows, shard)
    ins = (grad_x, inputs, misc_all, grad_hidden, hidden_rows, mixture, d_w, d_o, sums)
    outs = [
        ((slots, shard, double), F32),
        ((slots, hidden, shard), F32),
        ((tokens, width), BF16),
        ((tokens, width), F32),
        ((shard, QUERY_HEADS * HEAD_DIMENSION), F32),
        ((shard, KEY_VALUE_HEADS * HEAD_DIMENSION), F32),
        ((shard, KEY_VALUE_HEADS * HEAD_DIMENSION), F32),
        ((shard, width), F32),
        ((router_weight.shape[1], shard), F32),
        ((1, shard), F32),
        ((1, shard), F32),
    ]
    d_up, d_down, output, grad_inputs, d_q, d_k, d_v, d_o, d_router, gain_one, gain_two = call(
        functools.partial(finish, ranks, n_expert, slots, early, heads, tokens),
        "finish",
        outs,
        (og_all, norm_slices, og_slices, meta_group, grad_both, both_all, both_late, inner, inner_all) + ins,
        [pltpu.VMEM((ranks, n_expert, slots * SLOT_ROWS, shard), BF16)] * 2
        + [pltpu.VMEM((2, n_expert, tokens, shard), BF16)] * 2
        + [pltpu.SemaphoreType.DMA((2, 2))],
        us=20,
        grid=(slots,),
        in_specs=[ANY] * 3
        + [
            fixed(meta_group.shape),
            moving((rows, double)),
            gathered((rows, double), lambda s: jnp.minimum(s, early - 1)),
            gathered((rows, double), lambda s: jnp.maximum(s - early, 0)),
            moving((rows, hidden)),
            gathered((rows, hidden), lambda s: s),
        ]
        + [fixed(array.shape) for array in ins],
        out_specs=[moving((shard, double)), moving((hidden, shard))] + [fixed(shape) for shape, _ in outs[2:]],
    )
    return (
        output,
        grad_inputs,
        gain_one.reshape(shard),
        d_q,
        d_k,
        d_v,
        d_o,
        gain_two.reshape(shard),
        d_router.T,
        d_up,
        d_down,
    )


def solution(mesh):
    tokens = P(("dp", "expert"), None)
    rows = P("dp", None)
    return jax.shard_map(
        on_device,
        mesh=mesh,
        in_specs=(
            tokens,
            tokens,
            tokens,
            P(),
            P("dp"),
            rows,
            rows,
            rows,
            rows,
            P("dp"),
            rows,
            P("expert", None, None),
            P("expert", None, None),
            tokens,
        ),
        out_specs=(
            tokens,
            tokens,
            P("dp"),
            rows,
            rows,
            rows,
            rows,
            P("dp"),
            rows,
            P("expert", "dp", None),
            P("expert", None, "dp"),
        ),
        check_vma=False,
    )
```

```python
import functools
import math

import jax
import jax.numpy as jnp
import numpy as np
from jax import lax
from jax.experimental import pallas as pl
from jax.experimental.pallas import tpu as pltpu
from jax.sharding import PartitionSpec as P

QUERY_HEADS = 24
KEY_VALUE_HEADS = 8
HEAD_DIMENSION = 64
EXPERT_COUNT = 40
BLK = 4
SLOT_ROWS = 32
SLOT_STRIDE = 8

NORM_EPSILON = 1e-06
SCORE_SCALE = 0.015625
RESIDUAL_SCALE = 0.22
ROPE_BASE = 10000.0
MASKED_SCORE = -1e30

MESH = pl.DeviceIdType.MESH
F32, BF16 = jnp.float32, jnp.bfloat16
MEBI = 1024 * 1024
VMEM_MOST = 67_043_328


class Grid:
    def __init__(self, axis, A, B, step_a=None, step_b=1):
        self.axis, self.A, self.B = axis, A, B
        self.step_a, self.step_b = B if step_a is None else step_a, step_b
        self.me = lax.axis_index(axis)
        self.a, self.b = self.me // self.step_a % A, self.me // self.step_b % B

    def at(self, a, b):
        return a * self.step_a + b * self.step_b

    def dev(self, a, b):
        return {self.axis: self.at(a, b)}

    def here(self):
        return {self.axis: self.me}

    def near(self):
        found = []
        if self.A > 1:
            found += [
                (self.a > 0, self.dev(self.a - 1, self.b)),
                (self.a < self.A - 1, self.dev(self.a + 1, self.b)),
            ]
        found += [(self.me >= 0, self.dev(self.a, (self.b + r) % self.B)) for r in range(1, self.B)]
        return found

    def all(self):
        n = self.A * self.B
        return [(self.me >= 0, {self.axis: (self.me + r) % n}) for r in range(1, n)]

    def next(self, kind, way):
        step = 1 if way == 0 else -1
        if kind == "a":
            return self.ahead("a", way, 1), self.dev(self.a + step, self.b)
        return self.ahead("b", way, 1), self.dev(self.a, self.b + step)

    def behind(self, kind, way, far):
        at, size = (self.a, self.A) if kind == "a" else (self.b, self.B)
        return (at - far >= 0) if way == 0 else (at + far <= size - 1)

    def ahead(self, kind, way, far):
        return self.behind(kind, 1 - way, far)


def greet(peers):
    barrier = pltpu.get_barrier_semaphore()
    for there, device in peers:

        @pl.when(there)
        def _():
            pl.semaphore_signal(barrier, inc=1, device_id=device, device_id_type=MESH)

    pl.semaphore_wait(barrier, sum(jnp.where(there, 1, 0) for there, _ in peers))


def remote(src, dst, send, recv, device):
    return pltpu.make_async_remote_copy(
        src_ref=src, dst_ref=dst, send_sem=send, recv_sem=recv, device_id=device, device_id_type=MESH
    )


class Part:
    def __init__(self, ref, *rest):
        self.ref, self.rest, self.at = ref, rest, self

    def __getitem__(self, i):
        return self.ref.at[(i,) + self.rest]


def begin(step):
    next(step)
    return step


def advance(step, count):
    for _ in range(count):
        next(step)


def run(*steps):
    steps = list(steps)
    while steps:
        left = []
        for step in steps:
            try:
                next(step)
                left.append(step)
            except StopIteration:
                pass
        steps = left


def line_sems(A, B):
    dma = pltpu.SemaphoreType.DMA
    return [dma((2, A)), dma((2, A)), dma((2, A, B)), dma((2, A, B))]


def gather(g, own, out, sems, arrived=lambda i, block: None):
    send_a, recv_a, send_b, recv_b = sems
    A, B = g.A, g.B
    row = lambda way, k: g.a - k if way == 0 else g.a + k
    col = lambda way, k: g.b - k if way == 0 else g.b + k
    rows = [(0, 0)] + [(way, k) for k in range(1, A) for way in (0, 1)]

    def along_a(way, k, src, do):
        if k < A - 1:
            there, device = g.next("a", way)
            i = g.at(row(way, k), g.b)

            @pl.when(there)
            def _():
                do(remote(src, out.at[i], send_a.at[way, k], recv_a.at[way, k + 1], device))

    def along_b(way, j, a, i, src, do):
        if j < B - 1:
            there, device = g.next("b", way)

            @pl.when(there)
            def _():
                do(remote(src, out.at[i], send_b.at[way, a, j], recv_b.at[way, a, j + 1], device))

    def start(copy):
        copy.start()

    def sent(copy):
        copy.wait_send()

    for way in (0, 1):
        along_a(way, 0, own, start)
    for way in (0, 1):
        along_b(way, 0, g.a, g.me, own, start)
    arrived(g.me, own)
    yield
    for k in range(1, A):
        for way in (0, 1):
            i = g.at(row(way, k), g.b)

            @pl.when(g.behind("a", way, k))
            def _():
                remote(out.at[i], out.at[i], send_a.at[way, k], recv_a.at[way, k], g.here()).wait_recv()
                along_a(way, k, out.at[i], start)
                for w in (0, 1):
                    along_b(w, 0, row(way, k), i, out.at[i], start)
                arrived(i, out.at[i])

            yield
    for j in range(1, B):
        for way, k in rows:
            for w in (0, 1):
                i = g.at(row(way, k), col(w, j))

                @pl.when(g.behind("a", way, k) & g.behind("b", w, j))
                def _():
                    a = row(way, k)
                    remote(out.at[i], out.at[i], send_b.at[w, a, j], recv_b.at[w, a, j], g.here()).wait_recv()
                    along_b(w, j, a, i, out.at[i], start)
                    arrived(i, out.at[i])

            yield
    for way, k in rows:
        for w in (0, 1) if k == 0 else (way,):

            @pl.when(g.behind("a", w, k))
            def _():
                along_a(w, k, own, sent)

        @pl.when(g.behind("a", way, k))
        def _():
            for w in (0, 1):
                for j in range(B - 1):

                    @pl.when(g.behind("b", w, j))
                    def _():
                        along_b(w, j, row(way, k), g.me, own, sent)


def sum_slots(A, B, block, dtype=BF16):
    return [
        pltpu.VMEM((A + 1,) + block, dtype),
        pltpu.VMEM((A,) + block, dtype),
        pltpu.VMEM((A, B - 1) + block, dtype),
    ]


def reduce(g, part, finish, sems, slots):
    send_a, recv_a, send_b, recv_b = sems
    land_a, out_a, land_b = slots
    A, B = g.A, g.B
    row = lambda way, k: g.a + k if way == 0 else g.a - k
    rows = [(way, k) for k in range(A - 1, 0, -1) for way in (0, 1)] + [(0, 0)]
    here = g.here()

    def across(a, r):
        to = (g.b + r) % B
        return remote(part(g.at(a, to)), land_b.at[a, r - 1], send_b.at[0, a, r], recv_b.at[0, a, r], g.dev(g.a, to))

    def landing(way, k):
        return land_a.at[A if k == 0 and way == 1 else row(way, k)]

    def along(way, k):
        to = A if k == 1 and way == 1 else row(way, k)
        return remote(
            out_a.at[row(way, k)], land_a.at[to], send_a.at[way, k], recv_a.at[way, k - 1], g.next("a", way)[1]
        )

    def landed(way, k):
        remote(landing(way, k), landing(way, k), send_a.at[way, k], recv_a.at[way, k], here).wait_recv()

    for way, k in rows:

        @pl.when(g.ahead("a", way, k))
        def _():
            for r in range(1, B):
                across(row(way, k), r).start()

    yield
    for way, k in rows:

        @pl.when(g.ahead("a", way, k))
        def _():
            a = row(way, k)
            for r in range(1, B):
                mine = land_b.at[a, r - 1]
                remote(mine, mine, send_b.at[0, a, r], recv_b.at[0, a, r], here).wait_recv()

            def near():
                total = part(g.at(a, g.b))[...].astype(F32)
                for r in range(1, B):
                    total = total + land_b[a, r - 1].astype(F32)
                return total

            if k > 0:
                if k < A - 1:

                    @pl.when(g.behind("a", way, 1))
                    def _():
                        landed(way, k)
                        out_a[a] = (near() + landing(way, k)[...].astype(F32)).astype(out_a.dtype)

                @pl.when(jnp.logical_not(g.behind("a", way, 1)))
                def _():
                    out_a[a] = near().astype(out_a.dtype)

                along(way, k).start()
            else:
                for w in (0, 1):
                    if A > 1:

                        @pl.when(g.behind("a", w, 1))
                        def _():
                            landed(w, 0)

                total = near()
                if A == 2:
                    total = total + land_a[jnp.where(g.a == 1, 1, A)].astype(F32)
                else:
                    for w in (0, 1):
                        if A > 1:
                            total = total + jnp.where(g.behind("a", w, 1), landing(w, 0)[...].astype(F32), 0.0)
                finish(total)

        yield
    for way, k in rows:

        @pl.when(g.ahead("a", way, k))
        def _():
            for r in range(1, B):
                across(row(way, k), r).wait_send()
            if k > 0:
                along(way, k).wait_send()


def total_sems(A, B):
    dma = pltpu.SemaphoreType.DMA
    return [dma((2, A, B)), dma((2, A)), dma((2, A)), dma((2, A, B))]


def total_slots(A, B, block, dtype=BF16):
    return [
        pltpu.VMEM(block, dtype),
        pltpu.VMEM((A, B - 1) + block, dtype),
        pltpu.VMEM((A - 1,) + block, dtype),
        pltpu.VMEM((A - 1,) + block, dtype),
    ]


def total(g, part, out, sems, slots):
    first, second, third, fourth = sems
    kept, land_b, out_a, land_a = slots
    A, B = g.A, g.B
    here = g.here()
    row = lambda k: (g.a + k) % A
    col = lambda r: (g.b + r) % B

    def terms(a, r):
        return remote(part(g.at(a, col(r))), land_b.at[a, r - 1], first.at[0, a, r], first.at[1, a, r], g.dev(g.a, col(r)))

    def sums(k):
        return remote(out_a.at[k - 1], land_a.at[k - 1], second.at[0, k], second.at[1, k], g.dev(row(k), g.b))

    def rows(k):
        return remote(kept, out(g.me), third.at[0, k], third.at[1, k], g.dev(row(k), g.b))

    def cols(a, r, src):
        return remote(src, out(g.at(a, g.b)), fourth.at[0, a, r], fourth.at[1, a, r], g.dev(g.a, col(r)))

    def near(a):
        value = part(g.at(a, g.b))[...].astype(F32)
        for r in range(1, B):
            terms(a, r).wait_recv()
            value = value + land_b[a, r - 1].astype(F32)
        return value

    for k in [*range(1, A), 0]:
        for r in range(1, B):
            terms(row(k), r).start()
    yield
    for k in range(1, A):
        out_a[k - 1] = near(row(k)).astype(BF16)
        sums(k).start()
        yield
    value = near(g.a)
    for k in range(1, A):
        sums(k).wait_recv()
        value = value + land_a[k - 1].astype(F32)
    kept[...] = value.astype(BF16)
    out(g.me)[...] = kept[...]
    for r in range(1, B):
        cols(g.a, r, kept).start()
    for k in range(1, A):
        rows(k).start()
    yield
    for k in range(1, A):
        a = (g.a + A - k) % A
        mine = out(g.at(a, g.b))
        remote(mine, mine, third.at[0, k], third.at[1, k], here).wait_recv()
        for r in range(1, B):
            cols(a, r, mine).start()
        yield
    for k in [0, *range(1, A)]:
        a = (g.a + A - k) % A
        for r in range(1, B):
            mine = out(g.at(a, (g.b + B - r) % B))
            remote(mine, mine, fourth.at[0, a, r], fourth.at[1, a, r], here).wait_recv()
        yield
    for k in range(A):
        for r in range(1, B):
            terms(row(k), r).wait_send()
            cols(row(k), r, kept).wait_send()
        if k:
            sums(k).wait_send()
            rows(k).wait_send()


def exchange_sems(n):
    return [pltpu.SemaphoreType.DMA((n,)), pltpu.SemaphoreType.DMA((n,))]


def pass_slices(g, out, sems):
    send, recv = sems
    n = g.A * g.B

    def copies(i, block):
        for r in range(1, n):
            to = (g.me + r) % n
            yield remote(block.at[to], out.at[g.me, i], send.at[i, r], recv.at[i, r], {g.axis: to})

    def arrived(i, block):
        for copy in copies(i, block):
            copy.start()

    def end(blocks, block):
        for i in blocks:
            for r in range(1, n):
                mine = out.at[(g.me + n - r) % n, i]
                remote(mine, mine, send.at[i, r], recv.at[i, r], g.here()).wait_recv()
            for copy in copies(i, block):
                copy.wait_send()

    return arrived, end


def exchange(g, part, out, sems):
    send, recv = sems
    n = g.A * g.B
    copies = []
    for r in range(1, n):
        to = (g.me + r) % n
        copies.append(remote(part.at[to], out.at[g.me], send.at[r], recv.at[r], {g.axis: to}))
        copies[-1].start()
    out[g.me] = part[g.me]
    yield
    for r in range(1, n):
        origin = (g.me + n - r) % n
        remote(part.at[origin], out.at[origin], send.at[r], recv.at[r], g.here()).wait_recv()
    yield
    for copy in copies:
        copy.wait_send()


VMEM = pl.BlockSpec(memory_space=pltpu.VMEM)
ANY = pl.BlockSpec(memory_space=pl.ANY)


def call(body, name, outs, ins, scratch=(), cid=None, us=10.0, **grid):
    whole = VMEM
    params = dict(vmem_limit_bytes=VMEM_MOST)
    if cid is not None:
        params |= dict(collective_id=cid, has_side_effects=True)
    return pl.pallas_call(
        body,
        out_shape=[jax.ShapeDtypeStruct(shape, dtype) for shape, dtype in outs],
        in_specs=grid.pop("in_specs", [whole] * len(ins)),
        out_specs=grid.pop("out_specs", [whole] * len(outs)),
        scratch_shapes=list(scratch),
        compiler_params=pltpu.CompilerParams(**params),
        cost_estimate=pl.CostEstimate(flops=0, transcendentals=0, bytes_accessed=int(us * 3e6)),
        name=name,
        **grid,
    )(*ins)


def taker(refs):
    refs = list(refs)

    def take(n=None):
        if n is None:
            return refs.pop(0)
        return [refs.pop(0) for _ in range(n)]

    return take


def dot(left, right, contract=((1,), (0,))):
    return lax.dot_general(left, right, (contract, ((), ())), preferred_element_type=F32)


def halves(values):
    high = values.astype(BF16)
    return high, (values - high.astype(F32)).astype(BF16)


def norm_scale(values):
    return lax.rsqrt(jnp.mean(values * values, axis=-1, keepdims=True) + NORM_EPSILON)


def norm_back(grad, normed, scale, gain):
    grad_hat = grad * gain
    return scale * (grad_hat - normed * jnp.mean(grad_hat * normed, axis=-1, keepdims=True))


def rotary(values, cosine, sine, back=False):
    width, half = values.shape[1], HEAD_DIMENSION // 2
    later = pltpu.roll(values, width - half, 1)
    earlier = pltpu.roll(values, half, 1)
    front = lax.broadcasted_iota(jnp.int32, values.shape, 1) % HEAD_DIMENSION < half
    other = jnp.where(front, -later, earlier)
    return values * cosine - other * sine if back else values * cosine + other * sine


def allowed_pairs(segment_row):
    size = segment_row.shape[1]
    across = jnp.broadcast_to(segment_row, (size, size))
    rows = lax.broadcasted_iota(jnp.int32, (size, size), 0)
    cols = lax.broadcasted_iota(jnp.int32, (size, size), 1)
    return (cols <= rows) & (across == across.T)


def attention_weights(stacked, keys, allowed):
    scores = dot(stacked, keys, ((1,), (1,))) * SCORE_SCALE
    scores = jnp.where(allowed, scores, MASKED_SCORE)
    row_max = jnp.max(scores, axis=-1, keepdims=True)
    log_total = row_max + jnp.log(jnp.sum(jnp.exp(scores - row_max), axis=-1, keepdims=True))
    return jnp.exp(scores - log_total)


class Heads:
    def __init__(self, ranks):
        self.q, self.kv = QUERY_HEADS // ranks, KEY_VALUE_HEADS // ranks
        self.group = QUERY_HEADS // KEY_VALUE_HEADS
        self.q_cols, self.kv_cols = self.q * HEAD_DIMENSION, self.kv * HEAD_DIMENSION
        self.cols = -(-(self.q_cols + 2 * self.kv_cols) // 128) * 128

    def stack(self, rows, kv):
        first = kv * self.group
        return jnp.concatenate([self.head(rows, first + i) for i in range(self.group)], axis=0)

    def head(self, rows, i):
        return rows[:, i * HEAD_DIMENSION : (i + 1) * HEAD_DIMENSION]

    def key(self, rows, kv):
        return self.head(rows, self.q + kv)

    def value(self, rows, kv):
        return self.head(rows, self.q + self.kv + kv)


def rope_tables(length, heads):
    frequency = np.float32(ROPE_BASE) ** (-(np.arange(HEAD_DIMENSION // 2, dtype=np.float32) * 2.0) / HEAD_DIMENSION)
    angles = np.arange(length, dtype=np.float32)[:, None] * frequency.astype(np.float32)[None, :]
    cosine, sine = (np.tile(f(angles.astype(np.float64)).astype(np.float32), (1, 2)) for f in (np.cos, np.sin))
    turned = heads.q + heads.kv
    rest = heads.cols - turned * HEAD_DIMENSION
    cosine = np.concatenate([np.tile(cosine, (1, turned)), np.ones((length, rest), np.float32)], axis=1)
    sine = np.concatenate([np.tile(sine, (1, turned)), np.zeros((length, rest), np.float32)], axis=1)
    return cosine, sine


def gain_row(misc_ref, ranks, which):
    return jnp.concatenate([misc_ref[i, which : which + 1, :] for i in range(ranks)], axis=1)


def attention_forward(ranks, heads, length, x_ref, w_ref, o_ref, misc_ref, cos_ref, sin_ref, part_ref, qkv_ref, att_ref, scale_ref):
    width = x_ref.shape[2]
    gain = gain_row(misc_ref, ranks, 0)
    weights = w_ref[...].reshape(width, heads.cols)

    def one(b, carry):
        x = x_ref[b].astype(F32)
        scale = norm_scale(x)
        scale_ref[b] = jnp.broadcast_to(scale, (length, 128))
        normed = (x * scale * gain).astype(BF16)
        qkv_ref[b] = rotary(dot(normed, weights), cos_ref[...], sin_ref[...]).astype(BF16)
        qkv = qkv_ref[b]
        allowed = allowed_pairs(misc_ref[b, 8:9, :length])
        allowed = jnp.concatenate([allowed] * heads.group, axis=0)
        outs = []
        for kv in range(heads.kv):
            probs = attention_weights(heads.stack(qkv, kv), heads.key(qkv, kv), allowed).astype(BF16)
            mixed = dot(probs, heads.value(qkv, kv)).astype(BF16)
            outs += [mixed[i * length : (i + 1) * length] for i in range(heads.group)]
        att_ref[b] = jnp.concatenate(outs, axis=1)
        part_ref[b] = dot(att_ref[b], o_ref[...]).astype(BF16)
        return carry

    lax.fori_loop(0, ranks, one, 0)


def column_experts(n_expert, slots, axis):
    column = lax.broadcasted_iota(jnp.int32, (1, 128) if axis else (128, 1), axis)
    owner, slot = column // SLOT_STRIDE, column % SLOT_STRIDE
    expert = slot * n_expert + owner
    real = (owner < n_expert) & (slot < slots) & (expert < EXPERT_COUNT)
    return real, jnp.where(real, expert, -1)


def column_picks(n_expert, slots):
    _, expert = column_experts(n_expert, slots, 1)
    return jnp.where(lax.broadcasted_iota(jnp.int32, (EXPERT_COUNT, 128), 0) == expert, 1.0, 0.0)


def route_tables(n_expert, slots, routes, blocks_ref):
    tokens = routes.shape[1]
    _, expert = column_experts(n_expert, slots, 0)
    named = jnp.zeros((128, tokens), F32)
    for k in range(routes.shape[0]):
        named = named + jnp.where(routes[k : k + 1, :] == expert, 1.0, 0.0)
    limit = jnp.zeros((128, 1), jnp.int32)
    for e in range(EXPERT_COUNT):
        limit = jnp.where(expert == e, blocks_ref[e] * BLK, limit)
    rows = lax.broadcasted_iota(jnp.int32, (tokens, tokens), 0)
    cols = lax.broadcasted_iota(jnp.int32, (tokens, tokens), 1)
    earlier = jnp.where(rows < cols, 1.0, 0.0).astype(BF16)
    rank = dot(named.astype(BF16), earlier)
    kept = (named > 0.0) & (rank < limit.astype(F32))
    return kept, jnp.where(kept, rank, -1.0)


def route_forward(ranks, n_expert, slots, x_ref, branch_ref, misc_ref, router_ref, routes_ref, blocks_ref, hidden_ref, norm_ref, scale_ref, probs_ref, meta_ref, table_ref):
    gain = gain_row(misc_ref, ranks, 1)
    width = x_ref.shape[1]
    shard = width // ranks
    hidden = x_ref[...].astype(F32) + RESIDUAL_SCALE * branch_ref[...]
    hidden_ref[...] = hidden
    scale = norm_scale(hidden)
    scale_ref[...] = jnp.broadcast_to(scale, scale_ref.shape)
    norm = (hidden * scale * gain).astype(BF16)
    picks = column_picks(n_expert, slots).astype(BF16)
    for i in range(ranks):
        here = slice(i * shard, (i + 1) * shard)
        norm_ref[i] = norm[:, here]
        table_ref[here, :] = dot(router_ref[i], picks, ((0,), (0,))).astype(BF16)
    kept, place = route_tables(n_expert, slots, routes_ref[...], blocks_ref)
    real, _ = column_experts(n_expert, slots, 1)
    logits = jnp.where(real, dot(norm, table_ref[...]), MASKED_SCORE)
    weight = jnp.exp(logits - jnp.max(logits, axis=-1, keepdims=True))
    probs = weight / jnp.sum(weight, axis=-1, keepdims=True)
    probs_ref[...] = probs
    used = n_expert * SLOT_STRIDE
    meta_ref[0] = place[:used]
    meta_ref[1] = jnp.where(kept, probs.T, 0.0)[:used]


def row_picks(slots, place):
    number = lax.broadcasted_iota(jnp.int32, (SLOT_ROWS, place.shape[1]), 0).astype(F32)
    return jnp.concatenate([jnp.where(number == place[s : s + 1], 1.0, 0.0) for s in range(slots)], axis=0)


def row_shares(slots, share):
    return jnp.concatenate(
        [jnp.broadcast_to(share[s : s + 1], (SLOT_ROWS, share.shape[1])) for s in range(slots)], axis=0
    )


def pick_rows(slots, n_expert, mine, meta_ref, block, to_sc):
    def one(q, carry):
        pick = row_picks(slots, meta_ref[q, 0, mine, :]).astype(BF16)
        ranks, _, shard = block(q).shape
        for i in range(ranks):
            to_sc[q, :, i * shard : (i + 1) * shard] = dot(pick, block(q)[i]).astype(BF16)
        return carry

    lax.fori_loop(0, n_expert, one, 0)


def expert_slot(n_expert, tokens, s, mine, meta_ref, up_ref, down_ref, gate_grad_ref, inner_ref, both_ref, x_sc, og_sc):
    width = x_sc.shape[2]
    hidden = down_ref.shape[0]
    place_of = pl.ds(pl.multiple_of(s * SLOT_ROWS, SLOT_ROWS), SLOT_ROWS)
    slot_row = lax.broadcasted_iota(jnp.int32, (SLOT_STRIDE, tokens), 0) == s
    number = lax.broadcasted_iota(jnp.int32, (SLOT_ROWS, tokens), 0).astype(F32)
    rows = n_expert * SLOT_ROWS
    both = dot(x_sc[:, place_of, :].reshape(rows, width), up_ref[...])
    gate, up = both[:, :hidden], both[:, hidden:]
    squash = jax.nn.sigmoid(gate)
    inner = (gate * squash * up).astype(BF16)
    inner_ref[s] = inner
    produced = dot(inner, down_ref[...]).astype(BF16)
    masks, gates = [], []
    for q in range(n_expert):
        place = jnp.sum(jnp.where(slot_row, meta_ref[q, 0, mine, :], 0.0), axis=0, keepdims=True)
        share = jnp.sum(jnp.where(slot_row, meta_ref[q, 1, mine, :], 0.0), axis=0, keepdims=True)
        masks.append(number == place)
        gates.append(jnp.sum(jnp.where(masks[q], share, 0.0), axis=1, keepdims=True))
    mix_grad = RESIDUAL_SCALE * og_sc[:, place_of, :].reshape(rows, width).astype(F32)
    grad_rows = (jnp.concatenate(gates, axis=0) * mix_grad).astype(BF16)
    gate_grad = jnp.sum(mix_grad * produced.astype(F32), axis=1, keepdims=True)
    og_sc[:, place_of, :] = produced.reshape(n_expert, SLOT_ROWS, width)
    for q in range(n_expert):
        spread = jnp.where(masks[q], gate_grad[q * SLOT_ROWS : (q + 1) * SLOT_ROWS], 0.0)
        gate_grad_ref[q] = jnp.where(slot_row, jnp.sum(spread, axis=0, keepdims=True), gate_grad_ref[q])
    grad_inner = dot(grad_rows, down_ref[...], ((1,), (1,)))
    grad_both = jnp.concatenate(
        [grad_inner * up * squash * (1.0 + gate * (1.0 - squash)), grad_inner * (gate * squash)], axis=1
    ).astype(BF16)
    both_ref[s] = grad_both
    x_sc[:, place_of, :] = dot(grad_both, up_ref[...], ((1,), (1,))).astype(BF16).reshape(n_expert, SLOT_ROWS, width)


def sum_rows_back(slots, n_expert, mine, meta_ref, out_ref, back_ref, eo_sc, gx_sc):
    def one(q, carry):
        pick = row_picks(slots, meta_ref[q, 0, mine, :])
        high, low = halves(pick * row_shares(slots, meta_ref[q, 1, mine, :]))
        over = ((0,), (0,))
        back_ref[q] = dot(pick.astype(BF16), gx_sc[q], over).astype(BF16)
        out_ref[q] = (dot(high, eo_sc[q], over) + dot(low, eo_sc[q], over)).astype(BF16)
        return carry

    lax.fori_loop(0, n_expert, one, 0)


def route_backward(ranks, n_expert, shard, hidden_ref, norm_ref, scale_ref, probs_ref, misc_ref, router_ref, og_ref, back_ref, gate_grad_ref, grad_hidden_ref, branch_ref, small_ref):
    tokens, width = hidden_ref.shape
    gain = gain_row(misc_ref, ranks, 1)
    hidden = hidden_ref[...]
    used = n_expert * SLOT_STRIDE
    spread = gate_grad_ref[...].reshape(used, tokens)
    if used < 128:
        spread = jnp.concatenate([spread, jnp.zeros((128 - used, tokens), F32)], axis=0)
    grad_probs = spread.T
    probs = probs_ref[...]
    grad_logits = probs * (grad_probs - jnp.sum(probs * grad_probs, axis=1, keepdims=True))
    high, low = halves(grad_logits)
    router = router_ref[...]
    across = ((1,), (1,))
    grad_norm = back_ref[...] + (dot(high, router, across) + dot(low, router, across))
    scale = scale_ref[:, 0:1]
    normed = hidden * scale
    grad_hidden = og_ref[...].astype(F32) + norm_back(grad_norm, normed, scale, gain)
    grad_hidden_ref[...] = grad_hidden
    branch_ref[...] = (RESIDUAL_SCALE * grad_hidden).astype(BF16)
    over = ((0,), (0,))
    grad_gain = jnp.sum(grad_norm * normed, axis=0, keepdims=True)
    for i in range(ranks):
        here = slice(i * shard, (i + 1) * shard)
        grad_router = dot(high, norm_ref[i], over) + dot(low, norm_ref[i], over)
        small_ref[i, :used, :] = grad_router[:used]
        small_ref[i, used:, :] = jnp.broadcast_to(grad_gain[:, here], (8, shard))


def store_blocks(ref, cols, values):
    count, rows = ref.shape[0], ref.shape[1]
    for i in range(count):
        ref[i, :, cols] = values[i * rows : (i + 1) * rows]


def attention_backward(ranks, heads, length, branch_ref, att_ref, qkv_ref, o_ref, misc_ref, cos_ref, sin_ref, grad_ref, d_o_ref):
    d_o = dot(att_ref[...].reshape(ranks * length, heads.q_cols), branch_ref[...].reshape(ranks * length, -1), ((0,), (0,)))
    store_blocks(d_o_ref, slice(None), d_o.astype(BF16))

    def one(b, carry):
        grad_att = dot(branch_ref[b], o_ref[...], ((1,), (1,))).astype(BF16)
        att, qkv = att_ref[b], qkv_ref[b]
        allowed = allowed_pairs(misc_ref[b, 8:9, :length])
        allowed = jnp.concatenate([allowed] * heads.group, axis=0)
        d_q, d_k, d_v = [], [], []
        for kv in range(heads.kv):
            queries, keys = heads.stack(qkv, kv), heads.key(qkv, kv)
            soft = attention_weights(queries, keys, allowed)
            grads = heads.stack(grad_att, kv)
            d_v.append(dot(soft.astype(BF16), grads, ((0,), (0,))))
            delta = jnp.sum(grads.astype(F32) * heads.stack(att, kv).astype(F32), axis=1, keepdims=True)
            inner = dot(grads, heads.value(qkv, kv), ((1,), (1,)))
            d_scores = (soft * (inner - delta) * SCORE_SCALE).astype(BF16)
            rows = dot(d_scores, keys)
            d_q += [rows[i * length : (i + 1) * length] for i in range(heads.group)]
            d_k.append(dot(d_scores, queries, ((0,), (0,))))
        spare = heads.cols - heads.q_cols - 2 * heads.kv_cols
        fill = [jnp.zeros((length, spare), F32)] if spare else []
        grads = jnp.concatenate(d_q + d_k + d_v + fill, axis=1)
        grad_ref[b] = rotary(grads, cos_ref[...], sin_ref[...], back=True).astype(BF16)
        return carry

    lax.fori_loop(0, ranks, one, 0)


def projection_backward(ranks, heads, shard, x_ref, scale_ref, gain_ref, grad_ref, w_ref, small_ref, grad_x_ref, d_w_ref, sums_ref):
    normed = x_ref[...].astype(F32) * scale_ref[:, 0:1]
    norm_input = (normed * gain_ref[0:1, :]).astype(BF16)
    total = None
    for i in range(ranks):
        grads = grad_ref[i].reshape(-1, heads.cols)
        term = dot(grads, w_ref[i], ((1,), (1,)))
        total = term if total is None else total + term
        store_blocks(d_w_ref, slice(i * heads.cols, (i + 1) * heads.cols), dot(norm_input, grads, ((0,), (0,))).astype(BF16))
    grad_x_ref[...] = total.reshape(grad_x_ref.shape)
    small = small_ref[0]
    for i in range(1, ranks):
        small = small + small_ref[i]
    gain_grad = jnp.sum(total * normed, axis=0, keepdims=True)
    used = small.shape[0] - 8
    sums_ref[...] = jnp.zeros_like(sums_ref)
    sums_ref[:used, :] = small[:used].astype(BF16)
    second = lax.broadcasted_iota(jnp.int32, (8, shard), 0)
    sums_ref[used : used + 8, :] = jnp.where(second == 0, small[used:], jnp.where(second == 1, gain_grad, 0.0)).astype(BF16)


def group_rows(ranks, n_expert, slots, at, x, og, meta_ref, x_rows, og_rows):
    def one(q, carry):
        pick = row_picks(slots, meta_ref[at, q, 0])
        share = jnp.sum(pick * row_shares(slots, meta_ref[at, q, 1]), axis=1, keepdims=True)
        pick = pick.astype(BF16)
        x_rows[at, q] = dot(pick, x[q]).astype(BF16)
        og_rows[at, q] = (share * (RESIDUAL_SCALE * dot(pick, og[q]))).astype(BF16)
        return carry

    lax.fori_loop(0, n_expert, one, 0)


def finish(ranks, n_expert, slots, early, heads, tokens, x_rows_ref, og_rows_ref, both_ref, late_both_ref, inner_ref, grad_ref, x_ref, misc_ref, grad_hidden_ref, hidden_ref, mixture_ref, d_w_ref, d_o_ref, sums_ref, d_up_ref, d_down_ref, output_ref, grad_inputs_ref, q_ref, k_ref, v_ref, o_ref, router_ref, gain_one_ref, gain_two_ref):
    step = pl.program_id(0)

    @pl.when(step == 0)
    def _():
        output_ref[...] = (hidden_ref[...] + RESIDUAL_SCALE * mixture_ref[...]).astype(BF16)
        gain = gain_row(misc_ref, ranks, 0)
        grad = jnp.concatenate([grad_ref[i] for i in range(ranks)], axis=1)
        x = x_ref[...].astype(F32)
        scale = norm_scale(x)
        grad_inputs_ref[...] = grad_hidden_ref[...] + norm_back(grad, x * scale, scale, gain)
        used = n_expert * SLOT_STRIDE
        router_ref[...] = dot(column_picks(n_expert, slots).astype(BF16), sums_ref[:128])
        ends = sums_ref[used : used + 16, :].astype(F32)
        gain_two_ref[...] = ends[0]
        gain_one_ref[...] = ends[1]
        o_ref[...] = d_o_ref[...].astype(F32)
        first, second = heads.q_cols, heads.q_cols + heads.kv_cols
        for i in range(ranks):
            start = i * heads.cols
            q_ref[:, i * heads.q_cols : (i + 1) * heads.q_cols] = d_w_ref[:, start : start + first].astype(F32)
            here = slice(i * heads.kv_cols, (i + 1) * heads.kv_cols)
            k_ref[:, here] = d_w_ref[:, start + first : start + second].astype(F32)
            v_ref[:, here] = d_w_ref[:, start + second : start + second + heads.kv_cols].astype(F32)

    flat = lambda value: value.reshape(-1, value.shape[-1])
    over = ((0,), (0,))
    x = flat(x_rows_ref[...])

    @pl.when(step < early)
    def _():
        d_up_ref[0] = dot(x, flat(both_ref[...]), over)

    @pl.when(step >= early)
    def _():
        d_up_ref[0] = dot(x, flat(late_both_ref[...]), over)

    d_down_ref[0] = dot(flat(inner_ref[...]), flat(og_rows_ref[...]), over)


def on_device(
    inputs,
    segment_ids,
    routes,
    expert_blocks,
    norm1_gain,
    q_weight,
    k_weight,
    value_matrix,
    o_weight,
    norm2_gain,
    router_weight,
    expert_gate_up,
    expert_down,
    out_grad,
):
    ranks, n_expert = lax.axis_size("dp"), lax.axis_size("expert")
    tokens, width = inputs.shape
    shard = q_weight.shape[0]
    slots, _, double = expert_gate_up.shape
    hidden = expert_down.shape[1]
    heads = Heads(ranks)
    group = ("dp", ranks // 2, 2)
    plane = ("expert", 4, n_expert // 4)
    used = n_expert * SLOT_STRIDE
    cosine, sine = rope_tables(tokens, heads)

    gains = jnp.stack([norm1_gain, norm2_gain]).astype(F32)
    dma = pltpu.SemaphoreType.DMA

    def forward(*refs):
        take = taker(refs)
        x, wq, wk, wv, rt, gn, sg, og, wo, cs, sn, routes_ref, blocks_ref = take(13)
        w, ms_all, og_all, qkv, att, scale_one, xc, hidden_ref, norm, scale_two, probs, meta, table = take(13)
        x_all, w_all, rt_all, ms, og_own, part, branch, own_sem = take(8)
        dp, ex = Grid(*group), Grid(*plane)
        for i in range(ranks):
            at = 0
            for ref, cols in ((wq, heads.q_cols), (wk, heads.kv_cols), (wv, heads.kv_cols)):
                w[i, :, at : at + cols] = ref[:, i * cols : (i + 1) * cols]
                at += cols
            if at < heads.cols:
                w[i, :, at:] = jnp.zeros((shard, heads.cols - at), BF16)
            og_own[i] = og[:, i * shard : (i + 1) * shard]
        ms[...] = jnp.zeros_like(ms)
        ms[0:2, :] = gn[...]
        ms[8:9, :tokens] = sg[...].astype(F32)
        x_all[dp.me] = x[...]
        rt_all[dp.me] = rt[...]
        ms_all[dp.me] = ms[...]
        greet(dp.all() + ex.near())
        keep = pltpu.make_async_copy(og_own, og_all.at[ex.me], own_sem)
        keep.start()
        small = [begin(gather(dp, ms, ms_all, take(4))), begin(gather(dp, rt, rt_all, take(4)))]
        xs = begin(gather(dp, x, x_all, take(4)))
        ws = begin(exchange(dp, w, w_all, take(2)))
        ogs = begin(gather(ex, og_own, og_all, take(4)))
        run(*small, xs)
        for i in range(ranks):

            @pl.when(dp.me == i)
            def _():
                for b in range(ranks):
                    xc[b * tokens : (b + 1) * tokens, :] = x_all[b, :, i * shard : (i + 1) * shard]

        advance(ogs, 2 * (plane[1] - 1))
        run(ws)
        attention_forward(ranks, heads, tokens, x_all, w_all, wo, ms_all, cs, sn, part, qkv, att, scale_one)

        def store(total):
            branch[...] = total

        run(reduce(dp, lambda i: part.at[i], store, take(4), take(3)))
        route_forward(ranks, n_expert, slots, x, branch, ms_all, rt_all, routes_ref, blocks_ref, hidden_ref, norm, scale_two, probs, meta, table)
        run(ogs)
        keep.wait()

    (
        weights,
        misc_all,
        og_all,
        qkv,
        att,
        scale_one,
        x_cols,
        hidden_rows,
        norm_hidden,
        scale_two,
        probs,
        meta,
        router,
    ) = call(
        forward,
        "forward",
        [
            ((ranks, shard, heads.cols), BF16),
            ((ranks, 16, shard), F32),
            ((n_expert, ranks, tokens, shard), BF16),
            ((ranks, tokens, heads.cols), BF16),
            ((ranks, tokens, heads.q_cols), BF16),
            ((ranks, tokens, 128), F32),
            ((ranks * tokens, shard), BF16),
            ((tokens, width), F32),
            ((ranks, tokens, shard), BF16),
            ((tokens, 128), F32),
            ((tokens, 128), F32),
            ((2, used, tokens), F32),
            ((width, 128), BF16),
        ],
        (
            inputs,
            q_weight,
            k_weight,
            value_matrix,
            router_weight.T,
            gains,
            segment_ids,
            out_grad,
            o_weight,
            cosine,
            sine,
            routes.T,
            expert_blocks,
        ),
        [
            pltpu.VMEM((ranks, tokens, width), BF16),
            pltpu.VMEM((ranks, shard, heads.cols), BF16),
            pltpu.VMEM((ranks, router_weight.shape[1], shard), BF16),
            pltpu.VMEM((16, shard), F32),
            pltpu.VMEM((ranks, tokens, shard), BF16),
            pltpu.VMEM((ranks, tokens, width), BF16),
            pltpu.VMEM((tokens, width), F32),
            dma(()),
        ]
        + line_sems(*group[1:]) * 3
        + exchange_sems(ranks)
        + line_sems(*plane[1:])
        + line_sems(*group[1:])
        + sum_slots(*group[1:], (tokens, width)),
        cid=0,
        us=70,
        in_specs=[VMEM] * 12 + [pl.BlockSpec(memory_space=pltpu.SMEM)],
        out_specs=[VMEM] * 2 + [ANY] + [VMEM] * 10,
    )

    fixed = lambda shape: pl.BlockSpec(shape, lambda s: (0,) * len(shape), pipeline_mode=pl.Buffered(1))
    moving = lambda shape: pl.BlockSpec((1,) + shape, lambda s: (s,) + (0,) * len(shape))
    rows = n_expert * SLOT_ROWS
    deep = 2 if ranks * rows <= 1024 else 1
    early = slots * 3 // 5

    def mixture_of_experts(*refs):
        take = taker(refs)
        nh, mt, hid, sc, pb, ms, tb, og_mine, og, up, down = take(11)
        out_part, inr, gb, grad_hidden_ref, branch_ref, small_ref, mt_group, xd, ogd, gb_all = take(10)
        nh_all, mt_all, gg, gg_all, back_part, mt_own, x_sc, og_sc, og_in, up_in, down_in = take(11)
        og_sems, up_sems, own_sems, own_sem = take(4)
        dp, ex = Grid(*group), Grid(*plane)
        mine = pl.ds(pl.multiple_of(ex.me * SLOT_STRIDE, SLOT_STRIDE), SLOT_STRIDE)
        nh_all[ex.me] = nh[...]
        mt_all[ex.me] = mt[...]
        gg[...] = jnp.zeros_like(gg)

        def fetch(s, do):
            do(pltpu.make_async_copy(up.at[s], up_in.at[s % deep], up_sems.at[0, s % deep]))
            do(pltpu.make_async_copy(down.at[s], down_in.at[s % deep], up_sems.at[1, s % deep]))

        for s in range(deep):
            fetch(s, lambda copy: copy.start())
        greet(dp.all() + ex.all())
        mts = begin(gather(ex, mt, mt_all, take(4)))
        og_passed, og_end = pass_slices(dp, ogd, take(2))
        for i in range(n_expert):
            og_passed(i, og.at[i])
        passed, end = pass_slices(dp, xd, take(2))

        def keep(i, block):
            return pltpu.make_async_copy(block.at[dp.me], xd.at[dp.me, i], own_sems.at[i])

        def arrived(i, block):
            passed(i, block)
            keep(i, block).start()

        nhs = begin(gather(ex, nh, nh_all, take(4), arrived))
        run(mts)

        def fetch_og(q):
            return pltpu.make_async_copy(og.at[q], og_in.at[q % 2], og_sems.at[q % 2])

        fetch_og(0).start()

        def pick_og(q, carry):
            @pl.when(q + 1 < n_expert)
            def _():
                fetch_og(q + 1).start()

            fetch_og(q).wait()
            pick = row_picks(slots, mt_all[q, 0, mine, :]).astype(BF16)
            for i in range(ranks):
                og_sc[q, :, i * shard : (i + 1) * shard] = dot(pick, og_in[q % 2, i]).astype(BF16)
            return carry

        lax.fori_loop(0, n_expert, pick_og, 0)
        mt_own[...] = mt_all[:, :, mine, :]
        mt_group[dp.me] = mt_own[...]
        mgs = begin(gather(dp, mt_own, mt_group, take(4)))
        run(nhs)
        pick_rows(slots, n_expert, mine, mt_all, lambda q: nh_all.at[q], x_sc)

        def one(s, carry):
            fetch(s, lambda copy: copy.wait())
            expert_slot(n_expert, tokens, s, mine, mt_all, up_in.at[s % deep], down_in.at[s % deep], gg, inr, gb, x_sc, og_sc)

            @pl.when(s + deep < slots)
            def _():
                fetch(s + deep, lambda copy: copy.start())

            return carry

        lax.fori_loop(0, slots, one, 0)
        run(mgs)
        gb_early = gb.at[pl.ds(0, early)]
        keep_gb = pltpu.make_async_copy(gb_early, gb_all.at[dp.me], own_sem)
        keep_gb.start()
        gbs = begin(gather(dp, gb_early, gb_all, take(4)))
        sum_rows_back(slots, n_expert, mine, mt_all, out_part, back_part, og_sc, x_sc)

        def store(total):
            grad_hidden_ref[...] = total

        ggs = begin(exchange(ex, gg, gg_all, take(2)))
        run(reduce(ex, lambda i: back_part.at[i], store, take(4), take(3)))
        run(ggs)
        route_backward(ranks, n_expert, shard, hid, nh, sc, pb, ms, tb, og_mine, grad_hidden_ref, gg_all, grad_hidden_ref, branch_ref, small_ref)
        run(gbs)
        keep_gb.wait()
        end(range(n_expert), nh)
        og_end(range(n_expert), og.at[0])
        for i in range(n_expert):
            keep(i, nh).wait()

    out_part, inner, grad_both, grad_hidden, grad_branch, small, meta_group, norm_slices, og_slices, both_all = call(
        mixture_of_experts,
        "mixture_of_experts",
        [
            ((n_expert, tokens, width), BF16),
            ((slots, rows, hidden), BF16),
            ((slots, rows, double), BF16),
            ((tokens, width), F32),
            ((tokens, width), BF16),
            ((ranks, used + 8, shard), F32),
            ((ranks, n_expert, 2, SLOT_STRIDE, tokens), F32),
            ((ranks, n_expert, tokens, shard), BF16),
            ((ranks, n_expert, tokens, shard), BF16),
            ((ranks, early, rows, double), BF16),
        ],
        (
            norm_hidden,
            meta,
            hidden_rows,
            scale_two,
            probs,
            misc_all,
            router,
            out_grad,
            og_all,
            expert_gate_up,
            expert_down,
        ),
        [
            pltpu.VMEM((n_expert, ranks, tokens, shard), BF16),
            pltpu.VMEM((n_expert, 2, used, tokens), F32),
            pltpu.VMEM((n_expert, SLOT_STRIDE, tokens), F32),
            pltpu.VMEM((n_expert, SLOT_STRIDE, tokens), F32),
            pltpu.VMEM((n_expert, tokens, width), BF16),
            pltpu.VMEM((n_expert, 2, SLOT_STRIDE, tokens), F32),
            pltpu.VMEM((n_expert, slots * SLOT_ROWS, width), BF16),
            pltpu.VMEM((n_expert, slots * SLOT_ROWS, width), BF16),
            pltpu.VMEM((2, ranks, tokens, shard), BF16),
            pltpu.VMEM((deep, width, double), BF16),
            pltpu.VMEM((deep, hidden, width), BF16),
            dma((2,)),
            dma((2, deep)),
            dma((n_expert,)),
            dma(()),
        ]
        + line_sems(*plane[1:])
        + [dma((n_expert, ranks))] * 4
        + line_sems(*plane[1:])
        + line_sems(*group[1:]) * 2
        + exchange_sems(n_expert)
        + line_sems(*plane[1:])
        + sum_slots(*plane[1:], (tokens, width)),
        cid=1,
        us=115,
        in_specs=[VMEM] * 8 + [ANY] * 3,
        out_specs=[VMEM] * 7 + [ANY] * 3,
    )

    sum_rows = 16 * n_expert
    part_rows = shard // n_expert
    o_block, w_block, s_block = (part_rows, width), (part_rows, ranks * heads.cols), (16, shard)

    halves_of = ranks * heads.cols // 2
    summed = lambda block: total_sems(*plane[1:]) + total_slots(*plane[1:], block)

    def backward(*refs):
        take = taker(refs)
        br, sm, at, qkv, wo, ms, cs, sn, xc, sc, gn, w, terms, mt, og, xd, ogd, gb, inr = take(19)
        mix, gx_all, do_all, dw_all, su_all, x_rows, og_rows, gb_all, inr_all = take(9)
        br_all, sm_all, gr, gr_all, do, dw, su, gx, x_in, og_in, in_sems, own_sems = take(12)
        dp, ex = Grid(*group), Grid(*plane)

        def fetch(j, do_):
            p, slot = (dp.me + j) % ranks, j % 2
            do_(pltpu.make_async_copy(xd.at[p], x_in.at[slot], in_sems.at[0, slot]))
            do_(pltpu.make_async_copy(og.at[:, dp.me] if j == 0 else ogd.at[p], og_in.at[slot], in_sems.at[1, slot]))

        fetch(0, lambda copy: copy.start())
        keeps = [
            pltpu.make_async_copy(inr, inr_all.at[dp.me], own_sems.at[0]),
            pltpu.make_async_copy(gb.at[pl.ds(early, slots - early)], gb_all.at[dp.me], own_sems.at[1]),
        ]
        for copy in keeps:
            copy.start()
        br_all[dp.me] = br[...]
        greet(dp.all() + ex.all())

        def store(value):
            mix[...] = value

        brs = begin(gather(dp, br, br_all, take(4)))
        sms = begin(exchange(dp, sm, sm_all, take(2)))
        outs = begin(reduce(ex, lambda i: terms.at[i], store, take(4), take(3)))
        for j in range(ranks):
            if j + 1 < ranks:
                fetch(j + 1, lambda copy: copy.start())
            fetch(j, lambda copy: copy.wait())
            group_rows(ranks, n_expert, slots, (dp.me + j) % ranks, x_in.at[j % 2], og_in.at[j % 2], mt, x_rows, og_rows)
        run(brs)
        inrs = begin(gather(dp, inr, inr_all, take(4)))
        advance(outs, 2)
        attention_backward(ranks, heads, tokens, br_all, at, qkv, wo, ms, cs, sn, gr, do)
        gr_all[dp.me] = gr[...]
        grs = begin(gather(dp, gr, gr_all, take(4)))
        dos = begin(total(ex, lambda i: do.at[i], lambda i: do_all.at[i], take(4), take(4)))
        advance(outs, 2)
        run(sms)
        run(grs)
        gbs = begin(gather(dp, gb.at[pl.ds(early, slots - early)], gb_all, take(4)))
        advance(outs, 2)
        projection_backward(ranks, heads, shard, xc, sc, gn, gr_all, w, sm_all, gx, dw, su)
        gxs = begin(exchange(dp, gx, gx_all, take(2)))
        dws = []
        for i in range(2):
            cols = pl.ds(i * halves_of, halves_of)
            block = lambda ref, cols=cols: lambda i: ref.at[i, :, cols]
            dws.append(begin(total(ex, block(dw), block(dw_all), take(4), take(4))))
        rows_of = lambda i: pl.ds(pl.multiple_of(i * 16, 16), 16)
        sus = begin(total(ex, lambda i: su.at[rows_of(i)], lambda i: su_all.at[i], take(4), take(4)))
        run(outs)
        run(dos)
        run(*dws, sus)
        run(gxs)
        run(inrs)
        run(gbs)
        for copy in keeps:
            copy.wait()

    row_block = (n_expert, slots * SLOT_ROWS, shard)
    mixture, grad_x, d_o, d_w, sums, x_rows, og_rows, both_late, inner_all = call(
        backward,
        "backward",
        [
            ((tokens, width), F32),
            ((ranks, tokens, shard), F32),
            ((n_expert,) + o_block, BF16),
            ((n_expert,) + w_block, BF16),
            ((n_expert,) + s_block, BF16),
            ((ranks,) + row_block, BF16),
            ((ranks,) + row_block, BF16),
            ((ranks, slots - early, rows, double), BF16),
            ((ranks, slots, rows, hidden), BF16),
        ],
        (
            grad_branch,
            small,
            att,
            qkv,
            o_weight,
            misc_all,
            cosine,
            sine,
            x_cols,
            scale_one.reshape(ranks * tokens, 128),
            gains,
            weights,
            out_part,
            meta_group,
            og_all,
            norm_slices,
            og_slices,
            grad_both,
            inner,
        ),
        [
            pltpu.VMEM((ranks, tokens, width), BF16),
            pltpu.VMEM((ranks, used + 8, shard), F32),
            pltpu.VMEM((ranks, tokens, heads.cols), BF16),
            pltpu.VMEM((ranks, ranks, tokens, heads.cols), BF16),
            pltpu.VMEM((n_expert,) + o_block, BF16),
            pltpu.VMEM((n_expert,) + w_block, BF16),
            pltpu.VMEM((sum_rows, shard), BF16),
            pltpu.VMEM((ranks, tokens, shard), F32),
            pltpu.VMEM((2, n_expert, tokens, shard), BF16),
            pltpu.VMEM((2, n_expert, tokens, shard), BF16),
            dma((2, 2)),
            dma((2,)),
        ]
        + line_sems(*group[1:])
        + exchange_sems(ranks)
        + line_sems(*plane[1:])
        + sum_slots(*plane[1:], (tokens, width))
        + line_sems(*group[1:]) * 2
        + summed(o_block)
        + line_sems(*group[1:])
        + exchange_sems(ranks)
        + summed((part_rows, halves_of)) * 2
        + summed(s_block),
        cid=2,
        us=125,
        in_specs=[VMEM] * 14 + [ANY] * 5,
        out_specs=[VMEM] * 7 + [ANY] * 2,
    )

    held = pl.Buffered(deep)
    gathered = lambda shape, at: pl.BlockSpec(
        (ranks, 1) + shape, lambda s: (0, at(s)) + (0,) * len(shape), pipeline_mode=held
    )
    d_w = d_w.reshape(shard, ranks * heads.cols)
    d_o = d_o.reshape(shard, width)
    sums = sums.reshape(sum_rows, shard)
    ins = (grad_x, inputs, misc_all, grad_hidden, hidden_rows, mixture, d_w, d_o, sums)
    outs = [
        ((slots, shard, double), F32),
        ((slots, hidden, shard), F32),
        ((tokens, width), BF16),
        ((tokens, width), F32),
        ((shard, QUERY_HEADS * HEAD_DIMENSION), F32),
        ((shard, KEY_VALUE_HEADS * HEAD_DIMENSION), F32),
        ((shard, KEY_VALUE_HEADS * HEAD_DIMENSION), F32),
        ((shard, width), F32),
        ((router_weight.shape[1], shard), F32),
        ((shard,), F32),
        ((shard,), F32),
    ]
    d_up, d_down, output, grad_inputs, d_q, d_k, d_v, d_o, d_router, gain_one, gain_two = call(
        functools.partial(finish, ranks, n_expert, slots, early, heads, tokens),
        "finish",
        outs,
        (x_rows, og_rows, both_all, both_late, inner_all) + ins,
        us=15,
        grid=(slots,),
        in_specs=[
            pl.BlockSpec((ranks, n_expert, SLOT_ROWS, shard), lambda s: (0, 0, s, 0)),
            pl.BlockSpec((ranks, n_expert, SLOT_ROWS, shard), lambda s: (0, 0, s, 0)),
            gathered((rows, double), lambda s: jnp.minimum(s, early - 1)),
            gathered((rows, double), lambda s: jnp.maximum(s - early, 0)),
            gathered((rows, hidden), lambda s: s),
        ]
        + [fixed(array.shape) for array in ins],
        out_specs=[moving((shard, double)), moving((hidden, shard))] + [fixed(shape) for shape, _ in outs[2:]],
    )
    return (
        output,
        grad_inputs,
        gain_one,
        d_q,
        d_k,
        d_v,
        d_o,
        gain_two,
        d_router.T,
        d_up,
        d_down,
    )


def solution(mesh):
    tokens = P(("dp", "expert"), None)
    rows = P("dp", None)
    return jax.shard_map(
        on_device,
        mesh=mesh,
        in_specs=(
            tokens,
            tokens,
            tokens,
            P(),
            P("dp"),
            rows,
            rows,
            rows,
            rows,
            P("dp"),
            rows,
            P("expert", None, None),
            P("expert", None, None),
            tokens,
        ),
        out_specs=(
            tokens,
            tokens,
            P("dp"),
            rows,
            rows,
            rows,
            rows,
            P("dp"),
            rows,
            P("expert", "dp", None),
            P("expert", None, "dp"),
        ),
        check_vma=False,
    )
```

```python
import functools
import math

import jax
import jax.numpy as jnp
import numpy as np
from jax import lax
from jax.experimental import pallas as pl
from jax.experimental.pallas import tpu as pltpu
from jax.sharding import PartitionSpec as P

QUERY_HEADS = 24
KEY_VALUE_HEADS = 8
HEAD_DIMENSION = 64
EXPERT_COUNT = 40
BLK = 4
SLOT_ROWS = 32
SLOT_STRIDE = 8

NORM_EPSILON = 1e-06
SCORE_SCALE = 0.015625
RESIDUAL_SCALE = 0.22
ROPE_BASE = 10000.0
MASKED_SCORE = -1e30

MESH = pl.DeviceIdType.MESH
F32, BF16 = jnp.float32, jnp.bfloat16
MEBI = 1024 * 1024
VMEM_MOST = 67_043_328


class Grid:
    def __init__(self, axis, A, B, step_a=None, step_b=1):
        self.axis, self.A, self.B = axis, A, B
        self.step_a, self.step_b = B if step_a is None else step_a, step_b
        self.me = lax.axis_index(axis)
        self.a, self.b = self.me // self.step_a % A, self.me // self.step_b % B

    def at(self, a, b):
        return a * self.step_a + b * self.step_b

    def dev(self, a, b):
        return {self.axis: self.at(a, b)}

    def here(self):
        return {self.axis: self.me}

    def near(self):
        found = []
        if self.A > 1:
            found += [
                (self.a > 0, self.dev(self.a - 1, self.b)),
                (self.a < self.A - 1, self.dev(self.a + 1, self.b)),
            ]
        found += [(self.me >= 0, self.dev(self.a, (self.b + r) % self.B)) for r in range(1, self.B)]
        return found

    def all(self):
        n = self.A * self.B
        return [(self.me >= 0, {self.axis: (self.me + r) % n}) for r in range(1, n)]

    def next(self, kind, way):
        step = 1 if way == 0 else -1
        if kind == "a":
            return self.ahead("a", way, 1), self.dev(self.a + step, self.b)
        return self.ahead("b", way, 1), self.dev(self.a, self.b + step)

    def behind(self, kind, way, far):
        at, size = (self.a, self.A) if kind == "a" else (self.b, self.B)
        return (at - far >= 0) if way == 0 else (at + far <= size - 1)

    def ahead(self, kind, way, far):
        return self.behind(kind, 1 - way, far)


def greet(peers):
    barrier = pltpu.get_barrier_semaphore()
    for there, device in peers:

        @pl.when(there)
        def _():
            pl.semaphore_signal(barrier, inc=1, device_id=device, device_id_type=MESH)

    pl.semaphore_wait(barrier, sum(jnp.where(there, 1, 0) for there, _ in peers))


def remote(src, dst, send, recv, device):
    return pltpu.make_async_remote_copy(
        src_ref=src, dst_ref=dst, send_sem=send, recv_sem=recv, device_id=device, device_id_type=MESH
    )


class Part:
    def __init__(self, ref, *rest):
        self.ref, self.rest, self.at = ref, rest, self

    def __getitem__(self, i):
        return self.ref.at[(i,) + self.rest]


class Ring:
    def __init__(self, stage, out, sems):
        self.stage, self.out, self.sems = stage, out, sems

    def copy(self, i):
        return pltpu.make_async_copy(self.stage.at[i % 2], self.out.at[i], self.sems.at[i % 2])

    def free(self, i):
        @pl.when(i >= 2)
        def _():
            self.copy(i - 2).wait()

        return self.stage.at[i % 2]

    def end(self, count):
        for i in range(max(count - 2, 0), count):
            self.copy(i).wait()


def begin(step):
    next(step)
    return step


def advance(step, count):
    for _ in range(count):
        next(step)


def run_behind(*steps):
    steps, turn = list(steps), 0
    while steps:
        left = []
        for lag, step in steps:
            try:
                if turn >= lag:
                    next(step)
                left.append((lag, step))
            except StopIteration:
                pass
        steps, turn = left, turn + 1


def run(*steps):
    steps = list(steps)
    while steps:
        left = []
        for step in steps:
            try:
                next(step)
                left.append(step)
            except StopIteration:
                pass
        steps = left


def line_sems(A, B):
    dma = pltpu.SemaphoreType.DMA
    return [dma((2, A)), dma((2, A)), dma((2, A, B)), dma((2, A, B))]


def gather(g, own, out, sems, arrived=lambda i, block: None):
    send_a, recv_a, send_b, recv_b = sems
    A, B = g.A, g.B
    row = lambda way, k: g.a - k if way == 0 else g.a + k
    col = lambda way, k: g.b - k if way == 0 else g.b + k
    rows = [(0, 0)] + [(way, k) for k in range(1, A) for way in (0, 1)]

    def along_a(way, k, src, do):
        if k < A - 1:
            there, device = g.next("a", way)
            i = g.at(row(way, k), g.b)

            @pl.when(there)
            def _():
                do(remote(src, out.at[i], send_a.at[way, k], recv_a.at[way, k + 1], device))

    def along_b(way, j, a, i, src, do):
        if j < B - 1:
            there, device = g.next("b", way)

            @pl.when(there)
            def _():
                do(remote(src, out.at[i], send_b.at[way, a, j], recv_b.at[way, a, j + 1], device))

    def start(copy):
        copy.start()

    def sent(copy):
        copy.wait_send()

    for way in (0, 1):
        along_a(way, 0, own, start)
    for way in (0, 1):
        along_b(way, 0, g.a, g.me, own, start)
    arrived(g.me, own)
    yield
    for k in range(1, A):
        for way in (0, 1):
            i = g.at(row(way, k), g.b)

            @pl.when(g.behind("a", way, k))
            def _():
                remote(out.at[i], out.at[i], send_a.at[way, k], recv_a.at[way, k], g.here()).wait_recv()
                along_a(way, k, out.at[i], start)
                for w in (0, 1):
                    along_b(w, 0, row(way, k), i, out.at[i], start)
                arrived(i, out.at[i])

            yield
    for j in range(1, B):
        for way, k in rows:
            for w in (0, 1):
                i = g.at(row(way, k), col(w, j))

                @pl.when(g.behind("a", way, k) & g.behind("b", w, j))
                def _():
                    a = row(way, k)
                    remote(out.at[i], out.at[i], send_b.at[w, a, j], recv_b.at[w, a, j], g.here()).wait_recv()
                    along_b(w, j, a, i, out.at[i], start)
                    arrived(i, out.at[i])

            yield
    for way, k in rows:
        for w in (0, 1) if k == 0 else (way,):

            @pl.when(g.behind("a", w, k))
            def _():
                along_a(w, k, own, sent)

        @pl.when(g.behind("a", way, k))
        def _():
            for w in (0, 1):
                for j in range(B - 1):

                    @pl.when(g.behind("b", w, j))
                    def _():
                        along_b(w, j, row(way, k), g.me, own, sent)


def sum_slots(A, B, block, dtype=BF16):
    return [
        pltpu.VMEM((A + 1,) + block, dtype),
        pltpu.VMEM((A,) + block, dtype),
        pltpu.VMEM((A, B - 1) + block, dtype),
    ]


def reduce(g, part, finish, sems, slots, sent=None):
    send_a, recv_a, send_b, recv_b = sems
    land_a, out_a, land_b = slots
    sent = sent or part
    A, B = g.A, g.B
    row = lambda way, k: g.a + k if way == 0 else g.a - k
    rows = [(way, k) for k in range(A - 1, 0, -1) for way in (0, 1)] + [(0, 0)]
    here = g.here()

    def across(a, r):
        to = (g.b + r) % B
        return remote(sent(g.at(a, to)), land_b.at[a, r - 1], send_b.at[0, a, r], recv_b.at[0, a, r], g.dev(g.a, to))

    def landing(way, k):
        return land_a.at[A if k == 0 and way == 1 else row(way, k)]

    def along(way, k):
        to = A if k == 1 and way == 1 else row(way, k)
        return remote(
            out_a.at[row(way, k)], land_a.at[to], send_a.at[way, k], recv_a.at[way, k - 1], g.next("a", way)[1]
        )

    def landed(way, k):
        remote(landing(way, k), landing(way, k), send_a.at[way, k], recv_a.at[way, k], here).wait_recv()

    for way, k in rows:

        @pl.when(g.ahead("a", way, k))
        def _():
            for r in range(1, B):
                across(row(way, k), r).start()

    yield
    for way, k in rows:

        @pl.when(g.ahead("a", way, k))
        def _():
            a = row(way, k)
            for r in range(1, B):
                mine = land_b.at[a, r - 1]
                remote(mine, mine, send_b.at[0, a, r], recv_b.at[0, a, r], here).wait_recv()

            def near():
                total = part(g.at(a, g.b))[...].astype(F32)
                for r in range(1, B):
                    total = total + land_b[a, r - 1].astype(F32)
                return total

            if k > 0:
                if k < A - 1:

                    @pl.when(g.behind("a", way, 1))
                    def _():
                        landed(way, k)
                        out_a[a] = (near() + landing(way, k)[...].astype(F32)).astype(out_a.dtype)

                @pl.when(jnp.logical_not(g.behind("a", way, 1)))
                def _():
                    out_a[a] = near().astype(out_a.dtype)

                along(way, k).start()
            else:
                for w in (0, 1):
                    if A > 1:

                        @pl.when(g.behind("a", w, 1))
                        def _():
                            landed(w, 0)

                total = near()
                if A == 2:
                    total = total + land_a[jnp.where(g.a == 1, 1, A)].astype(F32)
                else:
                    for w in (0, 1):
                        if A > 1:
                            total = total + jnp.where(g.behind("a", w, 1), landing(w, 0)[...].astype(F32), 0.0)
                finish(total)

        yield
    for way, k in rows:

        @pl.when(g.ahead("a", way, k))
        def _():
            for r in range(1, B):
                across(row(way, k), r).wait_send()
            if k > 0:
                along(way, k).wait_send()


def total_scratch(A, B, block):
    return [pltpu.VMEM(block, BF16)] + line_sems(A, B) * 2 + sum_slots(A, B, block)


def total(g, part, out, take):
    kept, sems, slots = take(), take(8), take(3)

    def finish(value):
        kept[...] = value.astype(kept.dtype)

    yield from reduce(g, part, finish, sems[:4], slots)
    out.at[g.me][...] = kept[...]
    yield from gather(g, kept, out, sems[4:])


def exchange_sems(n):
    return [pltpu.SemaphoreType.DMA((n,)), pltpu.SemaphoreType.DMA((n,))]


def pass_slices(g, out, sems):
    send, recv = sems
    n = g.A * g.B

    def copies(i, block):
        for r in range(1, n):
            to = (g.me + r) % n
            yield remote(block.at[to], out.at[g.me, i], send.at[i, r], recv.at[i, r], {g.axis: to})

    def arrived(i, block):
        for copy in copies(i, block):
            copy.start()

    def end(blocks, block):
        for i in blocks:
            for r in range(1, n):
                mine = out.at[(g.me + n - r) % n, i]
                remote(mine, mine, send.at[i, r], recv.at[i, r], g.here()).wait_recv()
            for copy in copies(i, block):
                copy.wait_send()

    return arrived, end


def exchange(g, part, out, sems):
    send, recv = sems
    n = g.A * g.B
    copies = []
    for r in range(1, n):
        to = (g.me + r) % n
        copies.append(remote(part.at[to], out.at[g.me], send.at[r], recv.at[r], {g.axis: to}))
        copies[-1].start()
    out[g.me] = part[g.me]
    yield
    for r in range(1, n):
        origin = (g.me + n - r) % n
        remote(part.at[origin], out.at[origin], send.at[r], recv.at[r], g.here()).wait_recv()
    yield
    for copy in copies:
        copy.wait_send()


VMEM = pl.BlockSpec(memory_space=pltpu.VMEM)
ANY = pl.BlockSpec(memory_space=pl.ANY)


def call(body, name, outs, ins, scratch=(), cid=None, us=10.0, **grid):
    whole = VMEM
    params = dict(vmem_limit_bytes=VMEM_MOST)
    if cid is not None:
        params |= dict(collective_id=cid, has_side_effects=True)
    return pl.pallas_call(
        body,
        out_shape=[jax.ShapeDtypeStruct(shape, dtype) for shape, dtype in outs],
        in_specs=grid.pop("in_specs", [whole] * len(ins)),
        out_specs=grid.pop("out_specs", [whole] * len(outs)),
        scratch_shapes=list(scratch),
        compiler_params=pltpu.CompilerParams(**params),
        cost_estimate=pl.CostEstimate(flops=0, transcendentals=0, bytes_accessed=int(us * 3e6)),
        name=name,
        **grid,
    )(*ins)


def taker(refs):
    refs = list(refs)

    def take(n=None):
        if n is None:
            return refs.pop(0)
        return [refs.pop(0) for _ in range(n)]

    return take


def dot(left, right, contract=((1,), (0,))):
    return lax.dot_general(left, right, (contract, ((), ())), preferred_element_type=F32)


def halves(values):
    high = values.astype(BF16)
    return high, (values - high.astype(F32)).astype(BF16)


def norm_scale(values):
    return lax.rsqrt(jnp.mean(values * values, axis=-1, keepdims=True) + NORM_EPSILON)


def norm_back(grad, normed, scale, gain):
    grad_hat = grad * gain
    return scale * (grad_hat - normed * jnp.mean(grad_hat * normed, axis=-1, keepdims=True))


def rotary(values, cosine, sine, back=False):
    width, half = values.shape[1], HEAD_DIMENSION // 2
    later = pltpu.roll(values, width - half, 1)
    earlier = pltpu.roll(values, half, 1)
    front = lax.broadcasted_iota(jnp.int32, values.shape, 1) % HEAD_DIMENSION < half
    other = jnp.where(front, -later, earlier)
    return values * cosine - other * sine if back else values * cosine + other * sine


def allowed_pairs(segment_row):
    size = segment_row.shape[1]
    across = jnp.broadcast_to(segment_row, (size, size))
    rows = lax.broadcasted_iota(jnp.int32, (size, size), 0)
    cols = lax.broadcasted_iota(jnp.int32, (size, size), 1)
    return (cols <= rows) & (across == across.T)


def attention_weights(stacked, keys, allowed):
    scores = dot(stacked, keys, ((1,), (1,))) * SCORE_SCALE
    scores = jnp.where(allowed, scores, MASKED_SCORE)
    row_max = jnp.max(scores, axis=-1, keepdims=True)
    log_total = row_max + jnp.log(jnp.sum(jnp.exp(scores - row_max), axis=-1, keepdims=True))
    return jnp.exp(scores - log_total)


class Heads:
    def __init__(self, ranks):
        self.q, self.kv = QUERY_HEADS // ranks, KEY_VALUE_HEADS // ranks
        self.group = QUERY_HEADS // KEY_VALUE_HEADS
        self.q_cols, self.kv_cols = self.q * HEAD_DIMENSION, self.kv * HEAD_DIMENSION
        self.cols = -(-(self.q_cols + 2 * self.kv_cols) // 128) * 128

    def stack(self, rows, kv):
        first = kv * self.group
        return jnp.concatenate([self.head(rows, first + i) for i in range(self.group)], axis=0)

    def head(self, rows, i):
        return rows[:, i * HEAD_DIMENSION : (i + 1) * HEAD_DIMENSION]

    def key(self, rows, kv):
        return self.head(rows, self.q + kv)

    def value(self, rows, kv):
        return self.head(rows, self.q + self.kv + kv)


def rope_tables(length, heads):
    frequency = np.float32(ROPE_BASE) ** (-(np.arange(HEAD_DIMENSION // 2, dtype=np.float32) * 2.0) / HEAD_DIMENSION)
    angles = np.arange(length, dtype=np.float32)[:, None] * frequency.astype(np.float32)[None, :]
    cosine, sine = (np.tile(f(angles.astype(np.float64)).astype(np.float32), (1, 2)) for f in (np.cos, np.sin))
    turned = heads.q + heads.kv
    rest = heads.cols - turned * HEAD_DIMENSION
    cosine = np.concatenate([np.tile(cosine, (1, turned)), np.ones((length, rest), np.float32)], axis=1)
    sine = np.concatenate([np.tile(sine, (1, turned)), np.zeros((length, rest), np.float32)], axis=1)
    return cosine, sine


def gain_row(misc_ref, ranks, which):
    return jnp.concatenate([misc_ref[i, which : which + 1, :] for i in range(ranks)], axis=1)


def attention_forward(ranks, heads, length, x_ref, w_ref, o_ref, misc_ref, cos_ref, sin_ref, part_ref, qkv_ref, att_ref, scale_ref):
    width = x_ref.shape[2]
    gain = gain_row(misc_ref, ranks, 0)
    weights = w_ref[...].reshape(width, heads.cols)

    def one(b, carry):
        x = x_ref[b].astype(F32)
        scale = norm_scale(x)
        scale_ref[b] = jnp.broadcast_to(scale, (length, 128))
        normed = (x * scale * gain).astype(BF16)
        qkv_ref[b] = rotary(dot(normed, weights), cos_ref[...], sin_ref[...]).astype(BF16)
        qkv = qkv_ref[b]
        allowed = allowed_pairs(misc_ref[b, 8:9, :length])
        allowed = jnp.concatenate([allowed] * heads.group, axis=0)
        outs = []
        for kv in range(heads.kv):
            probs = attention_weights(heads.stack(qkv, kv), heads.key(qkv, kv), allowed).astype(BF16)
            mixed = dot(probs, heads.value(qkv, kv)).astype(BF16)
            outs += [mixed[i * length : (i + 1) * length] for i in range(heads.group)]
        att_ref[b] = jnp.concatenate(outs, axis=1)
        part_ref[b] = dot(att_ref[b], o_ref[...]).astype(BF16)
        return carry

    lax.fori_loop(0, ranks, one, 0)


def column_experts(n_expert, slots, axis):
    column = lax.broadcasted_iota(jnp.int32, (1, 128) if axis else (128, 1), axis)
    owner, slot = column // SLOT_STRIDE, column % SLOT_STRIDE
    expert = slot * n_expert + owner
    real = (owner < n_expert) & (slot < slots) & (expert < EXPERT_COUNT)
    return real, jnp.where(real, expert, -1)


def column_picks(n_expert, slots):
    _, expert = column_experts(n_expert, slots, 1)
    return jnp.where(lax.broadcasted_iota(jnp.int32, (EXPERT_COUNT, 128), 0) == expert, 1.0, 0.0)


def route_tables(n_expert, slots, routes, blocks_ref):
    tokens = routes.shape[1]
    _, expert = column_experts(n_expert, slots, 0)
    named = jnp.zeros((128, tokens), F32)
    for k in range(routes.shape[0]):
        named = named + jnp.where(routes[k : k + 1, :] == expert, 1.0, 0.0)
    limit = jnp.zeros((128, 1), jnp.int32)
    for e in range(EXPERT_COUNT):
        limit = jnp.where(expert == e, blocks_ref[e] * BLK, limit)
    rows = lax.broadcasted_iota(jnp.int32, (tokens, tokens), 0)
    cols = lax.broadcasted_iota(jnp.int32, (tokens, tokens), 1)
    earlier = jnp.where(rows < cols, 1.0, 0.0).astype(BF16)
    rank = dot(named.astype(BF16), earlier)
    kept = (named > 0.0) & (rank < limit.astype(F32))
    return kept, jnp.where(kept, rank, -1.0)


def route_forward(ranks, n_expert, slots, x_ref, branch_ref, misc_ref, router_ref, routes_ref, blocks_ref, hidden_ref, norm_ref, scale_ref, probs_ref, meta_ref, table_ref):
    gain = gain_row(misc_ref, ranks, 1)
    width = x_ref.shape[1]
    shard = width // ranks
    hidden = x_ref[...].astype(F32) + RESIDUAL_SCALE * branch_ref[...]
    hidden_ref[...] = hidden
    scale = norm_scale(hidden)
    scale_ref[...] = jnp.broadcast_to(scale, scale_ref.shape)
    norm = (hidden * scale * gain).astype(BF16)
    picks = column_picks(n_expert, slots).astype(BF16)
    for i in range(ranks):
        here = slice(i * shard, (i + 1) * shard)
        norm_ref[i] = norm[:, here]
        table_ref[here, :] = dot(router_ref[i], picks, ((0,), (0,))).astype(BF16)
    kept, place = route_tables(n_expert, slots, routes_ref[...], blocks_ref)
    real, _ = column_experts(n_expert, slots, 1)
    logits = jnp.where(real, dot(norm, table_ref[...]), MASKED_SCORE)
    weight = jnp.exp(logits - jnp.max(logits, axis=-1, keepdims=True))
    probs = weight / jnp.sum(weight, axis=-1, keepdims=True)
    probs_ref[...] = probs
    used = n_expert * SLOT_STRIDE
    meta_ref[0] = place[:used]
    meta_ref[1] = jnp.where(kept, probs.T, 0.0)[:used]


def row_picks(slots, place):
    number = lax.broadcasted_iota(jnp.int32, (SLOT_ROWS, place.shape[1]), 0).astype(F32)
    return jnp.concatenate([jnp.where(number == place[s : s + 1], 1.0, 0.0) for s in range(slots)], axis=0)


def row_shares(slots, share):
    return jnp.concatenate(
        [jnp.broadcast_to(share[s : s + 1], (SLOT_ROWS, share.shape[1])) for s in range(slots)], axis=0
    )


def pick_rows(slots, n_expert, mine, meta_ref, block, to_sc):
    def one(q, carry):
        pick = row_picks(slots, meta_ref[q, 0, mine, :]).astype(BF16)
        ranks, _, shard = block(q).shape
        for i in range(ranks):
            to_sc[q, :, i * shard : (i + 1) * shard] = dot(pick, block(q)[i]).astype(BF16)
        return carry

    lax.fori_loop(0, n_expert, one, 0)


def expert_slot(n_expert, tokens, s, mine, meta_ref, up_ref, down_ref, gate_grad_ref, inner_ring, both_ring, x_sc, og_sc):
    width = x_sc.shape[2]
    hidden = down_ref.shape[0]
    place_of = pl.ds(pl.multiple_of(s * SLOT_ROWS, SLOT_ROWS), SLOT_ROWS)
    slot_row = lax.broadcasted_iota(jnp.int32, (SLOT_STRIDE, tokens), 0) == s
    number = lax.broadcasted_iota(jnp.int32, (SLOT_ROWS, tokens), 0).astype(F32)
    rows = n_expert * SLOT_ROWS
    both = dot(x_sc[:, place_of, :].reshape(rows, width), up_ref[...])
    gate, up = both[:, :hidden], both[:, hidden:]
    squash = jax.nn.sigmoid(gate)
    inner = (gate * squash * up).astype(BF16)
    inner_ring.free(s)[...] = inner
    inner_ring.copy(s).start()
    produced = dot(inner, down_ref[...]).astype(BF16)
    masks, gates = [], []
    for q in range(n_expert):
        place = jnp.sum(jnp.where(slot_row, meta_ref[q, 0, mine, :], 0.0), axis=0, keepdims=True)
        share = jnp.sum(jnp.where(slot_row, meta_ref[q, 1, mine, :], 0.0), axis=0, keepdims=True)
        masks.append(number == place)
        gates.append(jnp.sum(jnp.where(masks[q], share, 0.0), axis=1, keepdims=True))
    mix_grad = RESIDUAL_SCALE * og_sc[:, place_of, :].reshape(rows, width).astype(F32)
    grad_rows = (jnp.concatenate(gates, axis=0) * mix_grad).astype(BF16)
    gate_grad = jnp.sum(mix_grad * produced.astype(F32), axis=1, keepdims=True)
    og_sc[:, place_of, :] = produced.reshape(n_expert, SLOT_ROWS, width)
    for q in range(n_expert):
        spread = jnp.where(masks[q], gate_grad[q * SLOT_ROWS : (q + 1) * SLOT_ROWS], 0.0)
        gate_grad_ref[q] = jnp.where(slot_row, jnp.sum(spread, axis=0, keepdims=True), gate_grad_ref[q])
    grad_inner = dot(grad_rows, down_ref[...], ((1,), (1,)))
    grad_both = jnp.concatenate(
        [grad_inner * up * squash * (1.0 + gate * (1.0 - squash)), grad_inner * (gate * squash)], axis=1
    ).astype(BF16)
    both_ring.free(s)[...] = grad_both
    both_ring.copy(s).start()
    x_sc[:, place_of, :] = dot(grad_both, up_ref[...], ((1,), (1,))).astype(BF16).reshape(n_expert, SLOT_ROWS, width)


def sum_rows_back(slots, n_expert, mine, meta_ref, out_ring, back_ring, eo_sc, gx_sc):
    def one(q, carry):
        pick = row_picks(slots, meta_ref[q, 0, mine, :])
        high, low = halves(pick * row_shares(slots, meta_ref[q, 1, mine, :]))
        over = ((0,), (0,))
        back_ring.free(q)[...] = dot(pick.astype(BF16), gx_sc[q], over).astype(BF16)
        back_ring.copy(q).start()
        out_ring.free(q)[...] = (dot(high, eo_sc[q], over) + dot(low, eo_sc[q], over)).astype(BF16)
        out_ring.copy(q).start()
        return carry

    lax.fori_loop(0, n_expert, one, 0)


def route_backward(ranks, n_expert, shard, hidden_ref, norm_ref, scale_ref, probs_ref, misc_ref, router_ref, og_ref, back_ref, gate_grad_ref, grad_hidden_ref, branch_ref, small_ref):
    tokens, width = hidden_ref.shape
    gain = gain_row(misc_ref, ranks, 1)
    hidden = hidden_ref[...]
    used = n_expert * SLOT_STRIDE
    spread = gate_grad_ref[...].reshape(used, tokens)
    if used < 128:
        spread = jnp.concatenate([spread, jnp.zeros((128 - used, tokens), F32)], axis=0)
    grad_probs = spread.T
    probs = probs_ref[...]
    grad_logits = probs * (grad_probs - jnp.sum(probs * grad_probs, axis=1, keepdims=True))
    high, low = halves(grad_logits)
    router = router_ref[...]
    across = ((1,), (1,))
    grad_norm = back_ref[...] + (dot(high, router, across) + dot(low, router, across))
    scale = scale_ref[:, 0:1]
    normed = hidden * scale
    grad_hidden = og_ref[...].astype(F32) + norm_back(grad_norm, normed, scale, gain)
    grad_hidden_ref[...] = grad_hidden
    branch_ref[...] = (RESIDUAL_SCALE * grad_hidden).astype(BF16)
    over = ((0,), (0,))
    grad_gain = jnp.sum(grad_norm * normed, axis=0, keepdims=True)
    for i in range(ranks):
        here = slice(i * shard, (i + 1) * shard)
        grad_router = dot(high, norm_ref[i], over) + dot(low, norm_ref[i], over)
        small_ref[i, :used, :] = grad_router[:used].astype(BF16)
        small_ref[i, used:, :] = jnp.broadcast_to(grad_gain[:, here], (16, shard)).astype(BF16)


def store_blocks(ref, cols, values):
    count, rows = ref.shape[0], ref.shape[1]
    for i in range(count):
        ref[i, :, cols] = values[i * rows : (i + 1) * rows]


def attention_backward(ranks, heads, length, branch_ref, att_ref, qkv_ref, o_ref, misc_ref, cos_ref, sin_ref, grad_ref, d_o_ref):
    d_o = dot(att_ref[...].reshape(ranks * length, heads.q_cols), branch_ref[...].reshape(ranks * length, -1), ((0,), (0,)))
    store_blocks(d_o_ref, slice(None), d_o.astype(BF16))

    def one(b, carry):
        grad_att = dot(branch_ref[b], o_ref[...], ((1,), (1,))).astype(BF16)
        att, qkv = att_ref[b], qkv_ref[b]
        allowed = allowed_pairs(misc_ref[b, 8:9, :length])
        allowed = jnp.concatenate([allowed] * heads.group, axis=0)
        d_q, d_k, d_v = [], [], []
        for kv in range(heads.kv):
            queries, keys = heads.stack(qkv, kv), heads.key(qkv, kv)
            soft = attention_weights(queries, keys, allowed)
            grads = heads.stack(grad_att, kv)
            d_v.append(dot(soft.astype(BF16), grads, ((0,), (0,))))
            delta = jnp.sum(grads.astype(F32) * heads.stack(att, kv).astype(F32), axis=1, keepdims=True)
            inner = dot(grads, heads.value(qkv, kv), ((1,), (1,)))
            d_scores = (soft * (inner - delta) * SCORE_SCALE).astype(BF16)
            rows = dot(d_scores, keys)
            d_q += [rows[i * length : (i + 1) * length] for i in range(heads.group)]
            d_k.append(dot(d_scores, queries, ((0,), (0,))))
        spare = heads.cols - heads.q_cols - 2 * heads.kv_cols
        fill = [jnp.zeros((length, spare), F32)] if spare else []
        grads = jnp.concatenate(d_q + d_k + d_v + fill, axis=1)
        grad_ref[b] = rotary(grads, cos_ref[...], sin_ref[...], back=True).astype(BF16)
        return carry

    lax.fori_loop(0, ranks, one, 0)


def projection_backward(ranks, heads, shard, x_ref, scale_ref, gain_ref, grad_ref, w_ref, small_ref, grad_x_ref, d_w_ref, sums_ref):
    normed = x_ref[...].astype(F32) * scale_ref[:, 0:1]
    norm_input = (normed * gain_ref[0:1, :]).astype(BF16)
    total = None
    for i in range(ranks):
        grads = grad_ref[i].reshape(-1, heads.cols)
        term = dot(grads, w_ref[i], ((1,), (1,)))
        total = term if total is None else total + term
        store_blocks(d_w_ref, slice(i * heads.cols, (i + 1) * heads.cols), dot(norm_input, grads, ((0,), (0,))).astype(BF16))
    grad_x_ref[...] = total.reshape(grad_x_ref.shape)
    small = small_ref[0].astype(F32)
    for i in range(1, ranks):
        small = small + small_ref[i].astype(F32)
    gain_grad = jnp.sum(total * normed, axis=0, keepdims=True)
    used = small.shape[0] - 16
    sums_ref[...] = jnp.zeros_like(sums_ref)
    sums_ref[:used, :] = small[:used].astype(BF16)
    second = lax.broadcasted_iota(jnp.int32, (16, shard), 0)
    sums_ref[used : used + 16, :] = jnp.where(second == 0, small[used:], jnp.where(second == 1, gain_grad, 0.0)).astype(BF16)


def group_rows(n_expert, slots, at, x, og, meta_ref, x_rows, og_rows):
    def one(q, carry):
        pick = row_picks(slots, meta_ref[at, q, 0])
        share = jnp.sum(pick * row_shares(slots, meta_ref[at, q, 1]), axis=1, keepdims=True)
        pick = pick.astype(BF16)
        x_rows[q] = dot(pick, x[q]).astype(BF16)
        og_rows[q] = (share * (RESIDUAL_SCALE * dot(pick, og[q]))).astype(BF16)
        return carry

    lax.fori_loop(0, n_expert, one, 0)


def finish(ranks, n_expert, slots, heads, tokens, x_rows_ref, og_rows_ref, both_ref, inner_ref, grad_ref, x_ref, misc_ref, grad_hidden_ref, hidden_ref, mixture_ref, d_w_ref, d_o_ref, sums_ref, d_up_ref, d_down_ref, output_ref, grad_inputs_ref, q_ref, k_ref, v_ref, o_ref, router_ref, gain_one_ref, gain_two_ref):
    step = pl.program_id(0)

    @pl.when(step == 0)
    def _():
        output_ref[...] = (hidden_ref[...] + RESIDUAL_SCALE * mixture_ref[...]).astype(BF16)
        gain = gain_row(misc_ref, ranks, 0)
        grad = jnp.concatenate([grad_ref[i] for i in range(ranks)], axis=1)
        x = x_ref[...].astype(F32)
        scale = norm_scale(x)
        grad_inputs_ref[...] = grad_hidden_ref[...] + norm_back(grad, x * scale, scale, gain)
        used = n_expert * SLOT_STRIDE
        router_ref[...] = dot(column_picks(n_expert, slots).astype(BF16), sums_ref[:128])
        ends = sums_ref[used : used + 16, :].astype(F32)
        gain_two_ref[...] = ends[0]
        gain_one_ref[...] = ends[1]
        o_ref[...] = d_o_ref[...].astype(F32)
        first, second = heads.q_cols, heads.q_cols + heads.kv_cols
        for i in range(ranks):
            start = i * heads.cols
            q_ref[:, i * heads.q_cols : (i + 1) * heads.q_cols] = d_w_ref[:, start : start + first].astype(F32)
            here = slice(i * heads.kv_cols, (i + 1) * heads.kv_cols)
            k_ref[:, here] = d_w_ref[:, start + first : start + second].astype(F32)
            v_ref[:, here] = d_w_ref[:, start + second : start + second + heads.kv_cols].astype(F32)

    flat = lambda value: value.reshape(-1, value.shape[-1])
    over = ((0,), (0,))
    d_up_ref[0] = dot(flat(x_rows_ref[...]), flat(both_ref[...]), over)
    d_down_ref[0] = dot(flat(inner_ref[...]), flat(og_rows_ref[...]), over)


def on_device(
    inputs,
    segment_ids,
    routes,
    expert_blocks,
    norm1_gain,
    q_weight,
    k_weight,
    value_matrix,
    o_weight,
    norm2_gain,
    router_weight,
    expert_gate_up,
    expert_down,
    out_grad,
):
    ranks, n_expert = lax.axis_size("dp"), lax.axis_size("expert")
    tokens, width = inputs.shape
    shard = q_weight.shape[0]
    slots, _, double = expert_gate_up.shape
    hidden = expert_down.shape[1]
    heads = Heads(ranks)
    group = ("dp", ranks // 2, 2)
    plane = ("expert", 4, n_expert // 4)
    used = n_expert * SLOT_STRIDE
    cosine, sine = rope_tables(tokens, heads)

    gains = jnp.stack([norm1_gain, norm2_gain]).astype(F32)
    dma = pltpu.SemaphoreType.DMA

    def forward(*refs):
        take = taker(refs)
        x, wq, wk, wv, rt, gn, sg, og, wo, cs, sn, routes_ref, blocks_ref = take(13)
        w, ms_all, og_all, qkv, att, scale_one, xc, hidden_ref, norm, scale_two, probs, meta, table = take(13)
        x_all, w_all, rt_all, ms, og_own, part, branch, own_sem = take(8)
        dp, ex = Grid(*group), Grid(*plane)
        for i in range(ranks):
            at = 0
            for ref, cols in ((wq, heads.q_cols), (wk, heads.kv_cols), (wv, heads.kv_cols)):
                w[i, :, at : at + cols] = ref[:, i * cols : (i + 1) * cols]
                at += cols
            if at < heads.cols:
                w[i, :, at:] = jnp.zeros((shard, heads.cols - at), BF16)
            og_own[i] = og[:, i * shard : (i + 1) * shard]
        ms[...] = jnp.zeros_like(ms)
        ms[0:2, :] = gn[...]
        ms[8:9, :tokens] = sg[...].astype(F32)
        x_all[dp.me] = x[...]
        rt_all[dp.me] = rt[...]
        ms_all[dp.me] = ms[...]
        greet(dp.all() + ex.near())
        keep = pltpu.make_async_copy(og_own, og_all.at[ex.me], own_sem)
        keep.start()
        small = [begin(gather(dp, ms, ms_all, take(4))), begin(gather(dp, rt, rt_all, take(4)))]
        xs = begin(gather(dp, x, x_all, take(4)))
        ws = begin(exchange(dp, w, w_all, take(2)))
        ogs = begin(gather(ex, og_own, og_all, take(4)))
        run(*small, xs)
        for i in range(ranks):

            @pl.when(dp.me == i)
            def _():
                for b in range(ranks):
                    xc[b * tokens : (b + 1) * tokens, :] = x_all[b, :, i * shard : (i + 1) * shard]

        advance(ogs, 2 * (plane[1] - 1))
        run(ws)
        attention_forward(ranks, heads, tokens, x_all, w_all, wo, ms_all, cs, sn, part, qkv, att, scale_one)

        def store(total):
            branch[...] = total

        run(reduce(dp, lambda i: part.at[i], store, take(4), take(3)))
        route_forward(ranks, n_expert, slots, x, branch, ms_all, rt_all, routes_ref, blocks_ref, hidden_ref, norm, scale_two, probs, meta, table)
        run(ogs)
        keep.wait()

    (
        weights,
        misc_all,
        og_all,
        qkv,
        att,
        scale_one,
        x_cols,
        hidden_rows,
        norm_hidden,
        scale_two,
        probs,
        meta,
        router,
    ) = call(
        forward,
        "forward",
        [
            ((ranks, shard, heads.cols), BF16),
            ((ranks, 16, shard), F32),
            ((n_expert, ranks, tokens, shard), BF16),
            ((ranks, tokens, heads.cols), BF16),
            ((ranks, tokens, heads.q_cols), BF16),
            ((ranks, tokens, 128), F32),
            ((ranks * tokens, shard), BF16),
            ((tokens, width), F32),
            ((ranks, tokens, shard), BF16),
            ((tokens, 128), F32),
            ((tokens, 128), F32),
            ((2, used, tokens), F32),
            ((width, 128), BF16),
        ],
        (
            inputs,
            q_weight,
            k_weight,
            value_matrix,
            router_weight.T,
            gains,
            segment_ids,
            out_grad,
            o_weight,
            cosine,
            sine,
            routes.T,
            expert_blocks,
        ),
        [
            pltpu.VMEM((ranks, tokens, width), BF16),
            pltpu.VMEM((ranks, shard, heads.cols), BF16),
            pltpu.VMEM((ranks, router_weight.shape[1], shard), BF16),
            pltpu.VMEM((16, shard), F32),
            pltpu.VMEM((ranks, tokens, shard), BF16),
            pltpu.VMEM((ranks, tokens, width), BF16),
            pltpu.VMEM((tokens, width), F32),
            dma(()),
        ]
        + line_sems(*group[1:]) * 3
        + exchange_sems(ranks)
        + line_sems(*plane[1:])
        + line_sems(*group[1:])
        + sum_slots(*group[1:], (tokens, width)),
        cid=0,
        us=70,
        in_specs=[VMEM] * 12 + [pl.BlockSpec(memory_space=pltpu.SMEM)],
        out_specs=[VMEM] * 2 + [ANY] + [VMEM] * 10,
    )

    fixed = lambda shape: pl.BlockSpec(shape, lambda s: (0,) * len(shape), pipeline_mode=pl.Buffered(1))
    moving = lambda shape: pl.BlockSpec((1,) + shape, lambda s: (s,) + (0,) * len(shape))
    rows = n_expert * SLOT_ROWS
    deep = 2 if ranks * rows <= 1024 else 1

    def mixture_of_experts(*refs):
        take = taker(refs)
        nh, mt, og, up, down = take(5)
        gg, mt_group, out_part, back_part, inr, gb, xd, ogd = take(8)
        nh_all, mt_all, mt_own, x_sc, og_sc, og_in, up_in, down_in = take(8)
        stages, ring_sems, og_sems, up_sems, own_sems = take(4), take(), take(), take(), take()
        dp, ex = Grid(*group), Grid(*plane)
        out_ring, back_ring, inner_ring, both_ring = (
            Ring(stage, out, ring_sems.at[i])
            for i, (stage, out) in enumerate(zip(stages, (out_part, back_part, inr.at[dp.me], gb.at[dp.me])))
        )
        mine = pl.ds(pl.multiple_of(ex.me * SLOT_STRIDE, SLOT_STRIDE), SLOT_STRIDE)
        nh_all[ex.me] = nh[...]
        mt_all[ex.me] = mt[...]
        gg[...] = jnp.zeros_like(gg)

        def fetch(s, do):
            do(pltpu.make_async_copy(up.at[s], up_in.at[s % deep], up_sems.at[0, s % deep]))
            do(pltpu.make_async_copy(down.at[s], down_in.at[s % deep], up_sems.at[1, s % deep]))

        for s in range(deep):
            fetch(s, lambda copy: copy.start())
        greet(dp.all() + ex.near())
        mts = begin(gather(ex, mt, mt_all, take(4)))
        og_passed, og_end = pass_slices(dp, ogd, take(2))
        for i in range(n_expert):
            og_passed(i, og.at[i])
        passed, end = pass_slices(dp, xd, take(2))

        def keep(i, block):
            return pltpu.make_async_copy(block.at[dp.me], xd.at[dp.me, i], own_sems.at[i])

        def arrived(i, block):
            passed(i, block)
            keep(i, block).start()

        nhs = begin(gather(ex, nh, nh_all, take(4), arrived))
        run(mts)

        def fetch_og(q):
            return pltpu.make_async_copy(og.at[q], og_in.at[q % 2], og_sems.at[q % 2])

        fetch_og(0).start()

        def pick_og(q, carry):
            @pl.when(q + 1 < n_expert)
            def _():
                fetch_og(q + 1).start()

            fetch_og(q).wait()
            pick = row_picks(slots, mt_all[q, 0, mine, :]).astype(BF16)
            for i in range(ranks):
                og_sc[q, :, i * shard : (i + 1) * shard] = dot(pick, og_in[q % 2, i]).astype(BF16)
            return carry

        lax.fori_loop(0, n_expert, pick_og, 0)
        mt_own[...] = mt_all[:, :, mine, :]
        mt_group[dp.me] = mt_own[...]
        mgs = begin(gather(dp, mt_own, mt_group, take(4)))
        run(nhs)
        pick_rows(slots, n_expert, mine, mt_all, lambda q: nh_all.at[q], x_sc)

        def one(s, carry):
            fetch(s, lambda copy: copy.wait())
            expert_slot(
                n_expert, tokens, s, mine, mt_all, up_in.at[s % deep], down_in.at[s % deep], gg, inner_ring, both_ring, x_sc, og_sc
            )

            @pl.when(s + deep < slots)
            def _():
                fetch(s + deep, lambda copy: copy.start())

            return carry

        lax.fori_loop(0, slots, one, 0)
        run(mgs)
        sum_rows_back(slots, n_expert, mine, mt_all, out_ring, back_ring, og_sc, x_sc)
        inner_ring.end(slots)
        both_ring.end(slots)
        out_ring.end(n_expert)
        back_ring.end(n_expert)
        end(range(n_expert), nh)
        og_end(range(n_expert), og.at[0])
        for i in range(n_expert):
            keep(i, nh).wait()

    gate_grad, meta_group, out_part, back_part, inner, grad_both, norm_slices, og_slices = call(
        mixture_of_experts,
        "mixture_of_experts",
        [
            ((n_expert, SLOT_STRIDE, tokens), F32),
            ((ranks, n_expert, 2, SLOT_STRIDE, tokens), F32),
            ((n_expert, tokens, width), BF16),
            ((n_expert, tokens, width), BF16),
            ((ranks, slots, rows, hidden), BF16),
            ((ranks, slots, rows, double), BF16),
            ((ranks, n_expert, tokens, shard), BF16),
            ((ranks, n_expert, tokens, shard), BF16),
        ],
        (norm_hidden, meta, og_all, expert_gate_up, expert_down),
        [
            pltpu.VMEM((n_expert, ranks, tokens, shard), BF16),
            pltpu.VMEM((n_expert, 2, used, tokens), F32),
            pltpu.VMEM((n_expert, 2, SLOT_STRIDE, tokens), F32),
            pltpu.VMEM((n_expert, slots * SLOT_ROWS, width), BF16),
            pltpu.VMEM((n_expert, slots * SLOT_ROWS, width), BF16),
            pltpu.VMEM((2, ranks, tokens, shard), BF16),
            pltpu.VMEM((deep, width, double), BF16),
            pltpu.VMEM((deep, hidden, width), BF16),
            pltpu.VMEM((2, tokens, width), BF16),
            pltpu.VMEM((2, tokens, width), BF16),
            pltpu.VMEM((2, rows, hidden), BF16),
            pltpu.VMEM((2, rows, double), BF16),
            dma((4, 2)),
            dma((2,)),
            dma((2, deep)),
            dma((n_expert,)),
        ]
        + line_sems(*plane[1:])
        + [dma((n_expert, ranks))] * 4
        + line_sems(*plane[1:])
        + line_sems(*group[1:]),
        cid=1,
        us=80,
        in_specs=[VMEM] * 2 + [ANY] * 3,
        out_specs=[VMEM] * 2 + [ANY] * 6,
    )

    sum_rows = 16 * n_expert
    part_rows = shard // n_expert
    o_block, w_block, s_block = (part_rows, width), (part_rows, ranks * heads.cols), (16, shard)

    halves_of = ranks * heads.cols // 2
    summed = lambda block: total_scratch(*plane[1:], block)

    lead = max(slots // 5, 1)

    def backward(*refs):
        take = taker(refs)
        hid, nh, sc2, pb, ms, tb, og_mine, gg, cs, sn, sc, gn, mt = take(13)
        brought, (og, xd, ogd, _, _, terms, back_terms) = take(5), take(7)
        grad_hidden_ref, mix, gx_all, do_all, dw_all, su_all, x_rows, og_rows, gb_all, inr_all = take(10)
        places, bring_sems = take(5), take()
        wo, qkv, at, xc, w = places
        out_in, back_in, term_sems = take(3)
        gg_all, sm, br_all, sm_all, gr_all, do, dw, su, gx, x_in, og_in, x_out, og_out, in_sems, out_sems = take(15)
        dp, ex = Grid(*group), Grid(*plane)
        brings = [pltpu.make_async_copy(*pair, bring_sems.at[i]) for i, pair in enumerate(zip(brought, places))]
        holds = [
            pltpu.make_async_copy(back_terms, back_in, term_sems.at[0]),
            pltpu.make_async_copy(terms, out_in, term_sems.at[1]),
        ]

        def fetch(j, do_):
            p, slot = (dp.me + j) % ranks, j % deep
            do_(pltpu.make_async_copy(xd.at[p], x_in.at[slot], in_sems.at[0, slot]))
            do_(pltpu.make_async_copy(og.at[:, dp.me] if j == 0 else ogd.at[p], og_in.at[slot], in_sems.at[1, slot]))

        for copy in holds + brings:
            copy.start()
        for j in range(deep):
            fetch(j, lambda copy: copy.start())
        greet(dp.all() + ex.all())

        def store(to):
            def finish_(value):
                to[...] = value

            return finish_

        ggs = begin(exchange(ex, gg, gg_all, take(2)))
        backs = begin(reduce(ex, lambda i: back_in.at[i], store(grad_hidden_ref), take(4), take(3), lambda i: back_terms.at[i]))
        outs = begin(reduce(ex, lambda i: out_in.at[i], store(mix), take(4), take(3), lambda i: terms.at[i]))
        inrs = begin(gather(dp, inr_all.at[dp.me], inr_all, take(4)))
        share = lambda start, count: begin(
            gather(dp, gb_all.at[dp.me, pl.ds(start, count)], Part(gb_all, pl.ds(start, count)), take(4))
        )
        gbs = [share(0, lead)]
        for copy in holds:
            copy.wait()

        def out_copies(j):
            p, slot = (dp.me + j) % ranks, j % deep
            return [
                pltpu.make_async_copy(x_out.at[slot], x_rows.at[p], out_sems.at[0, slot]),
                pltpu.make_async_copy(og_out.at[slot], og_rows.at[p], out_sems.at[1, slot]),
            ]

        def build(j):
            fetch(j, lambda copy: copy.wait())
            if j >= deep:
                for copy in out_copies(j - deep):
                    copy.wait()
            p, slot = (dp.me + j) % ranks, j % deep
            group_rows(n_expert, slots, p, x_in.at[slot], og_in.at[slot], mt, x_out.at[slot], og_out.at[slot])
            for copy in out_copies(j):
                copy.start()
            if j + deep < ranks:
                fetch(j + deep, lambda copy: copy.start())

        for j in range(ranks):
            build(j)
            if j < 2 * (plane[1] - 1):
                advance(backs, 1)
        for j in range(ranks - deep, ranks):
            for copy in out_copies(j):
                copy.wait()
        run(backs)
        run(ggs)
        route_backward(ranks, n_expert, shard, hid, nh, sc2, pb, ms, tb, og_mine, grad_hidden_ref, gg_all, grad_hidden_ref, br_all.at[dp.me], sm)
        brs = begin(gather(dp, br_all.at[dp.me], br_all, take(4)))
        sms = begin(exchange(dp, sm, sm_all, take(2)))
        for copy in brings:
            copy.wait()
        advance(outs, 2)
        run(brs)
        advance(outs, 2)
        attention_backward(ranks, heads, tokens, br_all, at, qkv, wo, ms, cs, sn, gr_all.at[dp.me], do)
        grs = begin(gather(dp, gr_all.at[dp.me], gr_all, take(4)))
        dos = begin(total(ex, lambda i: do.at[i], do_all, take))
        advance(outs, 2)
        run(sms)
        advance(dos, 2 * plane[1])
        run(grs)
        gbs.append(share(lead, slots - lead))
        projection_backward(ranks, heads, shard, xc, sc, gn, gr_all, w, sm_all, gx, dw, su)
        gxs = begin(exchange(dp, gx, gx_all, take(2)))
        dws = []
        for i in range(2):
            cols = pl.ds(i * halves_of, halves_of)
            part = Part(dw, slice(None), cols)
            dws.append(begin(total(ex, part.__getitem__, Part(dw_all, slice(None), cols), take)))
        rows_of = lambda i: pl.ds(pl.multiple_of(i * 16, 16), 16)
        sus = begin(total(ex, lambda i: su.at[rows_of(i)], su_all, take))
        run_behind((0, dos), (0, outs), (1, sus), (1, dws[0]), (6, dws[1]))
        run(gxs)
        run(inrs, *gbs)

    row_block = (n_expert, slots * SLOT_ROWS, shard)
    grad_hidden, mixture, grad_x, d_o, d_w, sums, x_rows, og_rows, both_all, inner_all = call(
        backward,
        "backward",
        [
            ((tokens, width), F32),
            ((tokens, width), F32),
            ((ranks, tokens, shard), F32),
            ((n_expert,) + o_block, BF16),
            ((n_expert,) + w_block, BF16),
            ((n_expert,) + s_block, BF16),
            ((ranks,) + row_block, BF16),
            ((ranks,) + row_block, BF16),
            ((ranks, slots, rows, double), BF16),
            ((ranks, slots, rows, hidden), BF16),
        ],
        (
            hidden_rows,
            norm_hidden,
            scale_two,
            probs,
            misc_all,
            router,
            out_grad,
            gate_grad,
            cosine,
            sine,
            scale_one.reshape(ranks * tokens, 128),
            gains,
            meta_group,
            o_weight,
            qkv,
            att,
            x_cols,
            weights,
            og_all,
            norm_slices,
            og_slices,
            grad_both,
            inner,
            out_part,
            back_part,
        ),
        [
            pltpu.VMEM(o_weight.shape, BF16),
            pltpu.VMEM(qkv.shape, BF16),
            pltpu.VMEM(att.shape, BF16),
            pltpu.VMEM(x_cols.shape, BF16),
            pltpu.VMEM(weights.shape, BF16),
            dma((5,)),
            pltpu.VMEM((n_expert, tokens, width), BF16),
            pltpu.VMEM((n_expert, tokens, width), BF16),
            dma((2,)),
            pltpu.VMEM((n_expert, SLOT_STRIDE, tokens), F32),
            pltpu.VMEM((ranks, used + 16, shard), BF16),
            pltpu.VMEM((ranks, tokens, width), BF16),
            pltpu.VMEM((ranks, used + 16, shard), BF16),
            pltpu.VMEM((ranks, ranks, tokens, heads.cols), BF16),
            pltpu.VMEM((n_expert,) + o_block, BF16),
            pltpu.VMEM((n_expert,) + w_block, BF16),
            pltpu.VMEM((sum_rows, shard), BF16),
            pltpu.VMEM((ranks, tokens, shard), F32),
            pltpu.VMEM((deep, n_expert, tokens, shard), BF16),
            pltpu.VMEM((deep, n_expert, tokens, shard), BF16),
            pltpu.VMEM((deep,) + row_block, BF16),
            pltpu.VMEM((deep,) + row_block, BF16),
            dma((2, deep)),
            dma((2, deep)),
        ]
        + exchange_sems(n_expert)
        + (line_sems(*plane[1:]) + sum_slots(*plane[1:], (tokens, width))) * 2
        + line_sems(*group[1:]) * 3
        + exchange_sems(ranks)
        + line_sems(*group[1:])
        + summed(o_block)
        + line_sems(*group[1:])
        + exchange_sems(ranks)
        + summed((part_rows, halves_of)) * 2
        + summed(s_block),
        cid=2,
        us=165,
        in_specs=[VMEM] * 13 + [ANY] * 12,
        out_specs=[VMEM] * 6 + [ANY] * 4,
        input_output_aliases={21: 8, 22: 9},
    )

    held = pl.Buffered(deep)
    gathered = lambda shape, at: pl.BlockSpec(
        (ranks, 1) + shape, lambda s: (0, at(s)) + (0,) * len(shape), pipeline_mode=held
    )
    d_w = d_w.reshape(shard, ranks * heads.cols)
    d_o = d_o.reshape(shard, width)
    sums = sums.reshape(sum_rows, shard)
    ins = (grad_x, inputs, misc_all, grad_hidden, hidden_rows, mixture, d_w, d_o, sums)
    outs = [
        ((slots, shard, double), F32),
        ((slots, hidden, shard), F32),
        ((tokens, width), BF16),
        ((tokens, width), F32),
        ((shard, QUERY_HEADS * HEAD_DIMENSION), F32),
        ((shard, KEY_VALUE_HEADS * HEAD_DIMENSION), F32),
        ((shard, KEY_VALUE_HEADS * HEAD_DIMENSION), F32),
        ((shard, width), F32),
        ((router_weight.shape[1], shard), F32),
        ((shard,), F32),
        ((shard,), F32),
    ]
    d_up, d_down, output, grad_inputs, d_q, d_k, d_v, d_o, d_router, gain_one, gain_two = call(
        functools.partial(finish, ranks, n_expert, slots, heads, tokens),
        "finish",
        outs,
        (x_rows, og_rows, both_all, inner_all) + ins,
        us=15,
        grid=(slots,),
        in_specs=[
            pl.BlockSpec((ranks, n_expert, SLOT_ROWS, shard), lambda s: (0, 0, s, 0)),
            pl.BlockSpec((ranks, n_expert, SLOT_ROWS, shard), lambda s: (0, 0, s, 0)),
            gathered((rows, double), lambda s: s),
            gathered((rows, hidden), lambda s: s),
        ]
        + [fixed(array.shape) for array in ins],
        out_specs=[moving((shard, double)), moving((hidden, shard))] + [fixed(shape) for shape, _ in outs[2:]],
    )
    return (
        output,
        grad_inputs,
        gain_one,
        d_q,
        d_k,
        d_v,
        d_o,
        gain_two,
        d_router.T,
        d_up,
        d_down,
    )


def solution(mesh):
    tokens = P(("dp", "expert"), None)
    rows = P("dp", None)
    return jax.shard_map(
        on_device,
        mesh=mesh,
        in_specs=(
            tokens,
            tokens,
            tokens,
            P(),
            P("dp"),
            rows,
            rows,
            rows,
            rows,
            P("dp"),
            rows,
            P("expert", None, None),
            P("expert", None, None),
            tokens,
        ),
        out_specs=(
            tokens,
            tokens,
            P("dp"),
            rows,
            rows,
            rows,
            rows,
            P("dp"),
            rows,
            P("expert", "dp", None),
            P("expert", None, "dp"),
        ),
        check_vma=False,
    )
```

```python
import functools
import math

import jax
import jax.numpy as jnp
import numpy as np
from jax import lax
from jax.experimental import pallas as pl
from jax.experimental.pallas import tpu as pltpu
from jax.sharding import PartitionSpec as P

QUERY_HEADS = 24
KEY_VALUE_HEADS = 8
HEAD_DIMENSION = 64
EXPERT_COUNT = 40
BLK = 4
SLOT_ROWS = 32
SLOT_STRIDE = 8

NORM_EPSILON = 1e-06
SCORE_SCALE = 0.015625
RESIDUAL_SCALE = 0.22
ROPE_BASE = 10000.0
MASKED_SCORE = -1e30

MESH = pl.DeviceIdType.MESH
F32, BF16 = jnp.float32, jnp.bfloat16
MEBI = 1024 * 1024
VMEM_MOST = 67_043_328


class Grid:
    def __init__(self, axis, A, B):
        self.axis, self.A, self.B = axis, A, B
        self.me = lax.axis_index(axis)
        self.a, self.b = self.me // B, self.me % B

    def at(self, a, b):
        return a * self.B + b

    def dev(self, a, b):
        return {self.axis: self.at(a, b)}

    def here(self):
        return {self.axis: self.me}

    def near(self):
        found = []
        if self.A > 1:
            found += [
                (self.a > 0, self.dev(self.a - 1, self.b)),
                (self.a < self.A - 1, self.dev(self.a + 1, self.b)),
            ]
        found += [(self.me >= 0, self.dev(self.a, (self.b + r) % self.B)) for r in range(1, self.B)]
        return found

    def all(self):
        n = self.A * self.B
        return [(self.me >= 0, {self.axis: (self.me + r) % n}) for r in range(1, n)]

    def next(self, kind, way):
        step = 1 if way == 0 else -1
        if kind == "a":
            return self.ahead("a", way, 1), self.dev(self.a + step, self.b)
        return self.ahead("b", way, 1), self.dev(self.a, self.b + step)

    def behind(self, kind, way, far):
        at, size = (self.a, self.A) if kind == "a" else (self.b, self.B)
        return (at - far >= 0) if way == 0 else (at + far <= size - 1)

    def ahead(self, kind, way, far):
        return self.behind(kind, 1 - way, far)


def greet(peers):
    barrier = pltpu.get_barrier_semaphore()
    for there, device in peers:

        @pl.when(there)
        def _():
            pl.semaphore_signal(barrier, inc=1, device_id=device, device_id_type=MESH)

    pl.semaphore_wait(barrier, sum(jnp.where(there, 1, 0) for there, _ in peers))


def remote(src, dst, send, recv, device):
    return pltpu.make_async_remote_copy(
        src_ref=src, dst_ref=dst, send_sem=send, recv_sem=recv, device_id=device, device_id_type=MESH
    )


class Part:
    def __init__(self, ref, *rest):
        self.ref, self.rest, self.at = ref, rest, self

    def __getitem__(self, i):
        return self.ref.at[(i,) + self.rest]


class Ring:
    def __init__(self, stage, out, sems):
        self.stage, self.out, self.sems = stage, out, sems

    def copy(self, i):
        return pltpu.make_async_copy(self.stage.at[i % 2], self.out.at[i], self.sems.at[i % 2])

    def free(self, i):
        @pl.when(i >= 2)
        def _():
            self.copy(i - 2).wait()

        return self.stage.at[i % 2]

    def end(self, count):
        for i in range(max(count - 2, 0), count):
            self.copy(i).wait()


def begin(step):
    next(step)
    return step


def advance(step, count):
    for _ in range(count):
        next(step)


def run_behind(*steps):
    steps, turn = list(steps), 0
    while steps:
        left = []
        for lag, step in steps:
            try:
                if turn >= lag:
                    next(step)
                left.append((lag, step))
            except StopIteration:
                pass
        steps, turn = left, turn + 1


def run(*steps):
    steps = list(steps)
    while steps:
        left = []
        for step in steps:
            try:
                next(step)
                left.append(step)
            except StopIteration:
                pass
        steps = left


def line_sems(A, B):
    dma = pltpu.SemaphoreType.DMA
    return [dma((2, A)), dma((2, A)), dma((2, A, B)), dma((2, A, B))]


def gather(g, own, out, sems, arrived=lambda i, block: None, near_first=False, started=False):
    send_a, recv_a, send_b, recv_b = sems
    A, B = g.A, g.B
    row = lambda way, k: g.a - k if way == 0 else g.a + k
    col = lambda way, k: g.b - k if way == 0 else g.b + k
    rows = [(0, 0)] + [(way, k) for k in range(1, A) for way in (0, 1)]

    def along_a(way, k, src, do):
        if k < A - 1:
            there, device = g.next("a", way)
            i = g.at(row(way, k), g.b)

            @pl.when(there)
            def _():
                do(remote(src, out.at[i], send_a.at[way, k], recv_a.at[way, k + 1], device))

    def along_b(way, j, a, i, src, do):
        if j < B - 1:
            there, device = g.next("b", way)

            @pl.when(there)
            def _():
                do(remote(src, out.at[i], send_b.at[way, a, j], recv_b.at[way, a, j + 1], device))

    def from_b(way, k, j):
        for w in (0, 1):
            i = g.at(row(way, k), col(w, j))

            @pl.when(g.behind("a", way, k) & g.behind("b", w, j))
            def _():
                a = row(way, k)
                remote(out.at[i], out.at[i], send_b.at[w, a, j], recv_b.at[w, a, j], g.here()).wait_recv()
                along_b(w, j, a, i, out.at[i], start)
                arrived(i, out.at[i])

    def start(copy):
        copy.start()

    def sent(copy):
        copy.wait_send()

    if not started:
        for way in (0, 1):
            along_a(way, 0, own, start)
        for way in (0, 1):
            along_b(way, 0, g.a, g.me, own, start)
        arrived(g.me, own)
    yield
    if near_first:
        for j in range(1, B):
            from_b(0, 0, j)
        yield
    for k in range(1, A):
        for way in (0, 1):
            i = g.at(row(way, k), g.b)

            @pl.when(g.behind("a", way, k))
            def _():
                remote(out.at[i], out.at[i], send_a.at[way, k], recv_a.at[way, k], g.here()).wait_recv()
                along_a(way, k, out.at[i], start)
                for w in (0, 1):
                    along_b(w, 0, row(way, k), i, out.at[i], start)
                arrived(i, out.at[i])

            yield
    for j in range(1, B):
        for way, k in rows[1:] if near_first else rows:
            from_b(way, k, j)
            yield
    for way, k in rows:
        for w in (0, 1) if k == 0 else (way,):

            @pl.when(g.behind("a", w, k))
            def _():
                along_a(w, k, own, sent)

        @pl.when(g.behind("a", way, k))
        def _():
            for w in (0, 1):
                for j in range(B - 1):

                    @pl.when(g.behind("b", w, j))
                    def _():
                        along_b(w, j, row(way, k), g.me, own, sent)


def sum_slots(A, B, block, dtype=BF16):
    return [
        pltpu.VMEM((A + 1,) + block, dtype),
        pltpu.VMEM((A,) + block, dtype),
        pltpu.VMEM((A, B - 1) + block, dtype),
    ]


def across(g, part, sems, slots, a, r):
    to = (g.b + r) % g.B
    return remote(part(g.at(a, to)), slots[2].at[a, r - 1], sems[2].at[0, a, r], sems[3].at[0, a, r], g.dev(g.a, to))


def reduce(g, part, finish, sems, slots, sent=None, started=False):
    send_a, recv_a, send_b, recv_b = sems
    land_a, out_a, land_b = slots
    sent = sent or part
    A, B = g.A, g.B
    row = lambda way, k: g.a + k if way == 0 else g.a - k
    rows = [(way, k) for k in range(A - 1, 0, -1) for way in (0, 1)] + [(0, 0)]
    here = g.here()

    def landing(way, k):
        return land_a.at[A if k == 0 and way == 1 else row(way, k)]

    def along(way, k):
        to = A if k == 1 and way == 1 else row(way, k)
        return remote(
            out_a.at[row(way, k)], land_a.at[to], send_a.at[way, k], recv_a.at[way, k - 1], g.next("a", way)[1]
        )

    def landed(way, k):
        remote(landing(way, k), landing(way, k), send_a.at[way, k], recv_a.at[way, k], here).wait_recv()

    for way, k in [] if started else rows:

        @pl.when(g.ahead("a", way, k))
        def _():
            for r in range(1, B):
                across(g, sent, sems, slots, row(way, k), r).start()

    yield
    for way, k in rows:

        @pl.when(g.ahead("a", way, k))
        def _():
            a = row(way, k)
            for r in range(1, B):
                mine = land_b.at[a, r - 1]
                remote(mine, mine, send_b.at[0, a, r], recv_b.at[0, a, r], here).wait_recv()

            def near():
                total = part(g.at(a, g.b))[...].astype(F32)
                for r in range(1, B):
                    total = total + land_b[a, r - 1].astype(F32)
                return total

            if k > 0:
                if k < A - 1:

                    @pl.when(g.behind("a", way, 1))
                    def _():
                        landed(way, k)
                        out_a[a] = (near() + landing(way, k)[...].astype(F32)).astype(out_a.dtype)

                @pl.when(jnp.logical_not(g.behind("a", way, 1)))
                def _():
                    out_a[a] = near().astype(out_a.dtype)

                along(way, k).start()
            else:
                for w in (0, 1):
                    if A > 1:

                        @pl.when(g.behind("a", w, 1))
                        def _():
                            landed(w, 0)

                total = near()
                if A == 2:
                    total = total + land_a[jnp.where(g.a == 1, 1, A)].astype(F32)
                else:
                    for w in (0, 1):
                        if A > 1:
                            total = total + jnp.where(g.behind("a", w, 1), landing(w, 0)[...].astype(F32), 0.0)
                finish(total)

        yield
    for way, k in rows:

        @pl.when(g.ahead("a", way, k))
        def _():
            for r in range(1, B):
                across(g, sent, sems, slots, row(way, k), r).wait_send()
            if k > 0:
                along(way, k).wait_send()


def total_scratch(A, B, block):
    return [pltpu.VMEM(block, BF16)] + line_sems(A, B) * 2 + sum_slots(A, B, block)


def total(g, part, out, take):
    kept, sems, slots = take(), take(8), take(3)

    def finish(value):
        kept[...] = value.astype(kept.dtype)

    yield from reduce(g, part, finish, sems[:4], slots)
    out.at[g.me][...] = kept[...]
    yield from gather(g, kept, out, sems[4:])


def exchange_sems(n):
    return [pltpu.SemaphoreType.DMA((n,)), pltpu.SemaphoreType.DMA((n,))]


def pass_slices(g, out, sems):
    send, recv = sems
    n = g.A * g.B

    def copies(i, block):
        for r in range(1, n):
            to = (g.me + r) % n
            yield remote(block.at[to], out.at[g.me, i], send.at[i, r], recv.at[i, r], {g.axis: to})

    def arrived(i, block):
        for copy in copies(i, block):
            copy.start()

    def end(blocks, block):
        for i in blocks:
            for r in range(1, n):
                mine = out.at[(g.me + n - r) % n, i]
                remote(mine, mine, send.at[i, r], recv.at[i, r], g.here()).wait_recv()
            for copy in copies(i, block):
                copy.wait_send()

    return arrived, end


def exchange(g, part, out, sems):
    send, recv = sems
    n = g.A * g.B
    copies = []
    for r in range(1, n):
        to = (g.me + r) % n
        copies.append(remote(part.at[to], out.at[g.me], send.at[r], recv.at[r], {g.axis: to}))
        copies[-1].start()
    out[g.me] = part[g.me]
    yield
    for r in range(1, n):
        origin = (g.me + n - r) % n
        remote(part.at[origin], out.at[origin], send.at[r], recv.at[r], g.here()).wait_recv()
    yield
    for copy in copies:
        copy.wait_send()


VMEM = pl.BlockSpec(memory_space=pltpu.VMEM)
ANY = pl.BlockSpec(memory_space=pl.ANY)


def call(body, name, outs, ins, scratch=(), cid=None, us=10.0, **grid):
    whole = VMEM
    params = dict(vmem_limit_bytes=VMEM_MOST)
    if cid is not None:
        params |= dict(collective_id=cid, has_side_effects=True)
    return pl.pallas_call(
        body,
        out_shape=[jax.ShapeDtypeStruct(shape, dtype) for shape, dtype in outs],
        in_specs=grid.pop("in_specs", [whole] * len(ins)),
        out_specs=grid.pop("out_specs", [whole] * len(outs)),
        scratch_shapes=list(scratch),
        compiler_params=pltpu.CompilerParams(**params),
        cost_estimate=pl.CostEstimate(flops=0, transcendentals=0, bytes_accessed=int(us * 3e6)),
        name=name,
        **grid,
    )(*ins)


def taker(refs):
    refs = list(refs)

    def take(n=None):
        if n is None:
            return refs.pop(0)
        return [refs.pop(0) for _ in range(n)]

    return take


def dot(left, right, contract=((1,), (0,))):
    return lax.dot_general(left, right, (contract, ((), ())), preferred_element_type=F32)


def halves(values):
    high = values.astype(BF16)
    return high, (values - high.astype(F32)).astype(BF16)


def norm_scale(values):
    return lax.rsqrt(jnp.mean(values * values, axis=-1, keepdims=True) + NORM_EPSILON)


def norm_back(grad, normed, scale, gain):
    grad_hat = grad * gain
    return scale * (grad_hat - normed * jnp.mean(grad_hat * normed, axis=-1, keepdims=True))


def rotary(values, cosine, sine, back=False):
    width, half = values.shape[1], HEAD_DIMENSION // 2
    later = pltpu.roll(values, width - half, 1)
    earlier = pltpu.roll(values, half, 1)
    front = lax.broadcasted_iota(jnp.int32, values.shape, 1) % HEAD_DIMENSION < half
    other = jnp.where(front, -later, earlier)
    return values * cosine - other * sine if back else values * cosine + other * sine


def allowed_pairs(segment_row):
    size = segment_row.shape[1]
    across = jnp.broadcast_to(segment_row, (size, size))
    rows = lax.broadcasted_iota(jnp.int32, (size, size), 0)
    cols = lax.broadcasted_iota(jnp.int32, (size, size), 1)
    return (cols <= rows) & (across == across.T)


def attention_weights(stacked, keys, allowed):
    scores = dot(stacked, keys, ((1,), (1,))) * SCORE_SCALE
    scores = jnp.where(allowed, scores, MASKED_SCORE)
    row_max = jnp.max(scores, axis=-1, keepdims=True)
    log_total = row_max + jnp.log(jnp.sum(jnp.exp(scores - row_max), axis=-1, keepdims=True))
    return jnp.exp(scores - log_total)


class Heads:
    def __init__(self, ranks):
        self.q, self.kv = QUERY_HEADS // ranks, KEY_VALUE_HEADS // ranks
        self.group = QUERY_HEADS // KEY_VALUE_HEADS
        self.q_cols, self.kv_cols = self.q * HEAD_DIMENSION, self.kv * HEAD_DIMENSION
        self.cols = -(-(self.q_cols + 2 * self.kv_cols) // 128) * 128

    def stack(self, rows, kv):
        first = kv * self.group
        return jnp.concatenate([self.head(rows, first + i) for i in range(self.group)], axis=0)

    def head(self, rows, i):
        return rows[:, i * HEAD_DIMENSION : (i + 1) * HEAD_DIMENSION]

    def key(self, rows, kv):
        return self.head(rows, self.q + kv)

    def value(self, rows, kv):
        return self.head(rows, self.q + self.kv + kv)


def rope_tables(length, heads):
    frequency = np.float32(ROPE_BASE) ** (-(np.arange(HEAD_DIMENSION // 2, dtype=np.float32) * 2.0) / HEAD_DIMENSION)
    angles = np.arange(length, dtype=np.float32)[:, None] * frequency.astype(np.float32)[None, :]
    cosine, sine = (np.tile(f(angles.astype(np.float64)).astype(np.float32), (1, 2)) for f in (np.cos, np.sin))
    turned = heads.q + heads.kv
    rest = heads.cols - turned * HEAD_DIMENSION
    cosine = np.concatenate([np.tile(cosine, (1, turned)), np.ones((length, rest), np.float32)], axis=1)
    sine = np.concatenate([np.tile(sine, (1, turned)), np.zeros((length, rest), np.float32)], axis=1)
    return cosine, sine


def gain_row(misc_ref, ranks, which):
    return jnp.concatenate([misc_ref[i, which : which + 1, :] for i in range(ranks)], axis=1)


def attention_forward(ranks, heads, length, b, x_ref, w_ref, o_ref, misc_ref, cos_ref, sin_ref, part_ref, qkv_ref, att_ref, scale_ref):
    width = x_ref.shape[2]
    x = x_ref[b].astype(F32)
    scale = norm_scale(x)
    scale_ref[b] = jnp.broadcast_to(scale, (length, 128))
    normed = (x * scale * gain_row(misc_ref, ranks, 0)).astype(BF16)
    qkv_ref[b] = rotary(dot(normed, w_ref[...].reshape(width, heads.cols)), cos_ref[...], sin_ref[...]).astype(BF16)
    qkv = qkv_ref[b]
    allowed = allowed_pairs(misc_ref[b, 8:9, :length])
    allowed = jnp.concatenate([allowed] * heads.group, axis=0)
    outs = []
    for kv in range(heads.kv):
        probs = attention_weights(heads.stack(qkv, kv), heads.key(qkv, kv), allowed).astype(BF16)
        mixed = dot(probs, heads.value(qkv, kv)).astype(BF16)
        outs += [mixed[i * length : (i + 1) * length] for i in range(heads.group)]
    att_ref[b] = jnp.concatenate(outs, axis=1)
    part_ref[b] = dot(att_ref[b], o_ref[...]).astype(BF16)


def column_experts(n_expert, slots, axis):
    column = lax.broadcasted_iota(jnp.int32, (1, 128) if axis else (128, 1), axis)
    owner, slot = column // SLOT_STRIDE, column % SLOT_STRIDE
    expert = slot * n_expert + owner
    real = (owner < n_expert) & (slot < slots) & (expert < EXPERT_COUNT)
    return real, jnp.where(real, expert, -1)


def column_picks(n_expert, slots):
    _, expert = column_experts(n_expert, slots, 1)
    return jnp.where(lax.broadcasted_iota(jnp.int32, (EXPERT_COUNT, 128), 0) == expert, 1.0, 0.0)


def route_tables(n_expert, slots, routes, blocks_ref):
    tokens = routes.shape[1]
    _, expert = column_experts(n_expert, slots, 0)
    named = jnp.zeros((128, tokens), F32)
    for k in range(routes.shape[0]):
        named = named + jnp.where(routes[k : k + 1, :] == expert, 1.0, 0.0)
    limit = jnp.zeros((128, 1), jnp.int32)
    for e in range(EXPERT_COUNT):
        limit = jnp.where(expert == e, blocks_ref[e] * BLK, limit)
    rows = lax.broadcasted_iota(jnp.int32, (tokens, tokens), 0)
    cols = lax.broadcasted_iota(jnp.int32, (tokens, tokens), 1)
    earlier = jnp.where(rows < cols, 1.0, 0.0).astype(BF16)
    rank = dot(named.astype(BF16), earlier)
    kept = (named > 0.0) & (rank < limit.astype(F32))
    return kept, jnp.where(kept, rank, -1.0)


def route_forward(ranks, n_expert, slots, x_ref, branch_ref, misc_ref, router_ref, routes_ref, blocks_ref, hidden_ref, norm_ref, scale_ref, probs_ref, meta_ref, table_ref):
    gain = gain_row(misc_ref, ranks, 1)
    width = x_ref.shape[1]
    shard = width // ranks
    hidden = x_ref[...].astype(F32) + RESIDUAL_SCALE * branch_ref[...]
    hidden_ref[...] = hidden
    scale = norm_scale(hidden)
    scale_ref[...] = jnp.broadcast_to(scale, scale_ref.shape)
    norm = (hidden * scale * gain).astype(BF16)
    picks = column_picks(n_expert, slots).astype(BF16)
    for i in range(ranks):
        here = slice(i * shard, (i + 1) * shard)
        norm_ref[i] = norm[:, here]
        table_ref[here, :] = dot(router_ref[i], picks, ((0,), (0,))).astype(BF16)
    kept, place = route_tables(n_expert, slots, routes_ref[...], blocks_ref)
    real, _ = column_experts(n_expert, slots, 1)
    logits = jnp.where(real, dot(norm, table_ref[...]), MASKED_SCORE)
    weight = jnp.exp(logits - jnp.max(logits, axis=-1, keepdims=True))
    probs = weight / jnp.sum(weight, axis=-1, keepdims=True)
    probs_ref[...] = probs
    used = n_expert * SLOT_STRIDE
    meta_ref[0] = place[:used]
    meta_ref[1] = jnp.where(kept, probs.T, 0.0)[:used]


def row_picks(slots, place):
    number = lax.broadcasted_iota(jnp.int32, (SLOT_ROWS, place.shape[1]), 0).astype(F32)
    return jnp.concatenate([jnp.where(number == place[s : s + 1], 1.0, 0.0) for s in range(slots)], axis=0)


def row_shares(slots, share):
    return jnp.concatenate(
        [jnp.broadcast_to(share[s : s + 1], (SLOT_ROWS, share.shape[1])) for s in range(slots)], axis=0
    )


def pick_rows(slots, n_expert, mine, meta_ref, block, to_sc):
    def one(q, carry):
        pick = row_picks(slots, meta_ref[q, 0, mine, :]).astype(BF16)
        ranks, _, shard = block(q).shape
        for i in range(ranks):
            to_sc[q, :, i * shard : (i + 1) * shard] = dot(pick, block(q)[i]).astype(BF16)
        return carry

    lax.fori_loop(0, n_expert, one, 0)


def expert_slot(n_expert, tokens, s, mine, meta_ref, up_ref, down_ref, gate_grad_ref, inner_ring, both_ring, x_sc, og_sc):
    width = x_sc.shape[2]
    hidden = down_ref.shape[0]
    place_of = pl.ds(pl.multiple_of(s * SLOT_ROWS, SLOT_ROWS), SLOT_ROWS)
    slot_row = lax.broadcasted_iota(jnp.int32, (SLOT_STRIDE, tokens), 0) == s
    number = lax.broadcasted_iota(jnp.int32, (SLOT_ROWS, tokens), 0).astype(F32)
    rows = n_expert * SLOT_ROWS
    both = dot(x_sc[:, place_of, :].reshape(rows, width), up_ref[...])
    gate, up = both[:, :hidden], both[:, hidden:]
    squash = jax.nn.sigmoid(gate)
    inner = (gate * squash * up).astype(BF16)
    inner_ring.free(s)[...] = inner
    inner_ring.copy(s).start()
    produced = dot(inner, down_ref[...]).astype(BF16)
    masks, gates = [], []
    for q in range(n_expert):
        place = jnp.sum(jnp.where(slot_row, meta_ref[q, 0, mine, :], 0.0), axis=0, keepdims=True)
        share = jnp.sum(jnp.where(slot_row, meta_ref[q, 1, mine, :], 0.0), axis=0, keepdims=True)
        masks.append(number == place)
        gates.append(jnp.sum(jnp.where(masks[q], share, 0.0), axis=1, keepdims=True))
    mix_grad = RESIDUAL_SCALE * og_sc[:, place_of, :].reshape(rows, width).astype(F32)
    grad_rows = (jnp.concatenate(gates, axis=0) * mix_grad).astype(BF16)
    gate_grad = jnp.sum(mix_grad * produced.astype(F32), axis=1, keepdims=True)
    og_sc[:, place_of, :] = produced.reshape(n_expert, SLOT_ROWS, width)
    for q in range(n_expert):
        spread = jnp.where(masks[q], gate_grad[q * SLOT_ROWS : (q + 1) * SLOT_ROWS], 0.0)
        gate_grad_ref[q] = jnp.where(slot_row, jnp.sum(spread, axis=0, keepdims=True), gate_grad_ref[q])
    grad_inner = dot(grad_rows, down_ref[...], ((1,), (1,)))
    grad_both = jnp.concatenate(
        [grad_inner * up * squash * (1.0 + gate * (1.0 - squash)), grad_inner * (gate * squash)], axis=1
    ).astype(BF16)
    both_ring.free(s)[...] = grad_both
    both_ring.copy(s).start()
    x_sc[:, place_of, :] = dot(grad_both, up_ref[...], ((1,), (1,))).astype(BF16).reshape(n_expert, SLOT_ROWS, width)


def sum_rows_back(slots, n_expert, mine, meta_ref, out_ring, back_ring, eo_sc, gx_sc):
    def one(q, carry):
        pick = row_picks(slots, meta_ref[q, 0, mine, :])
        high, low = halves(pick * row_shares(slots, meta_ref[q, 1, mine, :]))
        over = ((0,), (0,))
        back_ring.free(q)[...] = dot(pick.astype(BF16), gx_sc[q], over).astype(BF16)
        back_ring.copy(q).start()
        out_ring.free(q)[...] = (dot(high, eo_sc[q], over) + dot(low, eo_sc[q], over)).astype(BF16)
        out_ring.copy(q).start()
        return carry

    lax.fori_loop(0, n_expert, one, 0)


def route_backward(ranks, n_expert, shard, hidden_ref, norm_ref, scale_ref, probs_ref, misc_ref, router_ref, og_ref, back_ref, gate_grad_ref, grad_hidden_ref, branch_ref, small_ref):
    tokens, width = hidden_ref.shape
    gain = gain_row(misc_ref, ranks, 1)
    hidden = hidden_ref[...]
    used = n_expert * SLOT_STRIDE
    spread = gate_grad_ref[...].reshape(used, tokens)
    if used < 128:
        spread = jnp.concatenate([spread, jnp.zeros((128 - used, tokens), F32)], axis=0)
    grad_probs = spread.T
    probs = probs_ref[...]
    grad_logits = probs * (grad_probs - jnp.sum(probs * grad_probs, axis=1, keepdims=True))
    high, low = halves(grad_logits)
    router = router_ref[...]
    across = ((1,), (1,))
    grad_norm = back_ref[...] + (dot(high, router, across) + dot(low, router, across))
    scale = scale_ref[:, 0:1]
    normed = hidden * scale
    grad_hidden = og_ref[...].astype(F32) + norm_back(grad_norm, normed, scale, gain)
    grad_hidden_ref[...] = grad_hidden
    branch_ref[...] = (RESIDUAL_SCALE * grad_hidden).astype(BF16)
    over = ((0,), (0,))
    grad_gain = jnp.sum(grad_norm * normed, axis=0, keepdims=True)
    for i in range(ranks):
        here = slice(i * shard, (i + 1) * shard)
        grad_router = dot(high, norm_ref[i], over) + dot(low, norm_ref[i], over)
        small_ref[i, :used, :] = grad_router[:used].astype(BF16)
        small_ref[i, used:, :] = jnp.broadcast_to(grad_gain[:, here], (16, shard)).astype(BF16)


def store_blocks(ref, cols, values):
    count, rows = ref.shape[0], ref.shape[1]
    for i in range(count):
        ref[i, :, cols] = values[i * rows : (i + 1) * rows]


def attention_backward(heads, length, b, branch_ref, att_ref, qkv_ref, o_ref, misc_ref, cos_ref, sin_ref, grad_ref):
    grad_att = dot(branch_ref[b], o_ref[...], ((1,), (1,))).astype(BF16)
    att, qkv = att_ref[b], qkv_ref[b]
    allowed = allowed_pairs(misc_ref[b, 8:9, :length])
    allowed = jnp.concatenate([allowed] * heads.group, axis=0)
    d_q, d_k, d_v = [], [], []
    for kv in range(heads.kv):
        queries, keys = heads.stack(qkv, kv), heads.key(qkv, kv)
        soft = attention_weights(queries, keys, allowed)
        grads = heads.stack(grad_att, kv)
        d_v.append(dot(soft.astype(BF16), grads, ((0,), (0,))))
        delta = jnp.sum(grads.astype(F32) * heads.stack(att, kv).astype(F32), axis=1, keepdims=True)
        inner = dot(grads, heads.value(qkv, kv), ((1,), (1,)))
        d_scores = (soft * (inner - delta) * SCORE_SCALE).astype(BF16)
        rows = dot(d_scores, keys)
        d_q += [rows[i * length : (i + 1) * length] for i in range(heads.group)]
        d_k.append(dot(d_scores, queries, ((0,), (0,))))
    spare = heads.cols - heads.q_cols - 2 * heads.kv_cols
    fill = [jnp.zeros((length, spare), F32)] if spare else []
    grads = jnp.concatenate(d_q + d_k + d_v + fill, axis=1)
    grad_ref[b] = rotary(grads, cos_ref[...], sin_ref[...], back=True).astype(BF16)


def output_weight_backward(heads, branch_ref, att_ref, d_o_ref):
    branch = branch_ref[...].reshape(-1, branch_ref.shape[-1])
    store_blocks(d_o_ref, slice(None), dot(att_ref[...].reshape(-1, heads.q_cols), branch, ((0,), (0,))).astype(BF16))


def projection_products(ranks, heads, x_ref, scale_ref, gain_ref, grad_ref, d_w_ref, done):
    norm_input = (x_ref[...].astype(F32) * scale_ref[:, 0:1] * gain_ref[0:1, :]).astype(BF16)
    for i in range(ranks):
        grads = grad_ref[i].reshape(-1, heads.cols)
        store_blocks(d_w_ref, slice(i * heads.cols, (i + 1) * heads.cols), dot(norm_input, grads, ((0,), (0,))).astype(BF16))
        done(i)


def projection_backward(ranks, heads, shard, x_ref, scale_ref, grad_ref, w_ref, small_ref, grad_x_ref, sums_ref):
    normed = x_ref[...].astype(F32) * scale_ref[:, 0:1]
    total = None
    for i in range(ranks):
        term = dot(grad_ref[i].reshape(-1, heads.cols), w_ref[i], ((1,), (1,)))
        total = term if total is None else total + term
    grad_x_ref[...] = total.reshape(grad_x_ref.shape)
    small = small_ref[0].astype(F32)
    for i in range(1, ranks):
        small = small + small_ref[i].astype(F32)
    gain_grad = jnp.sum(total * normed, axis=0, keepdims=True)
    used = small.shape[0] - 16
    sums_ref[...] = jnp.zeros_like(sums_ref)
    sums_ref[:used, :] = small[:used].astype(BF16)
    second = lax.broadcasted_iota(jnp.int32, (16, shard), 0)
    sums_ref[used : used + 16, :] = jnp.where(second == 0, small[used:], jnp.where(second == 1, gain_grad, 0.0)).astype(BF16)


def group_rows(n_expert, slots, at, x, og, meta_ref, x_rows, og_rows):
    def one(q, carry):
        pick = row_picks(slots, meta_ref[at, q, 0])
        share = jnp.sum(pick * row_shares(slots, meta_ref[at, q, 1]), axis=1, keepdims=True)
        pick = pick.astype(BF16)
        x_rows[q] = dot(pick, x[q]).astype(BF16)
        og_rows[q] = (share * (RESIDUAL_SCALE * dot(pick, og[q]))).astype(BF16)
        return carry

    lax.fori_loop(0, n_expert, one, 0)


def finish(ranks, n_expert, slots, heads, tokens, x_rows_ref, og_rows_ref, both_ref, inner_ref, grad_ref, x_ref, misc_ref, grad_hidden_ref, hidden_ref, mixture_ref, d_w_ref, d_o_ref, sums_ref, d_up_ref, d_down_ref, output_ref, grad_inputs_ref, q_ref, k_ref, v_ref, o_ref, router_ref, gain_one_ref, gain_two_ref):
    step = pl.program_id(0)

    @pl.when(step == 0)
    def _():
        output_ref[...] = (hidden_ref[...] + RESIDUAL_SCALE * mixture_ref[...]).astype(BF16)
        gain = gain_row(misc_ref, ranks, 0)
        grad = jnp.concatenate([grad_ref[i] for i in range(ranks)], axis=1)
        x = x_ref[...].astype(F32)
        scale = norm_scale(x)
        grad_inputs_ref[...] = grad_hidden_ref[...] + norm_back(grad, x * scale, scale, gain)
        used = n_expert * SLOT_STRIDE
        router_ref[...] = dot(column_picks(n_expert, slots).astype(BF16), sums_ref[:128])
        ends = sums_ref[used : used + 16, :].astype(F32)
        gain_two_ref[...] = ends[0]
        gain_one_ref[...] = ends[1]
        o_ref[...] = d_o_ref[...].astype(F32)
        first, second = heads.q_cols, heads.q_cols + heads.kv_cols
        for i in range(ranks):
            start = i * heads.cols
            q_ref[:, i * heads.q_cols : (i + 1) * heads.q_cols] = d_w_ref[:, start : start + first].astype(F32)
            here = slice(i * heads.kv_cols, (i + 1) * heads.kv_cols)
            k_ref[:, here] = d_w_ref[:, start + first : start + second].astype(F32)
            v_ref[:, here] = d_w_ref[:, start + second : start + second + heads.kv_cols].astype(F32)

    flat = lambda value: value.reshape(-1, value.shape[-1])
    over = ((0,), (0,))
    d_up_ref[0] = dot(flat(x_rows_ref[...]), flat(both_ref[...]), over)
    d_down_ref[0] = dot(flat(inner_ref[...]), flat(og_rows_ref[...]), over)


def on_device(
    inputs,
    segment_ids,
    routes,
    expert_blocks,
    norm1_gain,
    q_weight,
    k_weight,
    value_matrix,
    o_weight,
    norm2_gain,
    router_weight,
    expert_gate_up,
    expert_down,
    out_grad,
):
    ranks, n_expert = lax.axis_size("dp"), lax.axis_size("expert")
    tokens, width = inputs.shape
    shard = q_weight.shape[0]
    slots, _, double = expert_gate_up.shape
    hidden = expert_down.shape[1]
    heads = Heads(ranks)
    group = ("dp", ranks // 2, 2)
    plane = ("expert", 4, n_expert // 4)
    used = n_expert * SLOT_STRIDE
    cosine, sine = rope_tables(tokens, heads)

    gains = jnp.stack([norm1_gain, norm2_gain]).astype(F32)
    dma = pltpu.SemaphoreType.DMA

    def forward(*refs):
        take = taker(refs)
        x, wq, wk, wv, rt, gn, sg, og, wo, cs, sn, routes_ref, blocks_ref = take(13)
        w, ms_all, og_all, qkv, att, scale_one, xc, hidden_ref, norm, scale_two, probs, meta, table = take(13)
        x_all, w_all, rt_all, ms, og_own, part, branch, own_sem = take(8)
        dp, ex = Grid(*group), Grid(*plane)
        for i in range(ranks):
            at = 0
            for ref, cols in ((wq, heads.q_cols), (wk, heads.kv_cols), (wv, heads.kv_cols)):
                w[i, :, at : at + cols] = ref[:, i * cols : (i + 1) * cols]
                at += cols
            if at < heads.cols:
                w[i, :, at:] = jnp.zeros((shard, heads.cols - at), BF16)
            og_own[i] = og[:, i * shard : (i + 1) * shard]
        ms[...] = jnp.zeros_like(ms)
        ms[0:2, :] = gn[...]
        ms[8:9, :tokens] = sg[...].astype(F32)
        x_all[dp.me] = x[...]
        rt_all[dp.me] = rt[...]
        ms_all[dp.me] = ms[...]
        greet(dp.all() + ex.near())
        keep = pltpu.make_async_copy(og_own, og_all.at[ex.me], own_sem)
        keep.start()
        small = [begin(gather(dp, ms, ms_all, take(4))), begin(gather(dp, rt, rt_all, take(4)))]
        xs = begin(gather(dp, x, x_all, take(4)))
        ws = begin(exchange(dp, w, w_all, take(2)))
        ogs = begin(gather(ex, og_own, og_all, take(4)))
        run(*small, xs)
        for i in range(ranks):

            @pl.when(dp.me == i)
            def _():
                for b in range(ranks):
                    xc[b * tokens : (b + 1) * tokens, :] = x_all[b, :, i * shard : (i + 1) * shard]

        advance(ogs, 2 * (plane[1] - 1))
        run(ws)

        def store(total):
            branch[...] = total

        dp_sems, dp_slots = take(4), take(3)
        sums = begin(reduce(dp, lambda i: part.at[i], store, dp_sems, dp_slots, started=True))

        def one(t, carry):
            a, r = (dp.a + 1 + t // 2) % dp.A, 1 + t % 2

            @pl.when(t == 2 * (dp.A - 1))
            def _():
                advance(sums, 2 * (dp.A - 1))

            b = dp.at(a, (dp.b + r) % 2)
            attention_forward(ranks, heads, tokens, b, x_all, w_all, wo, ms_all, cs, sn, part, qkv, att, scale_one)

            @pl.when(r < 2)
            def _():
                across(dp, lambda i: part.at[i], dp_sems, dp_slots, a, 1).start()

            return carry

        lax.fori_loop(0, ranks, one, 0)
        run(sums)
        route_forward(ranks, n_expert, slots, x, branch, ms_all, rt_all, routes_ref, blocks_ref, hidden_ref, norm, scale_two, probs, meta, table)
        run(ogs)
        keep.wait()

    (
        weights,
        misc_all,
        og_all,
        qkv,
        att,
        scale_one,
        x_cols,
        hidden_rows,
        norm_hidden,
        scale_two,
        probs,
        meta,
        router,
    ) = call(
        forward,
        "forward",
        [
            ((ranks, shard, heads.cols), BF16),
            ((ranks, 16, shard), F32),
            ((n_expert, ranks, tokens, shard), BF16),
            ((ranks, tokens, heads.cols), BF16),
            ((ranks, tokens, heads.q_cols), BF16),
            ((ranks, tokens, 128), F32),
            ((ranks * tokens, shard), BF16),
            ((tokens, width), F32),
            ((ranks, tokens, shard), BF16),
            ((tokens, 128), F32),
            ((tokens, 128), F32),
            ((2, used, tokens), F32),
            ((width, 128), BF16),
        ],
        (
            inputs,
            q_weight,
            k_weight,
            value_matrix,
            router_weight.T,
            gains,
            segment_ids,
            out_grad,
            o_weight,
            cosine,
            sine,
            routes.T,
            expert_blocks,
        ),
        [
            pltpu.VMEM((ranks, tokens, width), BF16),
            pltpu.VMEM((ranks, shard, heads.cols), BF16),
            pltpu.VMEM((ranks, router_weight.shape[1], shard), BF16),
            pltpu.VMEM((16, shard), F32),
            pltpu.VMEM((ranks, tokens, shard), BF16),
            pltpu.VMEM((ranks, tokens, width), BF16),
            pltpu.VMEM((tokens, width), F32),
            dma(()),
        ]
        + line_sems(*group[1:]) * 3
        + exchange_sems(ranks)
        + line_sems(*plane[1:])
        + line_sems(*group[1:])
        + sum_slots(*group[1:], (tokens, width)),
        cid=0,
        us=60,
        in_specs=[VMEM] * 12 + [pl.BlockSpec(memory_space=pltpu.SMEM)],
        out_specs=[VMEM] * 2 + [ANY] + [VMEM] * 10,
    )

    fixed = lambda shape: pl.BlockSpec(shape, lambda s: (0,) * len(shape), pipeline_mode=pl.Buffered(1))
    moving = lambda shape: pl.BlockSpec((1,) + shape, lambda s: (s,) + (0,) * len(shape))
    rows = n_expert * SLOT_ROWS
    deep = 2 if ranks * rows <= 1024 else 1

    def mixture_of_experts(*refs):
        take = taker(refs)
        nh, mt, og, up, down = take(5)
        gg, mt_group, out_part, back_part, inr, gb, xd, ogd = take(8)
        nh_all, mt_all, mt_own, x_sc, og_sc, og_in, up_in, down_in = take(8)
        stages, ring_sems, og_sems, up_sems, own_sems = take(4), take(), take(), take(), take()
        dp, ex = Grid(*group), Grid(*plane)
        out_ring, back_ring, inner_ring, both_ring = (
            Ring(stage, out, ring_sems.at[i])
            for i, (stage, out) in enumerate(zip(stages, (out_part, back_part, inr.at[dp.me], gb.at[dp.me])))
        )
        mine = pl.ds(pl.multiple_of(ex.me * SLOT_STRIDE, SLOT_STRIDE), SLOT_STRIDE)
        nh_all[ex.me] = nh[...]
        mt_all[ex.me] = mt[...]
        gg[...] = jnp.zeros_like(gg)

        def fetch(s, do):
            do(pltpu.make_async_copy(up.at[s], up_in.at[s % deep], up_sems.at[0, s % deep]))
            do(pltpu.make_async_copy(down.at[s], down_in.at[s % deep], up_sems.at[1, s % deep]))

        for s in range(deep):
            fetch(s, lambda copy: copy.start())
        greet(dp.all() + ex.near())
        mts = begin(gather(ex, mt, mt_all, take(4)))
        og_passed, og_end = pass_slices(dp, ogd, take(2))
        for i in range(n_expert):
            og_passed(i, og.at[i])
        passed, end = pass_slices(dp, xd, take(2))

        def keep(i, block):
            return pltpu.make_async_copy(block.at[dp.me], xd.at[dp.me, i], own_sems.at[i])

        def arrived(i, block):
            passed(i, block)
            keep(i, block).start()

        nhs = begin(gather(ex, nh, nh_all, take(4), arrived))
        run(mts)

        def fetch_og(q):
            return pltpu.make_async_copy(og.at[q], og_in.at[q % 2], og_sems.at[q % 2])

        fetch_og(0).start()

        def pick_og(q, carry):
            @pl.when(q + 1 < n_expert)
            def _():
                fetch_og(q + 1).start()

            fetch_og(q).wait()
            pick = row_picks(slots, mt_all[q, 0, mine, :]).astype(BF16)
            for i in range(ranks):
                og_sc[q, :, i * shard : (i + 1) * shard] = dot(pick, og_in[q % 2, i]).astype(BF16)
            return carry

        lax.fori_loop(0, n_expert, pick_og, 0)
        mt_own[...] = mt_all[:, :, mine, :]
        mt_group[dp.me] = mt_own[...]
        mgs = begin(gather(dp, mt_own, mt_group, take(4)))
        run(nhs)
        pick_rows(slots, n_expert, mine, mt_all, lambda q: nh_all.at[q], x_sc)

        def one(s, carry):
            fetch(s, lambda copy: copy.wait())
            expert_slot(
                n_expert, tokens, s, mine, mt_all, up_in.at[s % deep], down_in.at[s % deep], gg, inner_ring, both_ring, x_sc, og_sc
            )

            @pl.when(s + deep < slots)
            def _():
                fetch(s + deep, lambda copy: copy.start())

            return carry

        lax.fori_loop(0, slots, one, 0)
        run(mgs)
        sum_rows_back(slots, n_expert, mine, mt_all, out_ring, back_ring, og_sc, x_sc)
        inner_ring.end(slots)
        both_ring.end(slots)
        out_ring.end(n_expert)
        back_ring.end(n_expert)
        end(range(n_expert), nh)
        for i in range(n_expert):
            keep(i, nh).wait()
        og_end(range(n_expert), og.at[0])

    gate_grad, meta_group, out_part, back_part, inner, grad_both, norm_slices, og_slices = call(
        mixture_of_experts,
        "mixture_of_experts",
        [
            ((n_expert, SLOT_STRIDE, tokens), F32),
            ((ranks, n_expert, 2, SLOT_STRIDE, tokens), F32),
            ((n_expert, tokens, width), BF16),
            ((n_expert, tokens, width), BF16),
            ((ranks, slots, rows, hidden), BF16),
            ((ranks, slots, rows, double), BF16),
            ((ranks, n_expert, tokens, shard), BF16),
            ((ranks, n_expert, tokens, shard), BF16),
        ],
        (norm_hidden, meta, og_all, expert_gate_up, expert_down),
        [
            pltpu.VMEM((n_expert, ranks, tokens, shard), BF16),
            pltpu.VMEM((n_expert, 2, used, tokens), F32),
            pltpu.VMEM((n_expert, 2, SLOT_STRIDE, tokens), F32),
            pltpu.VMEM((n_expert, slots * SLOT_ROWS, width), BF16),
            pltpu.VMEM((n_expert, slots * SLOT_ROWS, width), BF16),
            pltpu.VMEM((2, ranks, tokens, shard), BF16),
            pltpu.VMEM((deep, width, double), BF16),
            pltpu.VMEM((deep, hidden, width), BF16),
            pltpu.VMEM((2, tokens, width), BF16),
            pltpu.VMEM((2, tokens, width), BF16),
            pltpu.VMEM((2, rows, hidden), BF16),
            pltpu.VMEM((2, rows, double), BF16),
            dma((4, 2)),
            dma((2,)),
            dma((2, deep)),
            dma((n_expert,)),
        ]
        + line_sems(*plane[1:])
        + [dma((n_expert, ranks))] * 4
        + line_sems(*plane[1:])
        + line_sems(*group[1:]),
        cid=1,
        us=75,
        in_specs=[VMEM] * 2 + [ANY] * 3,
        out_specs=[VMEM] * 2 + [ANY] * 6,
    )

    sum_rows = 16 * n_expert
    part_rows = shard // n_expert
    o_block, w_block, s_block = (part_rows, width), (part_rows, ranks * heads.cols), (16, shard)

    half = ranks * heads.cols // 2
    summed = lambda block: total_scratch(*plane[1:], block)

    lead = max(slots // 5, 1)

    def backward(*refs):
        take = taker(refs)
        hid, nh, sc2, pb, ms, tb, og_mine, gg, cs, sn, sc, gn, mt = take(13)
        brought, (og, xd, ogd, _, _, terms, back_terms) = take(5), take(7)
        grad_hidden_ref, mix, gx_all, do_all, dw_all, su_all, x_rows, og_rows, gb_all, inr_all = take(10)
        places, bring_sems = take(5), take()
        wo, qkv, at, xc, w = places
        out_in, back_in, term_sems = take(3)
        gg_all, sm, br_all, sm_all, gr_all, do, dw, su, gx, x_in, og_in, x_out, og_out, in_sems, out_sems = take(15)
        dp, ex = Grid(*group), Grid(*plane)
        brings = [pltpu.make_async_copy(*pair, bring_sems.at[i]) for i, pair in enumerate(zip(brought, places))]
        holds = [
            pltpu.make_async_copy(back_terms, back_in, term_sems.at[0]),
            pltpu.make_async_copy(terms, out_in, term_sems.at[1]),
        ]

        def fetch(j, do_):
            p, slot = (dp.me + j) % ranks, j % deep
            do_(pltpu.make_async_copy(xd.at[p], x_in.at[slot], in_sems.at[0, slot]))
            do_(pltpu.make_async_copy(og.at[:, dp.me] if j == 0 else ogd.at[p], og_in.at[slot], in_sems.at[1, slot]))

        for copy in holds + brings:
            copy.start()
        for j in range(deep):
            fetch(j, lambda copy: copy.start())
        greet(dp.all() + ex.all())

        def token_sum(to, kept, sent):
            def store(value):
                to[...] = value

            return begin(reduce(ex, lambda i: kept.at[i], store, take(4), take(3), lambda i: sent.at[i]))

        ggs = begin(exchange(ex, gg, gg_all, take(2)))
        backs = token_sum(grad_hidden_ref, back_in, back_terms)
        outs = token_sum(mix, out_in, terms)
        inrs = begin(gather(dp, inr_all.at[dp.me], inr_all, take(4)))
        share = lambda start, count: begin(
            gather(dp, gb_all.at[dp.me, pl.ds(start, count)], Part(gb_all, pl.ds(start, count)), take(4))
        )
        gbs = [share(0, lead)]
        for copy in holds:
            copy.wait()

        def out_copies(j):
            p, slot = (dp.me + j) % ranks, j % deep
            return [
                pltpu.make_async_copy(x_out.at[slot], x_rows.at[p], out_sems.at[0, slot]),
                pltpu.make_async_copy(og_out.at[slot], og_rows.at[p], out_sems.at[1, slot]),
            ]

        def build(j):
            fetch(j, lambda copy: copy.wait())
            if j >= deep:
                for copy in out_copies(j - deep):
                    copy.wait()
            p, slot = (dp.me + j) % ranks, j % deep
            group_rows(n_expert, slots, p, x_in.at[slot], og_in.at[slot], mt, x_out.at[slot], og_out.at[slot])
            for copy in out_copies(j):
                copy.start()
            if j + deep < ranks:
                fetch(j + deep, lambda copy: copy.start())

        for j in range(ranks):
            build(j)
            if j < 2 * (plane[1] - 1):
                advance(backs, 1)
        for j in range(ranks - deep, ranks):
            for copy in out_copies(j):
                copy.wait()
        run(backs)
        run(ggs)
        route_backward(ranks, n_expert, shard, hid, nh, sc2, pb, ms, tb, og_mine, grad_hidden_ref, gg_all, grad_hidden_ref, br_all.at[dp.me], sm)
        brs = begin(gather(dp, br_all.at[dp.me], br_all, take(4), near_first=True))
        sms = begin(exchange(dp, sm, sm_all, take(2)))
        for copy in brings:
            copy.wait()
        advance(outs, 2)
        gr_sems = take(4)
        share_gr = lambda p, started: gather(
            dp, gr_all.at[dp.me, p], Part(gr_all, p), [sems.at[p] for sems in gr_sems], started=started
        )

        def one(t, carry):
            @pl.when(t == 1)
            def _():
                advance(brs, 1)

            @pl.when(t == 2)
            def _():
                run(brs)

            p = dp.at((dp.a + t // 2) % dp.A, (dp.b + t % 2) % 2)
            attention_backward(heads, tokens, p, br_all, at, qkv, wo, ms, cs, sn, gr_all.at[dp.me])
            begin(share_gr(p, False))
            return carry

        lax.fori_loop(0, ranks, one, 0)
        output_weight_backward(heads, br_all, at, do)
        dos = begin(total(ex, lambda i: do.at[i], do_all, take))
        advance(outs, 2)
        run(sms)
        advance(dos, 2)
        run(*[share_gr(p, True) for p in range(ranks)])
        gbs.append(share(lead, slots - lead))
        dws = []

        def done(i):
            if (i + 1) % (ranks // 2) == 0:
                cols = pl.ds(len(dws) * half, half)
                part = Part(dw, slice(None), cols)
                dws.append(begin(total(ex, part.__getitem__, Part(dw_all, slice(None), cols), take)))

        projection_products(ranks, heads, xc, sc, gn, gr_all, dw, done)
        projection_backward(ranks, heads, shard, xc, sc, gr_all, w, sm_all, gx, su)
        gxs = begin(exchange(dp, gx, gx_all, take(2)))
        rows_of = lambda i: pl.ds(pl.multiple_of(i * 16, 16), 16)
        sus = begin(total(ex, lambda i: su.at[rows_of(i)], su_all, take))
        run_behind((0, dos), (0, outs), (0, dws[0]), (2, sus), (5, dws[1]))
        run(gxs)
        run(inrs, *gbs)

    row_block = (n_expert, slots * SLOT_ROWS, shard)
    grad_hidden, mixture, grad_x, d_o, d_w, sums, x_rows, og_rows, both_all, inner_all = call(
        backward,
        "backward",
        [
            ((tokens, width), F32),
            ((tokens, width), F32),
            ((ranks, tokens, shard), F32),
            ((n_expert,) + o_block, BF16),
            ((n_expert,) + w_block, BF16),
            ((n_expert,) + s_block, BF16),
            ((ranks,) + row_block, BF16),
            ((ranks,) + row_block, BF16),
            ((ranks, slots, rows, double), BF16),
            ((ranks, slots, rows, hidden), BF16),
        ],
        (
            hidden_rows,
            norm_hidden,
            scale_two,
            probs,
            misc_all,
            router,
            out_grad,
            gate_grad,
            cosine,
            sine,
            scale_one.reshape(ranks * tokens, 128),
            gains,
            meta_group,
            o_weight,
            qkv,
            att,
            x_cols,
            weights,
            og_all,
            norm_slices,
            og_slices,
            grad_both,
            inner,
            out_part,
            back_part,
        ),
        [
            pltpu.VMEM(o_weight.shape, BF16),
            pltpu.VMEM(qkv.shape, BF16),
            pltpu.VMEM(att.shape, BF16),
            pltpu.VMEM(x_cols.shape, BF16),
            pltpu.VMEM(weights.shape, BF16),
            dma((5,)),
            pltpu.VMEM((n_expert, tokens, width), BF16),
            pltpu.VMEM((n_expert, tokens, width), BF16),
            dma((2,)),
            pltpu.VMEM((n_expert, SLOT_STRIDE, tokens), F32),
            pltpu.VMEM((ranks, used + 16, shard), BF16),
            pltpu.VMEM((ranks, tokens, width), BF16),
            pltpu.VMEM((ranks, used + 16, shard), BF16),
            pltpu.VMEM((ranks, ranks, tokens, heads.cols), BF16),
            pltpu.VMEM((n_expert,) + o_block, BF16),
            pltpu.VMEM((n_expert,) + w_block, BF16),
            pltpu.VMEM((sum_rows, shard), BF16),
            pltpu.VMEM((ranks, tokens, shard), F32),
            pltpu.VMEM((deep, n_expert, tokens, shard), BF16),
            pltpu.VMEM((deep, n_expert, tokens, shard), BF16),
            pltpu.VMEM((deep,) + row_block, BF16),
            pltpu.VMEM((deep,) + row_block, BF16),
            dma((2, deep)),
            dma((2, deep)),
        ]
        + exchange_sems(n_expert)
        + (line_sems(*plane[1:]) + sum_slots(*plane[1:], (tokens, width))) * 2
        + line_sems(*group[1:]) * 3
        + exchange_sems(ranks)
        + [dma((ranks,) + sems.shape) for sems in line_sems(*group[1:])]
        + summed(o_block)
        + line_sems(*group[1:])
        + summed((part_rows, half)) * 2
        + exchange_sems(ranks)
        + summed(s_block),
        cid=2,
        us=165,
        in_specs=[VMEM] * 13 + [ANY] * 12,
        out_specs=[VMEM] * 6 + [ANY] * 4,
        input_output_aliases={21: 8, 22: 9},
    )

    held = pl.Buffered(deep)
    gathered = lambda shape, at: pl.BlockSpec(
        (ranks, 1) + shape, lambda s: (0, at(s)) + (0,) * len(shape), pipeline_mode=held
    )
    d_w = d_w.reshape(shard, ranks * heads.cols)
    d_o = d_o.reshape(shard, width)
    sums = sums.reshape(sum_rows, shard)
    ins = (grad_x, inputs, misc_all, grad_hidden, hidden_rows, mixture, d_w, d_o, sums)
    outs = [
        ((slots, shard, double), F32),
        ((slots, hidden, shard), F32),
        ((tokens, width), BF16),
        ((tokens, width), F32),
        ((shard, QUERY_HEADS * HEAD_DIMENSION), F32),
        ((shard, KEY_VALUE_HEADS * HEAD_DIMENSION), F32),
        ((shard, KEY_VALUE_HEADS * HEAD_DIMENSION), F32),
        ((shard, width), F32),
        ((router_weight.shape[1], shard), F32),
        ((shard,), F32),
        ((shard,), F32),
    ]
    d_up, d_down, output, grad_inputs, d_q, d_k, d_v, d_o, d_router, gain_one, gain_two = call(
        functools.partial(finish, ranks, n_expert, slots, heads, tokens),
        "finish",
        outs,
        (x_rows, og_rows, both_all, inner_all) + ins,
        us=15,
        grid=(slots,),
        in_specs=[
            pl.BlockSpec((ranks, n_expert, SLOT_ROWS, shard), lambda s: (0, 0, s, 0)),
            pl.BlockSpec((ranks, n_expert, SLOT_ROWS, shard), lambda s: (0, 0, s, 0)),
            gathered((rows, double), lambda s: s),
            gathered((rows, hidden), lambda s: s),
        ]
        + [fixed(array.shape) for array in ins],
        out_specs=[moving((shard, double)), moving((hidden, shard))] + [fixed(shape) for shape, _ in outs[2:]],
    )
    return (
        output,
        grad_inputs,
        gain_one,
        d_q,
        d_k,
        d_v,
        d_o,
        gain_two,
        d_router.T,
        d_up,
        d_down,
    )


def solution(mesh):
    tokens = P(("dp", "expert"), None)
    rows = P("dp", None)
    return jax.shard_map(
        on_device,
        mesh=mesh,
        in_specs=(
            tokens,
            tokens,
            tokens,
            P(),
            P("dp"),
            rows,
            rows,
            rows,
            rows,
            P("dp"),
            rows,
            P("expert", None, None),
            P("expert", None, None),
            tokens,
        ),
        out_specs=(
            tokens,
            tokens,
            P("dp"),
            rows,
            rows,
            rows,
            rows,
            P("dp"),
            rows,
            P("expert", "dp", None),
            P("expert", None, "dp"),
        ),
        check_vma=False,
    )
```

```python
import functools
import math

import jax
import jax.numpy as jnp
import numpy as np
from jax import lax
from jax.experimental import pallas as pl
from jax.experimental.pallas import tpu as pltpu
from jax.sharding import PartitionSpec as P

QUERY_HEADS = 24
KEY_VALUE_HEADS = 8
HEAD_DIMENSION = 64
EXPERT_COUNT = 40
BLK = 4
SLOT_ROWS = 32
SLOT_STRIDE = 8

NORM_EPSILON = 1e-06
SCORE_SCALE = 0.015625
RESIDUAL_SCALE = 0.22
ROPE_BASE = 10000.0
MASKED_SCORE = -1e30

MESH = pl.DeviceIdType.MESH
F32, BF16 = jnp.float32, jnp.bfloat16
MEBI = 1024 * 1024
VMEM_MOST = 67_043_328


class Grid:
    def __init__(self, axis, A, B):
        self.axis, self.A, self.B = axis, A, B
        self.me = lax.axis_index(axis)
        self.a, self.b = self.me // B, self.me % B

    def at(self, a, b):
        return a * self.B + b

    def dev(self, a, b):
        return {self.axis: self.at(a, b)}

    def here(self):
        return {self.axis: self.me}

    def near(self):
        found = []
        if self.A > 1:
            found += [
                (self.a > 0, self.dev(self.a - 1, self.b)),
                (self.a < self.A - 1, self.dev(self.a + 1, self.b)),
            ]
        found += [(self.me >= 0, self.dev(self.a, (self.b + r) % self.B)) for r in range(1, self.B)]
        return found

    def all(self):
        n = self.A * self.B
        return [(self.me >= 0, {self.axis: (self.me + r) % n}) for r in range(1, n)]

    def next(self, kind, way):
        step = 1 if way == 0 else -1
        if kind == "a":
            return self.ahead("a", way, 1), self.dev(self.a + step, self.b)
        return self.ahead("b", way, 1), self.dev(self.a, self.b + step)

    def behind(self, kind, way, far):
        at, size = (self.a, self.A) if kind == "a" else (self.b, self.B)
        return (at - far >= 0) if way == 0 else (at + far <= size - 1)

    def ahead(self, kind, way, far):
        return self.behind(kind, 1 - way, far)


def greet(peers):
    barrier = pltpu.get_barrier_semaphore()
    for there, device in peers:

        @pl.when(there)
        def _():
            pl.semaphore_signal(barrier, inc=1, device_id=device, device_id_type=MESH)

    pl.semaphore_wait(barrier, sum(jnp.where(there, 1, 0) for there, _ in peers))


def remote(src, dst, send, recv, device):
    return pltpu.make_async_remote_copy(
        src_ref=src, dst_ref=dst, send_sem=send, recv_sem=recv, device_id=device, device_id_type=MESH
    )


class Part:
    def __init__(self, ref, *rest):
        self.ref, self.rest, self.at = ref, rest, self

    def __getitem__(self, i):
        return self.ref.at[(i,) + self.rest]


class Ring:
    def __init__(self, stage, out, sems):
        self.stage, self.out, self.sems = stage, out, sems

    def copy(self, i):
        return pltpu.make_async_copy(self.stage.at[i % 2], self.out.at[i], self.sems.at[i % 2])

    def free(self, i):
        @pl.when(i >= 2)
        def _():
            self.copy(i - 2).wait()

        return self.stage.at[i % 2]

    def end(self, count):
        for i in range(max(count - 2, 0), count):
            self.copy(i).wait()


def begin(step):
    next(step)
    return step


def advance(step, count):
    for _ in range(count):
        next(step)


def run_behind(*steps):
    steps, turn = list(steps), 0
    while steps:
        left = []
        for lag, step in steps:
            try:
                if turn >= lag:
                    next(step)
                left.append((lag, step))
            except StopIteration:
                pass
        steps, turn = left, turn + 1


def run(*steps):
    steps = list(steps)
    while steps:
        left = []
        for step in steps:
            try:
                next(step)
                left.append(step)
            except StopIteration:
                pass
        steps = left


def line_sems(A, B):
    dma = pltpu.SemaphoreType.DMA
    return [dma((2, A)), dma((2, A)), dma((2, A, B)), dma((2, A, B))]


def gather(g, own, out, sems, arrived=lambda i, block: None, near_first=False, started=False):
    send_a, recv_a, send_b, recv_b = sems
    A, B = g.A, g.B
    row = lambda way, k: g.a - k if way == 0 else g.a + k
    col = lambda way, k: g.b - k if way == 0 else g.b + k
    rows = [(0, 0)] + [(way, k) for k in range(1, A) for way in (0, 1)]

    def along_a(way, k, src, do):
        if k < A - 1:
            there, device = g.next("a", way)
            i = g.at(row(way, k), g.b)

            @pl.when(there)
            def _():
                do(remote(src, out.at[i], send_a.at[way, k], recv_a.at[way, k + 1], device))

    def along_b(way, j, a, i, src, do):
        if j < B - 1:
            there, device = g.next("b", way)

            @pl.when(there)
            def _():
                do(remote(src, out.at[i], send_b.at[way, a, j], recv_b.at[way, a, j + 1], device))

    def from_b(way, k, j):
        for w in (0, 1):
            i = g.at(row(way, k), col(w, j))

            @pl.when(g.behind("a", way, k) & g.behind("b", w, j))
            def _():
                a = row(way, k)
                remote(out.at[i], out.at[i], send_b.at[w, a, j], recv_b.at[w, a, j], g.here()).wait_recv()
                along_b(w, j, a, i, out.at[i], start)
                arrived(i, out.at[i])

    def start(copy):
        copy.start()

    def sent(copy):
        copy.wait_send()

    if not started:
        for way in (0, 1):
            along_a(way, 0, own, start)
        for way in (0, 1):
            along_b(way, 0, g.a, g.me, own, start)
        arrived(g.me, own)
    yield
    if near_first:
        for j in range(1, B):
            from_b(0, 0, j)
        yield
    for k in range(1, A):
        for way in (0, 1):
            i = g.at(row(way, k), g.b)

            @pl.when(g.behind("a", way, k))
            def _():
                remote(out.at[i], out.at[i], send_a.at[way, k], recv_a.at[way, k], g.here()).wait_recv()
                along_a(way, k, out.at[i], start)
                for w in (0, 1):
                    along_b(w, 0, row(way, k), i, out.at[i], start)
                arrived(i, out.at[i])

            yield
    for j in range(1, B):
        for way, k in rows[1:] if near_first else rows:
            from_b(way, k, j)
            yield
    for way, k in rows:
        for w in (0, 1) if k == 0 else (way,):

            @pl.when(g.behind("a", w, k))
            def _():
                along_a(w, k, own, sent)

        @pl.when(g.behind("a", way, k))
        def _():
            for w in (0, 1):
                for j in range(B - 1):

                    @pl.when(g.behind("b", w, j))
                    def _():
                        along_b(w, j, row(way, k), g.me, own, sent)


def sum_slots(A, B, block, dtype=BF16):
    return [
        pltpu.VMEM((A + 1,) + block, dtype),
        pltpu.VMEM((A,) + block, dtype),
        pltpu.VMEM((A, B - 1) + block, dtype),
    ]


def across(g, part, sems, slots, a, r):
    to = (g.b + r) % g.B
    return remote(part(g.at(a, to)), slots[2].at[a, r - 1], sems[2].at[0, a, r], sems[3].at[0, a, r], g.dev(g.a, to))


def reduce(g, part, finish, sems, slots, sent=None, started=False):
    send_a, recv_a, send_b, recv_b = sems
    land_a, out_a, land_b = slots
    sent = sent or part
    A, B = g.A, g.B
    row = lambda way, k: g.a + k if way == 0 else g.a - k
    rows = [(way, k) for k in range(A - 1, 0, -1) for way in (0, 1)] + [(0, 0)]
    here = g.here()

    def landing(way, k):
        return land_a.at[A if k == 0 and way == 1 else row(way, k)]

    def along(way, k):
        to = A if k == 1 and way == 1 else row(way, k)
        return remote(
            out_a.at[row(way, k)], land_a.at[to], send_a.at[way, k], recv_a.at[way, k - 1], g.next("a", way)[1]
        )

    def landed(way, k):
        remote(landing(way, k), landing(way, k), send_a.at[way, k], recv_a.at[way, k], here).wait_recv()

    for way, k in [] if started else rows:

        @pl.when(g.ahead("a", way, k))
        def _():
            for r in range(1, B):
                across(g, sent, sems, slots, row(way, k), r).start()

    yield
    for way, k in rows:

        @pl.when(g.ahead("a", way, k))
        def _():
            a = row(way, k)
            for r in range(1, B):
                mine = land_b.at[a, r - 1]
                remote(mine, mine, send_b.at[0, a, r], recv_b.at[0, a, r], here).wait_recv()

            def near():
                total = part(g.at(a, g.b))[...].astype(F32)
                for r in range(1, B):
                    total = total + land_b[a, r - 1].astype(F32)
                return total

            if k > 0:
                if k < A - 1:

                    @pl.when(g.behind("a", way, 1))
                    def _():
                        landed(way, k)
                        out_a[a] = (near() + landing(way, k)[...].astype(F32)).astype(out_a.dtype)

                @pl.when(jnp.logical_not(g.behind("a", way, 1)))
                def _():
                    out_a[a] = near().astype(out_a.dtype)

                along(way, k).start()
            else:
                for w in (0, 1):
                    if A > 1:

                        @pl.when(g.behind("a", w, 1))
                        def _():
                            landed(w, 0)

                total = near()
                if A == 2:
                    total = total + land_a[jnp.where(g.a == 1, 1, A)].astype(F32)
                else:
                    for w in (0, 1):
                        if A > 1:
                            total = total + jnp.where(g.behind("a", w, 1), landing(w, 0)[...].astype(F32), 0.0)
                finish(total)

        yield
    for way, k in rows:

        @pl.when(g.ahead("a", way, k))
        def _():
            for r in range(1, B):
                across(g, sent, sems, slots, row(way, k), r).wait_send()
            if k > 0:
                along(way, k).wait_send()


def total_scratch(A, B, block):
    return [pltpu.VMEM(block, BF16)] + line_sems(A, B) * 2 + sum_slots(A, B, block)


def total(g, part, out, take):
    kept, sems, slots = take(), take(8), take(3)

    def finish(value):
        kept[...] = value.astype(kept.dtype)

    yield from reduce(g, part, finish, sems[:4], slots)
    out.at[g.me][...] = kept[...]
    yield from gather(g, kept, out, sems[4:])


def exchange_sems(n):
    return [pltpu.SemaphoreType.DMA((n,)), pltpu.SemaphoreType.DMA((n,))]


def pass_slices(g, out, sems):
    send, recv = sems
    n = g.A * g.B

    def copies(i, block):
        for r in range(1, n):
            to = (g.me + r) % n
            yield remote(block.at[to], out.at[g.me, i], send.at[i, r], recv.at[i, r], {g.axis: to})

    def arrived(i, block):
        for copy in copies(i, block):
            copy.start()

    def end(blocks, block):
        for i in blocks:
            for r in range(1, n):
                mine = out.at[(g.me + n - r) % n, i]
                remote(mine, mine, send.at[i, r], recv.at[i, r], g.here()).wait_recv()
            for copy in copies(i, block):
                copy.wait_send()

    return arrived, end


def exchange(g, part, out, sems):
    send, recv = sems
    n = g.A * g.B
    copies = []
    for r in range(1, n):
        to = (g.me + r) % n
        copies.append(remote(part.at[to], out.at[g.me], send.at[r], recv.at[r], {g.axis: to}))
        copies[-1].start()
    out[g.me] = part[g.me]
    yield
    for r in range(1, n):
        origin = (g.me + n - r) % n
        remote(part.at[origin], out.at[origin], send.at[r], recv.at[r], g.here()).wait_recv()
    yield
    for copy in copies:
        copy.wait_send()


VMEM = pl.BlockSpec(memory_space=pltpu.VMEM)
ANY = pl.BlockSpec(memory_space=pl.ANY)


def call(body, name, outs, ins, scratch=(), cid=None, us=10.0, **grid):
    whole = VMEM
    params = dict(vmem_limit_bytes=VMEM_MOST)
    if cid is not None:
        params |= dict(collective_id=cid, has_side_effects=True)
    return pl.pallas_call(
        body,
        out_shape=[jax.ShapeDtypeStruct(shape, dtype) for shape, dtype in outs],
        in_specs=grid.pop("in_specs", [whole] * len(ins)),
        out_specs=grid.pop("out_specs", [whole] * len(outs)),
        scratch_shapes=list(scratch),
        compiler_params=pltpu.CompilerParams(**params),
        cost_estimate=pl.CostEstimate(flops=0, transcendentals=0, bytes_accessed=int(us * 3e6)),
        name=name,
        **grid,
    )(*ins)


def taker(refs):
    refs = list(refs)

    def take(n=None):
        if n is None:
            return refs.pop(0)
        return [refs.pop(0) for _ in range(n)]

    return take


def dot(left, right, contract=((1,), (0,))):
    return lax.dot_general(left, right, (contract, ((), ())), preferred_element_type=F32)


def halves(values):
    high = values.astype(BF16)
    return high, (values - high.astype(F32)).astype(BF16)


def norm_scale(values):
    return lax.rsqrt(jnp.mean(values * values, axis=-1, keepdims=True) + NORM_EPSILON)


def norm_back(grad, normed, scale, gain):
    grad_hat = grad * gain
    return scale * (grad_hat - normed * jnp.mean(grad_hat * normed, axis=-1, keepdims=True))


def rotary(values, cosine, sine, back=False):
    width, half = values.shape[1], HEAD_DIMENSION // 2
    later = pltpu.roll(values, width - half, 1)
    earlier = pltpu.roll(values, half, 1)
    front = lax.broadcasted_iota(jnp.int32, values.shape, 1) % HEAD_DIMENSION < half
    other = jnp.where(front, -later, earlier)
    return values * cosine - other * sine if back else values * cosine + other * sine


def allowed_pairs(segment_row):
    size = segment_row.shape[1]
    across = jnp.broadcast_to(segment_row, (size, size))
    rows = lax.broadcasted_iota(jnp.int32, (size, size), 0)
    cols = lax.broadcasted_iota(jnp.int32, (size, size), 1)
    return (cols <= rows) & (across == across.T)


def attention_weights(stacked, keys, allowed):
    scores = dot(stacked, keys, ((1,), (1,))) * SCORE_SCALE
    scores = jnp.where(allowed, scores, MASKED_SCORE)
    row_max = jnp.max(scores, axis=-1, keepdims=True)
    log_total = row_max + jnp.log(jnp.sum(jnp.exp(scores - row_max), axis=-1, keepdims=True))
    return jnp.exp(scores - log_total)


class Heads:
    def __init__(self, ranks):
        self.q, self.kv = QUERY_HEADS // ranks, KEY_VALUE_HEADS // ranks
        self.group = QUERY_HEADS // KEY_VALUE_HEADS
        self.q_cols, self.kv_cols = self.q * HEAD_DIMENSION, self.kv * HEAD_DIMENSION
        self.cols = -(-(self.q_cols + 2 * self.kv_cols) // 128) * 128

    def stack(self, rows, kv):
        first = kv * self.group
        return jnp.concatenate([self.head(rows, first + i) for i in range(self.group)], axis=0)

    def head(self, rows, i):
        return rows[:, i * HEAD_DIMENSION : (i + 1) * HEAD_DIMENSION]

    def key(self, rows, kv):
        return self.head(rows, self.q + kv)

    def value(self, rows, kv):
        return self.head(rows, self.q + self.kv + kv)


def rope_tables(length, heads):
    frequency = np.float32(ROPE_BASE) ** (-(np.arange(HEAD_DIMENSION // 2, dtype=np.float32) * 2.0) / HEAD_DIMENSION)
    angles = np.arange(length, dtype=np.float32)[:, None] * frequency.astype(np.float32)[None, :]
    cosine, sine = (np.tile(f(angles.astype(np.float64)).astype(np.float32), (1, 2)) for f in (np.cos, np.sin))
    turned = heads.q + heads.kv
    rest = heads.cols - turned * HEAD_DIMENSION
    cosine = np.concatenate([np.tile(cosine, (1, turned)), np.ones((length, rest), np.float32)], axis=1)
    sine = np.concatenate([np.tile(sine, (1, turned)), np.zeros((length, rest), np.float32)], axis=1)
    return cosine, sine


def gain_row(misc_ref, ranks, which):
    return jnp.concatenate([misc_ref[i, which : which + 1, :] for i in range(ranks)], axis=1)


def attention_forward(ranks, heads, length, b, x_ref, w_ref, o_ref, misc_ref, cos_ref, sin_ref, part_ref, qkv_ref, att_ref, scale_ref):
    width = x_ref.shape[2]
    x = x_ref[b].astype(F32)
    scale = norm_scale(x)
    scale_ref[b] = jnp.broadcast_to(scale, (length, 128))
    normed = (x * scale * gain_row(misc_ref, ranks, 0)).astype(BF16)
    qkv_ref[b] = rotary(dot(normed, w_ref[...].reshape(width, heads.cols)), cos_ref[...], sin_ref[...]).astype(BF16)
    qkv = qkv_ref[b]
    allowed = allowed_pairs(misc_ref[b, 8:9, :length])
    allowed = jnp.concatenate([allowed] * heads.group, axis=0)
    outs = []
    for kv in range(heads.kv):
        probs = attention_weights(heads.stack(qkv, kv), heads.key(qkv, kv), allowed).astype(BF16)
        mixed = dot(probs, heads.value(qkv, kv)).astype(BF16)
        outs += [mixed[i * length : (i + 1) * length] for i in range(heads.group)]
    att_ref[b] = jnp.concatenate(outs, axis=1)
    part_ref[b] = dot(att_ref[b], o_ref[...]).astype(BF16)


def column_experts(n_expert, slots, axis):
    column = lax.broadcasted_iota(jnp.int32, (1, 128) if axis else (128, 1), axis)
    owner, slot = column // SLOT_STRIDE, column % SLOT_STRIDE
    expert = slot * n_expert + owner
    real = (owner < n_expert) & (slot < slots) & (expert < EXPERT_COUNT)
    return real, jnp.where(real, expert, -1)


def column_picks(n_expert, slots):
    _, expert = column_experts(n_expert, slots, 1)
    return jnp.where(lax.broadcasted_iota(jnp.int32, (EXPERT_COUNT, 128), 0) == expert, 1.0, 0.0)


def route_tables(n_expert, slots, routes, blocks_ref):
    tokens = routes.shape[1]
    _, expert = column_experts(n_expert, slots, 0)
    named = jnp.zeros((128, tokens), F32)
    for k in range(routes.shape[0]):
        named = named + jnp.where(routes[k : k + 1, :] == expert, 1.0, 0.0)
    limit = jnp.zeros((128, 1), jnp.int32)
    for e in range(EXPERT_COUNT):
        limit = jnp.where(expert == e, blocks_ref[e] * BLK, limit)
    rows = lax.broadcasted_iota(jnp.int32, (tokens, tokens), 0)
    cols = lax.broadcasted_iota(jnp.int32, (tokens, tokens), 1)
    earlier = jnp.where(rows < cols, 1.0, 0.0).astype(BF16)
    rank = dot(named.astype(BF16), earlier)
    kept = (named > 0.0) & (rank < limit.astype(F32))
    return kept, jnp.where(kept, rank, -1.0)


def route_forward(ranks, n_expert, slots, x_ref, branch_ref, misc_ref, router_ref, routes_ref, blocks_ref, hidden_ref, norm_ref, scale_ref, probs_ref, meta_ref, table_ref):
    gain = gain_row(misc_ref, ranks, 1)
    width = x_ref.shape[1]
    shard = width // ranks
    hidden = x_ref[...].astype(F32) + RESIDUAL_SCALE * branch_ref[...]
    hidden_ref[...] = hidden
    scale = norm_scale(hidden)
    scale_ref[...] = jnp.broadcast_to(scale, scale_ref.shape)
    norm = (hidden * scale * gain).astype(BF16)
    picks = column_picks(n_expert, slots).astype(BF16)
    for i in range(ranks):
        here = slice(i * shard, (i + 1) * shard)
        norm_ref[i] = norm[:, here]
        table_ref[here, :] = dot(router_ref[i], picks, ((0,), (0,))).astype(BF16)
    kept, place = route_tables(n_expert, slots, routes_ref[...], blocks_ref)
    real, _ = column_experts(n_expert, slots, 1)
    logits = jnp.where(real, dot(norm, table_ref[...]), MASKED_SCORE)
    weight = jnp.exp(logits - jnp.max(logits, axis=-1, keepdims=True))
    probs = weight / jnp.sum(weight, axis=-1, keepdims=True)
    probs_ref[...] = probs
    used = n_expert * SLOT_STRIDE
    meta_ref[0] = place[:used]
    meta_ref[1] = jnp.where(kept, probs.T, 0.0)[:used]


def row_picks(slots, place):
    number = lax.broadcasted_iota(jnp.int32, (SLOT_ROWS, place.shape[1]), 0).astype(F32)
    return jnp.concatenate([jnp.where(number == place[s : s + 1], 1.0, 0.0) for s in range(slots)], axis=0)


def row_shares(slots, share):
    return jnp.concatenate(
        [jnp.broadcast_to(share[s : s + 1], (SLOT_ROWS, share.shape[1])) for s in range(slots)], axis=0
    )


def pick_rows(slots, count, sequence, mine, meta_ref, block, to_sc):
    def one(t, carry):
        q = sequence(t)
        pick = row_picks(slots, meta_ref[q, 0, mine, :]).astype(BF16)
        ranks, _, shard = block(q).shape
        for i in range(ranks):
            to_sc[q, :, i * shard : (i + 1) * shard] = dot(pick, block(q)[i]).astype(BF16)
        return carry

    lax.fori_loop(0, count, one, 0)


def expert_slot(n_expert, tokens, s, mine, meta_ref, up_ref, down_ref, gate_grad_ref, inner_ring, both_ring, x_sc, og_sc):
    width = x_sc.shape[2]
    hidden = down_ref.shape[0]
    place_of = pl.ds(pl.multiple_of(s * SLOT_ROWS, SLOT_ROWS), SLOT_ROWS)
    slot_row = lax.broadcasted_iota(jnp.int32, (SLOT_STRIDE, tokens), 0) == s
    number = lax.broadcasted_iota(jnp.int32, (SLOT_ROWS, tokens), 0).astype(F32)
    rows = n_expert * SLOT_ROWS
    both = dot(x_sc[:, place_of, :].reshape(rows, width), up_ref[...])
    gate, up = both[:, :hidden], both[:, hidden:]
    squash = jax.nn.sigmoid(gate)
    inner = (gate * squash * up).astype(BF16)
    inner_ring.free(s)[...] = inner
    inner_ring.copy(s).start()
    produced = dot(inner, down_ref[...]).astype(BF16)
    masks, gates = [], []
    for q in range(n_expert):
        place = jnp.sum(jnp.where(slot_row, meta_ref[q, 0, mine, :], 0.0), axis=0, keepdims=True)
        share = jnp.sum(jnp.where(slot_row, meta_ref[q, 1, mine, :], 0.0), axis=0, keepdims=True)
        masks.append(number == place)
        gates.append(jnp.sum(jnp.where(masks[q], share, 0.0), axis=1, keepdims=True))
    mix_grad = RESIDUAL_SCALE * og_sc[:, place_of, :].reshape(rows, width).astype(F32)
    grad_rows = (jnp.concatenate(gates, axis=0) * mix_grad).astype(BF16)
    gate_grad = jnp.sum(mix_grad * produced.astype(F32), axis=1, keepdims=True)
    og_sc[:, place_of, :] = produced.reshape(n_expert, SLOT_ROWS, width)
    for q in range(n_expert):
        spread = jnp.where(masks[q], gate_grad[q * SLOT_ROWS : (q + 1) * SLOT_ROWS], 0.0)
        gate_grad_ref[q] = jnp.where(slot_row, jnp.sum(spread, axis=0, keepdims=True), gate_grad_ref[q])
    grad_inner = dot(grad_rows, down_ref[...], ((1,), (1,)))
    grad_both = jnp.concatenate(
        [grad_inner * up * squash * (1.0 + gate * (1.0 - squash)), grad_inner * (gate * squash)], axis=1
    ).astype(BF16)
    both_ring.free(s)[...] = grad_both
    both_ring.copy(s).start()
    x_sc[:, place_of, :] = dot(grad_both, up_ref[...], ((1,), (1,))).astype(BF16).reshape(n_expert, SLOT_ROWS, width)


def sum_rows_back(slots, n_expert, mine, meta_ref, out_ring, back_ring, eo_sc, gx_sc):
    def one(q, carry):
        pick = row_picks(slots, meta_ref[q, 0, mine, :])
        high, low = halves(pick * row_shares(slots, meta_ref[q, 1, mine, :]))
        over = ((0,), (0,))
        back_ring.free(q)[...] = dot(pick.astype(BF16), gx_sc[q], over).astype(BF16)
        back_ring.copy(q).start()
        out_ring.free(q)[...] = (dot(high, eo_sc[q], over) + dot(low, eo_sc[q], over)).astype(BF16)
        out_ring.copy(q).start()
        return carry

    lax.fori_loop(0, n_expert, one, 0)


def route_backward(ranks, n_expert, shard, hidden_ref, norm_ref, scale_ref, probs_ref, misc_ref, router_ref, og_ref, back_ref, gate_grad_ref, grad_hidden_ref, branch_ref, small_ref):
    tokens, width = hidden_ref.shape
    gain = gain_row(misc_ref, ranks, 1)
    hidden = hidden_ref[...]
    used = n_expert * SLOT_STRIDE
    spread = gate_grad_ref[...].reshape(used, tokens)
    if used < 128:
        spread = jnp.concatenate([spread, jnp.zeros((128 - used, tokens), F32)], axis=0)
    grad_probs = spread.T
    probs = probs_ref[...]
    grad_logits = probs * (grad_probs - jnp.sum(probs * grad_probs, axis=1, keepdims=True))
    high, low = halves(grad_logits)
    router = router_ref[...]
    across = ((1,), (1,))
    grad_norm = back_ref[...] + (dot(high, router, across) + dot(low, router, across))
    scale = scale_ref[:, 0:1]
    normed = hidden * scale
    grad_hidden = og_ref[...].astype(F32) + norm_back(grad_norm, normed, scale, gain)
    grad_hidden_ref[...] = grad_hidden
    branch_ref[...] = (RESIDUAL_SCALE * grad_hidden).astype(BF16)
    over = ((0,), (0,))
    grad_gain = jnp.sum(grad_norm * normed, axis=0, keepdims=True)
    for i in range(ranks):
        here = slice(i * shard, (i + 1) * shard)
        grad_router = dot(high, norm_ref[i], over) + dot(low, norm_ref[i], over)
        small_ref[i, :used, :] = grad_router[:used].astype(BF16)
        small_ref[i, used:, :] = jnp.broadcast_to(grad_gain[:, here], (16, shard)).astype(BF16)


def store_blocks(ref, cols, values):
    count, rows = ref.shape[0], ref.shape[1]
    for i in range(count):
        ref[i, :, cols] = values[i * rows : (i + 1) * rows]


def attention_backward(heads, length, b, branch_ref, att_ref, qkv_ref, o_ref, misc_ref, cos_ref, sin_ref, grad_ref):
    grad_att = dot(branch_ref[b], o_ref[...], ((1,), (1,))).astype(BF16)
    att, qkv = att_ref[b], qkv_ref[b]
    allowed = allowed_pairs(misc_ref[b, 8:9, :length])
    allowed = jnp.concatenate([allowed] * heads.group, axis=0)
    d_q, d_k, d_v = [], [], []
    for kv in range(heads.kv):
        queries, keys = heads.stack(qkv, kv), heads.key(qkv, kv)
        soft = attention_weights(queries, keys, allowed)
        grads = heads.stack(grad_att, kv)
        d_v.append(dot(soft.astype(BF16), grads, ((0,), (0,))))
        delta = jnp.sum(grads.astype(F32) * heads.stack(att, kv).astype(F32), axis=1, keepdims=True)
        inner = dot(grads, heads.value(qkv, kv), ((1,), (1,)))
        d_scores = (soft * (inner - delta) * SCORE_SCALE).astype(BF16)
        rows = dot(d_scores, keys)
        d_q += [rows[i * length : (i + 1) * length] for i in range(heads.group)]
        d_k.append(dot(d_scores, queries, ((0,), (0,))))
    spare = heads.cols - heads.q_cols - 2 * heads.kv_cols
    fill = [jnp.zeros((length, spare), F32)] if spare else []
    grads = jnp.concatenate(d_q + d_k + d_v + fill, axis=1)
    grad_ref[b] = rotary(grads, cos_ref[...], sin_ref[...], back=True).astype(BF16)


def output_weight_backward(heads, branch_ref, att_ref, d_o_ref):
    branch = branch_ref[...].reshape(-1, branch_ref.shape[-1])
    store_blocks(d_o_ref, slice(None), dot(att_ref[...].reshape(-1, heads.q_cols), branch, ((0,), (0,))).astype(BF16))


def projection_products(ranks, heads, x_ref, scale_ref, gain_ref, grad_ref, d_w_ref, done):
    norm_input = (x_ref[...].astype(F32) * scale_ref[:, 0:1] * gain_ref[0:1, :]).astype(BF16)
    for i in range(ranks):
        grads = grad_ref[i].reshape(-1, heads.cols)
        store_blocks(d_w_ref, slice(i * heads.cols, (i + 1) * heads.cols), dot(norm_input, grads, ((0,), (0,))).astype(BF16))
        done(i)


def projection_backward(ranks, heads, shard, x_ref, scale_ref, grad_ref, w_ref, small_ref, grad_x_ref, sums_ref):
    normed = x_ref[...].astype(F32) * scale_ref[:, 0:1]
    total = None
    for i in range(ranks):
        term = dot(grad_ref[i].reshape(-1, heads.cols), w_ref[i], ((1,), (1,)))
        total = term if total is None else total + term
    grad_x_ref[...] = total.reshape(grad_x_ref.shape)
    small = small_ref[0].astype(F32)
    for i in range(1, ranks):
        small = small + small_ref[i].astype(F32)
    gain_grad = jnp.sum(total * normed, axis=0, keepdims=True)
    used = small.shape[0] - 16
    sums_ref[...] = jnp.zeros_like(sums_ref)
    sums_ref[:used, :] = small[:used].astype(BF16)
    second = lax.broadcasted_iota(jnp.int32, (16, shard), 0)
    sums_ref[used : used + 16, :] = jnp.where(second == 0, small[used:], jnp.where(second == 1, gain_grad, 0.0)).astype(BF16)


def group_rows(n_expert, slots, at, x, og, meta_ref, x_rows, og_rows):
    def one(q, carry):
        pick = row_picks(slots, meta_ref[at, q, 0])
        share = jnp.sum(pick * row_shares(slots, meta_ref[at, q, 1]), axis=1, keepdims=True)
        pick = pick.astype(BF16)
        x_rows[q] = dot(pick, x[q]).astype(BF16)
        og_rows[q] = (share * (RESIDUAL_SCALE * dot(pick, og[q]))).astype(BF16)
        return carry

    lax.fori_loop(0, n_expert, one, 0)


def finish(ranks, n_expert, slots, heads, x_rows_ref, og_rows_ref, both_ref, inner_ref, *refs):
    step = pl.program_id(0)
    take = taker(refs)
    sources, d_up_ref, d_down_ref, targets = take(9), take(), take(), take(6)
    router_ref, gain_one_ref, gain_two_ref = take(3)
    places, stages, in_sems, out_sems = take(9), take(6), take(), take()
    grad_ref, x_ref, misc_ref, grad_hidden_ref, hidden_ref, mixture_ref, d_w_ref, d_o_ref, sums_ref = places
    output_ref, grad_inputs_ref, q_ref, k_ref, v_ref, o_ref = stages
    ins = [pltpu.make_async_copy(*pair, in_sems.at[i]) for i, pair in enumerate(zip(sources, places))]
    outs = [pltpu.make_async_copy(*pair, out_sems.at[i]) for i, pair in enumerate(zip(stages, targets))]

    @pl.when(step == 0)
    def _():
        for copy in ins:
            copy.start()

    @pl.when(step == min(1, slots - 1))
    def _():
        for copy in ins:
            copy.wait()
        output_ref[...] = (hidden_ref[...] + RESIDUAL_SCALE * mixture_ref[...]).astype(BF16)
        gain = gain_row(misc_ref, ranks, 0)
        grad = jnp.concatenate([grad_ref[i] for i in range(ranks)], axis=1)
        x = x_ref[...].astype(F32)
        scale = norm_scale(x)
        grad_inputs_ref[...] = grad_hidden_ref[...] + norm_back(grad, x * scale, scale, gain)
        used = n_expert * SLOT_STRIDE
        router_ref[...] = dot(column_picks(n_expert, slots).astype(BF16), sums_ref[:128])
        ends = sums_ref[used : used + 16, :].astype(F32)
        gain_two_ref[...] = ends[0]
        gain_one_ref[...] = ends[1]
        o_ref[...] = d_o_ref[...].astype(F32)
        first, second = heads.q_cols, heads.q_cols + heads.kv_cols
        for i in range(ranks):
            start = i * heads.cols
            q_ref[:, i * heads.q_cols : (i + 1) * heads.q_cols] = d_w_ref[:, start : start + first].astype(F32)
            here = slice(i * heads.kv_cols, (i + 1) * heads.kv_cols)
            k_ref[:, here] = d_w_ref[:, start + first : start + second].astype(F32)
            v_ref[:, here] = d_w_ref[:, start + second : start + second + heads.kv_cols].astype(F32)
        for copy in outs:
            copy.start()

    flat = lambda value: value.reshape(-1, value.shape[-1])
    over = ((0,), (0,))
    d_up_ref[0] = dot(flat(x_rows_ref[...]), flat(both_ref[...]), over)
    d_down_ref[0] = dot(flat(inner_ref[...]), flat(og_rows_ref[...]), over)

    @pl.when(step == slots - 1)
    def _():
        for copy in outs:
            copy.wait()


def on_device(
    inputs,
    segment_ids,
    routes,
    expert_blocks,
    norm1_gain,
    q_weight,
    k_weight,
    value_matrix,
    o_weight,
    norm2_gain,
    router_weight,
    expert_gate_up,
    expert_down,
    out_grad,
):
    ranks, n_expert = lax.axis_size("dp"), lax.axis_size("expert")
    tokens, width = inputs.shape
    shard = q_weight.shape[0]
    slots, _, double = expert_gate_up.shape
    hidden = expert_down.shape[1]
    heads = Heads(ranks)
    group = ("dp", ranks // 2, 2)
    plane = ("expert", 4, n_expert // 4)
    used = n_expert * SLOT_STRIDE
    cosine, sine = rope_tables(tokens, heads)

    dma = pltpu.SemaphoreType.DMA

    def forward(*refs):
        take = taker(refs)
        x, wq, wk, wv, rt, gain_one, gain_two, sg, og, wo, cs, sn, routes_ref, blocks_ref = take(14)
        w, ms_all, og_all, qkv, att, scale_one, xc, hidden_ref, norm, scale_two, probs, meta, table = take(13)
        x_all, w_all, rt_all, ms, og_own, part, branch, own_sem = take(8)
        dp, ex = Grid(*group), Grid(*plane)
        for i in range(ranks):
            at = 0
            for ref, cols in ((wq, heads.q_cols), (wk, heads.kv_cols), (wv, heads.kv_cols)):
                w[i, :, at : at + cols] = ref[:, i * cols : (i + 1) * cols]
                at += cols
            if at < heads.cols:
                w[i, :, at:] = jnp.zeros((shard, heads.cols - at), BF16)
            og_own[i] = og[:, i * shard : (i + 1) * shard]
        ms[...] = jnp.zeros_like(ms)
        ms[0, :] = gain_one[...].astype(F32)
        ms[1, :] = gain_two[...].astype(F32)
        ms[8:9, :tokens] = sg[...].astype(F32)
        x_all[dp.me] = x[...]
        rt_all[dp.me] = rt[...]
        ms_all[dp.me] = ms[...]
        greet(dp.all() + ex.near())
        keep = pltpu.make_async_copy(og_own, og_all.at[ex.me], own_sem)
        keep.start()
        small = [begin(gather(dp, ms, ms_all, take(4))), begin(gather(dp, rt, rt_all, take(4)))]
        xs = begin(gather(dp, x, x_all, take(4)))
        ws = begin(exchange(dp, w, w_all, take(2)))
        ogs = begin(gather(ex, og_own, og_all, take(4)))
        run(*small, xs)
        for i in range(ranks):

            @pl.when(dp.me == i)
            def _():
                for b in range(ranks):
                    xc[b * tokens : (b + 1) * tokens, :] = x_all[b, :, i * shard : (i + 1) * shard]

        advance(ogs, 2 * (plane[1] - 1))
        run(ws)

        def store(total):
            branch[...] = total

        dp_sems, dp_slots = take(4), take(3)
        sums = begin(reduce(dp, lambda i: part.at[i], store, dp_sems, dp_slots, started=True))

        def one(t, carry):
            a, r = (dp.a + 1 + t // 2) % dp.A, 1 + t % 2

            @pl.when(t == 2 * (dp.A - 1))
            def _():
                advance(sums, 2 * (dp.A - 1))

            b = dp.at(a, (dp.b + r) % 2)
            attention_forward(ranks, heads, tokens, b, x_all, w_all, wo, ms_all, cs, sn, part, qkv, att, scale_one)

            @pl.when(r < 2)
            def _():
                across(dp, lambda i: part.at[i], dp_sems, dp_slots, a, 1).start()

            return carry

        lax.fori_loop(0, ranks, one, 0)
        run(sums)
        route_forward(ranks, n_expert, slots, x, branch, ms_all, rt_all, routes_ref, blocks_ref, hidden_ref, norm, scale_two, probs, meta, table)
        run(ogs)
        keep.wait()

    (
        weights,
        misc_all,
        og_all,
        qkv,
        att,
        scale_one,
        x_cols,
        hidden_rows,
        norm_hidden,
        scale_two,
        probs,
        meta,
        router,
    ) = call(
        forward,
        "forward",
        [
            ((ranks, shard, heads.cols), BF16),
            ((ranks, 16, shard), F32),
            ((n_expert, ranks, tokens, shard), BF16),
            ((ranks, tokens, heads.cols), BF16),
            ((ranks, tokens, heads.q_cols), BF16),
            ((ranks, tokens, 128), F32),
            ((ranks * tokens, shard), BF16),
            ((tokens, width), F32),
            ((ranks, tokens, shard), BF16),
            ((tokens, 128), F32),
            ((tokens, 128), F32),
            ((2, used, tokens), F32),
            ((width, 128), BF16),
        ],
        (
            inputs,
            q_weight,
            k_weight,
            value_matrix,
            router_weight.T,
            norm1_gain,
            norm2_gain,
            segment_ids,
            out_grad,
            o_weight,
            cosine,
            sine,
            routes.T,
            expert_blocks,
        ),
        [
            pltpu.VMEM((ranks, tokens, width), BF16),
            pltpu.VMEM((ranks, shard, heads.cols), BF16),
            pltpu.VMEM((ranks, router_weight.shape[1], shard), BF16),
            pltpu.VMEM((16, shard), F32),
            pltpu.VMEM((ranks, tokens, shard), BF16),
            pltpu.VMEM((ranks, tokens, width), BF16),
            pltpu.VMEM((tokens, width), F32),
            dma(()),
        ]
        + line_sems(*group[1:]) * 3
        + exchange_sems(ranks)
        + line_sems(*plane[1:])
        + line_sems(*group[1:])
        + sum_slots(*group[1:], (tokens, width)),
        cid=0,
        us=60,
        in_specs=[VMEM] * 13 + [pl.BlockSpec(memory_space=pltpu.SMEM)],
        out_specs=[VMEM] * 2 + [ANY] + [VMEM] * 10,
    )

    fixed = lambda shape: pl.BlockSpec(shape, lambda s: (0,) * len(shape), pipeline_mode=pl.Buffered(1))
    moving = lambda shape: pl.BlockSpec((1,) + shape, lambda s: (s,) + (0,) * len(shape))
    rows = n_expert * SLOT_ROWS
    deep = 2 if ranks * rows <= 1024 else 1

    def mixture_of_experts(*refs):
        take = taker(refs)
        nh, mt, og, up, down = take(5)
        gg, mt_group, out_part, back_part, inr, gb, xd, ogd = take(8)
        nh_all, mt_all, mt_own, x_sc, og_sc, og_in, up_in, down_in = take(8)
        stages, ring_sems, og_sems, up_sems, own_sems = take(4), take(), take(), take(), take()
        dp, ex = Grid(*group), Grid(*plane)
        out_ring, back_ring, inner_ring, both_ring = (
            Ring(stage, out, ring_sems.at[i])
            for i, (stage, out) in enumerate(zip(stages, (out_part, back_part, inr.at[dp.me], gb.at[dp.me])))
        )
        mine = pl.ds(pl.multiple_of(ex.me * SLOT_STRIDE, SLOT_STRIDE), SLOT_STRIDE)
        nh_all[ex.me] = nh[...]
        mt_all[ex.me] = mt[...]
        gg[...] = jnp.zeros_like(gg)

        def fetch(s, do):
            do(pltpu.make_async_copy(up.at[s], up_in.at[s % deep], up_sems.at[0, s % deep]))
            do(pltpu.make_async_copy(down.at[s], down_in.at[s % deep], up_sems.at[1, s % deep]))

        for s in range(deep):
            fetch(s, lambda copy: copy.start())
        greet(dp.all() + ex.near())
        mts = begin(gather(ex, mt, mt_all, take(4)))
        og_passed, og_end = pass_slices(dp, ogd, take(2))
        for i in range(n_expert):
            og_passed(i, og.at[i])
        passed, end = pass_slices(dp, xd, take(2))

        def keep(i, block):
            return pltpu.make_async_copy(block.at[dp.me], xd.at[dp.me, i], own_sems.at[i])

        def arrived(i, block):
            passed(i, block)
            keep(i, block).start()

        nhs = begin(gather(ex, nh, nh_all, take(4), arrived))
        run(mts)

        def fetch_og(q):
            return pltpu.make_async_copy(og.at[q], og_in.at[q % 2], og_sems.at[q % 2])

        fetch_og(0).start()

        def pick_og(q, carry):
            @pl.when(q + 1 < n_expert)
            def _():
                fetch_og(q + 1).start()

            fetch_og(q).wait()
            pick = row_picks(slots, mt_all[q, 0, mine, :]).astype(BF16)
            for i in range(ranks):
                og_sc[q, :, i * shard : (i + 1) * shard] = dot(pick, og_in[q % 2, i]).astype(BF16)
            return carry

        lax.fori_loop(0, n_expert, pick_og, 0)
        mt_own[...] = mt_all[:, :, mine, :]
        mt_group[dp.me] = mt_own[...]
        mgs = begin(gather(dp, mt_own, mt_group, take(4)))
        advance(nhs, 2 * (ex.A - 1))
        block = lambda q: nh_all.at[q]
        pick_rows(slots, ex.A, lambda t: ex.at(t, ex.b), mine, mt_all, block, x_sc)
        run(nhs)
        others = ex.B - 1
        pick_rows(
            slots, ex.A * others, lambda t: ex.at(t // others, (ex.b + 1 + t % others) % ex.B), mine, mt_all, block, x_sc
        )

        def one(s, carry):
            fetch(s, lambda copy: copy.wait())
            expert_slot(
                n_expert, tokens, s, mine, mt_all, up_in.at[s % deep], down_in.at[s % deep], gg, inner_ring, both_ring, x_sc, og_sc
            )

            @pl.when(s + deep < slots)
            def _():
                fetch(s + deep, lambda copy: copy.start())

            return carry

        lax.fori_loop(0, slots, one, 0)
        run(mgs)
        sum_rows_back(slots, n_expert, mine, mt_all, out_ring, back_ring, og_sc, x_sc)
        inner_ring.end(slots)
        both_ring.end(slots)
        out_ring.end(n_expert)
        back_ring.end(n_expert)
        end(range(n_expert), nh)
        for i in range(n_expert):
            keep(i, nh).wait()
        og_end(range(n_expert), og.at[0])

    gate_grad, meta_group, out_part, back_part, inner, grad_both, norm_slices, og_slices = call(
        mixture_of_experts,
        "mixture_of_experts",
        [
            ((n_expert, SLOT_STRIDE, tokens), F32),
            ((ranks, n_expert, 2, SLOT_STRIDE, tokens), F32),
            ((n_expert, tokens, width), BF16),
            ((n_expert, tokens, width), BF16),
            ((ranks, slots, rows, hidden), BF16),
            ((ranks, slots, rows, double), BF16),
            ((ranks, n_expert, tokens, shard), BF16),
            ((ranks, n_expert, tokens, shard), BF16),
        ],
        (norm_hidden, meta, og_all, expert_gate_up, expert_down),
        [
            pltpu.VMEM((n_expert, ranks, tokens, shard), BF16),
            pltpu.VMEM((n_expert, 2, used, tokens), F32),
            pltpu.VMEM((n_expert, 2, SLOT_STRIDE, tokens), F32),
            pltpu.VMEM((n_expert, slots * SLOT_ROWS, width), BF16),
            pltpu.VMEM((n_expert, slots * SLOT_ROWS, width), BF16),
            pltpu.VMEM((2, ranks, tokens, shard), BF16),
            pltpu.VMEM((deep, width, double), BF16),
            pltpu.VMEM((deep, hidden, width), BF16),
            pltpu.VMEM((2, tokens, width), BF16),
            pltpu.VMEM((2, tokens, width), BF16),
            pltpu.VMEM((2, rows, hidden), BF16),
            pltpu.VMEM((2, rows, double), BF16),
            dma((4, 2)),
            dma((2,)),
            dma((2, deep)),
            dma((n_expert,)),
        ]
        + line_sems(*plane[1:])
        + [dma((n_expert, ranks))] * 4
        + line_sems(*plane[1:])
        + line_sems(*group[1:]),
        cid=1,
        us=75,
        in_specs=[VMEM] * 2 + [ANY] * 3,
        out_specs=[VMEM] * 2 + [ANY] * 6,
    )

    sum_rows = 16 * n_expert
    part_rows = shard // n_expert
    o_block, w_block, s_block = (part_rows, width), (part_rows, ranks * heads.cols), (16, shard)

    half = ranks * heads.cols // 2
    summed = lambda block: total_scratch(*plane[1:], block)

    lead = max(slots // 5, 1)

    def backward(*refs):
        take = taker(refs)
        hid, nh, sc2, pb, ms, tb, og_mine, gg, cs, sn, sc, mt = take(12)
        brought, (og, xd, ogd, _, _, terms, back_terms) = take(5), take(7)
        grad_hidden_ref, mix, gx_all, do_all, dw_all, su_all, x_rows, og_rows, gb_all, inr_all = take(10)
        places, bring_sems = take(5), take()
        wo, qkv, at, xc, w = places
        out_in, back_in, term_sems = take(3)
        gg_all, sm, br_all, sm_all, gr_all, do, dw, su, gx, x_in, og_in, x_out, og_out, in_sems, out_sems = take(15)
        dp, ex = Grid(*group), Grid(*plane)
        brings = [pltpu.make_async_copy(*pair, bring_sems.at[i]) for i, pair in enumerate(zip(brought, places))]
        holds = [
            pltpu.make_async_copy(back_terms, back_in, term_sems.at[0]),
            pltpu.make_async_copy(terms, out_in, term_sems.at[1]),
        ]

        def fetch(j, do_):
            p, slot = (dp.me + j) % ranks, j % deep
            do_(pltpu.make_async_copy(xd.at[p], x_in.at[slot], in_sems.at[0, slot]))
            do_(pltpu.make_async_copy(og.at[:, dp.me] if j == 0 else ogd.at[p], og_in.at[slot], in_sems.at[1, slot]))

        for copy in holds + brings:
            copy.start()
        for j in range(deep):
            fetch(j, lambda copy: copy.start())
        greet(dp.all() + ex.all())

        def token_sum(to, kept, sent):
            def store(value):
                to[...] = value

            return begin(reduce(ex, lambda i: kept.at[i], store, take(4), take(3), lambda i: sent.at[i]))

        ggs = begin(exchange(ex, gg, gg_all, take(2)))
        backs = token_sum(grad_hidden_ref, back_in, back_terms)
        outs = token_sum(mix, out_in, terms)
        inrs = begin(gather(dp, inr_all.at[dp.me], inr_all, take(4)))
        share = lambda start, count: begin(
            gather(dp, gb_all.at[dp.me, pl.ds(start, count)], Part(gb_all, pl.ds(start, count)), take(4))
        )
        gbs = [share(0, lead)]
        for copy in holds:
            copy.wait()

        def out_copies(j):
            p, slot = (dp.me + j) % ranks, j % deep
            return [
                pltpu.make_async_copy(x_out.at[slot], x_rows.at[p], out_sems.at[0, slot]),
                pltpu.make_async_copy(og_out.at[slot], og_rows.at[p], out_sems.at[1, slot]),
            ]

        def build(j):
            fetch(j, lambda copy: copy.wait())
            if j >= deep:
                for copy in out_copies(j - deep):
                    copy.wait()
            p, slot = (dp.me + j) % ranks, j % deep
            group_rows(n_expert, slots, p, x_in.at[slot], og_in.at[slot], mt, x_out.at[slot], og_out.at[slot])
            for copy in out_copies(j):
                copy.start()
            if j + deep < ranks:
                fetch(j + deep, lambda copy: copy.start())

        for j in range(ranks):
            build(j)
            if j < 2 * (plane[1] - 1):
                advance(backs, 1)
        for j in range(ranks - deep, ranks):
            for copy in out_copies(j):
                copy.wait()
        run(backs)
        run(ggs)
        route_backward(ranks, n_expert, shard, hid, nh, sc2, pb, ms, tb, og_mine, grad_hidden_ref, gg_all, grad_hidden_ref, br_all.at[dp.me], sm)
        brs = begin(gather(dp, br_all.at[dp.me], br_all, take(4), near_first=True))
        sms = begin(exchange(dp, sm, sm_all, take(2)))
        for copy in brings:
            copy.wait()
        advance(outs, 2)
        gr_sems = take(4)
        share_gr = lambda p, started: gather(
            dp, gr_all.at[dp.me, p], Part(gr_all, p), [sems.at[p] for sems in gr_sems], started=started
        )

        def one(t, carry):
            @pl.when(t == 1)
            def _():
                advance(brs, 1)

            @pl.when(t == 2)
            def _():
                run(brs)

            p = dp.at((dp.a + t // 2) % dp.A, (dp.b + t % 2) % 2)
            attention_backward(heads, tokens, p, br_all, at, qkv, wo, ms, cs, sn, gr_all.at[dp.me])
            begin(share_gr(p, False))
            return carry

        lax.fori_loop(0, ranks, one, 0)
        output_weight_backward(heads, br_all, at, do)
        dos = begin(total(ex, lambda i: do.at[i], do_all, take))
        advance(outs, 4)
        run(sms)
        advance(dos, 2)
        run(*[share_gr(p, True) for p in range(ranks)])
        gbs.append(share(lead, slots - lead))
        dws = []

        def done(i):
            if (i + 1) % (ranks // 2) == 0:
                cols = pl.ds(len(dws) * half, half)
                part = Part(dw, slice(None), cols)
                dws.append(begin(total(ex, part.__getitem__, Part(dw_all, slice(None), cols), take)))

        projection_products(ranks, heads, xc, sc, ms.at[dp.me], gr_all, dw, done)
        projection_backward(ranks, heads, shard, xc, sc, gr_all, w, sm_all, gx, su)
        gxs = begin(exchange(dp, gx, gx_all, take(2)))
        rows_of = lambda i: pl.ds(pl.multiple_of(i * 16, 16), 16)
        sus = begin(total(ex, lambda i: su.at[rows_of(i)], su_all, take))
        run_behind((0, dos), (0, outs), (0, dws[0]), (2, sus), (5, dws[1]))
        run(gxs)
        run(inrs, *gbs)

    row_block = (n_expert, slots * SLOT_ROWS, shard)
    grad_hidden, mixture, grad_x, d_o, d_w, sums, x_rows, og_rows, both_all, inner_all = call(
        backward,
        "backward",
        [
            ((tokens, width), F32),
            ((tokens, width), F32),
            ((ranks, tokens, shard), F32),
            ((n_expert,) + o_block, BF16),
            ((n_expert,) + w_block, BF16),
            ((n_expert,) + s_block, BF16),
            ((ranks,) + row_block, BF16),
            ((ranks,) + row_block, BF16),
            ((ranks, slots, rows, double), BF16),
            ((ranks, slots, rows, hidden), BF16),
        ],
        (
            hidden_rows,
            norm_hidden,
            scale_two,
            probs,
            misc_all,
            router,
            out_grad,
            gate_grad,
            cosine,
            sine,
            scale_one.reshape(ranks * tokens, 128),
            meta_group,
            o_weight,
            qkv,
            att,
            x_cols,
            weights,
            og_all,
            norm_slices,
            og_slices,
            grad_both,
            inner,
            out_part,
            back_part,
        ),
        [
            pltpu.VMEM(o_weight.shape, BF16),
            pltpu.VMEM(qkv.shape, BF16),
            pltpu.VMEM(att.shape, BF16),
            pltpu.VMEM(x_cols.shape, BF16),
            pltpu.VMEM(weights.shape, BF16),
            dma((5,)),
            pltpu.VMEM((n_expert, tokens, width), BF16),
            pltpu.VMEM((n_expert, tokens, width), BF16),
            dma((2,)),
            pltpu.VMEM((n_expert, SLOT_STRIDE, tokens), F32),
            pltpu.VMEM((ranks, used + 16, shard), BF16),
            pltpu.VMEM((ranks, tokens, width), BF16),
            pltpu.VMEM((ranks, used + 16, shard), BF16),
            pltpu.VMEM((ranks, ranks, tokens, heads.cols), BF16),
            pltpu.VMEM((n_expert,) + o_block, BF16),
            pltpu.VMEM((n_expert,) + w_block, BF16),
            pltpu.VMEM((sum_rows, shard), BF16),
            pltpu.VMEM((ranks, tokens, shard), F32),
            pltpu.VMEM((deep, n_expert, tokens, shard), BF16),
            pltpu.VMEM((deep, n_expert, tokens, shard), BF16),
            pltpu.VMEM((deep,) + row_block, BF16),
            pltpu.VMEM((deep,) + row_block, BF16),
            dma((2, deep)),
            dma((2, deep)),
        ]
        + exchange_sems(n_expert)
        + (line_sems(*plane[1:]) + sum_slots(*plane[1:], (tokens, width))) * 2
        + line_sems(*group[1:]) * 3
        + exchange_sems(ranks)
        + [dma((ranks,) + sems.shape) for sems in line_sems(*group[1:])]
        + summed(o_block)
        + line_sems(*group[1:])
        + summed((part_rows, half)) * 2
        + exchange_sems(ranks)
        + summed(s_block),
        cid=2,
        us=165,
        in_specs=[VMEM] * 12 + [ANY] * 12,
        out_specs=[VMEM] * 6 + [ANY] * 4,
        input_output_aliases={20: 8, 21: 9},
    )

    held = pl.Buffered(deep)
    gathered = lambda shape, at: pl.BlockSpec(
        (ranks, 1) + shape, lambda s: (0, at(s)) + (0,) * len(shape), pipeline_mode=held
    )
    d_w = d_w.reshape(shard, ranks * heads.cols)
    d_o = d_o.reshape(shard, width)
    sums = sums.reshape(sum_rows, shard)
    ins = (grad_x, inputs, misc_all, grad_hidden, hidden_rows, mixture, d_w, d_o, sums)
    outs = [
        ((slots, shard, double), F32),
        ((slots, hidden, shard), F32),
        ((tokens, width), BF16),
        ((tokens, width), F32),
        ((shard, QUERY_HEADS * HEAD_DIMENSION), F32),
        ((shard, KEY_VALUE_HEADS * HEAD_DIMENSION), F32),
        ((shard, KEY_VALUE_HEADS * HEAD_DIMENSION), F32),
        ((shard, width), F32),
        ((router_weight.shape[1], shard), F32),
        ((shard,), F32),
        ((shard,), F32),
    ]
    d_up, d_down, output, grad_inputs, d_q, d_k, d_v, d_o, d_router, gain_one, gain_two = call(
        functools.partial(finish, ranks, n_expert, slots, heads),
        "finish",
        outs,
        (x_rows, og_rows, both_all, inner_all) + ins,
        [pltpu.VMEM(array.shape, array.dtype) for array in ins]
        + [pltpu.VMEM(*out) for out in outs[2:8]]
        + [dma((9,)), dma((6,))],
        us=15,
        grid=(slots,),
        in_specs=[
            pl.BlockSpec((ranks, n_expert, SLOT_ROWS, shard), lambda s: (0, 0, s, 0)),
            pl.BlockSpec((ranks, n_expert, SLOT_ROWS, shard), lambda s: (0, 0, s, 0)),
            gathered((rows, double), lambda s: s),
            gathered((rows, hidden), lambda s: s),
        ]
        + [ANY] * 9,
        out_specs=[moving((shard, double)), moving((hidden, shard))]
        + [ANY] * 6
        + [fixed(shape) for shape, _ in outs[8:]],
    )
    return (
        output,
        grad_inputs,
        gain_one,
        d_q,
        d_k,
        d_v,
        d_o,
        gain_two,
        d_router.T,
        d_up,
        d_down,
    )


def solution(mesh):
    tokens = P(("dp", "expert"), None)
    rows = P("dp", None)
    return jax.shard_map(
        on_device,
        mesh=mesh,
        in_specs=(
            tokens,
            tokens,
            tokens,
            P(),
            P("dp"),
            rows,
            rows,
            rows,
            rows,
            P("dp"),
            rows,
            P("expert", None, None),
            P("expert", None, None),
            tokens,
        ),
        out_specs=(
            tokens,
            tokens,
            P("dp"),
            rows,
            rows,
            rows,
            rows,
            P("dp"),
            rows,
            P("expert", "dp", None),
            P("expert", None, "dp"),
        ),
        check_vma=False,
    )
```
